32 devices in a mesh: dp: 4 (over y, z), cp: 8 (over x, core).
Axes of the slice: x: 4, y: 2, z: 2, core: 2. Of those that a mesh axis runs over, the one named last changes fastest.
The devices are a block of a 4x4x8 slice.
Arguments:
- x_act: bfloat16 [8, 1024, 3584], P('dp', 'cp'), parts along dimension 0
- d_out: bfloat16 [8, 1024, 3584], P('dp', 'cp'), parts along dimension 0
- positions: int32 [8, 1024], P('dp', 'cp'), parts along dimension 0
- ln_gain: float32 [3584], replicated
- ln_bias: float32 [3584], replicated
- w_query: bfloat16 [3584, 28, 128], replicated
- w_key: bfloat16 [3584, 4, 128], replicated
- w_value: bfloat16 [3584, 4, 128], replicated
- w_out: bfloat16 [3584, 3584], replicated
Outputs:
- output 1: bfloat16 [8, 1024, 3584], P('dp', 'cp'), parts along dimension 0
- output 2: bfloat16 [8, 1024, 3584], P('dp', 'cp'), parts along dimension 0
- output 3: float32 [14336, 28, 128], P(('dp', 'cp')), parts along dimension 0
- output 4: float32 [14336, 4, 128], P(('dp', 'cp')), parts along dimension 0
- output 5: float32 [14336, 4, 128], P(('dp', 'cp')), parts along dimension 0
- output 6: float32 [14336, 3584], P(('dp', 'cp')), parts along dimension 0
- output 7: float32 [14336], P('dp'), parts along dimension 0
- output 8: float32 [14336], P('dp'), parts along dimension 0
There are 4 independent parts. The reference program is written for one: setup_inputs(seed, part) draws one part's arguments, and reference() takes and returns one part's arrays. A program takes and returns all parts, laid end to end along the dimension named above; an argument that names none is the same for every part.
All inputs are finite; a program needn't handle non-finite values.
Results may differ from the reference program's by a relative error of at most 0.00671658.
Values are sent between devices in bfloat16 or wider.
A program may use at most 768 MiB of HBM per device.

```python
import math
import jax
import jax.numpy as jnp
from jax import lax

BATCH = 2
SEQ = 1024
WIDTH = 3584
Q_HEADS = 28
KV_HEADS = 4
HEAD_DIM = 128
Q_TILE = 128
TOKEN_KINDS = 64
DOC_SPAN = 128
GROUPS = Q_HEADS // KV_HEADS
EPS = 1e-5
ROPE_BASE = 10000.0


def setup_inputs(seed: int = 0, part: int = 0) -> dict:
    part_keys = jax.random.split(jax.random.fold_in(jax.random.key(seed), part), 5)
    shared_keys = jax.random.split(jax.random.key(seed + 1), 6)
    tokens = jax.random.randint(part_keys[0], (BATCH, SEQ), 0, TOKEN_KINDS)
    token_table = jax.random.normal(part_keys[1], (TOKEN_KINDS, WIDTH), jnp.float32)
    noise_draw = jax.random.normal(part_keys[2], (BATCH, SEQ, WIDTH), jnp.float32)
    x_act = (token_table[tokens] + 0.5 * noise_draw).astype(jnp.bfloat16)
    d_out = jax.random.normal(part_keys[3], (BATCH, SEQ, WIDTH), jnp.float32).astype(jnp.bfloat16)
    doc_flags = jax.random.randint(part_keys[4], (BATCH, SEQ), 0, DOC_SPAN) == 0
    seq_index = jnp.arange(SEQ, dtype=jnp.int32)
    starts = jnp.where(doc_flags, seq_index[None, :], 0)
    positions = (seq_index[None, :] - lax.cummax(starts, axis=1)).astype(jnp.int32)
    fan_in = WIDTH ** -0.5
    w_query = jax.random.normal(shared_keys[0], (WIDTH, Q_HEADS, HEAD_DIM), jnp.float32) * fan_in
    key_noise = jax.random.normal(shared_keys[1], (WIDTH, KV_HEADS, HEAD_DIM), jnp.float32) * fan_in
    w_key = 0.8 * w_query[:, ::GROUPS, :] + 0.6 * key_noise
    w_value = jax.random.normal(shared_keys[2], (WIDTH, KV_HEADS, HEAD_DIM), jnp.float32) * fan_in
    w_out = jax.random.normal(shared_keys[3], (Q_HEADS * HEAD_DIM, WIDTH), jnp.float32) * (Q_HEADS * HEAD_DIM) ** -0.5
    ln_gain = 0.3 * jax.random.normal(shared_keys[4], (WIDTH,), jnp.float32)
    ln_bias = 0.3 * jax.random.normal(shared_keys[5], (WIDTH,), jnp.float32)
    return {'x_act': x_act, 'd_out': d_out, 'positions': positions, 'ln_gain': ln_gain, 'ln_bias': ln_bias, 'w_query': w_query.astype(jnp.bfloat16), 'w_key': w_key.astype(jnp.bfloat16), 'w_value': w_value.astype(jnp.bfloat16), 'w_out': w_out.astype(jnp.bfloat16)}


def norm_forward(x_act, ln_gain, ln_bias):
    x_f32 = x_act.astype(jnp.float32)
    centered = x_f32 - jnp.mean(x_f32, axis=-1, keepdims=True)
    inv_std = lax.rsqrt(jnp.mean(centered * centered, axis=-1, keepdims=True) + EPS)
    x_hat = centered * inv_std
    return (x_hat * (1.0 + ln_gain) + ln_bias).astype(jnp.bfloat16), x_hat, inv_std


def norm_backward(grad_h, x_hat, inv_std, ln_gain):
    grad_hat = grad_h * (1.0 + ln_gain)
    mean_one = jnp.mean(grad_hat, axis=-1, keepdims=True)
    mean_two = jnp.mean(grad_hat * x_hat, axis=-1, keepdims=True)
    return inv_std * (grad_hat - mean_one - x_hat * mean_two)


def rope_tables(positions):
    quarter = HEAD_DIM // 4
    freq_tab = jnp.exp(jnp.arange(quarter, dtype=jnp.float32) * (-2.0 * math.log(ROPE_BASE) / (HEAD_DIM // 2)))
    angles = positions.astype(jnp.float32)[..., None] * freq_tab
    return jnp.cos(angles)[..., None, :], jnp.sin(angles)[..., None, :]


def rope_rotate(values, cos_tab, sin_tab):
    quarter = cos_tab.shape[-1]
    first_half = values[..., :quarter]
    second_half = values[..., quarter:2 * quarter]
    return jnp.concatenate([first_half * cos_tab - second_half * sin_tab, second_half * cos_tab + first_half * sin_tab, values[..., 2 * quarter:]], axis=-1)


def tile_probs(q_tile, key_f, q_first):
    scores = jnp.einsum('bqkgd,blkd->bkgql', q_tile, key_f) * (HEAD_DIM ** -0.5)
    q_index = q_first + jnp.arange(Q_TILE)
    k_index = jnp.arange(SEQ)
    scores = jnp.where(k_index[None, :] <= q_index[:, None], scores, -1e30)
    shifted = jnp.exp(scores - jnp.max(scores, axis=-1, keepdims=True))
    return shifted / jnp.sum(shifted, axis=-1, keepdims=True)


def attention_forward(q_grouped, key_f, value_f):
    def one_tile(tile_idx):
        q_first = tile_idx * Q_TILE
        q_tile = lax.dynamic_slice_in_dim(q_grouped, q_first, Q_TILE, axis=1)
        tile_prob = tile_probs(q_tile, key_f, q_first)
        prob_bf16 = tile_prob.astype(jnp.bfloat16).astype(jnp.float32)
        return jnp.einsum('bkgql,blkd->bqkgd', prob_bf16, value_f).astype(jnp.bfloat16)
    out_tiles = lax.map(one_tile, jnp.arange(SEQ // Q_TILE))
    return jnp.moveaxis(out_tiles, 0, 1).reshape(BATCH * SEQ, Q_HEADS * HEAD_DIM)


def attention_backward(q_grouped, key_f, value_f, grad_attn):
    def one_tile(acc_pair, tile_idx):
        grad_k, grad_v = acc_pair
        q_first = tile_idx * Q_TILE
        q_tile = lax.dynamic_slice_in_dim(q_grouped, q_first, Q_TILE, axis=1)
        ga_tile = lax.dynamic_slice_in_dim(grad_attn, q_first, Q_TILE, axis=1)
        tile_prob = tile_probs(q_tile, key_f, q_first)
        grad_prob = jnp.einsum('bqkgd,blkd->bkgql', ga_tile, value_f)
        row_dot = jnp.sum(tile_prob * grad_prob, axis=-1, keepdims=True)
        grad_score = (tile_prob * (grad_prob - row_dot) * (HEAD_DIM ** -0.5)).astype(jnp.bfloat16).astype(jnp.float32)
        grad_q = jnp.einsum('bkgql,blkd->bqkgd', grad_score, key_f)
        grad_k = grad_k + jnp.einsum('bkgql,bqkgd->blkd', grad_score, q_tile)
        prob_bf16 = tile_prob.astype(jnp.bfloat16).astype(jnp.float32)
        grad_v = grad_v + jnp.einsum('bkgql,bqkgd->blkd', prob_bf16, ga_tile)
        return (grad_k, grad_v), grad_q
    zero_acc = jnp.zeros((BATCH, SEQ, KV_HEADS, HEAD_DIM), jnp.float32)
    (grad_k, grad_v), q_tiles = lax.scan(one_tile, (zero_acc, zero_acc), jnp.arange(SEQ // Q_TILE))
    grad_q = jnp.moveaxis(q_tiles, 0, 1).reshape(BATCH, SEQ, Q_HEADS, HEAD_DIM)
    return grad_q, grad_k, grad_v


def reference(x_act, d_out, positions, ln_gain, ln_bias, w_query, w_key, w_value, w_out):
    n_tokens = BATCH * SEQ
    wq_flat = w_query.reshape(WIDTH, Q_HEADS * HEAD_DIM)
    wk_flat = w_key.reshape(WIDTH, KV_HEADS * HEAD_DIM)
    wv_flat = w_value.reshape(WIDTH, KV_HEADS * HEAD_DIM)
    normed, x_hat, inv_std = norm_forward(x_act, ln_gain, ln_bias)
    flat_h = normed.reshape(n_tokens, WIDTH)
    cos_tab, sin_tab = rope_tables(positions)
    q_act = rope_rotate(jnp.dot(flat_h, wq_flat, preferred_element_type=jnp.float32).reshape(BATCH, SEQ, Q_HEADS, HEAD_DIM), cos_tab, sin_tab).astype(jnp.bfloat16)
    k_act = rope_rotate(jnp.dot(flat_h, wk_flat, preferred_element_type=jnp.float32).reshape(BATCH, SEQ, KV_HEADS, HEAD_DIM), cos_tab, sin_tab).astype(jnp.bfloat16)
    v_act = jnp.dot(flat_h, wv_flat, preferred_element_type=jnp.float32).astype(jnp.bfloat16).reshape(BATCH, SEQ, KV_HEADS, HEAD_DIM)
    q_grouped = q_act.reshape(BATCH, SEQ, KV_HEADS, GROUPS, HEAD_DIM).astype(jnp.float32)
    key_f = k_act.astype(jnp.float32)
    value_f = v_act.astype(jnp.float32)
    attn_act = attention_forward(q_grouped, key_f, value_f)
    block_out = (x_act.astype(jnp.float32) + jnp.dot(attn_act, w_out, preferred_element_type=jnp.float32).reshape(BATCH, SEQ, WIDTH)).astype(jnp.bfloat16)
    grad_flat = d_out.reshape(n_tokens, WIDTH)
    grad_wo = jnp.dot(attn_act.T, grad_flat, preferred_element_type=jnp.float32)
    grad_attn = jnp.dot(grad_flat, w_out.T, preferred_element_type=jnp.float32).astype(jnp.bfloat16)
    grad_q, grad_k, grad_v = attention_backward(q_grouped, key_f, value_f, grad_attn.reshape(BATCH, SEQ, KV_HEADS, GROUPS, HEAD_DIM).astype(jnp.float32))
    grad_q_pre = rope_rotate(grad_q, cos_tab, -sin_tab).astype(jnp.bfloat16).reshape(n_tokens, Q_HEADS * HEAD_DIM)
    grad_k_pre = rope_rotate(grad_k, cos_tab, -sin_tab).astype(jnp.bfloat16).reshape(n_tokens, KV_HEADS * HEAD_DIM)
    grad_v_pre = grad_v.astype(jnp.bfloat16).reshape(n_tokens, KV_HEADS * HEAD_DIM)
    grad_h = (jnp.dot(grad_q_pre, wq_flat.T, preferred_element_type=jnp.float32) + jnp.dot(grad_k_pre, wk_flat.T, preferred_element_type=jnp.float32) + jnp.dot(grad_v_pre, wv_flat.T, preferred_element_type=jnp.float32)).reshape(BATCH, SEQ, WIDTH)
    grad_wq = jnp.dot(flat_h.T, grad_q_pre, preferred_element_type=jnp.float32).reshape(WIDTH, Q_HEADS, HEAD_DIM)
    grad_wk = jnp.dot(flat_h.T, grad_k_pre, preferred_element_type=jnp.float32).reshape(WIDTH, KV_HEADS, HEAD_DIM)
    grad_wv = jnp.dot(flat_h.T, grad_v_pre, preferred_element_type=jnp.float32).reshape(WIDTH, KV_HEADS, HEAD_DIM)
    grad_x = (d_out.astype(jnp.float32) + norm_backward(grad_h, x_hat, inv_std, ln_gain)).astype(jnp.bfloat16)
    grad_gain = jnp.sum(grad_h * x_hat, axis=(0, 1))
    grad_bias = jnp.sum(grad_h, axis=(0, 1))
    return (block_out, grad_x, grad_wq, grad_wk, grad_wv, grad_wo, grad_gain, grad_bias)
```

```python
import functools
import math
import jax
import jax.numpy as jnp
from jax import lax
from jax.experimental import pallas as pl
from jax.experimental.pallas import tpu as pltpu
from jax.sharding import PartitionSpec as P

EPS = 1e-5
ROPE_BASE = 10000.0
BF16 = jnp.bfloat16
F32 = jnp.float32
VMEM_LIMIT = 56 * 1024 * 1024
NT = (((1,), (1,)), ((), ()))


def dot(a, b):
    return jnp.dot(a, b, preferred_element_type=F32)


def dot_nt(a, b):
    return lax.dot_general(a, b, NT, preferred_element_type=F32)


def call(body, out_shape, grid, in_specs, out_specs, scratch=(), prefetch=0, flops=0, nbytes=0, name=None, aliases={}):
    return pl.pallas_call(
        body,
        out_shape=out_shape,
        grid_spec=pltpu.PrefetchScalarGridSpec(num_scalar_prefetch=prefetch, grid=grid, in_specs=in_specs, out_specs=out_specs, scratch_shapes=list(scratch)),
        compiler_params=pltpu.CompilerParams(dimension_semantics=('arbitrary',) * len(grid), vmem_limit_bytes=VMEM_LIMIT),
        cost_estimate=pl.CostEstimate(flops=int(flops), bytes_accessed=int(nbytes), transcendentals=0),
        input_output_aliases=aliases,
        name=name,
    )


def sds(shape, dtype):
    return jax.ShapeDtypeStruct(shape, dtype)


def project_body(x_ref, gain_ref, bias_ref, cos_ref, sa_ref, sb_ref, pos_ref, wq_ref, wk_ref, wv_ref, qkv_ref, ht_ref, h_ref):
    n_tok, width = x_ref.shape
    heads, head_dim = wq_ref.shape[0], wq_ref.shape[2]

    @pl.when(pl.program_id(0) == 0)
    def _():
        rows = 16

        @pl.loop(0, n_tok // rows)
        def _(step):
            sl = pl.ds(pl.multiple_of(step * rows, rows), rows)
            x = x_ref[sl, :].astype(F32)
            cen = x - jnp.mean(x, axis=-1, keepdims=True)
            inv = lax.rsqrt(jnp.mean(cen * cen, axis=-1, keepdims=True) + EPS)
            h_ref[sl, :] = ((cen * inv) * (1.0 + gain_ref[...]) + bias_ref[...]).astype(BF16)

        @pl.loop(0, width // 128)
        def _(step):
            sl = pl.ds(pl.multiple_of(step * 128, 128), 128)
            ht_ref[sl, :] = h_ref[:, sl].T

    slabs = [wq_ref[j] for j in range(heads)] + [wk_ref[0], wv_ref[0]]
    y = dot(h_ref[...], jnp.concatenate(slabs, axis=1))
    n_batch = qkv_ref.shape[1]
    seq = n_tok // n_batch
    cos, sa, sb = cos_ref[...], sa_ref[...], sb_ref[...]
    for j in range(heads + 2):
        v = y[:, j * head_dim:(j + 1) * head_dim]
        if j < heads + 1:
            v = v * cos + pltpu.roll(v, head_dim - head_dim // 4, 1) * sa + pltpu.roll(v, head_dim // 4, 1) * sb
        v = v.astype(BF16)
        for b in range(n_batch):
            qkv_ref[0, b, 0:seq, j * head_dim:(j + 1) * head_dim] = v[b * seq:(b + 1) * seq]
    for b in range(n_batch):
        qkv_ref[0, b, seq:, :] = pos_ref[b]


def project(x, gain, bias, tables, pos_rows, wq, wk, wv):
    n_batch, seq, width = x.shape
    n_tok = n_batch * seq
    kv_heads = wk.shape[0]
    group, head_dim = wq.shape[0] // kv_heads, wq.shape[2]
    cols = (group + 2) * head_dim
    pad = pos_rows.shape[1]
    whole = lambda *s: pl.BlockSpec(s, lambda i: (0,) * len(s))
    return call(
        project_body,
        (sds((kv_heads, n_batch, seq + pad, cols), BF16), sds((width, n_tok), BF16)),
        (kv_heads,),
        [whole(n_tok, width), whole(1, width), whole(1, width)] + [whole(n_tok, head_dim)] * 3 + [whole(n_batch, pad, cols),
         pl.BlockSpec((group, width, head_dim), lambda i: (i, 0, 0)),
         pl.BlockSpec((1, width, head_dim), lambda i: (i, 0, 0)),
         pl.BlockSpec((1, width, head_dim), lambda i: (i, 0, 0))],
        (pl.BlockSpec((1, n_batch, seq + pad, cols), lambda i: (i, 0, 0, 0)), whole(width, n_tok)),
        scratch=[pltpu.VMEM((n_tok, width), BF16)],
        flops=2 * n_tok * width * cols * kv_heads, nbytes=width * cols * kv_heads * 2, name='project',
    )(x.reshape(n_tok, width), gain.reshape(1, width), bias.reshape(1, width), *tables, pos_rows, wq, wk, wv)


def masked_scores(k, q, limit, tile, scale):
    s = dot_nt(k[:limit], q) * scale
    row = lax.broadcasted_iota(jnp.int32, (tile, tile), 0)
    col = lax.broadcasted_iota(jnp.int32, (tile, tile), 1)
    tail = jnp.where(row <= col, s[limit - tile:], -1e30)
    return tail if limit == tile else jnp.concatenate([s[:limit - tile], tail], axis=0)


def attend_body(tile, q_ref, k_ref, v_ref, a_ref, at_ref, stat_ref, vt_ref):
    n_seq = q_ref.shape[0] * q_ref.shape[1]
    head_dim = q_ref.shape[2]
    scale = head_dim ** -0.5
    q = q_ref[...].reshape(n_seq, head_dim)
    k = k_ref[...].reshape(n_seq, head_dim)

    @pl.when(pl.program_id(0) == 0)
    def _():
        vt_ref[...] = v_ref[...].reshape(n_seq, head_dim).T

    for t in range(n_seq // tile):
        limit = (t + 1) * tile
        sl = slice(t * tile, limit)
        s = masked_scores(k, q[sl], limit, tile, scale)
        top = jnp.max(s, axis=0, keepdims=True)
        e = jnp.exp(s - top)
        inv = 1.0 / jnp.sum(e, axis=0, keepdims=True)
        p = (e * inv).astype(BF16)
        at = dot(vt_ref[:, :limit], p).astype(BF16)
        at_ref[:, sl] = at
        a_ref[sl, :] = at.T
        stat_ref[0, 0:1, sl] = top
        stat_ref[0, 1:2, sl] = inv


def attend(qkv, seq, group, tile):
    n_src, cols = qkv.shape[0], qkv.shape[2]
    head_dim = cols // (group + 2)
    n_seq = n_src * seq
    col = lambda f: pl.BlockSpec((n_src, seq, head_dim), lambda j: (0, 0, f(j)))
    return call(
        functools.partial(attend_body, tile),
        (sds((n_seq, group * head_dim), BF16), sds((group * head_dim, n_seq), BF16), sds((group, 8, n_seq), F32)),
        (group,),
        [col(lambda j: j), col(lambda j: group), col(lambda j: group + 1)],
        (pl.BlockSpec((n_seq, head_dim), lambda j: (0, j)), pl.BlockSpec((head_dim, n_seq), lambda j: (j, 0)), pl.BlockSpec((1, 8, n_seq), lambda j: (j, 0, 0))),
        scratch=[pltpu.VMEM((head_dim, n_seq), BF16)],
        flops=4 * group * n_seq * n_seq * head_dim, nbytes=3 * n_seq * cols * 2, name='attend',
    )(qkv, qkv, qkv)


def attend_back_body(tile, q_ref, k_ref, v_ref, da_ref, stat_ref, cos_ref, sin_ref, g_ref, kt_ref, dk_ref, dv_ref):
    n_seq = q_ref.shape[0] * q_ref.shape[1]
    head_dim = q_ref.shape[2]
    quarter = head_dim // 4
    group = pl.num_programs(0) - 2
    j = pl.program_id(0)
    scale = head_dim ** -0.5

    def rotate_back(t, sl):
        cos, sin = cos_ref[:, sl], sin_ref[:, sl]
        u, w = t[:quarter], t[quarter:2 * quarter]
        return jnp.concatenate([u * cos + w * sin, w * cos - u * sin, t[2 * quarter:]], axis=0)

    @pl.when(j == 0)
    def _():
        kt_ref[...] = k_ref[...].reshape(n_seq, head_dim).T
        dk_ref[...] = jnp.zeros_like(dk_ref)
        dv_ref[...] = jnp.zeros_like(dv_ref)

    @pl.when(j < group)
    def _():
        q = q_ref[...].reshape(n_seq, head_dim)
        k = k_ref[...].reshape(n_seq, head_dim)
        v = v_ref[...].reshape(n_seq, head_dim)
        for t in range(n_seq // tile):
            limit = (t + 1) * tile
            sl = slice(t * tile, limit)
            da = da_ref[sl, :]
            s = masked_scores(k, q[sl], limit, tile, scale)
            p = jnp.exp(s - stat_ref[0, 0:1, sl]) * stat_ref[0, 1:2, sl]
            dp = dot_nt(v[:limit], da)
            row_dot = jnp.sum(p * dp, axis=0, keepdims=True)
            ds = (p * (dp - row_dot) * scale).astype(BF16)
            dv_ref[:limit, :] += dot(p.astype(BF16), da)
            dk_ref[:limit, :] += dot(ds, q[sl])
            g_ref[sl, :] = rotate_back(dot(kt_ref[:, :limit], ds), sl).T.astype(BF16)

    @pl.when(j == group)
    def _():
        g_ref[...] = rotate_back(dk_ref[...].T, slice(0, n_seq)).T.astype(BF16)

    @pl.when(j == group + 1)
    def _():
        g_ref[...] = dv_ref[...].astype(BF16)


def attend_back(qkv, da, stats, cos_t, sin_t, seq, group, tile):
    n_src, cols = qkv.shape[0], qkv.shape[2]
    head_dim = cols // (group + 2)
    n_seq = n_src * seq
    last = group - 1
    col = lambda f: pl.BlockSpec((n_src, seq, head_dim), lambda j: (0, 0, f(j)))
    cap = lambda j: jnp.minimum(j, last)
    return call(
        functools.partial(attend_back_body, tile),
        sds((n_seq, cols), BF16),
        (group + 2,),
        [col(cap), col(lambda j: group), col(lambda j: group + 1),
         pl.BlockSpec((n_seq, head_dim), lambda j: (0, cap(j))),
         pl.BlockSpec((1, 8, n_seq), lambda j: (cap(j), 0, 0)),
         pl.BlockSpec(cos_t.shape, lambda j: (0, 0)), pl.BlockSpec(sin_t.shape, lambda j: (0, 0))],
        pl.BlockSpec((n_seq, head_dim), lambda j: (0, j)),
        scratch=[pltpu.VMEM((head_dim, n_seq), BF16), pltpu.VMEM((n_seq, head_dim), F32), pltpu.VMEM((n_seq, head_dim), F32)],
        flops=10 * group * n_seq * n_seq * head_dim, nbytes=4 * n_seq * cols * 2, name='attend_back',
    )(qkv, qkv, qkv, da, stats, cos_t, sin_t)


def grad_mix_body(where_ref, dy_ref, wo_ref, da_ref):
    rows = dy_ref.shape[0] * dy_ref.shape[2]
    da_ref[...] = dot_nt(dy_ref[...].reshape(rows, dy_ref.shape[3]), wo_ref[...]).astype(BF16)


def grad_mix(where, dy_all, w_out, n_rows):
    n_dev, n_batch, seq, width = dy_all.shape
    per = 2
    return call(
        grad_mix_body,
        sds((n_dev * seq, n_rows), BF16),
        (n_dev // per,),
        [pl.BlockSpec((per, 1, seq, width), lambda i, w: (i, w[1], 0, 0)), pl.BlockSpec((n_rows, width), lambda i, w: (w[0], 0))],
        pl.BlockSpec((per * seq, n_rows), lambda i, w: (i, 0)),
        prefetch=1, flops=2 * n_dev * seq * n_rows * width, nbytes=2 * width * (n_rows + n_dev * seq), name='grad_mix',
    )(where, dy_all, w_out)


def output_body(a_ref, wo_ref, x_ref, out_ref, mix_ref):
    n_src, seq, cols = a_ref.shape
    n_batch = x_ref.shape[0]

    @pl.when(pl.program_id(0) == 0)
    def _():
        for s in range(n_src):
            mix_ref[(s % n_batch) * seq:(s % n_batch + 1) * seq, (s // n_batch) * cols:(s // n_batch + 1) * cols] = a_ref[s]

    y = dot(mix_ref[...], wo_ref[...]).reshape(x_ref.shape)
    out_ref[...] = (x_ref[...].astype(F32) + y).astype(BF16)


def output(a_recv, w_out, x, tile):
    n_batch, seq, width = x.shape
    rows = w_out.shape[0]
    return call(
        output_body,
        sds(x.shape, BF16),
        (width // tile,),
        [pl.BlockSpec(a_recv.shape, lambda i: (0, 0, 0)), pl.BlockSpec((rows, tile), lambda i: (0, i)), pl.BlockSpec((n_batch, seq, tile), lambda i: (0, 0, i))],
        pl.BlockSpec((n_batch, seq, tile), lambda i: (0, 0, i)),
        scratch=[pltpu.VMEM((n_batch * seq, rows), BF16)],
        flops=2 * n_batch * seq * rows * width, nbytes=2 * rows * width, name='output',
    )(a_recv, w_out, x)


def grad_wo_body(where_ref, own_ref, other_ref, dy_ref, out_ref, at_ref):
    n_dev, n_batch, seq, tile = dy_ref.shape

    @pl.when(pl.program_id(0) == 0)
    def _():
        mine = where_ref[1]
        for d in range(n_dev):
            src = slice(d * seq, (d + 1) * seq)
            at_ref[:, pl.ds(pl.multiple_of((d * n_batch + mine) * seq, seq), seq)] = own_ref[:, src]
            at_ref[:, pl.ds(pl.multiple_of((d * n_batch + 1 - mine) * seq, seq), seq)] = other_ref[:, src]

    out_ref[...] = dot(at_ref[...], dy_ref[...].reshape(n_dev * n_batch * seq, tile))


def grad_wo_rows(where, own, other, dy_all, tile):
    n_dev, n_batch, seq, width = dy_all.shape
    rows, n_seq = own.shape
    return call(
        grad_wo_body,
        sds((rows, width), F32),
        (width // tile,),
        [pl.BlockSpec((rows, n_seq), lambda i, w: (0, 0))] * 2 + [pl.BlockSpec((n_dev, n_batch, seq, tile), lambda i, w: (0, 0, 0, i))],
        pl.BlockSpec((rows, tile), lambda i, w: (0, i)),
        scratch=[pltpu.VMEM((rows, n_batch * n_seq), BF16)],
        prefetch=1, flops=4 * n_seq * rows * width, nbytes=4 * n_seq * width + 4 * rows * width, name='grad_wo',
    )(where, own, other, dy_all)


def grad_qkv_body(ht_ref, g_ref, dq_ref, dk_ref, dv_ref, lhs_ref):
    n_dev, rows, n_tok = ht_ref.shape
    n_batch = g_ref.shape[0]
    seq = n_tok // n_batch
    head_dim = dq_ref.shape[2]
    group = dq_ref.shape[0]

    @pl.when(pl.program_id(0) == 0)
    def _():
        for d in range(n_dev):
            for b in range(n_batch):
                lhs_ref[:, (b * n_dev + d) * seq:(b * n_dev + d + 1) * seq] = ht_ref[d, :, b * seq:(b + 1) * seq]

    g = g_ref[...].reshape(n_batch * n_dev * seq, g_ref.shape[2])
    y = dot(lhs_ref[...], g)
    for j in range(group):
        dq_ref[j] = y[:, j * head_dim:(j + 1) * head_dim]
    dk_ref[0] = y[:, group * head_dim:(group + 1) * head_dim]
    dv_ref[0] = y[:, (group + 1) * head_dim:]


def grad_qkv(ht_all, g_all, group):
    n_dev, rows, n_tok = ht_all.shape
    _, n_seq, cols = g_all.shape
    head_dim = cols // (group + 2)
    n_batch = n_tok * n_dev // n_seq
    chips = n_dev // n_batch
    return call(
        grad_qkv_body,
        (sds((chips * group, rows, head_dim), F32), sds((chips, rows, head_dim), F32), sds((chips, rows, head_dim), F32)),
        (chips,),
        [pl.BlockSpec(ht_all.shape, lambda i: (0, 0, 0)), pl.BlockSpec((n_batch, n_seq, cols), lambda i: (i, 0, 0))],
        (pl.BlockSpec((group, rows, head_dim), lambda i: (i, 0, 0)), pl.BlockSpec((1, rows, head_dim), lambda i: (i, 0, 0)), pl.BlockSpec((1, rows, head_dim), lambda i: (i, 0, 0))),
        scratch=[pltpu.VMEM((rows, n_dev * n_tok), BF16)],
        flops=2 * n_dev * n_tok * rows * cols * chips, nbytes=2 * g_all.size + 4 * rows * cols * chips, name='grad_qkv',
    )(ht_all, g_all)


def grad_x_body(where_ref, g_ref, wq_ref, wk_ref, wv_ref, x_ref, dy_ref, gain_ref, dx_ref, sums_ref, acc_ref):
    n_batch, seq, cols = g_ref.shape
    n_tok = n_batch * seq
    group = wq_ref.shape[0]
    i = pl.program_id(0)
    w = jnp.concatenate([wq_ref[j] for j in range(group)] + [wk_ref[0], wv_ref[0]], axis=1)
    part = dot_nt(g_ref[...].reshape(n_tok, cols), w)

    @pl.when(i == 0)
    def _():
        acc_ref[...] = part

    @pl.when(i > 0)
    def _():
        acc_ref[...] += part

    @pl.when(i == pl.num_programs(0) - 1)
    def _():
        rows = 16
        sums_ref[...] = jnp.zeros_like(sums_ref)

        @pl.loop(0, n_tok // rows)
        def _(step):
            sl = pl.ds(pl.multiple_of(step * rows, rows), rows)
            x = x_ref[sl, :].astype(F32)
            cen = x - jnp.mean(x, axis=-1, keepdims=True)
            inv = lax.rsqrt(jnp.mean(cen * cen, axis=-1, keepdims=True) + EPS)
            hat = cen * inv
            dh = acc_ref[sl, :]
            gh = dh * (1.0 + gain_ref[...])
            one = jnp.mean(gh, axis=-1, keepdims=True)
            two = jnp.mean(gh * hat, axis=-1, keepdims=True)
            dx_ref[sl, :] = (dy_ref[sl, :].astype(F32) + inv * (gh - one - hat * two)).astype(BF16)
            sums_ref[0] += (dh * hat)[0:8] + (dh * hat)[8:16]
            sums_ref[1] += dh[0:8] + dh[8:16]


def grad_x(where, g_all, wq, wk, wv, x, dy, gain):
    n_batch, seq, width = x.shape
    n_tok = n_batch * seq
    cols = g_all.shape[2]
    kv_heads = wk.shape[0]
    group, head_dim = wq.shape[0] // kv_heads, wq.shape[2]
    whole = lambda *s: pl.BlockSpec(s, lambda i, w: (0,) * len(s))
    return call(
        grad_x_body,
        (sds((n_tok, width), BF16), sds((2, 8, width), F32)),
        (kv_heads,),
        [pl.BlockSpec((n_batch, seq, cols), lambda i, w: (i, w[2], 0)),
         pl.BlockSpec((group, width, head_dim), lambda i, w: (i, 0, 0)), pl.BlockSpec((1, width, head_dim), lambda i, w: (i, 0, 0)), pl.BlockSpec((1, width, head_dim), lambda i, w: (i, 0, 0)),
         whole(n_tok, width), whole(n_tok, width), whole(1, width)],
        (whole(n_tok, width), whole(2, 8, width)),
        scratch=[pltpu.VMEM((n_tok, width), F32)],
        prefetch=1, flops=2 * n_tok * width * cols * kv_heads, nbytes=2 * width * cols * kv_heads, name='grad_x',
    )(where, g_all, wq, wk, wv, x.reshape(n_tok, width), dy.reshape(n_tok, width), gain.reshape(1, width))


def solution(mesh):
    n_dev = mesh.shape['cp']

    def device_step(x_act, d_out, positions, ln_gain, ln_bias, w_query, w_key, w_value, w_out):
        n_batch, seq, width = x_act.shape
        q_heads, (kv_heads, head_dim) = w_query.shape[1], w_key.shape[1:]
        group = q_heads // kv_heads
        quarter = head_dim // 4
        chips = n_dev // n_batch
        assert chips == kv_heads and q_heads * head_dim == width
        me = lax.axis_index('cp')
        where = jnp.stack([me // n_batch, me % n_batch, me]).astype(jnp.int32)
        swap = [(i, i ^ 1) for i in range(n_dev)]

        dy_all = lax.all_gather(d_out, 'cp', axis=0)
        freq = jnp.exp(jnp.arange(quarter, dtype=F32) * (-2.0 * math.log(ROPE_BASE) / (head_dim // 2)))
        angles = positions.astype(F32).reshape(n_batch * seq, 1) * freq
        cos, sin = jnp.cos(angles), jnp.sin(angles)
        rest = jnp.zeros((n_batch * seq, head_dim - 2 * quarter), F32)
        none = jnp.zeros_like(sin)
        tables = (jnp.concatenate([cos, cos, rest + 1.0], axis=1), jnp.concatenate([-sin, none, rest], axis=1), jnp.concatenate([none, sin, rest], axis=1))
        cols = (group + 2) * head_dim
        pair = jnp.stack([positions // 256, positions % 256], axis=1).astype(BF16).reshape(n_batch, 1, 2 * seq)
        pos_rows = jnp.pad(pair, ((0, 0), (0, 7), (0, cols - 2 * seq)))
        wq = jnp.transpose(w_query, (1, 0, 2))
        wk = jnp.transpose(w_key, (1, 0, 2))
        wv = jnp.transpose(w_value, (1, 0, 2))

        qkv_send, ht = project(x_act, ln_gain, ln_bias, tables, pos_rows, wq, wk, wv)
        qkv = lax.all_to_all(qkv_send.reshape(n_dev, seq + 8, cols), 'cp', 0, 0, tiled=True)
        ht_all = lax.all_to_all(ht.reshape(n_dev, width // n_dev, n_batch * seq), 'cp', 0, 0, tiled=True)
        spots = qkv[:, seq, :2 * seq].astype(F32).reshape(n_dev, 2, seq)
        spots = (spots[:, 0] * 256.0 + spots[:, 1]).reshape(1, n_dev * seq)
        angles_t = freq[:, None] * spots
        cos_t, sin_t = jnp.cos(angles_t), jnp.sin(angles_t)

        attn, attn_t, stats = attend(qkv, seq, group, 256)
        a_recv = lax.all_to_all(attn.reshape(n_dev, seq, group * head_dim), 'cp', 0, 0, tiled=True)
        half = width // n_dev
        attn_t = attn_t.reshape(n_batch, half, n_dev * seq)
        at_own = lax.dynamic_index_in_dim(attn_t, where[1], 0, keepdims=False)
        at_other = lax.ppermute(lax.dynamic_index_in_dim(attn_t, 1 - where[1], 0, keepdims=False), 'cp', swap)
        da = grad_mix(where, dy_all, w_out, group * head_dim)
        g_own = attend_back(qkv, da, stats, cos_t, sin_t, seq, group, 256)
        g_all = lax.all_gather(g_own, 'cp', axis=0)
        block_out = output(a_recv, w_out, x_act, 512)
        grad_wo = grad_wo_rows(where, at_own, at_other, dy_all, 512)
        dx, sums = grad_x(where, g_all, wq, wk, wv, x_act, d_out, ln_gain)
        gq, gk, gv = grad_qkv(ht_all, g_all, group)
        total = jnp.sum(sums, axis=1)
        total = total + lax.ppermute(total, 'cp', swap)
        total = total + lax.ppermute(total, 'cp', [(i, (i // 2 ^ 1) * 2 + i % 2) for i in range(n_dev)])
        total = total + lax.ppermute(total, 'cp', [(i, (i // 2 ^ 3) * 2 + i % 2) for i in range(n_dev)])
        rows = lambda t: jnp.transpose(t, (1, 0, 2))
        return (block_out, dx.reshape(x_act.shape), rows(gq), rows(gk), rows(gv), grad_wo, total[0], total[1])

    return jax.shard_map(device_step, mesh=mesh, in_specs=(P('dp', 'cp', None), P('dp', 'cp', None), P('dp', 'cp'), P(None), P(None), P(None, None, None), P(None, None, None), P(None, None, None), P(None, None)), out_specs=(P('dp', 'cp', None), P('dp', 'cp', None), P(('dp', 'cp'), None, None), P(('dp', 'cp'), None, None), P(('dp', 'cp'), None, None), P(('dp', 'cp'), None), P('dp'), P('dp')), check_vma=False)
```

```python
import functools
import math
import jax
import jax.numpy as jnp
from jax import lax
from jax.experimental import pallas as pl
from jax.experimental.pallas import tpu as pltpu
from jax.sharding import PartitionSpec as P

EPS = 1e-5
ROPE_BASE = 10000.0
BF16 = jnp.bfloat16
F32 = jnp.float32
VMEM_LIMIT = 63 * 1024 * 1024
NT = (((1,), (1,)), ((), ()))
ANY = pl.BlockSpec(memory_space=pl.ANY)
VM = pl.BlockSpec(memory_space=pltpu.VMEM)
CORES = 2
PAD = 8
ATTN_TILE = 256
COL_TILE = 512
ROWS = 16


def dot(a, b):
    return jnp.dot(a, b, preferred_element_type=F32)


def dot_nt(a, b):
    return lax.dot_general(a, b, NT, preferred_element_type=F32)


def sds(shape, dtype):
    return jax.ShapeDtypeStruct(shape, dtype)


def block(i, size):
    return pl.ds(pl.multiple_of(i * size, size), size)


class Place:
    def __init__(self, n_dev):
        self.n_dev = n_dev
        self.chips = n_dev // CORES
        self.me = lax.axis_index('cp')
        self.chip = self.me // CORES
        self.core = self.me % CORES
        self.partner = self.chip * CORES + 1 - self.core

    def ring(self, step):
        return lax.rem(self.chip + self.chips + step, self.chips)

    def dev(self, step, core):
        return self.ring(step) * CORES + core

    def peers(self, far):
        near = [self.partner] + [self.dev(s, c) for s in (1, -1) for c in range(CORES)]
        return near + ([self.dev(2, c) for c in range(CORES)] if far else [])


def send(src, dst, ssem, rsem, to):
    return pltpu.make_async_remote_copy(src_ref=src, dst_ref=dst, send_sem=ssem, recv_sem=rsem, device_id={'cp': to}, device_id_type=pl.DeviceIdType.MESH)


def meet(peers):
    barrier = pltpu.get_barrier_semaphore()
    for peer in peers:
        pl.semaphore_signal(barrier, inc=1, device_id={'cp': peer}, device_id_type=pl.DeviceIdType.MESH)
    pl.semaphore_wait(barrier, len(peers))


class Exchange:
    def __init__(self, at, src, dst, relay, ssem, rsem):
        self.at, self.src, self.dst, self.relay, self.ssem, self.rsem = at, src, dst, relay, ssem, rsem
        near = [(0, 1 - at.core)] + [(s, c) for s in (1, -1) for c in range(CORES)]
        n = at.n_dev
        self.near = [send(src(at.dev(s, c)), dst(at.me), ssem.at[i], rsem.at[at.me], at.dev(s, c)) for i, (s, c) in enumerate(near)]
        self.far = [send(src(at.dev(2, i)), relay.at[i], ssem.at[5 + i], rsem.at[n + i], at.dev(step, at.core)) for i, step in enumerate((1, -1))]
        self.on = [send(relay.at[i], dst(at.dev(-step, at.core)), ssem.at[7 + i], rsem.at[at.dev(-step, at.core)], at.dev(step, i)) for i, step in enumerate((1, -1))]

    def start(self):
        for copy in self.far + self.near:
            copy.start()

    def pass_on(self):
        for far, on in zip(self.far, self.on):
            far.wait_recv()
            on.start()

    def wait_recv(self):
        at = self.at
        for j in range(1, at.n_dev):
            origin = lax.rem(at.me + j, at.n_dev)
            send(self.src(at.me), self.dst(origin), self.ssem.at[0], self.rsem.at[origin], at.partner).wait_recv()

    def wait_send(self):
        for copy in self.far + self.near + self.on:
            copy.wait_send()


def layer_norm(x, gain, bias=None):
    cen = x - jnp.mean(x, axis=-1, keepdims=True)
    inv = lax.rsqrt(jnp.mean(cen * cen, axis=-1, keepdims=True) + EPS)
    return cen * inv, inv


def masked_scores(k, q, limit, tile, scale):
    s = dot_nt(k[:limit], q) * scale
    row = lax.broadcasted_iota(jnp.int32, (tile, tile), 0)
    col = lax.broadcasted_iota(jnp.int32, (tile, tile), 1)
    tail = jnp.where(row <= col, s[limit - tile:], -1e30)
    return tail if limit == tile else jnp.concatenate([s[:limit - tile], tail], axis=0)


def front_body(n_dev, group, x_ref, gain_ref, bias_ref, cos_ref, sa_ref, sb_ref, pos_ref, freq_ref, dy_ref, wq_ref, wk_ref, wv_ref, wo_ref,
               dy_all, ht_all, a_all, g_out, dwo_out,
               h_ref, ht_ref, dyo_ref, qs_ref, qkv_ref, a_ref, at_ref, at2_ref, stat_ref, da_ref, g_ref, kt_ref, vt_ref, dk_ref, dv_ref,
               cost_ref, sint_ref, relay_q, relay_h, relay_a,
               dy_ssem, dy_rsem, q_ssem, q_rsem, h_ssem, h_rsem, a_ssem, a_rsem, t_sem, loc_sem, mix_sem):
    at = Place(n_dev)
    n_batch, seq, width = dy_ref.shape
    n_tok = n_batch * seq
    head_dim = wq_ref.shape[2]
    cols = (group + 2) * head_dim
    n_rows = group * head_dim
    half = n_rows // CORES
    n_seq = n_dev * seq
    quarter = head_dim // 4
    scale = head_dim ** -0.5
    core, me = at.core, at.me

    meet(at.peers(False))

    sub = seq // 2
    first = [send(dy_ref.at[b], dy_all.at[me, b], dy_ssem.at[b], dy_rsem.at[b], at.dev(step, core)) for b, step in enumerate((1, -1))]
    second = [[send(dy_ref.at[1 - b, pl.ds(p * sub, sub)], dy_all.at[me, 1 - b, pl.ds(p * sub, sub)], dy_ssem.at[2 + 2 * b + p], dy_rsem.at[2 + 2 * b + p], at.dev(step, core)) for p in range(2)] for b, step in enumerate((1, -1))]
    origin = [at.dev(-1, core), at.dev(1, core)]
    far_dev = at.dev(2, core)
    again = [send(dy_all.at[origin[b], b], dy_all.at[origin[b], b], dy_ssem.at[6 + b], dy_rsem.at[6 + b], at.dev(step, core)) for b, step in enumerate((1, -1))]
    own_across = send(dy_ref, dy_all.at[me], dy_ssem.at[8], dy_rsem.at[8], at.partner)
    first_across = [send(dy_all.at[origin[b], b], dy_all.at[origin[b], b], dy_ssem.at[9 + b], dy_rsem.at[9 + b], at.partner) for b in range(2)]
    second_across = [send(dy_all.at[origin[b], 1 - b], dy_all.at[origin[b], 1 - b], dy_ssem.at[11 + b], dy_rsem.at[11 + b], at.partner) for b in range(2)]
    far_across = [send(dy_all.at[far_dev, b], dy_all.at[far_dev, b], dy_ssem.at[13 + b], dy_rsem.at[13 + b], at.partner) for b in range(2)]
    for b in range(2):
        first[b].start()
        second[b][0].start()
    own_across.start()
    dy_in = pltpu.make_async_copy(dy_ref, dyo_ref, loc_sem.at[0])
    dy_in.start()

    @pl.loop(0, n_tok // ROWS)
    def _(step):
        sl = block(step, ROWS)
        hat, _ = layer_norm(x_ref[sl, :].astype(F32), None)
        h_ref[sl, :] = (hat * (1.0 + gain_ref[...]) + bias_ref[...]).astype(BF16)

    def project(wq, wk, wv):
        chip = pl.program_id(0)
        slabs = [wq[j] for j in range(group)] + [wk[0], wv[0]]
        y = dot(h_ref[...], jnp.concatenate(slabs, axis=1))
        cos, sa, sb = cos_ref[...], sa_ref[...], sb_ref[...]
        for j in range(group + 2):
            v = y[:, j * head_dim:(j + 1) * head_dim]
            if j < group + 1:
                v = v * cos + pltpu.roll(v, head_dim - quarter, 1) * sa + pltpu.roll(v, quarter, 1) * sb
            v = v.astype(BF16)
            for b in range(n_batch):
                qs_ref[chip * n_batch + b, 0:seq, j * head_dim:(j + 1) * head_dim] = v[b * seq:(b + 1) * seq]
        for b in range(n_batch):
            qs_ref[chip * n_batch + b, seq:, :] = pos_ref[b]

    pltpu.emit_pipeline(
        project,
        grid=(at.chips,),
        in_specs=[pl.BlockSpec((group, width, head_dim), lambda i: (i, 0, 0)), pl.BlockSpec((1, width, head_dim), lambda i: (i, 0, 0)), pl.BlockSpec((1, width, head_dim), lambda i: (i, 0, 0))],
        out_specs=[],
    )(wq_ref, wk_ref, wv_ref)

    qkv = Exchange(at, lambda d: qs_ref.at[d], lambda d: qkv_ref.at[d], relay_q, q_ssem, q_rsem)
    qkv.start()
    dy_in.wait()
    dy_keep = pltpu.make_async_copy(dyo_ref, dy_all.at[me], loc_sem.at[0])
    dy_keep.start()
    qkv_ref[me] = qs_ref[me]

    @pl.loop(0, width // 128)
    def _(step):
        sl = block(step, 128)
        ht_ref[sl, :] = h_ref[:, sl].T

    qkv.pass_on()
    for b in range(2):
        second[b][1].start()
    for b in range(2):
        first[b].wait_recv()
        again[b].start()
        first_across[b].start()
    hcols = Exchange(at, lambda d: ht_ref.at[block(d, half)], lambda d: ht_all.at[d], relay_h, h_ssem, h_rsem)
    hcols.start()
    h_keep = pltpu.make_async_copy(ht_ref.at[block(me, half)], ht_all.at[me], loc_sem.at[1])
    h_keep.start()

    qkv.wait_recv()
    k_all = lambda: qkv_ref[:, 0:seq, n_rows:n_rows + head_dim].reshape(n_seq, head_dim)
    v_all = lambda: qkv_ref[:, 0:seq, n_rows + head_dim:].reshape(n_seq, head_dim)
    q_head = lambda j: qkv_ref[:, 0:seq, block(j, head_dim)].reshape(n_seq, head_dim)
    kt_ref[...] = k_all().T
    vt_ref[...] = v_all().T

    @pl.loop(0, group)
    def _(j):
        q, k = q_head(j), k_all()
        for t in range(n_seq // ATTN_TILE):
            limit = (t + 1) * ATTN_TILE
            sl = slice(t * ATTN_TILE, limit)
            s = masked_scores(k, q[sl], limit, ATTN_TILE, scale)
            top = jnp.max(s, axis=0, keepdims=True)
            e = jnp.exp(s - top)
            inv = 1.0 / jnp.sum(e, axis=0, keepdims=True)
            mix_t = dot(vt_ref[:, :limit], (e * inv).astype(BF16)).astype(BF16)
            at_ref[block(j, head_dim), sl] = mix_t
            a_ref[sl, block(j, head_dim)] = mix_t.T
            stat_ref[j, 0:1, sl] = top
            stat_ref[j, 1:2, sl] = inv

    mixed = Exchange(at, lambda d: a_ref.at[block(d, seq)], lambda d: a_all.at[d], relay_a, a_ssem, a_rsem)
    mixed.start()
    a_keep = pltpu.make_async_copy(a_ref.at[block(me, seq)], a_all.at[me], loc_sem.at[2])
    a_keep.start()
    heads_across = send(at_ref.at[block(1 - core, half)], at2_ref.at[:, block(core, n_seq)], t_sem.at[0], t_sem.at[1], at.partner)
    heads_across.start()
    at2_ref[:, block(core, n_seq)] = at_ref[block(core, half), :]
    for d in range(n_dev):
        spots = qkv_ref[d, seq:seq + 1, 0:2 * seq].astype(F32)
        angle = freq_ref[...] * (spots[:, :seq] * 256.0 + spots[:, seq:])
        cost_ref[:, d * seq:(d + 1) * seq] = angle
    cost_all = cost_ref[...]
    cost_ref[...] = jnp.cos(cost_all)
    sint_ref[...] = jnp.sin(cost_all)

    for b in range(2):
        for p in range(2):
            second[b][p].wait_recv()
        second_across[b].start()
    own_across.wait_recv()
    for copy in first_across + second_across:
        copy.wait_recv()
    dy_keep.wait()

    def mix_grad(wo_vm, dyk):
        wo_in = pltpu.make_async_copy(wo_ref.at[block(at.chip, n_rows)], wo_vm, mix_sem.at[2])
        wo_in.start()

        def fetch(i, slot):
            step = jnp.where(i == 0, 0, jnp.where(i == 1, 1, jnp.where(i == 2, 3, 2)))
            chip = at.ring(step)
            return chip, pltpu.make_async_copy(dy_all.at[pl.ds(chip * CORES, CORES), core], dyk.at[slot], mix_sem.at[slot])

        fetch(0, 0)[1].start()
        wo_in.wait()

        @pl.loop(0, at.chips)
        def _(i):
            slot = lax.rem(i, 2)

            @pl.when(i == 1)
            def _():
                for b in range(2):
                    again[b].wait_recv()
                    far_across[b].start()

            @pl.when(i == at.chips - 2)
            def _():
                for b in range(2):
                    far_across[b].wait_recv()

            chip, copy = fetch(i, slot)
            copy.wait()

            @pl.when(i < at.chips - 1)
            def _():
                fetch(i + 1, 1 - slot)[1].start()

            rows = dyk[slot].reshape(CORES * seq, width)
            da_ref[block(chip, CORES * seq), :] = dot_nt(rows, wo_vm[...]).astype(BF16)

    pl.run_scoped(mix_grad, pltpu.VMEM((n_rows, width), BF16), pltpu.VMEM((2, CORES, seq, width), BF16))

    dk_ref[...] = jnp.zeros_like(dk_ref)
    dv_ref[...] = jnp.zeros_like(dv_ref)

    def rotate_back(t, cos, sin):
        u, w = t[:quarter], t[quarter:2 * quarter]
        return jnp.concatenate([u * cos + w * sin, w * cos - u * sin, t[2 * quarter:]], axis=0)

    @pl.loop(0, group)
    def _(j):
        @pl.when(j == 1)
        def _():
            hcols.pass_on()

        @pl.when(j == group - 1)
        def _():
            mixed.pass_on()

        q, k, v = q_head(j), k_all(), v_all()
        for t in range(n_seq // ATTN_TILE):
            limit = (t + 1) * ATTN_TILE
            sl = slice(t * ATTN_TILE, limit)
            da = da_ref[sl, block(j, head_dim)]
            s = masked_scores(k, q[sl], limit, ATTN_TILE, scale)
            p = jnp.exp(s - stat_ref[j, 0:1, sl]) * stat_ref[j, 1:2, sl]
            dp = dot_nt(v[:limit], da)
            row_dot = jnp.sum(p * dp, axis=0, keepdims=True)
            ds = (p * (dp - row_dot) * scale).astype(BF16)
            dv_ref[:limit, :] += dot(p.astype(BF16), da)
            dk_ref[:limit, :] += dot(ds, q[sl])
            back = rotate_back(dot(kt_ref[:, :limit], ds), cost_ref[:, sl], sint_ref[:, sl])
            g_ref[sl, block(j, head_dim)] = back.T.astype(BF16)

    g_ref[:, n_rows:n_rows + head_dim] = rotate_back(dk_ref[...].T, cost_ref[...], sint_ref[...]).T.astype(BF16)
    g_ref[:, n_rows + head_dim:] = dv_ref[...].astype(BF16)
    g_keep = pltpu.make_async_copy(g_ref, g_out, loc_sem.at[0])
    g_keep.start()

    heads_across.wait_recv()

    def wo_tile(dy, out):
        pieces = [dy[d, b] for b in range(n_batch) for d in range(n_dev)]
        out[...] = dot(at2_ref[...], jnp.concatenate(pieces, axis=0))

    pltpu.emit_pipeline(
        wo_tile,
        grid=(width // COL_TILE,),
        in_specs=[pl.BlockSpec((n_dev, n_batch, seq, COL_TILE), lambda i: (0, 0, 0, i))],
        out_specs=[pl.BlockSpec((half, COL_TILE), lambda i: (0, i))],
    )(dy_all, dwo_out)

    hcols.wait_recv()
    mixed.wait_recv()
    for copy in first + second[0] + second[1] + again + [own_across] + first_across + second_across + far_across + [heads_across]:
        copy.wait_send()
    for exchange in (qkv, hcols, mixed):
        exchange.wait_send()
    h_keep.wait()
    a_keep.wait()
    g_keep.wait()


def front(n_dev, x, gain, bias, tables, pos_rows, freq, dy, wq, wk, wv, wo):
    n_batch, seq, width = dy.shape
    n_tok = n_batch * seq
    kv_heads = wk.shape[0]
    group, head_dim = wq.shape[0] // kv_heads, wq.shape[2]
    cols = (group + 2) * head_dim
    n_rows = group * head_dim
    half = n_rows // CORES
    n_seq = n_dev * seq
    quarter = head_dim // 4
    dma = pltpu.SemaphoreType.DMA
    vm = pltpu.VMEM
    return pl.pallas_call(
        functools.partial(front_body, n_dev, group),
        out_shape=(sds((n_dev, n_batch, seq, width), BF16), sds((n_dev, half, n_tok), BF16), sds((n_dev, seq, n_rows), BF16), sds((n_seq, cols), BF16), sds((half, width), F32)),
        in_specs=[VM] * 8 + [ANY] * 5,
        out_specs=(ANY,) * 5,
        scratch_shapes=[
            vm((n_tok, width), BF16), vm((width, n_tok), BF16), vm(dy.shape, BF16), vm((n_dev, seq + PAD, cols), BF16), vm((n_dev, seq + PAD, cols), BF16),
            vm((n_seq, n_rows), BF16), vm((n_rows, n_seq), BF16), vm((half, n_batch * n_seq), BF16), vm((group, 8, n_seq), F32), vm((n_seq, n_rows), BF16), vm((n_seq, cols), BF16),
            vm((head_dim, n_seq), BF16), vm((head_dim, n_seq), BF16), vm((n_seq, head_dim), F32), vm((n_seq, head_dim), F32),
            vm((quarter, n_seq), F32), vm((quarter, n_seq), F32),
            vm((2, seq + PAD, cols), BF16), vm((2, half, n_tok), BF16), vm((2, seq, n_rows), BF16),
            dma((15,)), dma((15,)), dma((9,)), dma((n_dev + 2,)), dma((9,)), dma((n_dev + 2,)), dma((9,)), dma((n_dev + 2,)), dma((2,)), dma((3,)), dma((3,)),
        ],
        compiler_params=pltpu.CompilerParams(collective_id=0, has_side_effects=True, vmem_limit_bytes=VMEM_LIMIT),
        cost_estimate=pl.CostEstimate(flops=10 ** 11, bytes_accessed=10 ** 8, transcendentals=0),
        name='front',
    )(x.reshape(n_tok, width), gain.reshape(1, width), bias.reshape(1, width), *tables, pos_rows, freq.reshape(quarter, 1), dy, wq, wk, wv, wo)


def back_body(n_dev, group, x_ref, dy_ref, gain_ref, g_own, a_all, ht_all, wq_ref, wk_ref, wv_ref, wo_ref,
              out_ref, dx_ref, dwq_out, dwk_out, dwv_out, sum_ref,
              g_ref, mix_ref, lhs_ref, w_ref, acc_ref, dxv_ref, tile_ref, part_ref, all_ref,
              g_ssem, g_rsem, s_ssem, s_rsem, loc_sem, w_sem, t_sem):
    at = Place(n_dev)
    n_tok, width = x_ref.shape
    seq = a_all.shape[1]
    n_batch = n_tok // seq
    n_rows = a_all.shape[2]
    head_dim = wq_ref.shape[2]
    half = ht_all.shape[1]
    n_seq = g_own.shape[0]
    part = n_seq // 2
    core, me = at.core, at.me

    meet(at.peers(True))

    def piece(dev, h):
        return g_ref.at[dev, pl.ds(h * part, part)]

    first = [send(g_own.at[pl.ds(h * part, part)], piece(me, h), g_ssem.at[h], g_rsem.at[h], at.dev(step, core)) for h, step in enumerate((1, -1))]
    second = [send(g_own.at[pl.ds((1 - h) * part, part)], piece(me, 1 - h), g_ssem.at[2 + h], g_rsem.at[2 + h], at.dev(step, core)) for h, step in enumerate((1, -1))]
    origin = [at.dev(-1, core), at.dev(1, core)]
    far_dev = at.dev(2, core)
    again = [send(piece(origin[h], h), piece(origin[h], h), g_ssem.at[4 + h], g_rsem.at[4 + h], at.dev(step, core)) for h, step in enumerate((1, -1))]
    own_across = send(g_own, g_ref.at[me], g_ssem.at[6], g_rsem.at[6], at.partner)
    first_across = [send(piece(origin[h], h), piece(origin[h], h), g_ssem.at[7 + h], g_rsem.at[7 + h], at.partner) for h in range(2)]
    second_across = [send(piece(origin[h], 1 - h), piece(origin[h], 1 - h), g_ssem.at[9 + h], g_rsem.at[9 + h], at.partner) for h in range(2)]
    far_across = [send(piece(far_dev, h), piece(far_dev, h), g_ssem.at[11 + h], g_rsem.at[11 + h], at.partner) for h in range(2)]
    for copy in first + second + [own_across]:
        copy.start()
    g_in = pltpu.make_async_copy(g_own, g_ref.at[me], loc_sem.at[0])
    g_in.start()
    mix_in = [pltpu.make_async_copy(a_all.at[s], mix_ref.at[pl.ds((s % n_batch) * seq, seq), pl.ds((s // n_batch) * n_rows, n_rows)], loc_sem.at[1 + s]) for s in range(n_dev)]
    lhs_in = [pltpu.make_async_copy(ht_all.at[d, :, pl.ds(b * seq, seq)], lhs_ref.at[:, pl.ds((b * n_dev + d) * seq, seq)], loc_sem.at[1 + n_dev + b * n_dev + d]) for d in range(n_dev) for b in range(n_batch)]
    for copy in mix_in + lhs_in:
        copy.start()

    def chip_at(i):
        return at.ring(jnp.where(i == 0, 0, jnp.where(i == 1, 1, jnp.where(i == 2, 3, 2))))

    def weights(i, slot):
        chip = chip_at(i)
        return [
            pltpu.make_async_copy(wq_ref.at[block(chip, group)], w_ref.at[slot, pl.ds(0, group)], w_sem.at[slot, 0]),
            pltpu.make_async_copy(wk_ref.at[chip], w_ref.at[slot, group], w_sem.at[slot, 1]),
            pltpu.make_async_copy(wv_ref.at[chip], w_ref.at[slot, group + 1], w_sem.at[slot, 2]),
        ]

    def tiles(i):
        chip = chip_at(i)
        return [
            pltpu.make_async_copy(tile_ref.at[pl.ds(0, group)], dwq_out.at[block(chip, group)], t_sem.at[0]),
            pltpu.make_async_copy(tile_ref.at[group], dwk_out.at[chip], t_sem.at[1]),
            pltpu.make_async_copy(tile_ref.at[group + 1], dwv_out.at[chip], t_sem.at[2]),
        ]

    for copy in mix_in:
        copy.wait()

    def out_tile(wo, x, out):
        out[...] = (x[...].astype(F32) + dot(mix_ref[...], wo[...])).astype(BF16)

    pltpu.emit_pipeline(
        out_tile,
        grid=(width // COL_TILE,),
        in_specs=[pl.BlockSpec((width, COL_TILE), lambda i: (0, i)), pl.BlockSpec((n_tok, COL_TILE), lambda i: (0, i))],
        out_specs=[pl.BlockSpec((n_tok, COL_TILE), lambda i: (0, i))],
    )(wo_ref, x_ref, out_ref)

    for i in range(2):
        for copy in weights(i, i):
            copy.start()
    for copy in lhs_in:
        copy.wait()
    g_in.wait()
    own_across.wait_recv()

    sums = [send(all_ref.at[me], all_ref.at[me], s_ssem.at[j], s_rsem.at[me], peer) for j, peer in enumerate(at.peers(True))]

    @pl.loop(0, at.chips)
    def _(i):
        slot = lax.rem(i, 2)

        @pl.when(i == 1)
        def _():
            for h in range(2):
                first[h].wait_recv()
                again[h].start()
                first_across[h].start()
            for h in range(2):
                second[h].wait_recv()
                second_across[h].start()
            for copy in first_across + second_across:
                copy.wait_recv()

        @pl.when(i == at.chips - 1)
        def _():
            for h in range(2):
                again[h].wait_recv()
                far_across[h].start()
            for h in range(2):
                far_across[h].wait_recv()

        for copy in weights(i, slot):
            copy.wait()
        chip = chip_at(i)
        mine = jnp.concatenate([g_ref[chip * CORES + b, block(me, seq), :] for b in range(n_batch)], axis=0)
        w = jnp.concatenate([w_ref[slot, j] for j in range(group + 2)], axis=1)
        grow = dot_nt(mine, w)

        @pl.when(i == 0)
        def _():
            acc_ref[...] = grow

        @pl.when(i > 0)
        def _():
            acc_ref[...] += grow

        @pl.when(i < at.chips - 2)
        def _():
            for copy in weights(i + 2, slot):
                copy.start()

        @pl.when(i == at.chips - 1)
        def _():
            part_ref[...] = jnp.zeros_like(part_ref)

            @pl.loop(0, n_tok // ROWS)
            def _(step):
                sl = block(step, ROWS)
                hat, inv = layer_norm(x_ref[sl, :].astype(F32), None)
                dh = acc_ref[sl, :]
                gh = dh * (1.0 + gain_ref[...])
                one = jnp.mean(gh, axis=-1, keepdims=True)
                two = jnp.mean(gh * hat, axis=-1, keepdims=True)
                dxv_ref[sl, :] = (dy_ref[sl, :].astype(F32) + inv * (gh - one - hat * two)).astype(BF16)
                dg = dh * hat
                part_ref[0] += dg[0:8] + dg[8:16]
                part_ref[1] += dh[0:8] + dh[8:16]

            all_ref[me, 0:1, :] = jnp.sum(part_ref[0], axis=0, keepdims=True)
            all_ref[me, 1:2, :] = jnp.sum(part_ref[1], axis=0, keepdims=True)
            pltpu.make_async_copy(dxv_ref, dx_ref, loc_sem.at[0]).start()
            for copy in sums:
                copy.start()

        y = dot(lhs_ref[...], g_ref[pl.ds(chip * CORES, CORES)].reshape(n_batch * n_seq, (group + 2) * head_dim))

        @pl.when(i > 0)
        def _():
            for copy in tiles(i - 1):
                copy.wait()

        for j in range(group + 2):
            tile_ref[j] = y[:, j * head_dim:(j + 1) * head_dim]
        for copy in tiles(i):
            copy.start()

    for j in range(1, n_dev):
        source = lax.rem(me + j, n_dev)
        send(all_ref.at[me], all_ref.at[source], s_ssem.at[0], s_rsem.at[source], at.partner).wait_recv()
    total = all_ref[0]
    for d in range(1, n_dev):
        total = total + all_ref[d]
    sum_ref[...] = total
    for copy in sums + first + second + again + [own_across] + first_across + second_across + far_across:
        copy.wait_send()
    for copy in tiles(at.chips - 1):
        copy.wait()
    pltpu.make_async_copy(dxv_ref, dx_ref, loc_sem.at[0]).wait()


def back(n_dev, x, dy, gain, g_own, a_all, ht_all, wq, wk, wv, wo):
    n_batch, seq, width = dy.shape
    n_tok = n_batch * seq
    kv_heads = wk.shape[0]
    group, head_dim = wq.shape[0] // kv_heads, wq.shape[2]
    cols = (group + 2) * head_dim
    half = ht_all.shape[1]
    n_seq = n_dev * seq
    dma = pltpu.SemaphoreType.DMA
    vm = pltpu.VMEM
    return pl.pallas_call(
        functools.partial(back_body, n_dev, group),
        out_shape=(sds((n_tok, width), BF16), sds((n_tok, width), BF16), sds((kv_heads * group, half, head_dim), F32), sds((kv_heads, half, head_dim), F32), sds((kv_heads, half, head_dim), F32), sds((2, width), F32)),
        in_specs=[VM] * 3 + [ANY] * 7,
        out_specs=(ANY,) * 5 + (VM,),
        scratch_shapes=[
            vm((n_dev, n_seq, cols), BF16), vm((n_tok, width), BF16), vm((half, n_dev * n_tok), BF16), vm((2, group + 2, width, head_dim), BF16), vm((n_tok, width), F32), vm((n_tok, width), BF16),
            vm((group + 2, half, head_dim), F32), vm((2, 8, width), F32), vm((n_dev, 2, width), F32),
            dma((13,)), dma((13,)), dma((n_dev,)), dma((n_dev,)), dma((1 + 3 * n_dev,)), dma((2, 3)), dma((3,)),
        ],
        compiler_params=pltpu.CompilerParams(collective_id=1, has_side_effects=True, vmem_limit_bytes=VMEM_LIMIT),
        cost_estimate=pl.CostEstimate(flops=10 ** 11, bytes_accessed=10 ** 8, transcendentals=0),
        name='back',
    )(x.reshape(n_tok, width), dy.reshape(n_tok, width), gain.reshape(1, width), g_own, a_all, ht_all, wq, wk, wv, wo)


def solution(mesh):
    n_dev = mesh.shape['cp']

    def device_step(x_act, d_out, positions, ln_gain, ln_bias, w_query, w_key, w_value, w_out):
        n_batch, seq, width = x_act.shape
        q_heads, (kv_heads, head_dim) = w_query.shape[1], w_key.shape[1:]
        group = q_heads // kv_heads
        quarter = head_dim // 4
        assert n_batch == CORES and n_dev // CORES == kv_heads == 4 and q_heads * head_dim == width

        freq = jnp.exp(jnp.arange(quarter, dtype=F32) * (-2.0 * math.log(ROPE_BASE) / (head_dim // 2)))
        angles = positions.astype(F32).reshape(n_batch * seq, 1) * freq
        cos, sin = jnp.cos(angles), jnp.sin(angles)
        rest = jnp.zeros((n_batch * seq, head_dim - 2 * quarter), F32)
        none = jnp.zeros_like(sin)
        tables = (jnp.concatenate([cos, cos, rest + 1.0], axis=1), jnp.concatenate([-sin, none, rest], axis=1), jnp.concatenate([none, sin, rest], axis=1))
        cols = (group + 2) * head_dim
        pair = jnp.stack([positions // 256, positions % 256], axis=1).astype(BF16).reshape(n_batch, 1, 2 * seq)
        pos_rows = jnp.pad(pair, ((0, 0), (0, PAD - 1), (0, cols - 2 * seq)))
        by_head = lambda t: jnp.transpose(t, (1, 0, 2))
        wq, wk, wv = by_head(w_query), by_head(w_key), by_head(w_value)

        dy_all, ht_all, a_all, g_own, dwo = front(n_dev, x_act, ln_gain, ln_bias, tables, pos_rows, freq, d_out, wq, wk, wv, w_out)
        out, dx, dwq, dwk, dwv, sums = back(n_dev, x_act, d_out, ln_gain, g_own, a_all, ht_all, wq, wk, wv, w_out)
        return (out.reshape(x_act.shape), dx.reshape(x_act.shape), by_head(dwq), by_head(dwk), by_head(dwv), dwo, sums[0], sums[1])

    return jax.shard_map(device_step, mesh=mesh, in_specs=(P('dp', 'cp', None), P('dp', 'cp', None), P('dp', 'cp'), P(None), P(None), P(None, None, None), P(None, None, None), P(None, None, None), P(None, None)), out_specs=(P('dp', 'cp', None), P('dp', 'cp', None), P(('dp', 'cp'), None, None), P(('dp', 'cp'), None, None), P(('dp', 'cp'), None, None), P(('dp', 'cp'), None), P('dp'), P('dp')), check_vma=False)
```

```python
import functools
import math
import jax
import jax.numpy as jnp
import numpy as np
from jax import lax
from jax.experimental import pallas as pl
from jax.experimental.pallas import tpu as pltpu
from jax.sharding import PartitionSpec as P

EPS = 1e-5
ROPE_BASE = 10000.0
BF16 = jnp.bfloat16
F32 = jnp.float32
VMEM_LIMIT = 63 * 1024 * 1024
NT = (((1,), (1,)), ((), ()))
ANY = pl.BlockSpec(memory_space=pl.ANY)
VM = pl.BlockSpec(memory_space=pltpu.VMEM)
CORES = 2
ATTN_TILE = 256
COL_TILE = 512
ROWS = 16


def dot(a, b):
    return jnp.dot(a, b, preferred_element_type=F32)


def dot_nt(a, b):
    return lax.dot_general(a, b, NT, preferred_element_type=F32)


def sds(shape, dtype):
    return jax.ShapeDtypeStruct(shape, dtype)


def block(i, size):
    return pl.ds(pl.multiple_of(i * size, size), size)


class Place:
    def __init__(self, n_dev):
        self.n_dev = n_dev
        self.chips = n_dev // CORES
        self.me = lax.axis_index('cp')
        self.chip = self.me // CORES
        self.core = self.me % CORES
        self.partner = self.chip * CORES + 1 - self.core

    def ring(self, step):
        return lax.rem(self.chip + self.chips + step, self.chips)

    def dev(self, step, core):
        return self.ring(step) * CORES + core

    def peers(self, far):
        near = [self.partner] + [self.dev(s, c) for s in (1, -1) for c in range(CORES)]
        return near + ([self.dev(2, c) for c in range(CORES)] if far else [])


def send(src, dst, ssem, rsem, to):
    return pltpu.make_async_remote_copy(src_ref=src, dst_ref=dst, send_sem=ssem, recv_sem=rsem, device_id={'cp': to}, device_id_type=pl.DeviceIdType.MESH)


def meet(peers):
    barrier = pltpu.get_barrier_semaphore()
    for peer in peers:
        pl.semaphore_signal(barrier, inc=1, device_id={'cp': peer}, device_id_type=pl.DeviceIdType.MESH)
    pl.semaphore_wait(barrier, len(peers))


class Exchange:
    def __init__(self, at, src, dst, relay, ssem, rsem):
        self.at, self.src, self.dst, self.relay, self.ssem, self.rsem = at, src, dst, relay, ssem, rsem
        near = [(0, 1 - at.core)] + [(s, c) for s in (1, -1) for c in range(CORES)]
        n = at.n_dev
        self.near = [send(src(at.dev(s, c)), dst(at.me), ssem.at[i], rsem.at[at.me], at.dev(s, c)) for i, (s, c) in enumerate(near)]
        self.far = [send(src(at.dev(2, i)), relay.at[i], ssem.at[5 + i], rsem.at[n + i], at.dev(step, at.core)) for i, step in enumerate((1, -1))]
        self.on = [send(relay.at[i], dst(at.dev(-step, at.core)), ssem.at[7 + i], rsem.at[at.dev(-step, at.core)], at.dev(step, i)) for i, step in enumerate((1, -1))]

    def start(self):
        for copy in self.far + self.near:
            copy.start()

    def pass_on(self):
        for far, on in zip(self.far, self.on):
            far.wait_recv()
            on.start()

    def wait_recv(self):
        at = self.at
        for j in range(1, at.n_dev):
            origin = lax.rem(at.me + j, at.n_dev)
            send(self.src(at.me), self.dst(origin), self.ssem.at[0], self.rsem.at[origin], at.partner).wait_recv()

    def wait_send(self):
        for copy in self.far + self.near + self.on:
            copy.wait_send()


def layer_norm(x):
    cen = x - jnp.mean(x, axis=-1, keepdims=True)
    inv = lax.rsqrt(jnp.mean(cen * cen, axis=-1, keepdims=True) + EPS)
    return cen * inv, inv


def masked_scores(k, q, limit, tile, scale):
    s = dot_nt(k[:limit], q) * scale
    row = lax.broadcasted_iota(jnp.int32, (tile, tile), 0)
    col = lax.broadcasted_iota(jnp.int32, (tile, tile), 1)
    tail = jnp.where(row <= col, s[limit - tile:], -1e30)
    return tail if limit == tile else jnp.concatenate([s[:limit - tile], tail], axis=0)


def front_body(n_dev, group, x_ref, gain_ref, bias_ref, pos_ref, freq_ref, dy_ref, wq_ref, wk_ref, wv_ref, wo_ref,
               dy_all, ht_all, a_all, g_out, dwo_out, wkv_out,
               h_ref, ht_ref, dyo_ref, qs_ref, qkv_ref, a_ref, at_ref, at2_ref, stat_ref, da_ref, g_ref, kt_ref, vt_ref, dk_ref, dv_ref,
               cost_ref, sint_ref, tab_ref, spot_ref, relay_q, relay_h, relay_a,
               dy_ssem, dy_rsem, q_ssem, q_rsem, h_ssem, h_rsem, a_ssem, a_rsem, p_ssem, p_rsem, t_sem, loc_sem, mix_sem):
    at = Place(n_dev)
    n_batch, seq, width = dy_ref.shape
    n_tok = n_batch * seq
    head_dim = wq_ref.shape[2]
    cols = (group + 2) * head_dim
    n_rows = group * head_dim
    half = n_rows // CORES
    n_seq = n_dev * seq
    quarter = head_dim // 4
    scale = head_dim ** -0.5
    core, me = at.core, at.me

    meet(at.peers(True))

    sub = seq // 2
    first = [send(dy_ref.at[b], dy_all.at[me, b], dy_ssem.at[b], dy_rsem.at[b], at.dev(step, core)) for b, step in enumerate((1, -1))]
    second = [[send(dy_ref.at[1 - b, pl.ds(p * sub, sub)], dy_all.at[me, 1 - b, pl.ds(p * sub, sub)], dy_ssem.at[2 + 2 * b + p], dy_rsem.at[2 + 2 * b + p], at.dev(step, core)) for p in range(2)] for b, step in enumerate((1, -1))]
    origin = [at.dev(-1, core), at.dev(1, core)]
    far_dev = at.dev(2, core)
    again = [send(dy_all.at[origin[b], b], dy_all.at[origin[b], b], dy_ssem.at[6 + b], dy_rsem.at[6 + b], at.dev(step, core)) for b, step in enumerate((1, -1))]
    own_across = send(dy_ref, dy_all.at[me], dy_ssem.at[8], dy_rsem.at[8], at.partner)
    first_across = [send(dy_all.at[origin[b], b], dy_all.at[origin[b], b], dy_ssem.at[9 + b], dy_rsem.at[9 + b], at.partner) for b in range(2)]
    second_across = [send(dy_all.at[origin[b], 1 - b], dy_all.at[origin[b], 1 - b], dy_ssem.at[11 + b], dy_rsem.at[11 + b], at.partner) for b in range(2)]
    far_across = [send(dy_all.at[far_dev, b], dy_all.at[far_dev, b], dy_ssem.at[13 + b], dy_rsem.at[13 + b], at.partner) for b in range(2)]
    for b in range(2):
        first[b].start()
        second[b][0].start()
    own_across.start()
    spots = [send(pos_ref, spot_ref.at[me], p_ssem.at[j], p_rsem.at[me], peer) for j, peer in enumerate(at.peers(True))]
    for copy in spots:
        copy.start()
    dy_in = pltpu.make_async_copy(dy_ref, dyo_ref, loc_sem.at[0])
    dy_in.start()
    spot_ref[me] = pos_ref[...]

    freq = freq_ref[...]
    for b in range(n_batch):
        angle = freq * pos_ref[b:b + 1, :].astype(F32)
        cos, sin, none = jnp.cos(angle), jnp.sin(angle), jnp.zeros((quarter, seq), F32)
        rest = jnp.zeros((head_dim - 2 * quarter, seq), F32)
        for i, rows in enumerate(([cos, cos, rest + 1.0], [-sin, none, rest], [none, sin, rest])):
            tab_ref[i, b * seq:(b + 1) * seq, :] = jnp.concatenate(rows, axis=0).T

    gain = (1.0 + gain_ref[...]).reshape(1, width)
    bias = bias_ref[...].reshape(1, width)

    @pl.loop(0, n_tok // ROWS)
    def _(step):
        sl = block(step, ROWS)
        hat, _ = layer_norm(x_ref[sl, :].astype(F32))
        h_ref[sl, :] = (hat * gain + bias).astype(BF16)

    def project_all(wkv_ref, raw_ref):
        raw_in = [pltpu.make_async_copy(w, raw_ref.at[i], mix_sem.at[i]) for i, w in enumerate((wk_ref, wv_ref))]
        for copy in raw_in:
            copy.start()
        for copy in raw_in:
            copy.wait()
        span = 64 * at.chips
        row = lax.broadcasted_iota(jnp.int32, (span, span), 0)
        col = lax.broadcasted_iota(jnp.int32, (span, span), 1)
        pick = jnp.where(col == lax.rem(row, 64) * at.chips + lax.div(row, 64), 1.0, 0.0).astype(BF16)

        @pl.loop(0, width // 64)
        def _(step):
            sl = block(step, span)
            rows = dot(pick, jnp.concatenate([raw_ref[0, sl, :], raw_ref[1, sl, :]], axis=1)).astype(BF16)
            for n in range(at.chips):
                wkv_ref[n, block(step, 64), :] = rows[n * 64:(n + 1) * 64]

        keep = pltpu.make_async_copy(wkv_ref, wkv_out, mix_sem.at[2])
        keep.start()

        def project(wq):
            chip = pl.program_id(0)
            y = dot(h_ref[...], jnp.concatenate([wq[j] for j in range(group)] + [wkv_ref[chip]], axis=1))
            cos, sa, sb = tab_ref[0], tab_ref[1], tab_ref[2]
            for j in range(group + 2):
                v = y[:, j * head_dim:(j + 1) * head_dim]
                if j < group + 1:
                    v = v * cos + pltpu.roll(v, head_dim - quarter, 1) * sa + pltpu.roll(v, quarter, 1) * sb
                v = v.astype(BF16)
                for b in range(n_batch):
                    qs_ref[chip * n_batch + b, :, j * head_dim:(j + 1) * head_dim] = v[b * seq:(b + 1) * seq]

        pltpu.emit_pipeline(
            project,
            grid=(at.chips,),
            in_specs=[pl.BlockSpec((group, width, head_dim), lambda i: (i, 0, 0))],
            out_specs=[],
        )(wq_ref)
        keep.wait()

    pl.run_scoped(project_all, pltpu.VMEM((at.chips, width, 2 * head_dim), BF16), pltpu.VMEM((2, at.chips * width, head_dim), BF16))

    qkv = Exchange(at, lambda d: qs_ref.at[d], lambda d: qkv_ref.at[d], relay_q, q_ssem, q_rsem)
    qkv.start()
    dy_in.wait()
    dy_keep = pltpu.make_async_copy(dyo_ref, dy_all.at[me], loc_sem.at[0])
    dy_keep.start()
    qkv_ref[me] = qs_ref[me]

    @pl.loop(0, width // 128)
    def _(step):
        sl = block(step, 128)
        ht_ref[sl, :] = h_ref[:, sl].T

    qkv.pass_on()
    for b in range(2):
        second[b][1].start()
    for b in range(2):
        first[b].wait_recv()
        again[b].start()
        first_across[b].start()
    hcols = Exchange(at, lambda d: ht_ref.at[block(d, half)], lambda d: ht_all.at[d], relay_h, h_ssem, h_rsem)
    hcols.start()
    h_keep = pltpu.make_async_copy(ht_ref.at[block(me, half)], ht_all.at[me], loc_sem.at[1])
    h_keep.start()

    qkv.wait_recv()
    k_all = lambda: qkv_ref[:, :, n_rows:n_rows + head_dim].reshape(n_seq, head_dim)
    v_all = lambda: qkv_ref[:, :, n_rows + head_dim:].reshape(n_seq, head_dim)
    q_head = lambda j: qkv_ref[:, :, block(j, head_dim)].reshape(n_seq, head_dim)
    kt_ref[...] = k_all().T
    vt_ref[...] = v_all().T

    @pl.loop(0, group)
    def _(j):
        q, k = q_head(j), k_all()
        for t in range(n_seq // ATTN_TILE):
            limit = (t + 1) * ATTN_TILE
            sl = slice(t * ATTN_TILE, limit)
            s = masked_scores(k, q[sl], limit, ATTN_TILE, scale)
            top = jnp.max(s, axis=0, keepdims=True)
            e = jnp.exp(s - top)
            inv = 1.0 / jnp.sum(e, axis=0, keepdims=True)
            mix_t = dot(vt_ref[:, :limit], (e * inv).astype(BF16)).astype(BF16)
            at_ref[block(j, head_dim), sl] = mix_t
            a_ref[sl, block(j, head_dim)] = mix_t.T
            stat_ref[j, 0:1, sl] = top
            stat_ref[j, 1:2, sl] = inv

    mixed = Exchange(at, lambda d: a_ref.at[block(d, seq)], lambda d: a_all.at[d], relay_a, a_ssem, a_rsem)
    mixed.start()
    a_keep = pltpu.make_async_copy(a_ref.at[block(me, seq)], a_all.at[me], loc_sem.at[2])
    a_keep.start()
    heads_across = send(at_ref.at[block(1 - core, half)], at2_ref.at[:, block(core, n_seq)], t_sem.at[0], t_sem.at[1], at.partner)
    heads_across.start()
    at2_ref[:, block(core, n_seq)] = at_ref[block(core, half), :]
    for j in range(1, n_dev):
        source = lax.rem(me + j, n_dev)
        send(pos_ref, spot_ref.at[source], p_ssem.at[0], p_rsem.at[source], at.partner).wait_recv()
    for d in range(n_dev):
        angle = freq * spot_ref[d, pl.ds(core, 1), :].astype(F32)
        cost_ref[:, d * seq:(d + 1) * seq] = jnp.cos(angle)
        sint_ref[:, d * seq:(d + 1) * seq] = jnp.sin(angle)

    for b in range(2):
        for p in range(2):
            second[b][p].wait_recv()
        second_across[b].start()
    own_across.wait_recv()
    for copy in first_across + second_across:
        copy.wait_recv()
    dy_keep.wait()

    def mix_grad(wo_vm, dyk):
        wo_in = pltpu.make_async_copy(wo_ref.at[block(at.chip, n_rows)], wo_vm, mix_sem.at[2])
        wo_in.start()

        def fetch(i, slot):
            step = jnp.where(i == 0, 0, jnp.where(i == 1, 1, jnp.where(i == 2, 3, 2)))
            chip = at.ring(step)
            return chip, pltpu.make_async_copy(dy_all.at[pl.ds(chip * CORES, CORES), core], dyk.at[slot], mix_sem.at[slot])

        fetch(0, 0)[1].start()
        wo_in.wait()

        @pl.loop(0, at.chips)
        def _(i):
            slot = lax.rem(i, 2)

            @pl.when(i == 1)
            def _():
                for b in range(2):
                    again[b].wait_recv()
                    far_across[b].start()

            @pl.when(i == at.chips - 2)
            def _():
                for b in range(2):
                    far_across[b].wait_recv()

            chip, copy = fetch(i, slot)
            copy.wait()

            @pl.when(i < at.chips - 1)
            def _():
                fetch(i + 1, 1 - slot)[1].start()

            rows = dyk[slot].reshape(CORES * seq, width)
            da_ref[block(chip, CORES * seq), :] = dot_nt(rows, wo_vm[...]).astype(BF16)

    pl.run_scoped(mix_grad, pltpu.VMEM((n_rows, width), BF16), pltpu.VMEM((2, CORES, seq, width), BF16))

    dk_ref[...] = jnp.zeros_like(dk_ref)
    dv_ref[...] = jnp.zeros_like(dv_ref)

    def rotate_back(t, cos, sin):
        u, w = t[:quarter], t[quarter:2 * quarter]
        return jnp.concatenate([u * cos + w * sin, w * cos - u * sin, t[2 * quarter:]], axis=0)

    @pl.loop(0, group)
    def _(j):
        @pl.when(j == 1)
        def _():
            hcols.pass_on()

        @pl.when(j == group - 1)
        def _():
            mixed.pass_on()

        q, k, v = q_head(j), k_all(), v_all()
        for t in range(n_seq // ATTN_TILE):
            limit = (t + 1) * ATTN_TILE
            sl = slice(t * ATTN_TILE, limit)
            da = da_ref[sl, block(j, head_dim)]
            s = masked_scores(k, q[sl], limit, ATTN_TILE, scale)
            p = jnp.exp(s - stat_ref[j, 0:1, sl]) * stat_ref[j, 1:2, sl]
            dp = dot_nt(v[:limit], da)
            row_dot = jnp.sum(p * dp, axis=0, keepdims=True)
            ds = (p * (dp - row_dot) * scale).astype(BF16)
            dv_ref[:limit, :] += dot(p.astype(BF16), da)
            dk_ref[:limit, :] += dot(ds, q[sl])
            back = rotate_back(dot(kt_ref[:, :limit], ds), cost_ref[:, sl], sint_ref[:, sl])
            g_ref[sl, block(j, head_dim)] = back.T.astype(BF16)

    g_ref[:, n_rows:n_rows + head_dim] = rotate_back(dk_ref[...].T, cost_ref[...], sint_ref[...]).T.astype(BF16)
    g_ref[:, n_rows + head_dim:] = dv_ref[...].astype(BF16)
    g_keep = pltpu.make_async_copy(g_ref, g_out, loc_sem.at[0])
    g_keep.start()

    heads_across.wait_recv()

    def wo_tile(dy, out):
        pieces = [dy[d, b] for b in range(n_batch) for d in range(n_dev)]
        out[...] = dot(at2_ref[...], jnp.concatenate(pieces, axis=0))

    pltpu.emit_pipeline(
        wo_tile,
        grid=(width // COL_TILE,),
        in_specs=[pl.BlockSpec((n_dev, n_batch, seq, COL_TILE), lambda i: (0, 0, 0, i))],
        out_specs=[pl.BlockSpec((half, COL_TILE), lambda i: (0, i))],
    )(dy_all, dwo_out)

    hcols.wait_recv()
    mixed.wait_recv()
    for copy in first + second[0] + second[1] + again + [own_across] + first_across + second_across + far_across + [heads_across] + spots:
        copy.wait_send()
    for exchange in (qkv, hcols, mixed):
        exchange.wait_send()
    h_keep.wait()
    a_keep.wait()
    g_keep.wait()


def front(n_dev, x, gain, bias, positions, freq, dy, wq, wk, wv, wo):
    n_batch, seq, width = dy.shape
    n_tok = n_batch * seq
    head_dim = wq.shape[2]
    chips = n_dev // CORES
    group = wq.shape[0] // chips
    cols = (group + 2) * head_dim
    n_rows = group * head_dim
    half = n_rows // CORES
    n_seq = n_dev * seq
    quarter = head_dim // 4
    dma = pltpu.SemaphoreType.DMA
    vm = pltpu.VMEM
    return pl.pallas_call(
        functools.partial(front_body, n_dev, group),
        out_shape=(sds((n_dev, n_batch, seq, width), BF16), sds((n_dev, half, n_tok), BF16), sds((n_dev, seq, n_rows), BF16), sds((n_seq, cols), BF16), sds((half, width), F32), sds((chips, width, 2 * head_dim), BF16)),
        in_specs=[VM] * 5 + [ANY] * 5,
        out_specs=(ANY,) * 6,
        scratch_shapes=[
            vm((n_tok, width), BF16), vm((width, n_tok), BF16), vm(dy.shape, BF16), vm((n_dev, seq, cols), BF16), vm((n_dev, seq, cols), BF16),
            vm((n_seq, n_rows), BF16), vm((n_rows, n_seq), BF16), vm((half, n_batch * n_seq), BF16), vm((group, 8, n_seq), F32), vm((n_seq, n_rows), BF16), vm((n_seq, cols), BF16),
            vm((head_dim, n_seq), BF16), vm((head_dim, n_seq), BF16), vm((n_seq, head_dim), F32), vm((n_seq, head_dim), F32),
            vm((quarter, n_seq), F32), vm((quarter, n_seq), F32), vm((3, n_tok, head_dim), F32), vm((n_dev, n_batch, seq), jnp.int32),
            vm((2, seq, cols), BF16), vm((2, half, n_tok), BF16), vm((2, seq, n_rows), BF16),
            dma((15,)), dma((15,)), dma((9,)), dma((n_dev + 2,)), dma((9,)), dma((n_dev + 2,)), dma((9,)), dma((n_dev + 2,)), dma((n_dev,)), dma((n_dev,)), dma((2,)), dma((3,)), dma((3,)),
        ],
        compiler_params=pltpu.CompilerParams(collective_id=0, has_side_effects=True, vmem_limit_bytes=VMEM_LIMIT),
        cost_estimate=pl.CostEstimate(flops=10 ** 11, bytes_accessed=10 ** 8, transcendentals=0),
        name='front',
    )(x.reshape(n_tok, width), gain, bias, positions, freq, dy, wq, wk, wv, wo)


def back_body(n_dev, group, x_ref, dy_ref, gain_ref, g_own, a_all, ht_all, wq_ref, wkv_ref, wo_ref,
              out_ref, dx_ref, dwq_out, dwk_out, dwv_out, dgain_ref, dbias_ref,
              g_ref, mix_ref, lhs_ref, w_ref, wkv2_ref, acc_ref, hat_ref, inv_ref, dxv_ref, tile_ref, kv_ref, part_ref, all_ref,
              g_ssem, g_rsem, r_ssem, r_rsem, x_ssem, x_rsem, s_ssem, s_rsem, loc_sem, w_sem, t_sem):
    at = Place(n_dev)
    n_tok, width = x_ref.shape
    seq = a_all.shape[1]
    n_batch = n_tok // seq
    n_rows = a_all.shape[2]
    head_dim = wq_ref.shape[2]
    half = ht_all.shape[1]
    n_seq = g_own.shape[0]
    chips = at.chips
    part = n_seq // chips
    cols = (group + 2) * head_dim
    core, me = at.core, at.me

    meet(at.peers(True))

    def piece(dev, q):
        return g_ref.at[dev, block(q, part)]

    steps = (1, -1)
    turn = [[at.ring(2 + q) for q in range(chips)], [at.ring(q) for q in range(chips)]]
    direct = [[send(g_own.at[block(turn[i][q], part)], piece(me, turn[i][q]), g_ssem.at[i, q], g_rsem.at[i, q], at.dev(steps[i], core)) for q in range(chips)] for i in range(2)]
    origin = [at.dev(-1, core), at.dev(1, core)]
    came = [[at.ring(1 + q) for q in range(chips)], [at.ring(1 + q) for q in range(chips)]]
    again = [[send(piece(origin[i], came[i][q]), piece(origin[i], came[i][q]), r_ssem.at[i, q], r_rsem.at[i, q], at.dev(steps[i], core)) for q in range(2)] for i in range(2)]
    far_dev = at.dev(2, core)
    ends = [[at.ring(q) for q in range(2)], [at.ring(2 + q) for q in range(2)]]
    own_across = send(g_own, g_ref.at[me], x_ssem.at[0], x_rsem.at[0], at.partner)
    near_across = [send(g_ref.at[origin[i]], g_ref.at[origin[i]], x_ssem.at[1 + i], x_rsem.at[1 + i], at.partner) for i in range(2)]
    far_across = [[send(piece(far_dev, ends[i][q]), piece(far_dev, ends[i][q]), x_ssem.at[3 + 2 * i + q], x_rsem.at[3 + 2 * i + q], at.partner) for q in range(2)] for i in range(2)]
    for q in range(chips):
        for i in range(2):
            direct[i][q].start()
    own_across.start()
    g_in = pltpu.make_async_copy(g_own, g_ref.at[me], loc_sem.at[0])
    g_in.start()
    mix_in = [pltpu.make_async_copy(a_all.at[s], mix_ref.at[pl.ds((s % n_batch) * seq, seq), pl.ds((s // n_batch) * n_rows, n_rows)], loc_sem.at[1 + s]) for s in range(n_dev)]
    lhs_in = [pltpu.make_async_copy(ht_all.at[d, :, pl.ds(b * seq, seq)], lhs_ref.at[:, pl.ds((b * n_dev + d) * seq, seq)], loc_sem.at[1 + n_dev + b * n_dev + d]) for d in range(n_dev) for b in range(n_batch)]
    for copy in mix_in + lhs_in:
        copy.start()

    def chip_at(i):
        return at.ring(jnp.where(i == 0, 0, jnp.where(i == 1, 1, jnp.where(i == 2, 3, 2))))

    def weights(i, slot):
        chip = chip_at(i)
        return [
            pltpu.make_async_copy(wq_ref.at[block(chip, group)], w_ref.at[slot], w_sem.at[slot, 0]),
            pltpu.make_async_copy(wkv_ref.at[chip], wkv2_ref.at[slot], w_sem.at[slot, 1]),
        ]

    def tiles(i):
        return pltpu.make_async_copy(tile_ref, dwq_out.at[block(chip_at(i), group)], t_sem.at[0])

    gain = (1.0 + gain_ref[...]).reshape(1, width)

    @pl.loop(0, n_tok // ROWS)
    def _(step):
        sl = block(step, ROWS)
        hat, inv = layer_norm(x_ref[sl, :].astype(F32))
        hat_ref[sl, :] = hat
        inv_ref[sl, :] = jnp.broadcast_to(inv, (ROWS, 128))

    for copy in mix_in:
        copy.wait()

    def out_tile(wo, x, out):
        out[...] = (x[...].astype(F32) + dot(mix_ref[...], wo[...])).astype(BF16)

    pltpu.emit_pipeline(
        out_tile,
        grid=(width // COL_TILE,),
        in_specs=[pl.BlockSpec((width, COL_TILE), lambda i: (0, i)), pl.BlockSpec((n_tok, COL_TILE), lambda i: (0, i))],
        out_specs=[pl.BlockSpec((n_tok, COL_TILE), lambda i: (0, i))],
    )(wo_ref, x_ref, out_ref)

    for i in range(2):
        for copy in weights(i, i):
            copy.start()
    for copy in lhs_in:
        copy.wait()
    g_in.wait()
    own_across.wait_recv()
    sums = [send(all_ref.at[me], all_ref.at[me], s_ssem.at[j], s_rsem.at[me], peer) for j, peer in enumerate(at.peers(True))]
    last = chips - 1

    @pl.loop(0, chips)
    def _(i):
        slot = lax.rem(i, 2)
        chip = chip_at(i)

        @pl.when(i == 1)
        def _():
            for q in range(2):
                for j in range(2):
                    direct[j][q].wait_recv()
                    again[j][q].start()
            for j in range(2):
                for q in range(2, chips):
                    direct[j][q].wait_recv()
                near_across[j].start()
            for copy in near_across:
                copy.wait_recv()

        @pl.when(i == last)
        def _():
            for j in range(2):
                again[j][0].wait_recv()
                far_across[j][0].start()
            for j in range(2):
                far_across[j][0].wait_recv()

        for copy in weights(i, slot):
            copy.wait()
        mine = jnp.concatenate([g_ref[chip * CORES + b, block(me, seq), :] for b in range(n_batch)], axis=0)
        grow = dot_nt(mine, jnp.concatenate([w_ref[slot, j] for j in range(group)] + [wkv2_ref[slot]], axis=1))

        @pl.when(i == 0)
        def _():
            acc_ref[...] = grow

        @pl.when(i > 0)
        def _():
            acc_ref[...] += grow

        @pl.when(i < chips - 2)
        def _():
            for copy in weights(i + 2, slot):
                copy.start()

        @pl.when(i == last)
        def _():
            part_ref[...] = jnp.zeros_like(part_ref)

            @pl.loop(0, n_tok // ROWS)
            def _(step):
                sl = block(step, ROWS)
                hat = hat_ref[sl, :]
                inv = inv_ref[sl, 0:1]
                dh = acc_ref[sl, :]
                dg = dh * hat
                gh = dh * gain
                one = jnp.mean(gh, axis=-1, keepdims=True)
                two = jnp.mean(dg * gain, axis=-1, keepdims=True)
                dxv_ref[sl, :] = (dy_ref[sl, :].astype(F32) + inv * (gh - one - hat * two)).astype(BF16)
                part_ref[0] += dg[0:8] + dg[8:16]
                part_ref[1] += dh[0:8] + dh[8:16]

            all_ref[me, 0:1, :] = jnp.sum(part_ref[0], axis=0, keepdims=True)
            all_ref[me, 1:2, :] = jnp.sum(part_ref[1], axis=0, keepdims=True)
            pltpu.make_async_copy(dxv_ref, dx_ref, loc_sem.at[0]).start()
            for copy in sums:
                copy.start()

        @pl.when(i > 0)
        def _():
            tiles(i - 1).wait()

        def gather(halves):
            rows = [at.ring(q) for q in halves]
            lhs = [lhs_ref[:, pl.ds(pl.multiple_of(b * n_seq + q * part, part), part)] for b in range(n_batch) for q in rows]
            rhs = [g_ref[chip * CORES + b, block(q, part), :] for b in range(n_batch) for q in rows]
            return dot(jnp.concatenate(lhs, axis=1), jnp.concatenate(rhs, axis=0))

        def put(y, add):
            for j in range(group):
                v = y[:, j * head_dim:(j + 1) * head_dim]
                tile_ref[j] = tile_ref[j] + v if add else v
            for j in range(2):
                v = y[:, (group + j) * head_dim:(group + j + 1) * head_dim]
                rows = pl.ds(chip, half, stride=chips)
                kv_ref[j, rows, :] = kv_ref[j, rows, :] + v if add else v

        put(gather((0, 2)), False)

        @pl.when(i == last)
        def _():
            for j in range(2):
                again[j][1].wait_recv()
                far_across[j][1].start()
            for j in range(2):
                far_across[j][1].wait_recv()

        put(gather((1, 3)), True)
        tiles(i).start()

    kv_put = [pltpu.make_async_copy(kv_ref.at[j], ref, t_sem.at[1 + j]) for j, ref in enumerate((dwk_out, dwv_out))]
    for copy in kv_put:
        copy.start()
    for j in range(1, n_dev):
        source = lax.rem(me + j, n_dev)
        send(all_ref.at[me], all_ref.at[source], s_ssem.at[0], s_rsem.at[source], at.partner).wait_recv()
    total = all_ref[0]
    for d in range(1, n_dev):
        total = total + all_ref[d]
    dgain_ref[...] = total[0:1].reshape(width)
    dbias_ref[...] = total[1:2].reshape(width)
    for copy in sums + direct[0] + direct[1] + again[0] + again[1] + [own_across] + near_across + far_across[0] + far_across[1]:
        copy.wait_send()
    tiles(last).wait()
    for copy in kv_put:
        copy.wait()
    pltpu.make_async_copy(dxv_ref, dx_ref, loc_sem.at[0]).wait()


def back(n_dev, x, dy, gain, g_own, a_all, ht_all, wq, wkv, wo):
    n_batch, seq, width = dy.shape
    n_tok = n_batch * seq
    chips, _, pair = wkv.shape
    head_dim = wq.shape[2]
    group = wq.shape[0] // chips
    cols = (group + 2) * head_dim
    half = ht_all.shape[1]
    n_seq = n_dev * seq
    dma = pltpu.SemaphoreType.DMA
    vm = pltpu.VMEM
    return pl.pallas_call(
        functools.partial(back_body, n_dev, group),
        out_shape=(sds((n_tok, width), BF16), sds((n_tok, width), BF16), sds((chips * group, half, head_dim), F32), sds((chips * half, head_dim), F32), sds((chips * half, head_dim), F32), sds((width,), F32), sds((width,), F32)),
        in_specs=[VM] * 3 + [ANY] * 6,
        out_specs=(ANY,) * 5 + (VM, VM),
        scratch_shapes=[
            vm((n_dev, n_seq, cols), BF16), vm((n_tok, width), BF16), vm((half, n_dev * n_tok), BF16), vm((2, group, width, head_dim), BF16), vm((2, width, pair), BF16), vm((n_tok, width), F32), vm((n_tok, width), F32), vm((n_tok, 128), F32), vm((n_tok, width), BF16),
            vm((group, half, head_dim), F32), vm((2, chips * half, head_dim), F32), vm((2, 8, width), F32), vm((n_dev, 2, width), F32),
            dma((2, chips)), dma((2, chips)), dma((2, 2)), dma((2, 2)), dma((7,)), dma((7,)), dma((n_dev,)), dma((n_dev,)), dma((1 + 3 * n_dev,)), dma((2, 2)), dma((3,)),
        ],
        compiler_params=pltpu.CompilerParams(collective_id=1, has_side_effects=True, vmem_limit_bytes=VMEM_LIMIT),
        cost_estimate=pl.CostEstimate(flops=10 ** 11, bytes_accessed=10 ** 8, transcendentals=0),
        name='back',
    )(x.reshape(n_tok, width), dy.reshape(n_tok, width), gain, g_own, a_all, ht_all, wq, wkv, wo)


def solution(mesh):
    n_dev = mesh.shape['cp']

    def device_step(x_act, d_out, positions, ln_gain, ln_bias, w_query, w_key, w_value, w_out):
        n_batch, seq, width = x_act.shape
        q_heads, (kv_heads, head_dim) = w_query.shape[1], w_key.shape[1:]
        group = q_heads // kv_heads
        quarter = head_dim // 4
        assert n_batch == CORES and n_dev // CORES == kv_heads == 4 and q_heads * head_dim == width

        freq = np.exp(np.arange(quarter) * (-2.0 * math.log(ROPE_BASE) / (head_dim // 2))).astype(np.float32).reshape(quarter, 1)
        by_head = lambda t: jnp.transpose(t, (1, 0, 2))
        by_row = lambda t: t.reshape(width * kv_heads, head_dim)
        wq = by_head(w_query)

        dy_all, ht_all, a_all, g_own, dwo, wkv = front(n_dev, x_act, ln_gain, ln_bias, positions, jnp.asarray(freq), d_out, wq, by_row(w_key), by_row(w_value), w_out)
        out, dx, dwq, dwk, dwv, dgain, dbias = back(n_dev, x_act, d_out, ln_gain, g_own, a_all, ht_all, wq, wkv, w_out)
        kv_rows = lambda t: t.reshape(width // n_dev, kv_heads, head_dim)
        return (out.reshape(x_act.shape), dx.reshape(x_act.shape), by_head(dwq), kv_rows(dwk), kv_rows(dwv), dwo, dgain, dbias)

    return jax.shard_map(device_step, mesh=mesh, in_specs=(P('dp', 'cp', None), P('dp', 'cp', None), P('dp', 'cp'), P(None), P(None), P(None, None, None), P(None, None, None), P(None, None, None), P(None, None)), out_specs=(P('dp', 'cp', None), P('dp', 'cp', None), P(('dp', 'cp'), None, None), P(('dp', 'cp'), None, None), P(('dp', 'cp'), None, None), P(('dp', 'cp'), None), P('dp'), P('dp')), check_vma=False)
```

```python
import functools
import math
import jax
import jax.numpy as jnp
import numpy as np
from jax import lax
from jax.experimental import pallas as pl
from jax.experimental.pallas import tpu as pltpu
from jax.sharding import PartitionSpec as P

EPS = 1e-5
ROPE_BASE = 10000.0
BF16 = jnp.bfloat16
F32 = jnp.float32
VMEM_LIMIT = 46 * 1024 * 1024
NT = (((1,), (1,)), ((), ()))
ANY = pl.BlockSpec(memory_space=pl.ANY)
VM = pl.BlockSpec(memory_space=pltpu.VMEM)
HBM = pl.BlockSpec(memory_space=pltpu.HBM)
CORES = 2
ATTN_TILE = 256
COL_TILE = 512
ROWS = 16
W_SLOTS = 7
W_ROWS = 512


def dot(a, b):
    return jnp.dot(a, b, preferred_element_type=F32)


def dot_nt(a, b):
    return lax.dot_general(a, b, NT, preferred_element_type=F32)


def sds(shape, dtype):
    return jax.ShapeDtypeStruct(shape, dtype)


def block(i, size):
    return pl.ds(pl.multiple_of(i * size, size), size)


class Place:
    def __init__(self, n_dev):
        self.n_dev = n_dev
        self.chips = n_dev // CORES
        self.me = lax.axis_index('cp')
        self.chip = self.me // CORES
        self.core = self.me % CORES
        self.partner = self.chip * CORES + 1 - self.core

    def ring(self, step):
        return lax.rem(self.chip + self.chips + step, self.chips)

    def dev(self, step, core):
        return self.ring(step) * CORES + core

    def peers(self, far):
        near = [self.partner] + [self.dev(s, c) for s in (1, -1) for c in range(CORES)]
        return near + ([self.dev(2, c) for c in range(CORES)] if far else [])


def send(src, dst, ssem, rsem, to):
    return pltpu.make_async_remote_copy(src_ref=src, dst_ref=dst, send_sem=ssem, recv_sem=rsem, device_id={'cp': to}, device_id_type=pl.DeviceIdType.MESH)


def meet(peers):
    barrier = pltpu.get_barrier_semaphore()
    for peer in peers:
        pl.semaphore_signal(barrier, inc=1, device_id={'cp': peer}, device_id_type=pl.DeviceIdType.MESH)
    pl.semaphore_wait(barrier, len(peers))


class Exchange:
    def __init__(self, at, src, dst, relay, ssem, rsem):
        self.at, self.src, self.dst, self.relay, self.ssem, self.rsem = at, src, dst, relay, ssem, rsem
        near = [(0, 1 - at.core)] + [(s, c) for s in (1, -1) for c in range(CORES)]
        n = at.n_dev
        self.near = [send(src(at.dev(s, c)), dst(at.me), ssem.at[i], rsem.at[at.me], at.dev(s, c)) for i, (s, c) in enumerate(near)]
        self.far = [send(src(at.dev(2, i)), relay.at[i], ssem.at[5 + i], rsem.at[n + i], at.dev(step, at.core)) for i, step in enumerate((1, -1))]
        self.on = [send(relay.at[i], dst(at.dev(-step, at.core)), ssem.at[7 + i], rsem.at[at.dev(-step, at.core)], at.dev(step, i)) for i, step in enumerate((1, -1))]

    def start(self):
        for copy in self.far + self.near:
            copy.start()

    def pass_on(self):
        for far, on in zip(self.far, self.on):
            far.wait_recv()
            on.start()

    def wait_recv(self):
        at = self.at
        for j in range(1, at.n_dev):
            origin = lax.rem(at.me + j, at.n_dev)
            send(self.src(at.me), self.dst(origin), self.ssem.at[0], self.rsem.at[origin], at.partner).wait_recv()

    def wait_send(self):
        for copy in self.far + self.near + self.on:
            copy.wait_send()


def layer_norm(x):
    cen = x - jnp.mean(x, axis=-1, keepdims=True)
    inv = lax.rsqrt(jnp.mean(cen * cen, axis=-1, keepdims=True) + EPS)
    return cen * inv, inv


def masked_scores(k, q, limit, tile, scale):
    s = dot_nt(k[:limit], q) * scale
    row = lax.broadcasted_iota(jnp.int32, (tile, tile), 0)
    col = lax.broadcasted_iota(jnp.int32, (tile, tile), 1)
    tail = jnp.where(row <= col, s[limit - tile:], -1e30)
    return tail if limit == tile else jnp.concatenate([s[:limit - tile], tail], axis=0)


def block_body(n_dev, group, gain_ref, bias_ref, pos_ref, freq_ref, x_hbm, dy_ref, wq_ref, wk_ref, wv_ref, wo_ref,
               out_ref, dx_ref, dwq_ref, dwk_ref, dwv_ref, dwo_ref, dgain_ref, dbias_ref, dy_all, ht_all, a_all, g_all, wkv_all,
               h_ref, ht_ref, qs_ref, qkv_ref, a_ref, at_ref, at2_ref, stat_ref, da_ref, kt_ref, vt_ref, dk_ref, dv_ref,
               cost_ref, sint_ref, tab_ref, spot_ref, relay_q, relay_h, relay_a, far_ref, part_ref, all_ref,
               dy_ssem, dy_rsem, q_ssem, q_rsem, h_ssem, h_rsem, a_ssem, a_rsem, p_ssem, p_rsem, t_sem,
               g_ssem, g_rsem, r_ssem, r_rsem, x_ssem, x_rsem, s_ssem, s_rsem, loc_sem, mix_sem, lhs_sem, w_sem, job_sem):
    at = Place(n_dev)
    n_batch, seq, width = dy_ref.shape
    n_tok = n_batch * seq
    head_dim = wq_ref.shape[2]
    cols = (group + 2) * head_dim
    n_rows = group * head_dim
    half = n_rows // CORES
    n_seq = n_dev * seq
    quarter = head_dim // 4
    scale = head_dim ** -0.5
    chips = at.chips
    core, me = at.core, at.me
    steps = (1, -1)
    origin = [at.dev(-1, core), at.dev(1, core)]
    far_dev = at.dev(2, core)

    meet(at.peers(True))

    sub = seq // 2
    first = [send(dy_ref.at[b], dy_all.at[me, b], dy_ssem.at[b], dy_rsem.at[b], at.dev(steps[b], core)) for b in range(2)]
    second = [[send(dy_ref.at[1 - b, pl.ds(p * sub, sub)], dy_all.at[me, 1 - b, pl.ds(p * sub, sub)], dy_ssem.at[2 + 2 * b + p], dy_rsem.at[2 + 2 * b + p], at.dev(steps[b], core)) for p in range(2)] for b in range(2)]
    again = [send(dy_all.at[origin[b], b], dy_all.at[origin[b], b], dy_ssem.at[6 + b], dy_rsem.at[6 + b], at.dev(steps[b], core)) for b in range(2)]
    own_across = send(dy_ref, dy_all.at[me], dy_ssem.at[8], dy_rsem.at[8], at.partner)
    first_across = [send(dy_all.at[origin[b], b], dy_all.at[origin[b], b], dy_ssem.at[9 + b], dy_rsem.at[9 + b], at.partner) for b in range(2)]
    second_across = [send(dy_all.at[origin[b], 1 - b], dy_all.at[origin[b], 1 - b], dy_ssem.at[11 + b], dy_rsem.at[11 + b], at.partner) for b in range(2)]
    far_across = [send(dy_all.at[far_dev, b], dy_all.at[far_dev, b], dy_ssem.at[13 + b], dy_rsem.at[13 + b], at.partner) for b in range(2)]
    for b in range(2):
        first[b].start()
        second[b][0].start()
    x_in = pltpu.make_async_copy(x_hbm, dx_ref, loc_sem.at[1])
    x_in.start()
    own_across.start()
    spots = [send(pos_ref, spot_ref.at[me], p_ssem.at[j], p_rsem.at[me], peer) for j, peer in enumerate(at.peers(True))]
    for copy in spots:
        copy.start()
    spot_ref[me] = pos_ref[...]

    freq = freq_ref[...]
    for b in range(n_batch):
        angle = freq * pos_ref[b:b + 1, :].astype(F32)
        cos, sin, none = jnp.cos(angle), jnp.sin(angle), jnp.zeros((quarter, seq), F32)
        rest = jnp.zeros((head_dim - 2 * quarter, seq), F32)
        for i, rows in enumerate(([cos, cos, rest + 1.0], [-sin, none, rest], [none, sin, rest])):
            tab_ref[i, b * seq:(b + 1) * seq, :] = jnp.concatenate(rows, axis=0).T

    gain = (1.0 + gain_ref[...]).reshape(1, width)
    bias = bias_ref[...].reshape(1, width)
    x_in.wait()

    @pl.loop(0, n_tok // ROWS)
    def _(step):
        sl = block(step, ROWS)
        hat, _ = layer_norm(dx_ref[sl, :].astype(F32))
        h_ref[sl, :] = (hat * gain + bias).astype(BF16)

    def project_all(wkv_ref, dyo_ref):
        dy_in = pltpu.make_async_copy(dy_ref, dyo_ref, loc_sem.at[0])
        dy_in.start()
        span = 64 * chips
        row = lax.broadcasted_iota(jnp.int32, (span, span), 0)
        col = lax.broadcasted_iota(jnp.int32, (span, span), 1)
        pick = jnp.where(col == lax.rem(row, 64) * chips + lax.div(row, 64), 1.0, 0.0).astype(BF16)
        batch = 4

        def part_heads(wk, wv):
            for i in range(batch):
                sl = slice(i * span, (i + 1) * span)
                rows = dot(pick, jnp.concatenate([wk[sl, :], wv[sl, :]], axis=1)).astype(BF16)
                for n in range(chips):
                    wkv_ref[n, block(pl.program_id(0) * batch + i, 64), :] = rows[n * 64:(n + 1) * 64]

        pltpu.emit_pipeline(part_heads, grid=(width // (64 * batch),), in_specs=[pl.BlockSpec((span * batch, head_dim), lambda i: (i, 0))] * 2, out_specs=[])(wk_ref, wv_ref)
        keep = pltpu.make_async_copy(wkv_ref, wkv_all, mix_sem.at[2])
        keep.start()
        dy_in.wait()
        dy_keep = pltpu.make_async_copy(dyo_ref, dy_all.at[me], loc_sem.at[0])
        dy_keep.start()

        def place(v, chip, j, turn):
            if turn:
                v = v * tab_ref[0] + pltpu.roll(v, head_dim - quarter, 1) * tab_ref[1] + pltpu.roll(v, quarter, 1) * tab_ref[2]
            v = v.astype(BF16)
            for b in range(n_batch):
                qs_ref[chip * n_batch + b, :, block(j, head_dim)] = v[b * seq:(b + 1) * seq]

        def project(wq):
            y = dot(h_ref[...], jnp.concatenate([wq[0], wq[1]], axis=1))
            for i in range(2):
                head = pl.program_id(0) * 2 + i
                place(y[:, i * head_dim:(i + 1) * head_dim], lax.div(head, group), lax.rem(head, group), True)

        pltpu.emit_pipeline(project, grid=(chips * group // 2,), in_specs=[pl.BlockSpec((2, width, head_dim), lambda i: (i, 0, 0))], out_specs=[])(wq_ref)

        @pl.loop(0, chips)
        def _(chip):
            y = dot(h_ref[...], wkv_ref[chip])
            place(y[:, :head_dim], chip, group, True)
            place(y[:, head_dim:], chip, group + 1, False)

        keep.wait()
        dy_keep.wait()

    pl.run_scoped(project_all, pltpu.VMEM((chips, width, 2 * head_dim), BF16), pltpu.VMEM(dy_ref.shape, BF16))

    qkv = Exchange(at, lambda d: qs_ref.at[d], lambda d: qkv_ref.at[d], relay_q, q_ssem, q_rsem)
    qkv.start()
    qkv_ref[me] = qs_ref[me]

    @pl.loop(0, width // 128)
    def _(step):
        sl = block(step, 128)
        ht_ref[sl, :] = h_ref[:, sl].T

    qkv.pass_on()
    for b in range(2):
        second[b][1].start()
    for b in range(2):
        first[b].wait_recv()
        again[b].start()
        first_across[b].start()
    hcols = Exchange(at, lambda d: ht_ref.at[block(d, half)], lambda d: ht_all.at[d], relay_h, h_ssem, h_rsem)
    hcols.start()
    h_keep = pltpu.make_async_copy(ht_ref.at[block(me, half)], ht_all.at[me], loc_sem.at[1])
    h_keep.start()

    qkv.wait_recv()
    k_all = lambda: qkv_ref[:, :, n_rows:n_rows + head_dim].reshape(n_seq, head_dim)
    v_all = lambda: qkv_ref[:, :, n_rows + head_dim:].reshape(n_seq, head_dim)
    q_head = lambda j: qkv_ref[:, :, block(j, head_dim)].reshape(n_seq, head_dim)
    kt_ref[...] = k_all().T
    vt_ref[...] = v_all().T

    @pl.loop(0, group)
    def _(j):
        q, k = q_head(j), k_all()
        for t in range(n_seq // ATTN_TILE):
            limit = (t + 1) * ATTN_TILE
            sl = slice(t * ATTN_TILE, limit)
            s = masked_scores(k, q[sl], limit, ATTN_TILE, scale)
            top = jnp.max(s, axis=0, keepdims=True)
            e = jnp.exp(s - top)
            inv = 1.0 / jnp.sum(e, axis=0, keepdims=True)
            mix_t = dot(vt_ref[:, :limit], (e * inv).astype(BF16)).astype(BF16)
            at_ref[block(j, head_dim), sl] = mix_t
            a_ref[sl, block(j, head_dim)] = mix_t.T
            stat_ref[j, 0:1, sl] = top
            stat_ref[j, 1:2, sl] = inv

    mixed = Exchange(at, lambda d: a_ref.at[block(d, seq)], lambda d: a_all.at[d], relay_a, a_ssem, a_rsem)
    mixed.start()
    a_keep = pltpu.make_async_copy(a_ref.at[block(me, seq)], a_all.at[me], loc_sem.at[2])
    a_keep.start()
    heads_across = send(at_ref.at[block(1 - core, half)], at2_ref.at[:, block(core, n_seq)], t_sem.at[0], t_sem.at[1], at.partner)
    heads_across.start()
    at2_ref[:, block(core, n_seq)] = at_ref[block(core, half), :]
    for j in range(1, n_dev):
        source = lax.rem(me + j, n_dev)
        send(pos_ref, spot_ref.at[source], p_ssem.at[0], p_rsem.at[source], at.partner).wait_recv()
    for d in range(n_dev):
        angle = freq * spot_ref[d, pl.ds(core, 1), :].astype(F32)
        cost_ref[:, d * seq:(d + 1) * seq] = jnp.cos(angle)
        sint_ref[:, d * seq:(d + 1) * seq] = jnp.sin(angle)

    for b in range(2):
        for p in range(2):
            second[b][p].wait_recv()
        second_across[b].start()
    own_across.wait_recv()
    for copy in first_across + second_across:
        copy.wait_recv()

    def chip_at(i):
        return at.ring(jnp.where(i == 0, 0, jnp.where(i == 1, 1, jnp.where(i == 2, 3, 2))))

    def mix_grad(wo_vm, dyk):
        wo_in = pltpu.make_async_copy(wo_ref.at[block(at.chip, n_rows)], wo_vm, mix_sem.at[2])
        wo_in.start()

        def fetch(i, slot):
            return pltpu.make_async_copy(dy_all.at[block(chip_at(i), CORES), core], dyk.at[slot], mix_sem.at[slot])

        fetch(0, 0).start()
        wo_in.wait()

        @pl.loop(0, chips)
        def _(i):
            slot = lax.rem(i, 2)

            @pl.when(i == 1)
            def _():
                for b in range(2):
                    again[b].wait_recv()
                    far_across[b].start()

            @pl.when(i == chips - 2)
            def _():
                for b in range(2):
                    far_across[b].wait_recv()

            fetch(i, slot).wait()

            @pl.when(i < chips - 1)
            def _():
                fetch(i + 1, 1 - slot).start()

            rows = dyk[slot].reshape(CORES * seq, width)
            da_ref[block(chip_at(i), CORES * seq), :] = dot_nt(rows, wo_vm[...]).astype(BF16)

    pl.run_scoped(mix_grad, pltpu.VMEM((n_rows, width), BF16), pltpu.VMEM((2, CORES, seq, width), BF16))

    qkv.wait_send()
    g_ref = qs_ref
    dk_ref[...] = jnp.zeros_like(dk_ref)
    dv_ref[...] = jnp.zeros_like(dv_ref)

    def rotate_back(t, cos, sin):
        u, w = t[:quarter], t[quarter:2 * quarter]
        return jnp.concatenate([u * cos + w * sin, w * cos - u * sin, t[2 * quarter:]], axis=0)

    def by_dev(t):
        return t.astype(BF16).reshape(t.shape[0] // seq, seq, head_dim)

    @pl.loop(0, group)
    def _(j):
        @pl.when(j == 1)
        def _():
            hcols.pass_on()

        @pl.when(j == group - 1)
        def _():
            mixed.pass_on()

        q, k, v = q_head(j), k_all(), v_all()
        for t in range(n_seq // ATTN_TILE):
            limit = (t + 1) * ATTN_TILE
            sl = slice(t * ATTN_TILE, limit)
            da = da_ref[sl, block(j, head_dim)]
            s = masked_scores(k, q[sl], limit, ATTN_TILE, scale)
            p = jnp.exp(s - stat_ref[j, 0:1, sl]) * stat_ref[j, 1:2, sl]
            dp = dot_nt(v[:limit], da)
            row_dot = jnp.sum(p * dp, axis=0, keepdims=True)
            ds = (p * (dp - row_dot) * scale).astype(BF16)
            dv_ref[:limit, :] += dot(p.astype(BF16), da)
            dk_ref[:limit, :] += dot(ds, q[sl])
            back = rotate_back(dot(kt_ref[:, :limit], ds), cost_ref[:, sl], sint_ref[:, sl])
            g_ref[t * ATTN_TILE // seq:limit // seq, :, block(j, head_dim)] = by_dev(back.T)

    g_ref[:, :, n_rows:n_rows + head_dim] = by_dev(rotate_back(dk_ref[...].T, cost_ref[...], sint_ref[...]).T)
    g_ref[:, :, n_rows + head_dim:] = by_dev(dv_ref[...])

    def span_of(q):
        return block(q, CORES)

    turn = [[at.ring(2 + q) for q in range(chips)], [at.ring(q) for q in range(chips)]]
    direct = [[send(g_ref.at[span_of(turn[i][q])], g_all.at[me, span_of(turn[i][q])], g_ssem.at[i, q], g_rsem.at[i, q], at.dev(steps[i], core)) for q in range(chips)] for i in range(2)]
    came = [at.ring(1 + q) for q in range(chips)]
    onward = [[send(g_all.at[origin[i], span_of(came[q])], far_ref.at[core, span_of(came[q])], r_ssem.at[i, q], r_rsem.at[i, q], at.dev(steps[i], core)) for q in range(2)] for i in range(2)]
    ends = [[at.ring(q) for q in range(2)], [at.ring(2 + q) for q in range(2)]]
    g_across = send(g_ref, g_all.at[me], x_ssem.at[0], x_rsem.at[0], at.partner)
    near_across = [[send(g_all.at[origin[i], span_of(came[q])], g_all.at[origin[i], span_of(came[q])], x_ssem.at[1 + i * chips + q], x_rsem.at[1 + i * chips + q], at.partner) for q in range(chips)] for i in range(2)]
    end_across = [[send(far_ref.at[core, span_of(ends[i][q])], far_ref.at[core, span_of(ends[i][q])], x_ssem.at[1 + (2 + i) * chips + q], x_rsem.at[1 + (2 + i) * chips + q], at.partner) for q in range(2)] for i in range(2)]
    for q in range(chips):
        for i in range(2):
            direct[i][q].start()
    g_across.start()
    g_keep = pltpu.make_async_copy(g_ref, g_all.at[me], loc_sem.at[0])
    g_keep.start()

    heads_across.wait_recv()

    def wo_tile(dy):
        pieces = [dy[d, b] for b in range(n_batch) for d in range(n_dev)]
        dwo_ref[:, block(pl.program_id(0), COL_TILE)] = dot(at2_ref[...], jnp.concatenate(pieces, axis=0))

    pltpu.emit_pipeline(wo_tile, grid=(width // COL_TILE,), in_specs=[pl.BlockSpec((n_dev, n_batch, seq, COL_TILE), lambda i: (0, 0, 0, i))], out_specs=[])(dy_all)

    hcols.wait_recv()
    h_keep.wait()
    lhs_in = [pltpu.make_async_copy(ht_all.at[d, :, pl.ds(b * seq, seq)], at2_ref.at[:, pl.ds((b * n_dev + d) * seq, seq)], lhs_sem.at[b * n_dev + d]) for d in range(n_dev) for b in range(n_batch)]
    for copy in lhs_in:
        copy.start()
    mixed.wait_recv()
    a_keep.wait()
    mix_in = [pltpu.make_async_copy(a_all.at[s], h_ref.at[pl.ds((s % n_batch) * seq, seq), pl.ds((s // n_batch) * n_rows, n_rows)], loc_sem.at[1 + s]) for s in range(n_dev)]
    for copy in mix_in:
        copy.start()
    for copy in mix_in:
        copy.wait()

    def out_tile(wo):
        sl = block(pl.program_id(0), COL_TILE)
        out_ref[:, sl] = (dx_ref[:, sl].astype(F32) + dot(h_ref[...], wo[...])).astype(BF16)

    pltpu.emit_pipeline(out_tile, grid=(width // COL_TILE,), in_specs=[pl.BlockSpec((width, COL_TILE), lambda i: (0, i))], out_specs=[])(wo_ref)

    dy_back = [pltpu.make_async_copy(dy_ref.at[b], h_ref.at[pl.ds(b * seq, seq)], loc_sem.at[1 + b]) for b in range(n_batch)]
    for copy in dy_back:
        copy.start()
    for copy in lhs_in:
        copy.wait()
    g_keep.wait()
    g_across.wait_recv()
    sums = [send(all_ref.at[me], all_ref.at[me], s_ssem.at[j], s_rsem.at[me], peer) for j, peer in enumerate(at.peers(True))]

    def weight_grads(wq_vm, wkv_vm, acc_ref, job_ref, mine_ref):
        n_slots = wq_vm.shape[0]
        chunk = wq_vm.shape[2]
        n_chunks = width // chunk
        total = n_chunks * chips

        def weights(s):
            slot = lax.rem(s, n_slots)
            chip = chip_at(lax.div(s, n_chunks))
            rows = block(lax.rem(s, n_chunks), chunk)
            return [
                pltpu.make_async_copy(wq_ref.at[block(chip, group), rows], wq_vm.at[slot], w_sem.at[slot, 0]),
                pltpu.make_async_copy(wkv_all.at[chip, rows], wkv_vm.at[slot], w_sem.at[slot, 1]),
            ]

        for s in range(n_slots):
            for copy in weights(s):
                copy.start()

        def grow(i, read):
            @pl.loop(0, n_chunks)
            def _(n):
                s = i * n_chunks + n
                slot = lax.rem(s, n_slots)
                for copy in weights(s):
                    copy.wait()
                rows = jnp.concatenate([read(b) for b in range(n_batch)], axis=0)
                part = dot_nt(rows, jnp.concatenate([wq_vm[slot, j] for j in range(group)] + [wkv_vm[slot]], axis=1))
                sl = block(n, chunk)

                @pl.when(i == 0)
                def _():
                    acc_ref[:, sl] = part

                @pl.when(i > 0)
                def _():
                    acc_ref[:, sl] += part

                @pl.when(s + n_slots < total)
                def _():
                    for copy in weights(s + n_slots):
                        copy.start()

        def mine_in(chip):
            return [pltpu.make_async_copy(g_all.at[chip * CORES + b, me], mine_ref.at[b], job_sem.at[2, b, 0]) for b in range(n_batch)]

        def grow_near(i):
            copies = mine_in(chip_at(i))
            for copy in copies:
                copy.start()
            for copy in copies:
                copy.wait()
            grow(i, lambda b: mine_ref[b])

        def job_in(chip, quarters, slot):
            return [pltpu.make_async_copy(g_all.at[chip * CORES + b, span_of(q)], job_ref.at[slot, b, n], job_sem.at[slot, b, n]) for b in range(n_batch) for n, q in enumerate(quarters)]

        def job(chip, quarters, read, add):
            part = CORES * seq
            lhs = [at2_ref[:, pl.ds(pl.multiple_of(b * n_seq + q * part, part), part)] for b in range(n_batch) for q in quarters]
            rhs = [read(b, n, q).reshape(part, cols) for b in range(n_batch) for n, q in enumerate(quarters)]
            y = dot(jnp.concatenate(lhs, axis=1), jnp.concatenate(rhs, axis=0))
            for j in range(group):
                v = y[:, j * head_dim:(j + 1) * head_dim]
                dwq_ref[chip * group + j] = dwq_ref[chip * group + j] + v if add else v
            for j, ref in enumerate((dwk_ref, dwv_ref)):
                v = y[:, (group + j) * head_dim:(group + j + 1) * head_dim]
                rows = pl.ds(chip, half, stride=chips)
                ref[rows, :] = ref[rows, :] + v if add else v

        def near_pair(quarters, add):
            for slot, step in enumerate(steps):
                for copy in job_in(at.ring(step), quarters, slot):
                    copy.start()

            @pl.loop(0, 2)
            def _(slot):
                chip = at.ring(1 - 2 * slot)
                for copy in job_in(chip, quarters, slot):
                    copy.wait()
                job(chip, quarters, lambda b, n, q: job_ref[slot, b, n], add)

        for slot in range(2):
            for copy in job_in(at.chip, [at.ring(2 * slot), at.ring(2 * slot + 1)], slot):
                copy.start()
        grow_near(0)
        for slot in range(2):
            quarters = [at.ring(2 * slot), at.ring(2 * slot + 1)]
            for copy in job_in(at.chip, quarters, slot):
                copy.wait()
            job(at.chip, quarters, lambda b, n, q: job_ref[slot, b, n], slot == 1)

        for q in range(2):
            for i in range(2):
                direct[i][q].wait_recv()
                onward[i][q].start()
                near_across[i][q].start()
        for q in range(2):
            for i in range(2):
                near_across[i][q].wait_recv()
        near_pair(came[:2], False)
        for q in range(2, chips):
            for i in range(2):
                direct[i][q].wait_recv()
                near_across[i][q].start()
        for q in range(2, chips):
            for i in range(2):
                near_across[i][q].wait_recv()

        @pl.loop(1, chips - 1)
        def _(i):
            grow_near(i)

        near_pair(came[2:], True)
        far_chip = at.ring(2)
        for i in range(2):
            onward[i][0].wait_recv()
            end_across[i][0].start()
        for i in range(2):
            end_across[i][0].wait_recv()
        grow(chips - 1, lambda b: far_ref[b, me])
        for copy in dy_back:
            copy.wait()
        part_ref[...] = jnp.zeros_like(part_ref)

        @pl.loop(0, n_tok // ROWS)
        def _(step):
            sl = block(step, ROWS)
            hat, inv = layer_norm(dx_ref[sl, :].astype(F32))
            dh = acc_ref[sl, :]
            dg = dh * hat
            gh = dh * gain
            one = jnp.mean(gh, axis=-1, keepdims=True)
            two = jnp.mean(dg * gain, axis=-1, keepdims=True)
            dx_ref[sl, :] = (h_ref[sl, :].astype(F32) + inv * (gh - one - hat * two)).astype(BF16)
            part_ref[0] += dg[0:8] + dg[8:16]
            part_ref[1] += dh[0:8] + dh[8:16]

        all_ref[me, 0:1, :] = jnp.sum(part_ref[0], axis=0, keepdims=True)
        all_ref[me, 1:2, :] = jnp.sum(part_ref[1], axis=0, keepdims=True)
        read_far = lambda b, n, q: far_ref[b, span_of(q)]
        for copy in sums:
            copy.start()
        job(far_chip, [ends[0][0], ends[1][0]], read_far, False)
        for i in range(2):
            onward[i][1].wait_recv()
            end_across[i][1].start()
        for i in range(2):
            end_across[i][1].wait_recv()
        job(far_chip, [ends[0][1], ends[1][1]], read_far, True)

    pl.run_scoped(
        weight_grads,
        pltpu.VMEM((W_SLOTS, group, W_ROWS, head_dim), BF16), pltpu.VMEM((W_SLOTS, W_ROWS, 2 * head_dim), BF16), pltpu.VMEM((n_tok, width), F32),
        pltpu.VMEM((2, n_batch, 2, CORES, seq, cols), BF16), pltpu.VMEM((n_batch, seq, cols), BF16),
    )

    for j in range(1, n_dev):
        source = lax.rem(me + j, n_dev)
        send(all_ref.at[me], all_ref.at[source], s_ssem.at[0], s_rsem.at[source], at.partner).wait_recv()
    total = all_ref[0]
    for d in range(1, n_dev):
        total = total + all_ref[d]
    dgain_ref[...] = total[0:1].reshape(width)
    dbias_ref[...] = total[1:2].reshape(width)
    done = first + second[0] + second[1] + again + [own_across] + first_across + second_across + far_across + [heads_across] + spots
    done += direct[0] + direct[1] + onward[0] + onward[1] + [g_across] + near_across[0] + near_across[1] + end_across[0] + end_across[1] + sums
    for copy in done:
        copy.wait_send()
    hcols.wait_send()
    mixed.wait_send()


def whole_block(n_dev, x, gain, bias, positions, freq, dy, wq, wk, wv, wo):
    n_batch, seq, width = dy.shape
    n_tok = n_batch * seq
    head_dim = wq.shape[2]
    chips = n_dev // CORES
    group = wq.shape[0] // chips
    cols = (group + 2) * head_dim
    n_rows = group * head_dim
    half = n_rows // CORES
    n_seq = n_dev * seq
    quarter = head_dim // 4
    dma = pltpu.SemaphoreType.DMA
    vm = pltpu.VMEM
    shapes = [((n_tok, width), BF16)] * 2 + [((chips * group, half, head_dim), F32)] + [((chips * half, head_dim), F32)] * 2 + [((half, width), F32), ((width,), F32), ((width,), F32)]
    held = [((n_dev, n_batch, seq, width), BF16), ((n_dev, half, n_tok), BF16), ((n_dev, seq, n_rows), BF16), ((n_dev, n_dev, seq, cols), BF16), ((chips, width, 2 * head_dim), BF16)]
    return pl.pallas_call(
        functools.partial(block_body, n_dev, group),
        out_shape=tuple(pltpu.VMEM(*t) for t in shapes) + tuple(sds(*t) for t in held),
        in_specs=[VM] * 4 + [HBM] * 6,
        out_specs=(VM,) * len(shapes) + (HBM,) * len(held),
        scratch_shapes=[
            vm((n_tok, width), BF16), vm((width, n_tok), BF16), vm((n_dev, seq, cols), BF16), vm((n_dev, seq, cols), BF16),
            vm((n_seq, n_rows), BF16), vm((n_rows, n_seq), BF16), vm((half, n_batch * n_seq), BF16), vm((group, 8, n_seq), F32), vm((n_seq, n_rows), BF16),
            vm((head_dim, n_seq), BF16), vm((head_dim, n_seq), BF16), vm((n_seq, head_dim), F32), vm((n_seq, head_dim), F32),
            vm((quarter, n_seq), F32), vm((quarter, n_seq), F32), vm((3, n_tok, head_dim), F32), vm((n_dev, n_batch, seq), jnp.int32),
            vm((2, seq, cols), BF16), vm((2, half, n_tok), BF16), vm((2, seq, n_rows), BF16),
            vm((n_batch, n_dev, seq, cols), BF16), vm((2, 8, width), F32), vm((n_dev, 2, width), F32),
            dma((15,)), dma((15,)), dma((9,)), dma((n_dev + 2,)), dma((9,)), dma((n_dev + 2,)), dma((9,)), dma((n_dev + 2,)), dma((n_dev,)), dma((n_dev,)), dma((2,)),
            dma((2, chips)), dma((2, chips)), dma((2, 2)), dma((2, 2)), dma((1 + 4 * chips,)), dma((1 + 4 * chips,)), dma((n_dev,)), dma((n_dev,)),
            dma((1 + n_dev,)), dma((3,)), dma((n_batch * n_dev,)), dma((W_SLOTS, 2)), dma((3, n_batch, 2)),
        ],
        compiler_params=pltpu.CompilerParams(collective_id=0, has_side_effects=True, vmem_limit_bytes=VMEM_LIMIT),
        cost_estimate=pl.CostEstimate(flops=10 ** 11, bytes_accessed=10 ** 8, transcendentals=0),
        name='block',
    )(gain, bias, positions, freq, x.reshape(n_tok, width), dy, wq, wk, wv, wo)[:len(shapes)]


def settle_body(n, *refs):
    sems = refs[2 * n]
    copies = [pltpu.make_async_copy(refs[i], refs[n + i], sems.at[i]) for i in range(n)]
    for copy in copies:
        copy.start()
    for copy in copies:
        copy.wait()


def settle(arrays):
    n = len(arrays)
    return pl.pallas_call(
        functools.partial(settle_body, n),
        out_shape=tuple(sds(t.shape, t.dtype) for t in arrays),
        in_specs=[ANY] * n,
        out_specs=(HBM,) * n,
        scratch_shapes=[pltpu.SemaphoreType.DMA((n,))],
        compiler_params=pltpu.CompilerParams(vmem_limit_bytes=1024 * 1024),
        name='settle',
    )(*arrays)


def solution(mesh):
    n_dev = mesh.shape['cp']

    def device_step(x_act, d_out, positions, ln_gain, ln_bias, w_query, w_key, w_value, w_out):
        n_batch, seq, width = x_act.shape
        q_heads, (kv_heads, head_dim) = w_query.shape[1], w_key.shape[1:]
        group = q_heads // kv_heads
        quarter = head_dim // 4
        assert n_batch == CORES and n_dev // CORES == kv_heads == 4 and q_heads * head_dim == width

        freq = np.exp(np.arange(quarter) * (-2.0 * math.log(ROPE_BASE) / (head_dim // 2))).astype(np.float32).reshape(quarter, 1)
        by_head = lambda t: jnp.transpose(t, (1, 0, 2))
        by_row = lambda t: t.reshape(width * kv_heads, head_dim)
        wq = by_head(w_query)

        results = whole_block(n_dev, x_act, ln_gain, ln_bias, positions, jnp.asarray(freq), d_out, wq, by_row(w_key), by_row(w_value), w_out)
        out, dx, dwq, dwk, dwv, dwo, dgain, dbias = settle(results)
        kv_rows = lambda t: t.reshape(width // n_dev, kv_heads, head_dim)
        return (out.reshape(x_act.shape), dx.reshape(x_act.shape), by_head(dwq), kv_rows(dwk), kv_rows(dwv), dwo, dgain, dbias)

    return jax.shard_map(device_step, mesh=mesh, in_specs=(P('dp', 'cp', None), P('dp', 'cp', None), P('dp', 'cp'), P(None), P(None), P(None, None, None), P(None, None, None), P(None, None, None), P(None, None)), out_specs=(P('dp', 'cp', None), P('dp', 'cp', None), P(('dp', 'cp'), None, None), P(('dp', 'cp'), None, None), P(('dp', 'cp'), None, None), P(('dp', 'cp'), None), P('dp'), P('dp')), check_vma=False)
```

```python
import functools
import math
import jax
import jax.numpy as jnp
import numpy as np
from jax import lax
from jax.experimental import pallas as pl
from jax.experimental.pallas import tpu as pltpu
from jax.sharding import PartitionSpec as P

EPS = 1e-5
ROPE_BASE = 10000.0
BF16 = jnp.bfloat16
F32 = jnp.float32
VMEM_LIMIT = 46 * 1024 * 1024
NT = (((1,), (1,)), ((), ()))
ANY = pl.BlockSpec(memory_space=pl.ANY)
VM = pl.BlockSpec(memory_space=pltpu.VMEM)
HBM = pl.BlockSpec(memory_space=pltpu.HBM)
CORES = 2
ATTN_TILE = 256
COL_TILE = 512
ROWS = 16
W_SLOTS = 4
W_ROWS = 512
SETTLE = 4


def dot(a, b):
    return jnp.dot(a, b, preferred_element_type=F32)


def dot_nt(a, b):
    return lax.dot_general(a, b, NT, preferred_element_type=F32)


def sds(shape, dtype):
    return jax.ShapeDtypeStruct(shape, dtype)


def block(i, size):
    return pl.ds(pl.multiple_of(i * size, size), size)


class Place:
    def __init__(self, n_dev):
        self.n_dev = n_dev
        self.chips = n_dev // CORES
        self.me = lax.axis_index('cp')
        self.chip = self.me // CORES
        self.core = self.me % CORES
        self.partner = self.chip * CORES + 1 - self.core

    def ring(self, step):
        return lax.rem(self.chip + self.chips + step, self.chips)

    def dev(self, step, core):
        return self.ring(step) * CORES + core

    def peers(self, far):
        near = [self.partner] + [self.dev(s, c) for s in (1, -1) for c in range(CORES)]
        return near + ([self.dev(2, c) for c in range(CORES)] if far else [])


def send(src, dst, ssem, rsem, to):
    return pltpu.make_async_remote_copy(src_ref=src, dst_ref=dst, send_sem=ssem, recv_sem=rsem, device_id={'cp': to}, device_id_type=pl.DeviceIdType.MESH)


def meet(peers):
    barrier = pltpu.get_barrier_semaphore()
    for peer in peers:
        pl.semaphore_signal(barrier, inc=1, device_id={'cp': peer}, device_id_type=pl.DeviceIdType.MESH)
    pl.semaphore_wait(barrier, len(peers))


class Ring:
    def __init__(self, n, slots, copies):
        self.n, self.slots, self.copies = n, slots, copies

    def prime(self):
        for s in range(self.slots):
            for copy in self.copies(s, s):
                copy.start()

    def run(self, use):
        @pl.loop(0, self.n)
        def _(s):
            slot = lax.rem(s, self.slots)
            for copy in self.copies(s, slot):
                copy.wait()
            use(s, slot)

            @pl.when(s + self.slots < self.n)
            def _():
                for copy in self.copies(s + self.slots, slot):
                    copy.start()


class Exchange:
    def __init__(self, at, src, dst, relay, ssem, rsem):
        self.at, self.src, self.dst, self.relay, self.ssem, self.rsem = at, src, dst, relay, ssem, rsem
        near = [(0, 1 - at.core)] + [(s, c) for s in (1, -1) for c in range(CORES)]
        n = at.n_dev
        self.near = [send(src(at.dev(s, c)), dst(at.me), ssem.at[i], rsem.at[at.me], at.dev(s, c)) for i, (s, c) in enumerate(near)]
        self.far = [send(src(at.dev(2, i)), relay.at[i], ssem.at[5 + i], rsem.at[n + i], at.dev(step, at.core)) for i, step in enumerate((1, -1))]
        self.on = [send(relay.at[i], dst(at.dev(-step, at.core)), ssem.at[7 + i], rsem.at[at.dev(-step, at.core)], at.dev(step, i)) for i, step in enumerate((1, -1))]

    def start(self):
        for copy in self.far + self.near:
            copy.start()

    def pass_on(self):
        for far, on in zip(self.far, self.on):
            far.wait_recv()
            on.start()

    def wait_recv(self):
        at = self.at
        for j in range(1, at.n_dev):
            origin = lax.rem(at.me + j, at.n_dev)
            send(self.src(at.me), self.dst(origin), self.ssem.at[0], self.rsem.at[origin], at.partner).wait_recv()

    def wait_send(self):
        for copy in self.far + self.near + self.on:
            copy.wait_send()


def layer_norm(x):
    cen = x - jnp.mean(x, axis=-1, keepdims=True)
    inv = lax.rsqrt(jnp.mean(cen * cen, axis=-1, keepdims=True) + EPS)
    return cen * inv, inv


def masked_scores(k, q, limit, tile, scale):
    s = dot_nt(k[:limit], q) * scale
    row = lax.broadcasted_iota(jnp.int32, (tile, tile), 0)
    col = lax.broadcasted_iota(jnp.int32, (tile, tile), 1)
    tail = jnp.where(row <= col, s[limit - tile:], -1e30)
    return tail if limit == tile else jnp.concatenate([s[:limit - tile], tail], axis=0)


def block_body(n_dev, group, gain_ref, bias_ref, pos_ref, freq_ref, x_hbm, dy_ref, wq_ref, wk_ref, wv_ref, wo_ref,
               out_ref, dx_ref, dwq_ref, dwk_ref, dwv_ref, dwo_ref, dgain_ref, dbias_ref, dy_all, ht_all, a_all, g_all, wkv_all,
               h_ref, ht_ref, qs_ref, qkv_ref, a_ref, at_ref, at2_ref, stat_ref, da_ref, kt_ref, vt_ref, dk_ref, dv_ref,
               cost_ref, sint_ref, tab_ref, spot_ref, relay_q, relay_h, relay_a, far_ref, part_ref, all_ref,
               dy_ssem, dy_rsem, q_ssem, q_rsem, h_ssem, h_rsem, a_ssem, a_rsem, p_ssem, p_rsem, t_sem,
               g_ssem, g_rsem, r_ssem, r_rsem, x_ssem, x_rsem, s_ssem, s_rsem, loc_sem, mix_sem, lhs_sem, w_sem, job_sem):
    at = Place(n_dev)
    n_batch, seq, width = dy_ref.shape
    n_tok = n_batch * seq
    head_dim = wq_ref.shape[2]
    cols = (group + 2) * head_dim
    n_rows = group * head_dim
    half = n_rows // CORES
    n_seq = n_dev * seq
    quarter = head_dim // 4
    scale = head_dim ** -0.5
    chips = at.chips
    core, me = at.core, at.me
    steps = (1, -1)
    origin = [at.dev(-1, core), at.dev(1, core)]
    far_dev = at.dev(2, core)

    with jax.named_scope('meet'):
        meet(at.peers(True))

    first = [send(dy_ref.at[b], dy_all.at[me, b], dy_ssem.at[b], dy_rsem.at[b], at.dev(steps[b], core)) for b in range(2)]
    second = [send(dy_ref.at[1 - b], dy_all.at[me, 1 - b], dy_ssem.at[2 + b], dy_rsem.at[2 + b], at.dev(steps[b], core)) for b in range(2)]
    again = [send(dy_all.at[origin[b], b], dy_all.at[origin[b], b], dy_ssem.at[6 + b], dy_rsem.at[6 + b], at.dev(steps[b], core)) for b in range(2)]
    own_across = send(dy_ref, dy_all.at[me], dy_ssem.at[8], dy_rsem.at[8], at.partner)
    first_across = [send(dy_all.at[origin[b], b], dy_all.at[origin[b], b], dy_ssem.at[9 + b], dy_rsem.at[9 + b], at.partner) for b in range(2)]
    second_across = [send(dy_all.at[origin[b], 1 - b], dy_all.at[origin[b], 1 - b], dy_ssem.at[11 + b], dy_rsem.at[11 + b], at.partner) for b in range(2)]
    far_across = [send(dy_all.at[far_dev, b], dy_all.at[far_dev, b], dy_ssem.at[13 + b], dy_rsem.at[13 + b], at.partner) for b in range(2)]
    for copy in first + second:
        copy.start()
    x_in = pltpu.make_async_copy(x_hbm, dx_ref, loc_sem.at[1])
    x_in.start()
    own_across.start()
    spots = [send(pos_ref, spot_ref.at[me], p_ssem.at[j], p_rsem.at[me], peer) for j, peer in enumerate(at.peers(True))]
    for copy in spots:
        copy.start()
    spot_ref[me] = pos_ref[...]

    freq = freq_ref[...]
    for b in range(n_batch):
        angle = freq * pos_ref[b:b + 1, :].astype(F32)
        cos, sin, none = jnp.cos(angle), jnp.sin(angle), jnp.zeros((quarter, seq), F32)
        rest = jnp.zeros((head_dim - 2 * quarter, seq), F32)
        for i, rows in enumerate(([cos, cos, rest + 1.0], [-sin, none, rest], [none, sin, rest])):
            tab_ref[i, b * seq:(b + 1) * seq, :] = jnp.concatenate(rows, axis=0).T

    gain = (1.0 + gain_ref[...]).reshape(1, width)
    bias = bias_ref[...].reshape(1, width)

    def project_all(wkv_ref, raw_ref, wq_vm, raw_sem, wq_sem, stage_sem):
        pieces = [(b, i) for b in range(n_batch) for i in range(width // n_rows)]
        there = lambda n: da_ref.at[pl.ds(n * seq, seq)]
        dy_in = [pltpu.make_async_copy(dy_ref.at[b, :, pl.ds(i * n_rows, n_rows)], there(n), stage_sem.at[n]) for n, (b, i) in enumerate(pieces)]
        dy_keep = [pltpu.make_async_copy(there(n), dy_all.at[me, b, :, pl.ds(i * n_rows, n_rows)], stage_sem.at[n]) for n, (b, i) in enumerate(pieces)]
        span = 64 * chips
        batch = raw_ref.shape[2] // span
        row = lax.broadcasted_iota(jnp.int32, (span, span), 0)
        col = lax.broadcasted_iota(jnp.int32, (span, span), 1)
        pick = jnp.where(col == lax.rem(row, 64) * chips + lax.div(row, 64), 1.0, 0.0).astype(BF16)

        def raw_in(s, slot):
            return [pltpu.make_async_copy(w.at[block(s, span * batch)], raw_ref.at[slot, i], raw_sem.at[slot, i]) for i, w in enumerate((wk_ref, wv_ref))]

        def wq_in(s, slot):
            return [pltpu.make_async_copy(wq_ref.at[block(s, 2)], wq_vm.at[slot], wq_sem.at[slot])]

        def part_heads(s, slot):
            for i in range(batch):
                sl = slice(i * span, (i + 1) * span)
                rows = dot(pick, jnp.concatenate([raw_ref[slot, 0, sl, :], raw_ref[slot, 1, sl, :]], axis=1)).astype(BF16)
                for n in range(chips):
                    wkv_ref[n, block(s * batch + i, 64), :] = rows[n * 64:(n + 1) * 64]

        def place(v, chip, j, turn):
            if turn:
                v = v * tab_ref[0] + pltpu.roll(v, head_dim - quarter, 1) * tab_ref[1] + pltpu.roll(v, quarter, 1) * tab_ref[2]
            v = v.astype(BF16)
            for b in range(n_batch):
                qs_ref[chip * n_batch + b, :, block(j, head_dim)] = v[b * seq:(b + 1) * seq]

        def project(s, slot):
            y = dot(h_ref[...], jnp.concatenate([wq_vm[slot, 0], wq_vm[slot, 1]], axis=1))
            for i in range(2):
                head = s * 2 + i
                place(y[:, i * head_dim:(i + 1) * head_dim], lax.div(head, group), lax.rem(head, group), True)

        kv_ring = Ring(width // (64 * batch), raw_ref.shape[0], raw_in)
        q_ring = Ring(chips * group // 2, wq_vm.shape[0], wq_in)
        kv_ring.prime()
        q_ring.prime()
        for copy in dy_in:
            copy.start()
        x_in.wait()
        with jax.named_scope('norm'):
            @pl.loop(0, n_tok // (2 * ROWS))
            def _(step):
                for i in range(2):
                    sl = block(2 * step + i, ROWS)
                    hat, _ = layer_norm(dx_ref[sl, :].astype(F32))
                    h_ref[sl, :] = (hat * gain + bias).astype(BF16)

        with jax.named_scope('heads_kv'):
            kv_ring.run(part_heads)
        keep = pltpu.make_async_copy(wkv_ref, wkv_all, mix_sem.at[2])
        keep.start()
        for come, go in zip(dy_in, dy_keep):
            come.wait()
            go.start()
        with jax.named_scope('project_q'):
            q_ring.run(project)
        with jax.named_scope('project_kv'):
            @pl.loop(0, chips)
            def _(chip):
                y = dot(h_ref[...], wkv_ref[chip])
                place(y[:, :head_dim], chip, group, True)
                place(y[:, head_dim:], chip, group + 1, False)

        keep.wait()
        for copy in dy_keep:
            copy.wait()

    pl.run_scoped(
        project_all,
        pltpu.VMEM((chips, width, 2 * head_dim), BF16),
        pltpu.VMEM((3, 2, 4 * 64 * chips, head_dim), BF16), pltpu.VMEM((4, 2, width, head_dim), BF16),
        pltpu.SemaphoreType.DMA((3, 2)), pltpu.SemaphoreType.DMA((4,)), pltpu.SemaphoreType.DMA((n_batch * width // n_rows,)),
    )

    qkv = Exchange(at, lambda d: qs_ref.at[d], lambda d: qkv_ref.at[d], relay_q, q_ssem, q_rsem)
    qkv.start()
    qkv_ref[me] = qs_ref[me]

    with jax.named_scope('turn_h'):
        @pl.loop(0, width // 128)
        def _(step):
            sl = block(step, 128)
            ht_ref[sl, :] = h_ref[:, sl].T

    with jax.named_scope('qkv_pass'):
        qkv.pass_on()
    for b in range(2):
        first[b].wait_recv()
        again[b].start()
        first_across[b].start()
    for b in range(2):
        second[b].wait_recv()
        second_across[b].start()
    hcols = Exchange(at, lambda d: ht_ref.at[block(d, half)], lambda d: ht_all.at[d], relay_h, h_ssem, h_rsem)
    hcols.start()
    h_keep = pltpu.make_async_copy(ht_ref.at[block(me, half)], ht_all.at[me], loc_sem.at[1])
    h_keep.start()

    k_all = lambda: qkv_ref[:, :, n_rows:n_rows + head_dim].reshape(n_seq, head_dim)
    v_all = lambda: qkv_ref[:, :, n_rows + head_dim:].reshape(n_seq, head_dim)
    q_head = lambda j: qkv_ref[:, :, block(j, head_dim)].reshape(n_seq, head_dim)
    mixed = Exchange(at, lambda d: a_ref.at[block(d, seq)], lambda d: a_all.at[d], relay_a, a_ssem, a_rsem)
    a_keep = pltpu.make_async_copy(a_ref.at[block(me, seq)], a_all.at[me], loc_sem.at[2])
    heads_across = send(at_ref.at[block(1 - core, half)], at2_ref.at[:, block(core, n_seq)], t_sem.at[0], t_sem.at[1], at.partner)

    def chip_at(i):
        return at.ring(jnp.where(i == 0, 0, jnp.where(i == 1, 1, jnp.where(i == 2, 3, 2))))

    def middle(wo_vm, dyk):
        wo_in = pltpu.make_async_copy(wo_ref.at[block(at.chip, n_rows)], wo_vm, mix_sem.at[2])
        wo_in.start()
        with jax.named_scope('qkv_wait'):
            qkv.wait_recv()
        kt_ref[...] = k_all().T
        vt_ref[...] = v_all().T

        with jax.named_scope('attend'):
            @pl.loop(0, group)
            def _(j):
                q, k = q_head(j), k_all()
                for t in range(n_seq // ATTN_TILE):
                    limit = (t + 1) * ATTN_TILE
                    sl = slice(t * ATTN_TILE, limit)
                    s = masked_scores(k, q[sl], limit, ATTN_TILE, scale)
                    top = jnp.max(s, axis=0, keepdims=True)
                    e = jnp.exp(s - top)
                    inv = 1.0 / jnp.sum(e, axis=0, keepdims=True)
                    mix_t = dot(vt_ref[:, :limit], (e * inv).astype(BF16)).astype(BF16)
                    at_ref[block(j, head_dim), sl] = mix_t
                    a_ref[sl, block(j, head_dim)] = mix_t.T
                    stat_ref[j, 0:1, sl] = top
                    stat_ref[j, 1:2, sl] = inv

        mixed.start()
        a_keep.start()
        heads_across.start()
        with jax.named_scope('at2'):
            at2_ref[:, block(core, n_seq)] = at_ref[block(core, half), :]
        for j in range(1, n_dev):
            source = lax.rem(me + j, n_dev)
            send(pos_ref, spot_ref.at[source], p_ssem.at[0], p_rsem.at[source], at.partner).wait_recv()
        with jax.named_scope('angles'):
            for d in range(n_dev):
                angle = freq * spot_ref[d, pl.ds(core, 1), :].astype(F32)
                cost_ref[:, d * seq:(d + 1) * seq] = jnp.cos(angle)
                sint_ref[:, d * seq:(d + 1) * seq] = jnp.sin(angle)

        with jax.named_scope('dy_wait'):
            own_across.wait_recv()
            for copy in first_across + second_across:
                copy.wait_recv()

        def fetch(i, slot):
            return pltpu.make_async_copy(dy_all.at[block(chip_at(i), CORES), core], dyk.at[slot], mix_sem.at[slot])

        with jax.named_scope('wo_wait'):
            fetch(0, 0).start()
            wo_in.wait()

        @pl.loop(0, chips)
        def _(i):
            slot = lax.rem(i, 2)
            fetch(i, slot).wait()

            @pl.when(i < chips - 2)
            def _():
                fetch(i + 1, 1 - slot).start()

            rows = dyk[slot].reshape(CORES * seq, width)
            da_ref[block(chip_at(i), CORES * seq), :] = dot_nt(rows, wo_vm[...]).astype(BF16)

            @pl.when(i == chips - 2)
            def _():
                with jax.named_scope('dy_far'):
                    for b in range(2):
                        again[b].wait_recv()
                        far_across[b].start()
                with jax.named_scope('dy_far2'):
                    for b in range(2):
                        far_across[b].wait_recv()
                fetch(i + 1, 1 - slot).start()

    pl.run_scoped(middle, pltpu.VMEM((n_rows, width), BF16), pltpu.VMEM((2, CORES, seq, width), BF16))

    qkv.wait_send()
    g_ref = qs_ref
    dk_ref[...] = jnp.zeros_like(dk_ref)
    dv_ref[...] = jnp.zeros_like(dv_ref)

    def rotate_back(t, cos, sin):
        u, w = t[:quarter], t[quarter:2 * quarter]
        return jnp.concatenate([u * cos + w * sin, w * cos - u * sin, t[2 * quarter:]], axis=0)

    def by_dev(t):
        return t.astype(BF16).reshape(t.shape[0] // seq, seq, head_dim)

    with jax.named_scope('attend_back'):
        @pl.loop(0, group)
        def _(j):
            @pl.when(j == 1)
            def _():
                with jax.named_scope('h_pass'):
                    hcols.pass_on()

            @pl.when(j == group - 1)
            def _():
                with jax.named_scope('a_pass'):
                    mixed.pass_on()

            q, k, v = q_head(j), k_all(), v_all()
            for t in range(n_seq // ATTN_TILE):
                limit = (t + 1) * ATTN_TILE
                sl = slice(t * ATTN_TILE, limit)
                da = da_ref[sl, block(j, head_dim)]
                s = masked_scores(k, q[sl], limit, ATTN_TILE, scale)
                p = jnp.exp(s - stat_ref[j, 0:1, sl]) * stat_ref[j, 1:2, sl]
                dp = dot_nt(v[:limit], da)
                row_dot = jnp.sum(p * dp, axis=0, keepdims=True)
                ds = (p * (dp - row_dot) * scale).astype(BF16)
                dv_ref[:limit, :] += dot(p.astype(BF16), da)
                dk_ref[:limit, :] += dot(ds, q[sl])
                back = rotate_back(dot(kt_ref[:, :limit], ds), cost_ref[:, sl], sint_ref[:, sl])
                g_ref[t * ATTN_TILE // seq:limit // seq, :, block(j, head_dim)] = by_dev(back.T)

    g_ref[:, :, n_rows:n_rows + head_dim] = by_dev(rotate_back(dk_ref[...].T, cost_ref[...], sint_ref[...]).T)
    g_ref[:, :, n_rows + head_dim:] = by_dev(dv_ref[...])

    def span_of(q):
        return block(q, CORES)

    turn = [[at.ring(q) for q in (2, 1, 3, 0)], [at.ring(q) for q in (3, 0, 1, 2)]]
    direct = [[send(g_ref.at[span_of(turn[i][q])], g_all.at[me, span_of(turn[i][q])], g_ssem.at[i, q], g_rsem.at[i, q], at.dev(steps[i], core)) for q in range(chips)] for i in range(2)]
    came = [[at.ring(q) for q in (1, 0, 2, 3)], [at.ring(q) for q in (0, 1, 2, 3)]]
    onward = [[send(g_all.at[origin[i], span_of(came[i][q])], far_ref.at[core, span_of(came[i][q])], r_ssem.at[i, q], r_rsem.at[i, q], at.dev(steps[i], core)) for q in range(2)] for i in range(2)]
    ends = [[at.ring(q) for q in (0, 3)], [at.ring(q) for q in (1, 2)]]
    g_across = send(g_ref, g_all.at[me], x_ssem.at[0], x_rsem.at[0], at.partner)
    near_across = [[send(g_all.at[origin[i], span_of(came[i][q])], g_all.at[origin[i], span_of(came[i][q])], x_ssem.at[1 + i * chips + q], x_rsem.at[1 + i * chips + q], at.partner) for q in range(chips)] for i in range(2)]
    end_across = [[send(far_ref.at[core, span_of(ends[i][q])], far_ref.at[core, span_of(ends[i][q])], x_ssem.at[1 + (2 + i) * chips + q], x_rsem.at[1 + (2 + i) * chips + q], at.partner) for q in range(2)] for i in range(2)]
    for q in range(chips):
        for i in range(2):
            direct[i][q].start()
    g_across.start()
    g_keep = pltpu.make_async_copy(g_ref, g_all.at[me], loc_sem.at[0])
    g_keep.start()

    with jax.named_scope('heads_wait'):
        heads_across.wait_recv()

    def wo_tile(dy):
        pieces = [dy[d, b] for b in range(n_batch) for d in range(n_dev)]
        dwo_ref[:, block(pl.program_id(0), COL_TILE)] = dot(at2_ref[...], jnp.concatenate(pieces, axis=0))

    with jax.named_scope('grad_wo'):
        pltpu.emit_pipeline(wo_tile, grid=(width // COL_TILE,), in_specs=[pl.BlockSpec((n_dev, n_batch, seq, COL_TILE), lambda i: (0, 0, 0, i))], out_specs=[])(dy_all)

    with jax.named_scope('h_wait'):
        hcols.wait_recv()
        h_keep.wait()
    lhs_in = [pltpu.make_async_copy(ht_all.at[d, :, pl.ds(b * seq, seq)], at2_ref.at[:, pl.ds((b * n_dev + d) * seq, seq)], lhs_sem.at[b * n_dev + d]) for d in range(n_dev) for b in range(n_batch)]
    for copy in lhs_in:
        copy.start()
    with jax.named_scope('a_wait'):
        mixed.wait_recv()
        a_keep.wait()
    mix_in = [pltpu.make_async_copy(a_all.at[s], h_ref.at[pl.ds((s % n_batch) * seq, seq), pl.ds((s // n_batch) * n_rows, n_rows)], loc_sem.at[1 + s]) for s in range(n_dev)]
    for copy in mix_in:
        copy.start()
    with jax.named_scope('mix_in'):
        for copy in mix_in:
            copy.wait()

    def out_tile(wo):
        sl = block(pl.program_id(0), COL_TILE)
        out_ref[:, sl] = (dx_ref[:, sl].astype(F32) + dot(h_ref[...], wo[...])).astype(BF16)

    with jax.named_scope('output'):
        pltpu.emit_pipeline(out_tile, grid=(width // COL_TILE,), in_specs=[pl.BlockSpec((width, COL_TILE), lambda i: (0, i))], out_specs=[])(wo_ref)

    dy_back = [pltpu.make_async_copy(dy_ref.at[b], h_ref.at[pl.ds(b * seq, seq)], loc_sem.at[1 + b]) for b in range(n_batch)]
    for copy in dy_back:
        copy.start()
    with jax.named_scope('own_wait'):
        for copy in lhs_in:
            copy.wait()
        g_keep.wait()
        g_across.wait_recv()
    sums = [send(all_ref.at[me], all_ref.at[me], s_ssem.at[j], s_rsem.at[me], peer) for j, peer in enumerate(at.peers(True))]

    def weight_grads(wq_vm, wkv_vm, acc_ref, hat_ref, inv_ref, job_ref, mine_ref):
        n_slots = wq_vm.shape[0]
        chunk = wq_vm.shape[2]
        n_chunks = width // chunk
        total = n_chunks * chips

        def weights(s):
            slot = lax.rem(s, n_slots)
            chip = chip_at(lax.div(s, n_chunks))
            rows = block(lax.rem(s, n_chunks), chunk)
            return [
                pltpu.make_async_copy(wq_ref.at[block(chip, group), rows], wq_vm.at[slot], w_sem.at[slot, 0]),
                pltpu.make_async_copy(wkv_all.at[chip, rows], wkv_vm.at[slot], w_sem.at[slot, 1]),
            ]

        for s in range(n_slots):
            for copy in weights(s):
                copy.start()

        def grow(i, read):
            @pl.loop(0, n_chunks)
            def _(n):
                s = i * n_chunks + n
                slot = lax.rem(s, n_slots)
                for copy in weights(s):
                    copy.wait()
                rows = jnp.concatenate([read(b) for b in range(n_batch)], axis=0)
                part = dot_nt(rows, jnp.concatenate([wq_vm[slot, j] for j in range(group)] + [wkv_vm[slot]], axis=1))
                sl = block(n, chunk)

                @pl.when(i == 0)
                def _():
                    acc_ref[:, sl] = part

                @pl.when(i > 0)
                def _():
                    acc_ref[:, sl] += part

                @pl.when(s + n_slots < total)
                def _():
                    for copy in weights(s + n_slots):
                        copy.start()

        def mine_in(chip):
            return [pltpu.make_async_copy(g_all.at[chip * CORES + b, me], mine_ref.at[b], job_sem.at[2, b, 0]) for b in range(n_batch)]

        def grow_near(i):
            copies = mine_in(chip_at(i))
            for copy in copies:
                copy.start()
            for copy in copies:
                copy.wait()
            grow(i, lambda b: mine_ref[b])

        def job_in(chip, quarters, slot):
            return [pltpu.make_async_copy(g_all.at[chip * CORES + b, span_of(q)], job_ref.at[slot, b, n], job_sem.at[slot, b, n]) for b in range(n_batch) for n, q in enumerate(quarters)]

        def job(chip, quarters, read, add):
            part = CORES * seq
            lhs = [at2_ref[:, pl.ds(pl.multiple_of(b * n_seq + q * part, part), part)] for b in range(n_batch) for q in quarters]
            rhs = [read(b, n, q).reshape(part, cols) for b in range(n_batch) for n, q in enumerate(quarters)]
            y = dot(jnp.concatenate(lhs, axis=1), jnp.concatenate(rhs, axis=0))
            for j in range(group):
                v = y[:, j * head_dim:(j + 1) * head_dim]
                dwq_ref[chip * group + j] = dwq_ref[chip * group + j] + v if add else v
            for j, ref in enumerate((dwk_ref, dwv_ref)):
                v = y[:, (group + j) * head_dim:(group + j + 1) * head_dim]
                rows = pl.ds(chip, half, stride=chips)
                ref[rows, :] = ref[rows, :] + v if add else v

        def near_pair(quarters, add):
            for slot, step in enumerate(steps):
                for copy in job_in(at.ring(step), quarters, slot):
                    copy.start()

            @pl.loop(0, 2)
            def _(slot):
                chip = at.ring(1 - 2 * slot)
                for copy in job_in(chip, quarters, slot):
                    copy.wait()
                job(chip, quarters, lambda b, n, q: job_ref[slot, b, n], add)

        halves = [[at.ring(q) for q in half_of] for half_of in ((0, 1), (2, 3))]
        for slot in range(2):
            for copy in job_in(at.chip, [at.ring(2 * slot), at.ring(2 * slot + 1)], slot):
                copy.start()
        with jax.named_scope('own_dh'):
            grow_near(0)
        with jax.named_scope('own_job'):
            for slot in range(2):
                quarters = [at.ring(2 * slot), at.ring(2 * slot + 1)]
                for copy in job_in(at.chip, quarters, slot):
                    copy.wait()
                job(at.chip, quarters, lambda b, n, q: job_ref[slot, b, n], slot == 1)

        with jax.named_scope('d01_wait'):
            for q in range(2):
                for i in range(2):
                    direct[i][q].wait_recv()
                    onward[i][q].start()
                    near_across[i][q].start()
        with jax.named_scope('d01_across'):
            for q in range(2):
                for i in range(2):
                    near_across[i][q].wait_recv()
        with jax.named_scope('near_dh'):
            @pl.loop(1, chips - 1)
            def _(i):
                grow_near(i)

        with jax.named_scope('near_a'):
            near_pair(halves[0], False)
        with jax.named_scope('hat'):
            @pl.loop(0, n_tok // (2 * ROWS))
            def _(step):
                for i in range(2):
                    sl = block(2 * step + i, ROWS)
                    hat, inv = layer_norm(dx_ref[sl, :].astype(F32))
                    hat_ref[sl, :] = hat
                    inv_ref[sl, :] = jnp.broadcast_to(inv, (ROWS, 128))

        with jax.named_scope('d23_wait'):
            for q in range(2, chips):
                for i in range(2):
                    direct[i][q].wait_recv()
                    near_across[i][q].start()
        with jax.named_scope('d23_across'):
            for q in range(2, chips):
                for i in range(2):
                    near_across[i][q].wait_recv()

        with jax.named_scope('near_b'):
            near_pair(halves[1], True)
        far_chip = at.ring(2)
        with jax.named_scope('far0_wait'):
            for i in range(2):
                onward[i][0].wait_recv()
                end_across[i][0].start()
        with jax.named_scope('far0_across'):
            for i in range(2):
                end_across[i][0].wait_recv()
        with jax.named_scope('far_dh'):
            grow(chips - 1, lambda b: far_ref[b, me])
        for copy in dy_back:
            copy.wait()
        part_ref[...] = jnp.zeros_like(part_ref)

        with jax.named_scope('norm_back'):
            @pl.loop(0, n_tok // (2 * ROWS))
            def _(step):
                for i in range(2):
                    sl = block(2 * step + i, ROWS)
                    hat, inv = hat_ref[sl, :], inv_ref[sl, 0:1]
                    dh = acc_ref[sl, :]
                    dg = dh * hat
                    gh = dh * gain
                    one = jnp.mean(gh, axis=-1, keepdims=True)
                    two = jnp.mean(dg * gain, axis=-1, keepdims=True)
                    dx_ref[sl, :] = (h_ref[sl, :].astype(F32) + inv * (gh - one - hat * two)).astype(BF16)
                    part_ref[0] += dg[0:8] + dg[8:16]
                    part_ref[1] += dh[0:8] + dh[8:16]

        all_ref[me, 0:1, :] = jnp.sum(part_ref[0], axis=0, keepdims=True)
        all_ref[me, 1:2, :] = jnp.sum(part_ref[1], axis=0, keepdims=True)
        read_far = lambda b, n, q: far_ref[b, span_of(q)]
        for copy in sums:
            copy.start()
        with jax.named_scope('far_a'):
            job(far_chip, [ends[0][0], ends[1][0]], read_far, False)
        with jax.named_scope('far1_wait'):
            for i in range(2):
                onward[i][1].wait_recv()
                end_across[i][1].start()
        with jax.named_scope('far1_across'):
            for i in range(2):
                end_across[i][1].wait_recv()
        with jax.named_scope('far_b'):
            job(far_chip, [ends[0][1], ends[1][1]], read_far, True)

    pl.run_scoped(
        weight_grads,
        pltpu.VMEM((W_SLOTS, group, W_ROWS, head_dim), BF16), pltpu.VMEM((W_SLOTS, W_ROWS, 2 * head_dim), BF16), pltpu.VMEM((n_tok, width), F32),
        pltpu.VMEM((n_tok, width), F32), pltpu.VMEM((n_tok, 128), F32), pltpu.VMEM((2, n_batch, 2, CORES, seq, cols), BF16), pltpu.VMEM((n_batch, seq, cols), BF16),
    )

    with jax.named_scope('sums'):
        for j in range(1, n_dev):
            source = lax.rem(me + j, n_dev)
            send(all_ref.at[me], all_ref.at[source], s_ssem.at[0], s_rsem.at[source], at.partner).wait_recv()
        total = all_ref[0]
        for d in range(1, n_dev):
            total = total + all_ref[d]
        dgain_ref[...] = total[0:1].reshape(width)
        dbias_ref[...] = total[1:2].reshape(width)
    done = first + second + again + [own_across] + first_across + second_across + far_across + [heads_across] + spots
    done += direct[0] + direct[1] + onward[0] + onward[1] + [g_across] + near_across[0] + near_across[1] + end_across[0] + end_across[1] + sums
    with jax.named_scope('done'):
        for copy in done:
            copy.wait_send()
        hcols.wait_send()
        mixed.wait_send()


def whole_block(n_dev, x, gain, bias, positions, freq, dy, wq, wk, wv, wo):
    n_batch, seq, width = dy.shape
    n_tok = n_batch * seq
    head_dim = wq.shape[2]
    chips = n_dev // CORES
    group = wq.shape[0] // chips
    cols = (group + 2) * head_dim
    n_rows = group * head_dim
    half = n_rows // CORES
    n_seq = n_dev * seq
    quarter = head_dim // 4
    dma = pltpu.SemaphoreType.DMA
    vm = pltpu.VMEM
    shapes = [((n_tok, width), BF16)] * 2 + [((chips * group, half, head_dim), F32)] + [((chips * half, head_dim), F32)] * 2 + [((half, width), F32), ((width,), F32), ((width,), F32)]
    held = [((n_dev, n_batch, seq, width), BF16), ((n_dev, half, n_tok), BF16), ((n_dev, seq, n_rows), BF16), ((n_dev, n_dev, seq, cols), BF16), ((chips, width, 2 * head_dim), BF16)]
    return pl.pallas_call(
        functools.partial(block_body, n_dev, group),
        out_shape=tuple(pltpu.VMEM(*t) for t in shapes) + tuple(sds(*t) for t in held),
        in_specs=[VM] * 4 + [HBM] * 6,
        out_specs=(VM,) * len(shapes) + (HBM,) * len(held),
        scratch_shapes=[
            vm((n_tok, width), BF16), vm((width, n_tok), BF16), vm((n_dev, seq, cols), BF16), vm((n_dev, seq, cols), BF16),
            vm((n_seq, n_rows), BF16), vm((n_rows, n_seq), BF16), vm((half, n_batch * n_seq), BF16), vm((group, 8, n_seq), F32), vm((n_seq, n_rows), BF16),
            vm((head_dim, n_seq), BF16), vm((head_dim, n_seq), BF16), vm((n_seq, head_dim), F32), vm((n_seq, head_dim), F32),
            vm((quarter, n_seq), F32), vm((quarter, n_seq), F32), vm((3, n_tok, head_dim), F32), vm((n_dev, n_batch, seq), jnp.int32),
            vm((2, seq, cols), BF16), vm((2, half, n_tok), BF16), vm((2, seq, n_rows), BF16),
            vm((n_batch, n_dev, seq, cols), BF16), vm((2, 8, width), F32), vm((n_dev, 2, width), F32),
            dma((15,)), dma((15,)), dma((9,)), dma((n_dev + 2,)), dma((9,)), dma((n_dev + 2,)), dma((9,)), dma((n_dev + 2,)), dma((n_dev,)), dma((n_dev,)), dma((2,)),
            dma((2, chips)), dma((2, chips)), dma((2, 2)), dma((2, 2)), dma((1 + 4 * chips,)), dma((1 + 4 * chips,)), dma((n_dev,)), dma((n_dev,)),
            dma((1 + n_dev,)), dma((3,)), dma((n_batch * n_dev,)), dma((W_SLOTS, 2)), dma((3, n_batch, 2)),
        ],
        compiler_params=pltpu.CompilerParams(collective_id=0, has_side_effects=True, vmem_limit_bytes=VMEM_LIMIT),
        cost_estimate=pl.CostEstimate(flops=10 ** 11, bytes_accessed=10 ** 8, transcendentals=0),
        name='block',
    )(gain, bias, positions, freq, x.reshape(n_tok, width), dy, wq, wk, wv, wo)[:len(shapes)]


def settle_body(n, *refs):
    sems = refs[2 * n]
    copies = []
    for i in range(n):
        src, dst = refs[i], refs[n + i]
        pieces = SETTLE if len(src.shape) > 1 else 1
        size = src.shape[0] // pieces
        for p in range(pieces):
            copies.append(pltpu.make_async_copy(src.at[pl.ds(p * size, size)], dst.at[pl.ds(p * size, size)], sems.at[i, p]))
    for copy in copies:
        copy.start()
    for copy in copies:
        copy.wait()


def settle(arrays):
    n = len(arrays)
    return pl.pallas_call(
        functools.partial(settle_body, n),
        out_shape=tuple(sds(t.shape, t.dtype) for t in arrays),
        in_specs=[ANY] * n,
        out_specs=(HBM,) * n,
        scratch_shapes=[pltpu.SemaphoreType.DMA((n, SETTLE))],
        compiler_params=pltpu.CompilerParams(vmem_limit_bytes=1024 * 1024),
        name='settle',
    )(*arrays)


def solution(mesh):
    n_dev = mesh.shape['cp']

    def device_step(x_act, d_out, positions, ln_gain, ln_bias, w_query, w_key, w_value, w_out):
        n_batch, seq, width = x_act.shape
        q_heads, (kv_heads, head_dim) = w_query.shape[1], w_key.shape[1:]
        group = q_heads // kv_heads
        quarter = head_dim // 4
        assert n_batch == CORES and n_dev // CORES == kv_heads == 4 and q_heads * head_dim == width

        freq = np.exp(np.arange(quarter) * (-2.0 * math.log(ROPE_BASE) / (head_dim // 2))).astype(np.float32).reshape(quarter, 1)
        by_head = lambda t: jnp.transpose(t, (1, 0, 2))
        by_row = lambda t: t.reshape(width * kv_heads, head_dim)
        wq = by_head(w_query)

        results = whole_block(n_dev, x_act, ln_gain, ln_bias, positions, jnp.asarray(freq), d_out, wq, by_row(w_key), by_row(w_value), w_out)
        out, dx, dwq, dwk, dwv, dwo, dgain, dbias = settle(results)
        kv_rows = lambda t: t.reshape(width // n_dev, kv_heads, head_dim)
        return (out.reshape(x_act.shape), dx.reshape(x_act.shape), by_head(dwq), kv_rows(dwk), kv_rows(dwv), dwo, dgain, dbias)

    return jax.shard_map(device_step, mesh=mesh, in_specs=(P('dp', 'cp', None), P('dp', 'cp', None), P('dp', 'cp'), P(None), P(None), P(None, None, None), P(None, None, None), P(None, None, None), P(None, None)), out_specs=(P('dp', 'cp', None), P('dp', 'cp', None), P(('dp', 'cp'), None, None), P(('dp', 'cp'), None, None), P(('dp', 'cp'), None, None), P(('dp', 'cp'), None), P('dp'), P('dp')), check_vma=False)
```

```python
import functools
import math
import jax
import jax.numpy as jnp
import numpy as np
from jax import lax
from jax.experimental import pallas as pl
from jax.experimental.pallas import tpu as pltpu
from jax.sharding import PartitionSpec as P

EPS = 1e-5
ROPE_BASE = 10000.0
BF16 = jnp.bfloat16
F32 = jnp.float32
VMEM_LIMIT = 46 * 1024 * 1024
NT = (((1,), (1,)), ((), ()))
ANY = pl.BlockSpec(memory_space=pl.ANY)
VM = pl.BlockSpec(memory_space=pltpu.VMEM)
HBM = pl.BlockSpec(memory_space=pltpu.HBM)
CORES = 2
COL_TILE = 512
ROWS = 16
W_SLOTS = 4
W_ROWS = 512
SETTLE = 4


def dot(a, b):
    return jnp.dot(a, b, preferred_element_type=F32)


def dot_nt(a, b):
    return lax.dot_general(a, b, NT, preferred_element_type=F32)


def sds(shape, dtype):
    return jax.ShapeDtypeStruct(shape, dtype)


def block(i, size):
    return pl.ds(pl.multiple_of(i * size, size), size)


class Place:
    def __init__(self, n_dev):
        self.n_dev = n_dev
        self.chips = n_dev // CORES
        self.me = lax.axis_index('cp')
        self.chip = self.me // CORES
        self.core = self.me % CORES
        self.partner = self.chip * CORES + 1 - self.core

    def ring(self, step):
        return lax.rem(self.chip + self.chips + step, self.chips)

    def dev(self, step, core):
        return self.ring(step) * CORES + core

    def peers(self, far):
        near = [self.partner] + [self.dev(s, c) for s in (1, -1) for c in range(CORES)]
        return near + ([self.dev(2, c) for c in range(CORES)] if far else [])


def send(src, dst, ssem, rsem, to):
    return pltpu.make_async_remote_copy(src_ref=src, dst_ref=dst, send_sem=ssem, recv_sem=rsem, device_id={'cp': to}, device_id_type=pl.DeviceIdType.MESH)


def meet(peers):
    barrier = pltpu.get_barrier_semaphore()
    for peer in peers:
        pl.semaphore_signal(barrier, inc=1, device_id={'cp': peer}, device_id_type=pl.DeviceIdType.MESH)
    pl.semaphore_wait(barrier, len(peers))


class Ring:
    def __init__(self, n, slots, copies):
        self.n, self.slots, self.copies = n, slots, copies

    def prime(self):
        for s in range(self.slots):
            for copy in self.copies(s, s):
                copy.start()

    def run(self, use):
        @pl.loop(0, self.n)
        def _(s):
            slot = lax.rem(s, self.slots)
            for copy in self.copies(s, slot):
                copy.wait()
            use(s, slot)

            @pl.when(s + self.slots < self.n)
            def _():
                for copy in self.copies(s + self.slots, slot):
                    copy.start()


class Gather:
    def __init__(self, at, own, piece, both, ssem, rsem):
        steps = (1, -1)
        origin = [at.dev(-1, at.core), at.dev(1, at.core)]
        far = at.dev(2, at.core)
        link = lambda i, src, dst, to: send(src, dst, ssem.at[i], rsem.at[i], to)
        self.first = [link(b, own(b), piece(at.me, b), at.dev(steps[b], at.core)) for b in range(2)]
        self.second = [link(2 + b, own(1 - b), piece(at.me, 1 - b), at.dev(steps[b], at.core)) for b in range(2)]
        self.again = [link(4 + b, piece(origin[b], b), piece(origin[b], b), at.dev(steps[b], at.core)) for b in range(2)]
        self.own_across = link(6, both(None), both(at.me), at.partner)
        self.first_across = [link(7 + b, piece(origin[b], b), piece(origin[b], b), at.partner) for b in range(2)]
        self.second_across = [link(9 + b, piece(origin[b], 1 - b), piece(origin[b], 1 - b), at.partner) for b in range(2)]
        self.far_across = [link(11 + b, piece(far, b), piece(far, b), at.partner) for b in range(2)]

    def start_first(self):
        for copy in self.first + [self.own_across]:
            copy.start()

    def start_second(self):
        for copy in self.second:
            copy.start()

    def pass_on(self):
        for copy, again, across in zip(self.first, self.again, self.first_across):
            copy.wait_recv()
            again.start()
            across.start()

    def share_second(self):
        for copy, across in zip(self.second, self.second_across):
            copy.wait_recv()
            across.start()

    def share_far(self):
        for copy, across in zip(self.again, self.far_across):
            copy.wait_recv()
            across.start()

    def wait_near(self):
        for copy in [self.own_across] + self.first_across + self.second_across:
            copy.wait_recv()

    def wait_far(self):
        for copy in self.far_across:
            copy.wait_recv()

    def sent(self):
        return self.first + self.second + self.again + [self.own_across] + self.first_across + self.second_across + self.far_across


class Exchange:
    def __init__(self, at, src, dst, relay, ssem, rsem):
        self.at, self.src, self.dst, self.relay, self.ssem, self.rsem = at, src, dst, relay, ssem, rsem
        near = [(0, 1 - at.core)] + [(s, c) for s in (1, -1) for c in range(CORES)]
        n = at.n_dev
        self.near = [send(src(at.dev(s, c)), dst(at.me), ssem.at[i], rsem.at[at.me], at.dev(s, c)) for i, (s, c) in enumerate(near)]
        self.far = [send(src(at.dev(2, i)), relay.at[i], ssem.at[5 + i], rsem.at[n + i], at.dev(step, at.core)) for i, step in enumerate((1, -1))]
        self.on = [send(relay.at[i], dst(at.dev(-step, at.core)), ssem.at[7 + i], rsem.at[at.dev(-step, at.core)], at.dev(step, i)) for i, step in enumerate((1, -1))]

    def start(self):
        for copy in self.far + self.near:
            copy.start()

    def pass_on(self):
        for far, on in zip(self.far, self.on):
            far.wait_recv()
            on.start()

    def wait_recv(self):
        at = self.at
        for j in range(1, at.n_dev):
            origin = lax.rem(at.me + j, at.n_dev)
            send(self.src(at.me), self.dst(origin), self.ssem.at[0], self.rsem.at[origin], at.partner).wait_recv()

    def wait_send(self):
        for copy in self.far + self.near + self.on:
            copy.wait_send()


def layer_norm(x):
    cen = x - jnp.mean(x, axis=-1, keepdims=True)
    inv = lax.rsqrt(jnp.mean(cen * cen, axis=-1, keepdims=True) + EPS)
    return cen * inv, inv


def block_body(n_dev, group, gain_ref, bias_ref, pos_ref, freq_ref, x_hbm, dy_ref, wq_ref, wk_ref, wv_ref, wo_ref,
               out_ref, dx_ref, dwq_ref, dwk_ref, dwv_ref, dwo_ref, dgain_ref, dbias_ref, dy_all, ht_all, g_all, wkv_all,
               h_ref, ht_ref, g_ref, q_ref, at_ref, at2_ref, da_ref, kt_ref, vt_ref, dk_ref, dv_ref,
               cost_ref, sint_ref, tab_ref, spot_ref, relay_q, relay_h, far_ref, part_ref, all_ref,
               dy_ssem, dy_rsem, kv_ssem, kv_rsem, q_ssem, q_rsem, h_ssem, h_rsem, p_ssem, p_rsem, t_sem,
               g_ssem, g_rsem, r_ssem, r_rsem, x_ssem, x_rsem, s_ssem, s_rsem, loc_sem, mix_sem, lhs_sem, w_sem, job_sem):
    at = Place(n_dev)
    n_batch, seq, width = dy_ref.shape
    n_tok = n_batch * seq
    head_dim = wq_ref.shape[2]
    cols = (group + 2) * head_dim
    n_rows = group * head_dim
    half = n_rows // CORES
    n_seq = n_dev * seq
    quarter = head_dim // 4
    scale = head_dim ** -0.5
    chips = at.chips
    tile = CORES * seq
    core, me = at.core, at.me
    steps = (1, -1)
    origin = [at.dev(-1, core), at.dev(1, core)]
    far_dev = at.dev(2, core)
    scope = jax.named_scope

    with scope('meet'):
        meet(at.peers(True))

    kv_cols = 2 * head_dim * chips
    kv_piece = lambda d, b: far_ref.at[b, d, :, pl.ds(0, kv_cols)]
    kv_both = lambda d: far_ref.at[:, me if d is None else d, :, pl.ds(0, kv_cols)]
    dys = Gather(at, lambda b: dy_ref.at[b], lambda d, b: dy_all.at[d, b], lambda d: dy_ref if d is None else dy_all.at[d], dy_ssem, dy_rsem)
    kvs = Gather(at, lambda b: kv_piece(me, b), kv_piece, kv_both, kv_ssem, kv_rsem)
    q_part = pl.ds(0, n_rows)
    queries = Exchange(at, lambda d: g_ref.at[d, :, q_part], lambda d: q_ref.at[d], relay_q, q_ssem, q_rsem)
    hcols = Exchange(at, lambda d: ht_ref.at[block(d, half)], lambda d: ht_all.at[d], relay_h, h_ssem, h_rsem)
    heads_across = send(at_ref.at[block(1 - core, half)], at2_ref.at[:, block(core, n_seq)], t_sem.at[0], t_sem.at[1], at.partner)
    spots = [send(pos_ref, spot_ref.at[me], p_ssem.at[j], p_rsem.at[me], peer) for j, peer in enumerate(at.peers(True))]

    dys.start_first()
    x_in = pltpu.make_async_copy(x_hbm, dx_ref, loc_sem.at[1])
    x_in.start()
    for copy in spots:
        copy.start()
    spot_ref[me] = pos_ref[...]

    freq = freq_ref[...]
    for b in range(n_batch):
        angle = freq * pos_ref[b:b + 1, :].astype(F32)
        cos, sin, none = jnp.cos(angle), jnp.sin(angle), jnp.zeros((quarter, seq), F32)
        rest = jnp.zeros((head_dim - 2 * quarter, seq), F32)
        for i, rows in enumerate(([cos, cos, rest + 1.0], [-sin, none, rest], [none, sin, rest])):
            tab_ref[i, b * seq:(b + 1) * seq, :] = jnp.concatenate(rows, axis=0).T

    gain = (1.0 + gain_ref[...]).reshape(1, width)
    bias = bias_ref[...].reshape(1, width)

    def project_all(wkv_ref, raw_ref, wq_vm, raw_sem, wq_sem, stage_sem):
        pieces = [(b, i) for b in range(n_batch) for i in range(width // n_rows)]
        there = lambda n: da_ref.at[pl.ds(n * seq, seq)]
        dy_in = [pltpu.make_async_copy(dy_ref.at[b, :, pl.ds(i * n_rows, n_rows)], there(n), stage_sem.at[n]) for n, (b, i) in enumerate(pieces)]
        dy_keep = [pltpu.make_async_copy(there(n), dy_all.at[me, b, :, pl.ds(i * n_rows, n_rows)], stage_sem.at[n]) for n, (b, i) in enumerate(pieces)]
        span = 64 * chips
        batch = raw_ref.shape[2] // span
        row = lax.broadcasted_iota(jnp.int32, (span, span), 0)
        col = lax.broadcasted_iota(jnp.int32, (span, span), 1)
        pick = jnp.where(col == lax.rem(row, 64) * chips + lax.div(row, 64), 1.0, 0.0).astype(BF16)

        def raw_in(s, slot):
            return [pltpu.make_async_copy(w.at[block(s, span * batch)], raw_ref.at[slot, i], raw_sem.at[slot, i]) for i, w in enumerate((wk_ref, wv_ref))]

        def wq_in(s, slot):
            return [pltpu.make_async_copy(wq_ref.at[block(s, 2)], wq_vm.at[slot], wq_sem.at[slot])]

        def part_heads(s, slot):
            for i in range(batch):
                sl = slice(i * span, (i + 1) * span)
                rows = dot(pick, jnp.concatenate([raw_ref[slot, 0, sl, :], raw_ref[slot, 1, sl, :]], axis=1)).astype(BF16)
                for n in range(chips):
                    wkv_ref[n, block(s * batch + i, 64), :] = rows[n * 64:(n + 1) * 64]

        def turned(v):
            return v * tab_ref[0] + pltpu.roll(v, head_dim - quarter, 1) * tab_ref[1] + pltpu.roll(v, quarter, 1) * tab_ref[2]

        def project(s, slot):
            y = dot(h_ref[...], jnp.concatenate([wq_vm[slot, 0], wq_vm[slot, 1]], axis=1))
            for i in range(2):
                head = s * 2 + i
                v = turned(y[:, i * head_dim:(i + 1) * head_dim]).astype(BF16)
                for b in range(n_batch):
                    g_ref[lax.div(head, group) * n_batch + b, :, block(lax.rem(head, group), head_dim)] = v[b * seq:(b + 1) * seq]

        kv_ring = Ring(width // (64 * batch), raw_ref.shape[0], raw_in)
        q_ring = Ring(chips * group // 2, wq_vm.shape[0], wq_in)
        kv_ring.prime()
        q_ring.prime()
        for copy in dy_in:
            copy.start()
        x_in.wait()
        with scope('norm'):
            @pl.loop(0, n_tok // (2 * ROWS))
            def _(step):
                for i in range(2):
                    sl = block(2 * step + i, ROWS)
                    hat, _ = layer_norm(dx_ref[sl, :].astype(F32))
                    h_ref[sl, :] = (hat * gain + bias).astype(BF16)

        with scope('heads_kv'):
            kv_ring.run(part_heads)
        keep = pltpu.make_async_copy(wkv_ref, wkv_all, mix_sem.at[2])
        keep.start()
        for come, go in zip(dy_in, dy_keep):
            come.wait()
            go.start()
        with scope('project_kv'):
            @pl.loop(0, chips)
            def _(n):
                y = dot(h_ref[...], wkv_ref[n])
                v = jnp.concatenate([turned(y[:, :head_dim]), y[:, head_dim:]], axis=1).astype(BF16)
                for b in range(n_batch):
                    far_ref[b, me, :, block(n, 2 * head_dim)] = v[b * seq:(b + 1) * seq]

        kvs.start_first()
        kvs.start_second()
        with scope('project_q'):
            q_ring.run(project)
        keep.wait()
        for copy in dy_keep:
            copy.wait()

    pl.run_scoped(
        project_all,
        pltpu.VMEM((chips, width, 2 * head_dim), BF16),
        pltpu.VMEM((3, 2, 4 * 64 * chips, head_dim), BF16), pltpu.VMEM((4, 2, width, head_dim), BF16),
        pltpu.SemaphoreType.DMA((3, 2)), pltpu.SemaphoreType.DMA((4,)), pltpu.SemaphoreType.DMA((n_batch * width // n_rows,)),
    )

    with scope('kv_pass'):
        kvs.pass_on()
    queries.start()
    q_ref[me] = g_ref[me, :, q_part]
    with scope('turn_h'):
        @pl.loop(0, width // 128)
        def _(step):
            sl = block(step, 128)
            ht_ref[sl, :] = h_ref[:, sl].T

    with scope('kv_wait'):
        kvs.share_second()
        kvs.share_far()
        kvs.wait_near()
        kvs.wait_far()

    def chip_at(i):
        return at.ring(jnp.where(i == 0, 0, jnp.where(i == 1, 1, jnp.where(i == 2, 3, 2))))

    def soft(s, seen):
        s = s * scale
        tail = jnp.where(seen, s[s.shape[0] - tile:], -1e30)
        s = tail if s.shape[0] == tile else jnp.concatenate([s[:s.shape[0] - tile], tail], axis=0)
        e = jnp.exp(s - jnp.max(s, axis=0, keepdims=True))
        return e * (1.0 / jnp.sum(e, axis=0, keepdims=True))

    def attend(t):
        limit = (t + 1) * tile

        @pl.loop(0, n_batch * chips)
        def _(i):
            @pl.when(i == 1)
            def _():
                with scope('q_pass'):
                    queries.pass_on()
                dys.start_second()
                dys.pass_on()
                hcols.start()

            b, n = lax.rem(i, n_batch), lax.div(i, n_batch)
            k = far_ref[b, 0:limit // seq, :, block(2 * n, head_dim)].reshape(limit, head_dim)
            vt = far_ref[b, 0:limit // seq, :, block(2 * n + 1, head_dim)].reshape(limit, head_dim).T

            def heads(first, count):
                q = jnp.concatenate([g_ref[n * n_batch + b, :, block(first + j, head_dim)] for j in range(count)], axis=0)
                row = lax.broadcasted_iota(jnp.int32, (tile, count * seq), 0)
                col = lax.broadcasted_iota(jnp.int32, (tile, count * seq), 1)
                p = soft(dot_nt(k, q), row <= lax.rem(col, seq) + core * seq)
                mixed = dot(vt, p.astype(BF16)).astype(BF16)
                for j in range(count):
                    h_ref[block(b, seq), block(n * group + first + j, head_dim)] = mixed[:, j * seq:(j + 1) * seq].T

            @pl.loop(0, group // 2)
            def _(j):
                heads(2 * j, 2)

            heads(group - 1, 1)

    with scope('attend'):
        for t in range(chips):
            @pl.when(at.chip == t)
            def _(t=t):
                attend(t)

    h_keep = pltpu.make_async_copy(ht_ref.at[block(me, half)], ht_all.at[me], loc_sem.at[1])
    h_keep.start()

    def out_tile(wo):
        sl = block(pl.program_id(0), COL_TILE)
        out_ref[:, sl] = (dx_ref[:, sl].astype(F32) + dot(h_ref[...], wo[...])).astype(BF16)

    with scope('output'):
        pltpu.emit_pipeline(out_tile, grid=(width // COL_TILE,), in_specs=[pl.BlockSpec((width, COL_TILE), lambda i: (0, i))], out_specs=[])(wo_ref)

    dy_back = [pltpu.make_async_copy(dy_ref.at[b], h_ref.at[pl.ds(b * seq, seq)], loc_sem.at[2 + b]) for b in range(n_batch)]
    for copy in dy_back:
        copy.start()

    k_all = lambda n: far_ref[core, 0:n, :, block(2 * at.chip, head_dim)].reshape(n * seq, head_dim)
    v_all = lambda n: far_ref[core, 0:n, :, block(2 * at.chip + 1, head_dim)].reshape(n * seq, head_dim)

    def rotate_back(t, cos, sin):
        u, w = t[:quarter], t[quarter:2 * quarter]
        return jnp.concatenate([u * cos + w * sin, w * cos - u * sin, t[2 * quarter:]], axis=0)

    def by_dev(t):
        return t.astype(BF16).reshape(t.shape[0] // seq, seq, head_dim)

    def attend_back(t):
        limit = (t + 1) * tile
        sl = slice(t * tile, limit)
        devs = slice(t * CORES, (t + 1) * CORES)

        @pl.loop(0, group)
        def _(j):
            q = q_ref[devs, :, block(j, head_dim)].reshape(tile, head_dim)
            k, v = k_all(limit // seq), v_all(limit // seq)
            da = da_ref[sl, block(j, head_dim)]
            row = lax.broadcasted_iota(jnp.int32, (tile, tile), 0)
            col = lax.broadcasted_iota(jnp.int32, (tile, tile), 1)
            p = soft(dot_nt(k, q), row <= col)
            p_low = p.astype(BF16)
            at_ref[block(j, head_dim), sl] = dot(vt_ref[:, :limit], p_low).astype(BF16)
            dp = dot_nt(v, da)
            row_dot = jnp.sum(p * dp, axis=0, keepdims=True)
            ds = (p * (dp - row_dot) * scale).astype(BF16)
            dv_ref[:limit, :] += dot(p_low, da)
            dk_ref[:limit, :] += dot(ds, q)
            back = rotate_back(dot(kt_ref[:, :limit], ds), cost_ref[:, sl], sint_ref[:, sl])
            g_ref[devs, :, block(j, head_dim)] = by_dev(back.T)

    def middle(wo_vm, dyk):
        wo_in = pltpu.make_async_copy(wo_ref.at[block(at.chip, n_rows)], wo_vm, mix_sem.at[2])
        wo_in.start()
        for j in range(1, n_dev):
            source = lax.rem(me + j, n_dev)
            send(pos_ref, spot_ref.at[source], p_ssem.at[0], p_rsem.at[source], at.partner).wait_recv()
        for d in range(n_dev):
            angle = freq * spot_ref[d, pl.ds(core, 1), :].astype(F32)
            cost_ref[:, d * seq:(d + 1) * seq] = jnp.cos(angle)
            sint_ref[:, d * seq:(d + 1) * seq] = jnp.sin(angle)
        with scope('q_wait'):
            queries.wait_recv()
            queries.wait_send()
            for copy in kvs.sent():
                copy.wait_send()
        kt_ref[...] = k_all(n_dev).T
        vt_ref[...] = v_all(n_dev).T
        dk_ref[...] = jnp.zeros_like(dk_ref)
        dv_ref[...] = jnp.zeros_like(dv_ref)
        with scope('dy_wait'):
            dys.share_second()
            dys.wait_near()

        def fetch(i, slot):
            return pltpu.make_async_copy(dy_all.at[block(chip_at(i), CORES), core], dyk.at[slot], mix_sem.at[slot])

        with scope('wo_wait'):
            fetch(0, 0).start()
            wo_in.wait()

        @pl.loop(0, chips)
        def _(i):
            slot = lax.rem(i, 2)

            @pl.when(i == chips - 1)
            def _():
                with scope('dy_far'):
                    dys.share_far()
                with scope('dy_far2'):
                    dys.wait_far()
                fetch(i, slot).start()
                with scope('h_pass'):
                    hcols.pass_on()

            fetch(i, slot).wait()

            @pl.when(i < chips - 2)
            def _():
                fetch(i + 1, 1 - slot).start()

            chip = chip_at(i)
            with scope('da'):
                da_ref[block(chip, tile), :] = dot_nt(dyk[slot].reshape(tile, width), wo_vm[...]).astype(BF16)
            with scope('attend_back'):
                for t in range(chips):
                    @pl.when(chip == t)
                    def _(t=t):
                        attend_back(t)

    pl.run_scoped(middle, pltpu.VMEM((n_rows, width), BF16), pltpu.VMEM((2, CORES, seq, width), BF16))
    g_ref[:, :, n_rows:n_rows + head_dim] = by_dev(rotate_back(dk_ref[...].T, cost_ref[...], sint_ref[...]).T)
    g_ref[:, :, n_rows + head_dim:] = by_dev(dv_ref[...])

    def span_of(q):
        return block(q, CORES)

    turn = [[at.ring(q) for q in (2, 1, 3, 0)], [at.ring(q) for q in (3, 0, 1, 2)]]
    direct = [[send(g_ref.at[span_of(turn[i][q])], g_all.at[me, span_of(turn[i][q])], g_ssem.at[i, q], g_rsem.at[i, q], at.dev(steps[i], core)) for q in range(chips)] for i in range(2)]
    came = [[at.ring(q) for q in (1, 0, 2, 3)], [at.ring(q) for q in (0, 1, 2, 3)]]
    onward = [[send(g_all.at[origin[i], span_of(came[i][q])], far_ref.at[core, span_of(came[i][q])], r_ssem.at[i, q], r_rsem.at[i, q], at.dev(steps[i], core)) for q in range(2)] for i in range(2)]
    ends = [[at.ring(q) for q in (0, 3)], [at.ring(q) for q in (1, 2)]]
    g_across = send(g_ref, g_all.at[me], x_ssem.at[0], x_rsem.at[0], at.partner)
    near_across = [[send(g_all.at[origin[i], span_of(came[i][q])], g_all.at[origin[i], span_of(came[i][q])], x_ssem.at[1 + i * chips + q], x_rsem.at[1 + i * chips + q], at.partner) for q in range(chips)] for i in range(2)]
    end_across = [[send(far_ref.at[core, span_of(ends[i][q])], far_ref.at[core, span_of(ends[i][q])], x_ssem.at[1 + (2 + i) * chips + q], x_rsem.at[1 + (2 + i) * chips + q], at.partner) for q in range(2)] for i in range(2)]
    for q in range(chips):
        for i in range(2):
            direct[i][q].start()
    g_across.start()
    g_keep = pltpu.make_async_copy(g_ref, g_all.at[me], loc_sem.at[0])
    g_keep.start()
    heads_across.start()
    at2_ref[:, block(core, n_seq)] = at_ref[block(core, half), :]

    with jax.named_scope('heads_wait'):
        heads_across.wait_recv()

    def wo_tile(dy):
        pieces = [dy[d, b] for b in range(n_batch) for d in range(n_dev)]
        dwo_ref[:, block(pl.program_id(0), COL_TILE)] = dot(at2_ref[...], jnp.concatenate(pieces, axis=0))

    with jax.named_scope('grad_wo'):
        pltpu.emit_pipeline(wo_tile, grid=(width // COL_TILE,), in_specs=[pl.BlockSpec((n_dev, n_batch, seq, COL_TILE), lambda i: (0, 0, 0, i))], out_specs=[])(dy_all)

    with scope('h_wait'):
        hcols.wait_recv()
    h_keep.wait()
    lhs_in = [pltpu.make_async_copy(ht_all.at[d, :, pl.ds(b * seq, seq)], at2_ref.at[:, pl.ds((b * n_dev + d) * seq, seq)], lhs_sem.at[b * n_dev + d]) for d in range(n_dev) for b in range(n_batch)]
    for copy in lhs_in:
        copy.start()
    with jax.named_scope('own_wait'):
        for copy in lhs_in:
            copy.wait()
        g_keep.wait()
        g_across.wait_recv()
    sums = [send(all_ref.at[me], all_ref.at[me], s_ssem.at[j], s_rsem.at[me], peer) for j, peer in enumerate(at.peers(True))]

    def weight_grads(wq_vm, wkv_vm, acc_ref, hat_ref, inv_ref, job_ref, mine_ref):
        n_slots = wq_vm.shape[0]
        chunk = wq_vm.shape[2]
        n_chunks = width // chunk
        total = n_chunks * chips

        def weights(s):
            slot = lax.rem(s, n_slots)
            chip = chip_at(lax.div(s, n_chunks))
            rows = block(lax.rem(s, n_chunks), chunk)
            return [
                pltpu.make_async_copy(wq_ref.at[block(chip, group), rows], wq_vm.at[slot], w_sem.at[slot, 0]),
                pltpu.make_async_copy(wkv_all.at[chip, rows], wkv_vm.at[slot], w_sem.at[slot, 1]),
            ]

        for s in range(n_slots):
            for copy in weights(s):
                copy.start()

        def grow(i, read):
            @pl.loop(0, n_chunks)
            def _(n):
                s = i * n_chunks + n
                slot = lax.rem(s, n_slots)
                for copy in weights(s):
                    copy.wait()
                rows = jnp.concatenate([read(b) for b in range(n_batch)], axis=0)
                part = dot_nt(rows, jnp.concatenate([wq_vm[slot, j] for j in range(group)] + [wkv_vm[slot]], axis=1))
                sl = block(n, chunk)

                @pl.when(i == 0)
                def _():
                    acc_ref[:, sl] = part

                @pl.when(i > 0)
                def _():
                    acc_ref[:, sl] += part

                @pl.when(s + n_slots < total)
                def _():
                    for copy in weights(s + n_slots):
                        copy.start()

        def mine_in(chip):
            return [pltpu.make_async_copy(g_all.at[chip * CORES + b, me], mine_ref.at[b], job_sem.at[2, b, 0]) for b in range(n_batch)]

        def grow_near(i):
            copies = mine_in(chip_at(i))
            for copy in copies:
                copy.start()
            for copy in copies:
                copy.wait()
            grow(i, lambda b: mine_ref[b])

        def job_in(chip, quarters, slot):
            return [pltpu.make_async_copy(g_all.at[chip * CORES + b, span_of(q)], job_ref.at[slot, b, n], job_sem.at[slot, b, n]) for b in range(n_batch) for n, q in enumerate(quarters)]

        def job(chip, quarters, read, add):
            part = CORES * seq
            lhs = [at2_ref[:, pl.ds(pl.multiple_of(b * n_seq + q * part, part), part)] for b in range(n_batch) for q in quarters]
            rhs = [read(b, n, q).reshape(part, cols) for b in range(n_batch) for n, q in enumerate(quarters)]
            y = dot(jnp.concatenate(lhs, axis=1), jnp.concatenate(rhs, axis=0))
            for j in range(group):
                v = y[:, j * head_dim:(j + 1) * head_dim]
                dwq_ref[chip * group + j] = dwq_ref[chip * group + j] + v if add else v
            for j, ref in enumerate((dwk_ref, dwv_ref)):
                v = y[:, (group + j) * head_dim:(group + j + 1) * head_dim]
                rows = pl.ds(chip, half, stride=chips)
                ref[rows, :] = ref[rows, :] + v if add else v

        def near_pair(quarters, add):
            for slot, step in enumerate(steps):
                for copy in job_in(at.ring(step), quarters, slot):
                    copy.start()

            @pl.loop(0, 2)
            def _(slot):
                chip = at.ring(1 - 2 * slot)
                for copy in job_in(chip, quarters, slot):
                    copy.wait()
                job(chip, quarters, lambda b, n, q: job_ref[slot, b, n], add)

        halves = [[at.ring(q) for q in half_of] for half_of in ((0, 1), (2, 3))]
        for slot in range(2):
            for copy in job_in(at.chip, [at.ring(2 * slot), at.ring(2 * slot + 1)], slot):
                copy.start()
        with jax.named_scope('own_dh'):
            grow_near(0)
        with jax.named_scope('own_job'):
            for slot in range(2):
                quarters = [at.ring(2 * slot), at.ring(2 * slot + 1)]
                for copy in job_in(at.chip, quarters, slot):
                    copy.wait()
                job(at.chip, quarters, lambda b, n, q: job_ref[slot, b, n], slot == 1)

        with jax.named_scope('d01_wait'):
            for q in range(2):
                for i in range(2):
                    direct[i][q].wait_recv()
                for i in range(2):
                    onward[i][q].start()
                    near_across[i][q].start()
        with jax.named_scope('d01_across'):
            for q in range(2):
                for i in range(2):
                    near_across[i][q].wait_recv()
        with jax.named_scope('near_dh'):
            @pl.loop(1, chips - 1)
            def _(i):
                grow_near(i)

        with jax.named_scope('near_a'):
            near_pair(halves[0], False)
        with jax.named_scope('hat'):
            @pl.loop(0, n_tok // (2 * ROWS))
            def _(step):
                for i in range(2):
                    sl = block(2 * step + i, ROWS)
                    hat, inv = layer_norm(dx_ref[sl, :].astype(F32))
                    hat_ref[sl, :] = hat
                    inv_ref[sl, :] = jnp.broadcast_to(inv, (ROWS, 128))

        with jax.named_scope('d23_wait'):
            for q in range(2, chips):
                for i in range(2):
                    direct[i][q].wait_recv()
                    near_across[i][q].start()
        with jax.named_scope('d23_across'):
            for q in range(2, chips):
                for i in range(2):
                    near_across[i][q].wait_recv()

        with jax.named_scope('near_b'):
            near_pair(halves[1], True)
        far_chip = at.ring(2)
        with jax.named_scope('far0_wait'):
            for i in range(2):
                onward[i][0].wait_recv()
                end_across[i][0].start()
        with jax.named_scope('far0_across'):
            for i in range(2):
                end_across[i][0].wait_recv()
        with jax.named_scope('far_dh'):
            grow(chips - 1, lambda b: far_ref[b, me])
        for copy in dy_back:
            copy.wait()
        part_ref[...] = jnp.zeros_like(part_ref)

        with jax.named_scope('norm_back'):
            @pl.loop(0, n_tok // (2 * ROWS))
            def _(step):
                for i in range(2):
                    sl = block(2 * step + i, ROWS)
                    hat, inv = hat_ref[sl, :], inv_ref[sl, 0:1]
                    dh = acc_ref[sl, :]
                    dg = dh * hat
                    gh = dh * gain
                    one = jnp.mean(gh, axis=-1, keepdims=True)
                    two = jnp.mean(dg * gain, axis=-1, keepdims=True)
                    dx_ref[sl, :] = (h_ref[sl, :].astype(F32) + inv * (gh - one - hat * two)).astype(BF16)
                    part_ref[0] += dg[0:8] + dg[8:16]
                    part_ref[1] += dh[0:8] + dh[8:16]

        all_ref[me, 0:1, :] = jnp.sum(part_ref[0], axis=0, keepdims=True)
        all_ref[me, 1:2, :] = jnp.sum(part_ref[1], axis=0, keepdims=True)
        read_far = lambda b, n, q: far_ref[b, span_of(q)]
        for copy in sums:
            copy.start()
        with jax.named_scope('far_a'):
            job(far_chip, [ends[0][0], ends[1][0]], read_far, False)
        with jax.named_scope('far1_wait'):
            for i in range(2):
                onward[i][1].wait_recv()
                end_across[i][1].start()
        with jax.named_scope('far1_across'):
            for i in range(2):
                end_across[i][1].wait_recv()
        with jax.named_scope('far_b'):
            job(far_chip, [ends[0][1], ends[1][1]], read_far, True)

    pl.run_scoped(
        weight_grads,
        pltpu.VMEM((W_SLOTS, group, W_ROWS, head_dim), BF16), pltpu.VMEM((W_SLOTS, W_ROWS, 2 * head_dim), BF16), pltpu.VMEM((n_tok, width), F32),
        pltpu.VMEM((n_tok, width), F32), pltpu.VMEM((n_tok, 128), F32), pltpu.VMEM((2, n_batch, 2, CORES, seq, cols), BF16), pltpu.VMEM((n_batch, seq, cols), BF16),
    )

    with jax.named_scope('sums'):
        for j in range(1, n_dev):
            source = lax.rem(me + j, n_dev)
            send(all_ref.at[me], all_ref.at[source], s_ssem.at[0], s_rsem.at[source], at.partner).wait_recv()
        total = all_ref[0]
        for d in range(1, n_dev):
            total = total + all_ref[d]
        dgain_ref[...] = total[0:1].reshape(width)
        dbias_ref[...] = total[1:2].reshape(width)
    done = dys.sent() + [heads_across] + spots
    done += direct[0] + direct[1] + onward[0] + onward[1] + [g_across] + near_across[0] + near_across[1] + end_across[0] + end_across[1] + sums
    with jax.named_scope('done'):
        for copy in done:
            copy.wait_send()
        hcols.wait_send()


def whole_block(n_dev, x, gain, bias, positions, freq, dy, wq, wk, wv, wo):
    n_batch, seq, width = dy.shape
    n_tok = n_batch * seq
    head_dim = wq.shape[2]
    chips = n_dev // CORES
    group = wq.shape[0] // chips
    cols = (group + 2) * head_dim
    n_rows = group * head_dim
    half = n_rows // CORES
    n_seq = n_dev * seq
    quarter = head_dim // 4
    dma = pltpu.SemaphoreType.DMA
    vm = pltpu.VMEM
    shapes = [((n_tok, width), BF16)] * 2 + [((chips * group, half, head_dim), F32)] + [((chips * half, head_dim), F32)] * 2 + [((half, width), F32), ((width,), F32), ((width,), F32)]
    held = [((n_dev, n_batch, seq, width), BF16), ((n_dev, half, n_tok), BF16), ((n_dev, n_dev, seq, cols), BF16), ((chips, width, 2 * head_dim), BF16)]
    return pl.pallas_call(
        functools.partial(block_body, n_dev, group),
        out_shape=tuple(pltpu.VMEM(*t) for t in shapes) + tuple(sds(*t) for t in held),
        in_specs=[VM] * 4 + [HBM] * 6,
        out_specs=(VM,) * len(shapes) + (HBM,) * len(held),
        scratch_shapes=[
            vm((n_tok, width), BF16), vm((width, n_tok), BF16), vm((n_dev, seq, cols), BF16), vm((n_dev, seq, n_rows), BF16),
            vm((n_rows, n_seq), BF16), vm((half, n_batch * n_seq), BF16), vm((n_seq, n_rows), BF16),
            vm((head_dim, n_seq), BF16), vm((head_dim, n_seq), BF16), vm((n_seq, head_dim), F32), vm((n_seq, head_dim), F32),
            vm((quarter, n_seq), F32), vm((quarter, n_seq), F32), vm((3, n_tok, head_dim), F32), vm((n_dev, n_batch, seq), jnp.int32),
            vm((2, seq, n_rows), BF16), vm((2, half, n_tok), BF16),
            vm((n_batch, n_dev, seq, cols), BF16), vm((2, 8, width), F32), vm((n_dev, 2, width), F32),
            dma((13,)), dma((13,)), dma((13,)), dma((13,)), dma((9,)), dma((n_dev + 2,)), dma((9,)), dma((n_dev + 2,)), dma((n_dev,)), dma((n_dev,)), dma((2,)),
            dma((2, chips)), dma((2, chips)), dma((2, 2)), dma((2, 2)), dma((1 + 4 * chips,)), dma((1 + 4 * chips,)), dma((n_dev,)), dma((n_dev,)),
            dma((1 + n_dev,)), dma((3,)), dma((n_batch * n_dev,)), dma((W_SLOTS, 2)), dma((3, n_batch, 2)),
        ],
        compiler_params=pltpu.CompilerParams(collective_id=0, has_side_effects=True, vmem_limit_bytes=VMEM_LIMIT),
        cost_estimate=pl.CostEstimate(flops=10 ** 11, bytes_accessed=10 ** 8, transcendentals=0),
        name='block',
    )(gain, bias, positions, freq, x.reshape(n_tok, width), dy, wq, wk, wv, wo)[:len(shapes)]


def settle_body(n, *refs):
    sems = refs[2 * n]
    copies = []
    for i in range(n):
        src, dst = refs[i], refs[n + i]
        pieces = SETTLE if len(src.shape) > 1 else 1
        size = src.shape[0] // pieces
        for p in range(pieces):
            copies.append(pltpu.make_async_copy(src.at[pl.ds(p * size, size)], dst.at[pl.ds(p * size, size)], sems.at[i, p]))
    for copy in copies:
        copy.start()
    for copy in copies:
        copy.wait()


def settle(arrays):
    n = len(arrays)
    return pl.pallas_call(
        functools.partial(settle_body, n),
        out_shape=tuple(sds(t.shape, t.dtype) for t in arrays),
        in_specs=[ANY] * n,
        out_specs=(HBM,) * n,
        scratch_shapes=[pltpu.SemaphoreType.DMA((n, SETTLE))],
        compiler_params=pltpu.CompilerParams(vmem_limit_bytes=1024 * 1024),
        name='settle',
    )(*arrays)


def solution(mesh):
    n_dev = mesh.shape['cp']

    def device_step(x_act, d_out, positions, ln_gain, ln_bias, w_query, w_key, w_value, w_out):
        n_batch, seq, width = x_act.shape
        q_heads, (kv_heads, head_dim) = w_query.shape[1], w_key.shape[1:]
        group = q_heads // kv_heads
        quarter = head_dim // 4
        assert n_batch == CORES and n_dev // CORES == kv_heads == 4 and q_heads * head_dim == width

        freq = np.exp(np.arange(quarter) * (-2.0 * math.log(ROPE_BASE) / (head_dim // 2))).astype(np.float32).reshape(quarter, 1)
        by_head = lambda t: jnp.transpose(t, (1, 0, 2))
        by_row = lambda t: t.reshape(width * kv_heads, head_dim)
        wq = by_head(w_query)

        results = whole_block(n_dev, x_act, ln_gain, ln_bias, positions, jnp.asarray(freq), d_out, wq, by_row(w_key), by_row(w_value), w_out)
        out, dx, dwq, dwk, dwv, dwo, dgain, dbias = settle(results)
        kv_rows = lambda t: t.reshape(width // n_dev, kv_heads, head_dim)
        return (out.reshape(x_act.shape), dx.reshape(x_act.shape), by_head(dwq), kv_rows(dwk), kv_rows(dwv), dwo, dgain, dbias)

    return jax.shard_map(device_step, mesh=mesh, in_specs=(P('dp', 'cp', None), P('dp', 'cp', None), P('dp', 'cp'), P(None), P(None), P(None, None, None), P(None, None, None), P(None, None, None), P(None, None)), out_specs=(P('dp', 'cp', None), P('dp', 'cp', None), P(('dp', 'cp'), None, None), P(('dp', 'cp'), None, None), P(('dp', 'cp'), None, None), P(('dp', 'cp'), None), P('dp'), P('dp')), check_vma=False)
```

```python
import functools
import math
import jax
import jax.numpy as jnp
import numpy as np
from jax import lax
from jax.experimental import pallas as pl
from jax.experimental.pallas import tpu as pltpu
from jax.sharding import PartitionSpec as P

EPS = 1e-5
ROPE_BASE = 10000.0
BF16 = jnp.bfloat16
F32 = jnp.float32
VMEM_LIMIT = 46 * 1024 * 1024
NT = (((1,), (1,)), ((), ()))
ANY = pl.BlockSpec(memory_space=pl.ANY)
VM = pl.BlockSpec(memory_space=pltpu.VMEM)
HBM = pl.BlockSpec(memory_space=pltpu.HBM)
CORES = 2
COL_TILE = 512
ROWS = 16
W_SLOTS = 4
W_ROWS = 512
SETTLE = 4


def dot(a, b):
    return jnp.dot(a, b, preferred_element_type=F32)


def dot_nt(a, b):
    return lax.dot_general(a, b, NT, preferred_element_type=F32)


def sds(shape, dtype):
    return jax.ShapeDtypeStruct(shape, dtype)


def block(i, size):
    return pl.ds(pl.multiple_of(i * size, size), size)


class Place:
    def __init__(self, n_dev):
        self.n_dev = n_dev
        self.chips = n_dev // CORES
        self.me = lax.axis_index('cp')
        self.chip = self.me // CORES
        self.core = self.me % CORES
        self.partner = self.chip * CORES + 1 - self.core

    def ring(self, step):
        return lax.rem(self.chip + self.chips + step, self.chips)

    def dev(self, step, core):
        return self.ring(step) * CORES + core

    def peers(self, far):
        near = [self.partner] + [self.dev(s, c) for s in (1, -1) for c in range(CORES)]
        return near + ([self.dev(2, c) for c in range(CORES)] if far else [])


def send(src, dst, ssem, rsem, to):
    return pltpu.make_async_remote_copy(src_ref=src, dst_ref=dst, send_sem=ssem, recv_sem=rsem, device_id={'cp': to}, device_id_type=pl.DeviceIdType.MESH)


def meet(peers):
    barrier = pltpu.get_barrier_semaphore()
    for peer in peers:
        pl.semaphore_signal(barrier, inc=1, device_id={'cp': peer}, device_id_type=pl.DeviceIdType.MESH)
    pl.semaphore_wait(barrier, len(peers))


class Ring:
    def __init__(self, n, slots, copies):
        self.n, self.slots, self.copies = n, slots, copies

    def prime(self):
        for s in range(self.slots):
            for copy in self.copies(s, s):
                copy.start()

    def run(self, use):
        @pl.loop(0, self.n)
        def _(s):
            slot = lax.rem(s, self.slots)
            for copy in self.copies(s, slot):
                copy.wait()
            use(s, slot)

            @pl.when(s + self.slots < self.n)
            def _():
                for copy in self.copies(s + self.slots, slot):
                    copy.start()


class Gather:
    def __init__(self, at, own, piece, both, ssem, rsem):
        steps = (1, -1)
        origin = [at.dev(-1, at.core), at.dev(1, at.core)]
        far = at.dev(2, at.core)
        link = lambda i, src, dst, to: send(src, dst, ssem.at[i], rsem.at[i], to)
        self.first = [link(b, own(b), piece(at.me, b), at.dev(steps[b], at.core)) for b in range(2)]
        self.second = [link(2 + b, own(1 - b), piece(at.me, 1 - b), at.dev(steps[b], at.core)) for b in range(2)]
        self.again = [link(4 + b, piece(origin[b], b), piece(origin[b], b), at.dev(steps[b], at.core)) for b in range(2)]
        self.own_across = link(6, both(None), both(at.me), at.partner)
        self.first_across = [link(7 + b, piece(origin[b], b), piece(origin[b], b), at.partner) for b in range(2)]
        self.second_across = [link(9 + b, piece(origin[b], 1 - b), piece(origin[b], 1 - b), at.partner) for b in range(2)]
        self.far_across = [link(11 + b, piece(far, b), piece(far, b), at.partner) for b in range(2)]

    def start_first(self):
        for copy in self.first + [self.own_across]:
            copy.start()

    def start_second(self):
        for copy in self.second:
            copy.start()

    def pass_on(self):
        for copy, again, across in zip(self.first, self.again, self.first_across):
            copy.wait_recv()
            again.start()
            across.start()

    def share_second(self):
        for copy, across in zip(self.second, self.second_across):
            copy.wait_recv()
            across.start()

    def share_far(self):
        for copy, across in zip(self.again, self.far_across):
            copy.wait_recv()
            across.start()

    def wait_near(self):
        for copy in [self.own_across] + self.first_across + self.second_across:
            copy.wait_recv()

    def wait_far(self):
        for copy in self.far_across:
            copy.wait_recv()

    def sent(self):
        return self.first + self.second + self.again + [self.own_across] + self.first_across + self.second_across + self.far_across


class Exchange:
    def __init__(self, at, src, dst, relay, ssem, rsem):
        self.at, self.src, self.dst, self.relay, self.ssem, self.rsem = at, src, dst, relay, ssem, rsem
        near = [(0, 1 - at.core)] + [(s, c) for s in (1, -1) for c in range(CORES)]
        n = at.n_dev
        self.near = [send(src(at.dev(s, c)), dst(at.me), ssem.at[i], rsem.at[at.me], at.dev(s, c)) for i, (s, c) in enumerate(near)]
        self.far = [send(src(at.dev(2, i)), relay.at[i], ssem.at[5 + i], rsem.at[n + i], at.dev(step, at.core)) for i, step in enumerate((1, -1))]
        self.on = [send(relay.at[i], dst(at.dev(-step, at.core)), ssem.at[7 + i], rsem.at[at.dev(-step, at.core)], at.dev(step, i)) for i, step in enumerate((1, -1))]

    def start(self):
        for copy in self.far + self.near:
            copy.start()

    def pass_on(self):
        for far, on in zip(self.far, self.on):
            far.wait_recv()
            on.start()

    def wait_recv(self):
        at = self.at
        for j in range(1, at.n_dev):
            origin = lax.rem(at.me + j, at.n_dev)
            send(self.src(at.me), self.dst(origin), self.ssem.at[0], self.rsem.at[origin], at.partner).wait_recv()

    def wait_send(self):
        for copy in self.far + self.near + self.on:
            copy.wait_send()


def layer_norm(x):
    cen = x - jnp.mean(x, axis=-1, keepdims=True)
    inv = lax.rsqrt(jnp.mean(cen * cen, axis=-1, keepdims=True) + EPS)
    return cen * inv, inv


def block_body(n_dev, group, gain_ref, bias_ref, pos_ref, freq_ref, x_hbm, dy_ref, wq_ref, wk_ref, wv_ref, wo_ref,
               out_ref, dx_ref, dwq_ref, dwk_ref, dwv_ref, dwo_ref, dgain_ref, dbias_ref, dy_all, ht_all, g_all, wkv_all,
               h_ref, ht_ref, g_ref, q_ref, at_ref, at2_ref, da_ref, kt_ref, vt_ref, dk_ref, dv_ref,
               cost_ref, sint_ref, tab_ref, spot_ref, relay_q, relay_h, far_ref, part_ref, all_ref,
               dy_ssem, dy_rsem, kv_ssem, kv_rsem, q_ssem, q_rsem, h_ssem, h_rsem, p_ssem, p_rsem, t_sem,
               g_ssem, g_rsem, r_ssem, r_rsem, x_ssem, x_rsem, s_ssem, s_rsem, loc_sem, mix_sem, lhs_sem, w_sem, job_sem):
    at = Place(n_dev)
    n_batch, seq, width = dy_ref.shape
    n_tok = n_batch * seq
    head_dim = wq_ref.shape[2]
    cols = (group + 2) * head_dim
    n_rows = group * head_dim
    half = n_rows // CORES
    n_seq = n_dev * seq
    quarter = head_dim // 4
    scale = head_dim ** -0.5
    chips = at.chips
    tile = CORES * seq
    core, me = at.core, at.me
    steps = (1, -1)
    origin = [at.dev(-1, core), at.dev(1, core)]
    far_dev = at.dev(2, core)
    scope = jax.named_scope

    with scope('meet'):
        meet(at.peers(True))

    kv_cols = 2 * head_dim * chips
    kv_piece = lambda d, b: far_ref.at[b, d, :, pl.ds(0, kv_cols)]
    kv_both = lambda d: far_ref.at[:, me if d is None else d, :, pl.ds(0, kv_cols)]
    dys = Gather(at, lambda b: dy_ref.at[b], lambda d, b: dy_all.at[d, b], lambda d: dy_ref if d is None else dy_all.at[d], dy_ssem, dy_rsem)
    kvs = Gather(at, lambda b: kv_piece(me, b), kv_piece, kv_both, kv_ssem, kv_rsem)
    q_part = pl.ds(0, n_rows)
    queries = Exchange(at, lambda d: g_ref.at[d, :, q_part], lambda d: q_ref.at[d], relay_q, q_ssem, q_rsem)
    hcols = Exchange(at, lambda d: ht_ref.at[block(d, half)], lambda d: ht_all.at[d], relay_h, h_ssem, h_rsem)
    heads_across = send(at_ref.at[block(1 - core, half)], at2_ref.at[:, block(core, n_seq)], t_sem.at[0], t_sem.at[1], at.partner)
    spots = [send(pos_ref, spot_ref.at[me], p_ssem.at[j], p_rsem.at[me], peer) for j, peer in enumerate(at.peers(True))]

    dys.start_first()
    x_in = pltpu.make_async_copy(x_hbm, dx_ref, loc_sem.at[1])
    x_in.start()
    for copy in spots:
        copy.start()
    spot_ref[me] = pos_ref[...]

    freq = freq_ref[...]
    for b in range(n_batch):
        angle = freq * pos_ref[b:b + 1, :].astype(F32)
        cos, sin, none = jnp.cos(angle), jnp.sin(angle), jnp.zeros((quarter, seq), F32)
        rest = jnp.zeros((head_dim - 2 * quarter, seq), F32)
        for i, rows in enumerate(([cos, cos, rest + 1.0], [-sin, none, rest], [none, sin, rest])):
            tab_ref[i, b * seq:(b + 1) * seq, :] = jnp.concatenate(rows, axis=0).T

    gain = (1.0 + gain_ref[...]).reshape(1, width)
    bias = bias_ref[...].reshape(1, width)

    def project_all(wkv_ref, raw_ref, wq_vm, raw_sem, wq_sem, stage_sem):
        pieces = [(b, i) for b in range(n_batch) for i in range(width // n_rows)]
        there = lambda n: da_ref.at[pl.ds(n * seq, seq)]
        dy_in = [pltpu.make_async_copy(dy_ref.at[b, :, pl.ds(i * n_rows, n_rows)], there(n), stage_sem.at[n]) for n, (b, i) in enumerate(pieces)]
        dy_keep = [pltpu.make_async_copy(there(n), dy_all.at[me, b, :, pl.ds(i * n_rows, n_rows)], stage_sem.at[n]) for n, (b, i) in enumerate(pieces)]
        span = 64 * chips
        batch = raw_ref.shape[2] // span
        row = lax.broadcasted_iota(jnp.int32, (span, span), 0)
        col = lax.broadcasted_iota(jnp.int32, (span, span), 1)
        pick = jnp.where(col == lax.rem(row, 64) * chips + lax.div(row, 64), 1.0, 0.0).astype(BF16)

        def raw_in(s, slot):
            return [pltpu.make_async_copy(w.at[block(s, span * batch)], raw_ref.at[slot, i], raw_sem.at[slot, i]) for i, w in enumerate((wk_ref, wv_ref))]

        def wq_in(s, slot):
            return [pltpu.make_async_copy(wq_ref.at[block(s, 2)], wq_vm.at[slot], wq_sem.at[slot])]

        def part_heads(s, slot):
            for i in range(batch):
                sl = slice(i * span, (i + 1) * span)
                rows = dot(pick, jnp.concatenate([raw_ref[slot, 0, sl, :], raw_ref[slot, 1, sl, :]], axis=1)).astype(BF16)
                for n in range(chips):
                    wkv_ref[n, block(s * batch + i, 64), :] = rows[n * 64:(n + 1) * 64]

        def turned(v):
            return v * tab_ref[0] + pltpu.roll(v, head_dim - quarter, 1) * tab_ref[1] + pltpu.roll(v, quarter, 1) * tab_ref[2]

        def project(s, slot):
            y = dot(h_ref[...], jnp.concatenate([wq_vm[slot, 0], wq_vm[slot, 1]], axis=1))
            for i in range(2):
                head = s * 2 + i
                v = turned(y[:, i * head_dim:(i + 1) * head_dim]).astype(BF16)
                for b in range(n_batch):
                    g_ref[lax.div(head, group) * n_batch + b, :, block(lax.rem(head, group), head_dim)] = v[b * seq:(b + 1) * seq]

        kv_ring = Ring(width // (64 * batch), raw_ref.shape[0], raw_in)
        q_ring = Ring(chips * group // 2, wq_vm.shape[0], wq_in)
        kv_ring.prime()
        q_ring.prime()
        for copy in dy_in:
            copy.start()
        x_in.wait()
        with scope('norm'):
            @pl.loop(0, n_tok // (2 * ROWS))
            def _(step):
                for i in range(2):
                    sl = block(2 * step + i, ROWS)
                    hat, _ = layer_norm(dx_ref[sl, :].astype(F32))
                    h_ref[sl, :] = (hat * gain + bias).astype(BF16)

        with scope('heads_kv'):
            kv_ring.run(part_heads)
        keep = pltpu.make_async_copy(wkv_ref, wkv_all, mix_sem.at[2])
        keep.start()
        for come, go in zip(dy_in, dy_keep):
            come.wait()
            go.start()
        with scope('project_kv'):
            @pl.loop(0, chips)
            def _(n):
                y = dot(h_ref[...], wkv_ref[n])
                v = jnp.concatenate([turned(y[:, :head_dim]), y[:, head_dim:]], axis=1).astype(BF16)
                for b in range(n_batch):
                    far_ref[b, me, :, block(n, 2 * head_dim)] = v[b * seq:(b + 1) * seq]

        kvs.start_first()
        kvs.start_second()
        with scope('project_q'):
            q_ring.run(project)
        keep.wait()
        for copy in dy_keep:
            copy.wait()

    pl.run_scoped(
        project_all,
        pltpu.VMEM((chips, width, 2 * head_dim), BF16),
        pltpu.VMEM((3, 2, 4 * 64 * chips, head_dim), BF16), pltpu.VMEM((4, 2, width, head_dim), BF16),
        pltpu.SemaphoreType.DMA((3, 2)), pltpu.SemaphoreType.DMA((4,)), pltpu.SemaphoreType.DMA((n_batch * width // n_rows,)),
    )

    with scope('kv_pass'):
        kvs.pass_on()
    queries.start()
    q_ref[me] = g_ref[me, :, q_part]
    with scope('turn_h'):
        @pl.loop(0, width // 128)
        def _(step):
            sl = block(step, 128)
            ht_ref[sl, :] = h_ref[:, sl].T

    with scope('kv_wait'):
        kvs.share_second()
        kvs.share_far()
        kvs.wait_near()
        kvs.wait_far()

    def chip_at(i):
        return at.ring(jnp.where(i == 0, 0, jnp.where(i == 1, 1, jnp.where(i == 2, 3, 2))))

    def soft(s, seen):
        s = s * scale
        clear = s.shape[0] - seen.shape[0]
        tail = jnp.where(seen, s[clear:], -1e30)
        s = tail if clear == 0 else jnp.concatenate([s[:clear], tail], axis=0)
        e = jnp.exp(s - jnp.max(s, axis=0, keepdims=True))
        return e * (1.0 / jnp.sum(e, axis=0, keepdims=True))

    def attend(limit, clear):
        @pl.loop(0, n_batch * chips)
        def _(i):
            @pl.when(i == 1)
            def _():
                with scope('q_pass'):
                    queries.pass_on()
                dys.start_second()
                dys.pass_on()
                hcols.start()

            b, n = lax.rem(i, n_batch), lax.div(i, n_batch)
            k = far_ref[b, 0:limit // seq, :, block(2 * n, head_dim)].reshape(limit, head_dim)
            vt = far_ref[b, 0:limit // seq, :, block(2 * n + 1, head_dim)].reshape(limit, head_dim).T
            q = jnp.concatenate([g_ref[n * n_batch + b, :, block(j, head_dim)] for j in range(group)], axis=0)
            row = lax.broadcasted_iota(jnp.int32, (limit - clear, n_rows), 0)
            col = lax.broadcasted_iota(jnp.int32, (limit - clear, n_rows), 1)
            p = soft(dot_nt(k, q), row <= lax.rem(col, seq) + (me * seq - clear))
            mixed = dot(vt, p.astype(BF16)).astype(BF16)
            for j in range(group):
                h_ref[block(b, seq), block(n * group + j, head_dim)] = mixed[:, j * seq:(j + 1) * seq].T

    with scope('attend'):
        @pl.when(at.chip == chips - 1)
        def _():
            attend(chips * tile, (chips - 1) * tile)

        @pl.when(at.chip < chips - 1)
        def _():
            attend((chips - 1) * tile, 0)

    h_keep = pltpu.make_async_copy(ht_ref.at[block(me, half)], ht_all.at[me], loc_sem.at[1])
    h_keep.start()

    k_all = lambda n: far_ref[core, 0:n, :, block(2 * at.chip, head_dim)].reshape(n * seq, head_dim)
    v_all = lambda n: far_ref[core, 0:n, :, block(2 * at.chip + 1, head_dim)].reshape(n * seq, head_dim)

    def rotate_back(t, cos, sin):
        u, w = t[:quarter], t[quarter:2 * quarter]
        return jnp.concatenate([u * cos + w * sin, w * cos - u * sin, t[2 * quarter:]], axis=0)

    def by_dev(t):
        return t.astype(BF16).reshape(t.shape[0] // seq, seq, head_dim)

    def attend_back(t):
        limit = (t + 1) * tile
        sl = slice(t * tile, limit)
        devs = slice(t * CORES, (t + 1) * CORES)

        def heads(first, count):
            each = range(count)
            q = jnp.concatenate([q_ref[devs, :, block(first + j, head_dim)].reshape(tile, head_dim) for j in each], axis=0)
            da = jnp.concatenate([da_ref[sl, block(first + j, head_dim)] for j in each], axis=0)
            k, v = k_all(limit // seq), v_all(limit // seq)
            row = lax.broadcasted_iota(jnp.int32, (tile, count * tile), 0)
            col = lax.broadcasted_iota(jnp.int32, (tile, count * tile), 1)
            p = soft(dot_nt(k, q), row <= lax.rem(col, tile))
            p_low = p.astype(BF16)
            mixed = dot(vt_ref[:, :limit], p_low).astype(BF16)
            dp = dot_nt(v, da)
            row_dot = jnp.sum(p * dp, axis=0, keepdims=True)
            ds = (p * (dp - row_dot) * scale).astype(BF16)
            dv_ref[:limit, :] += dot(p_low, da)
            dk_ref[:limit, :] += dot(ds, q)
            back = dot(kt_ref[:, :limit], ds)
            for j in each:
                part = slice(j * tile, (j + 1) * tile)
                at_ref[block(first + j, head_dim), sl] = mixed[:, part]
                g_ref[devs, :, block(first + j, head_dim)] = by_dev(rotate_back(back[:, part], cost_ref[:, sl], sint_ref[:, sl]).T)

        @pl.loop(0, group // 2)
        def _(j):
            heads(2 * j, 2)

        heads(group - 1, 1)

    def middle(wo_vm, dyk):
        wo_in = pltpu.make_async_copy(wo_ref.at[block(at.chip, n_rows)], wo_vm, mix_sem.at[2])
        wo_in.start()
        for j in range(1, n_dev):
            source = lax.rem(me + j, n_dev)
            send(pos_ref, spot_ref.at[source], p_ssem.at[0], p_rsem.at[source], at.partner).wait_recv()
        for d in range(n_dev):
            angle = freq * spot_ref[d, pl.ds(core, 1), :].astype(F32)
            cost_ref[:, d * seq:(d + 1) * seq] = jnp.cos(angle)
            sint_ref[:, d * seq:(d + 1) * seq] = jnp.sin(angle)
        with scope('q_wait'):
            queries.wait_recv()
            queries.wait_send()
            for copy in kvs.sent():
                copy.wait_send()
        kt_ref[...] = k_all(n_dev).T
        vt_ref[...] = v_all(n_dev).T
        dk_ref[...] = jnp.zeros_like(dk_ref)
        dv_ref[...] = jnp.zeros_like(dv_ref)
        with scope('dy_wait'):
            dys.share_second()
            dys.wait_near()

        def fetch(i, slot):
            return pltpu.make_async_copy(dy_all.at[block(chip_at(i), CORES), core], dyk.at[slot], mix_sem.at[slot])

        with scope('wo_wait'):
            fetch(0, 0).start()
            wo_in.wait()

        @pl.loop(0, chips)
        def _(i):
            slot = lax.rem(i, 2)

            @pl.when(i == chips - 1)
            def _():
                with scope('dy_far'):
                    dys.share_far()
                with scope('dy_far2'):
                    dys.wait_far()
                fetch(i, slot).start()
                with scope('h_pass'):
                    hcols.pass_on()

            fetch(i, slot).wait()

            @pl.when(i < chips - 2)
            def _():
                fetch(i + 1, 1 - slot).start()

            chip = chip_at(i)
            with scope('da'):
                da_ref[block(chip, tile), :] = dot_nt(dyk[slot].reshape(tile, width), wo_vm[...]).astype(BF16)
            with scope('attend_back'):
                for t in range(chips):
                    @pl.when(chip == t)
                    def _(t=t):
                        attend_back(t)

    pl.run_scoped(middle, pltpu.VMEM((n_rows, width), BF16), pltpu.VMEM((2, CORES, seq, width), BF16))
    g_ref[:, :, n_rows:n_rows + head_dim] = by_dev(rotate_back(dk_ref[...].T, cost_ref[...], sint_ref[...]).T)
    g_ref[:, :, n_rows + head_dim:] = by_dev(dv_ref[...])

    def span_of(q):
        return block(q, CORES)

    turn = [[at.ring(q) for q in (2, 1, 3, 0)], [at.ring(q) for q in (3, 0, 1, 2)]]
    direct = [[send(g_ref.at[span_of(turn[i][q])], g_all.at[me, span_of(turn[i][q])], g_ssem.at[i, q], g_rsem.at[i, q], at.dev(steps[i], core)) for q in range(chips)] for i in range(2)]
    came = [[at.ring(q) for q in (1, 0, 2, 3)], [at.ring(q) for q in (0, 1, 2, 3)]]
    onward = [[send(g_all.at[origin[i], span_of(came[i][q])], far_ref.at[core, span_of(came[i][q])], r_ssem.at[i, q], r_rsem.at[i, q], at.dev(steps[i], core)) for q in range(2)] for i in range(2)]
    ends = [[at.ring(q) for q in (0, 3)], [at.ring(q) for q in (1, 2)]]
    g_across = send(g_ref, g_all.at[me], x_ssem.at[0], x_rsem.at[0], at.partner)
    near_across = [[send(g_all.at[origin[i], span_of(came[i][q])], g_all.at[origin[i], span_of(came[i][q])], x_ssem.at[1 + i * chips + q], x_rsem.at[1 + i * chips + q], at.partner) for q in range(chips)] for i in range(2)]
    end_across = [[send(far_ref.at[core, span_of(ends[i][q])], far_ref.at[core, span_of(ends[i][q])], x_ssem.at[1 + (2 + i) * chips + q], x_rsem.at[1 + (2 + i) * chips + q], at.partner) for q in range(2)] for i in range(2)]
    for q in range(chips):
        for i in range(2):
            direct[i][q].start()
    g_across.start()
    g_keep = pltpu.make_async_copy(g_ref, g_all.at[me], loc_sem.at[0])
    g_keep.start()
    heads_across.start()
    at2_ref[:, block(core, n_seq)] = at_ref[block(core, half), :]

    def out_tile(wo):
        sl = block(pl.program_id(0), COL_TILE)
        out_ref[:, sl] = (dx_ref[:, sl].astype(F32) + dot(h_ref[...], wo[...])).astype(BF16)

    with scope('output'):
        pltpu.emit_pipeline(out_tile, grid=(width // COL_TILE,), in_specs=[pl.BlockSpec((width, COL_TILE), lambda i: (0, i))], out_specs=[])(wo_ref)

    dy_back = [pltpu.make_async_copy(dy_ref.at[b], h_ref.at[pl.ds(b * seq, seq)], loc_sem.at[2 + b]) for b in range(n_batch)]
    for copy in dy_back:
        copy.start()

    with jax.named_scope('heads_wait'):
        heads_across.wait_recv()

    def wo_tile(dy):
        pieces = [dy[d, b] for b in range(n_batch) for d in range(n_dev)]
        dwo_ref[:, block(pl.program_id(0), COL_TILE)] = dot(at2_ref[...], jnp.concatenate(pieces, axis=0))

    with jax.named_scope('grad_wo'):
        pltpu.emit_pipeline(wo_tile, grid=(width // COL_TILE,), in_specs=[pl.BlockSpec((n_dev, n_batch, seq, COL_TILE), lambda i: (0, 0, 0, i))], out_specs=[])(dy_all)

    with scope('h_wait'):
        hcols.wait_recv()
    h_keep.wait()
    lhs_in = [pltpu.make_async_copy(ht_all.at[d, :, pl.ds(b * seq, seq)], at2_ref.at[:, pl.ds((b * n_dev + d) * seq, seq)], lhs_sem.at[b * n_dev + d]) for d in range(n_dev) for b in range(n_batch)]
    for copy in lhs_in:
        copy.start()
    with jax.named_scope('own_wait'):
        for copy in lhs_in:
            copy.wait()
        g_keep.wait()
        g_across.wait_recv()
    sums = [send(all_ref.at[me], all_ref.at[me], s_ssem.at[j], s_rsem.at[me], peer) for j, peer in enumerate(at.peers(True))]

    def weight_grads(wq_vm, wkv_vm, acc_ref, hat_ref, inv_ref, job_ref, mine_ref):
        n_slots = wq_vm.shape[0]
        chunk = wq_vm.shape[2]
        n_chunks = width // chunk
        total = n_chunks * chips

        def weights(s):
            slot = lax.rem(s, n_slots)
            chip = chip_at(lax.div(s, n_chunks))
            rows = block(lax.rem(s, n_chunks), chunk)
            return [
                pltpu.make_async_copy(wq_ref.at[block(chip, group), rows], wq_vm.at[slot], w_sem.at[slot, 0]),
                pltpu.make_async_copy(wkv_all.at[chip, rows], wkv_vm.at[slot], w_sem.at[slot, 1]),
            ]

        for s in range(n_slots):
            for copy in weights(s):
                copy.start()

        def grow(i, read):
            @pl.loop(0, n_chunks)
            def _(n):
                s = i * n_chunks + n
                slot = lax.rem(s, n_slots)
                for copy in weights(s):
                    copy.wait()
                rows = jnp.concatenate([read(b) for b in range(n_batch)], axis=0)
                part = dot_nt(rows, jnp.concatenate([wq_vm[slot, j] for j in range(group)] + [wkv_vm[slot]], axis=1))
                sl = block(n, chunk)

                @pl.when(i == 0)
                def _():
                    acc_ref[:, sl] = part

                @pl.when(i > 0)
                def _():
                    acc_ref[:, sl] += part

                @pl.when(s + n_slots < total)
                def _():
                    for copy in weights(s + n_slots):
                        copy.start()

        def mine_in(chip):
            return [pltpu.make_async_copy(g_all.at[chip * CORES + b, me], mine_ref.at[b], job_sem.at[2, b, 0]) for b in range(n_batch)]

        def grow_near(i):
            copies = mine_in(chip_at(i))
            for copy in copies:
                copy.start()
            for copy in copies:
                copy.wait()
            grow(i, lambda b: mine_ref[b])

        def job_in(chip, quarters, slot):
            return [pltpu.make_async_copy(g_all.at[chip * CORES + b, span_of(q)], job_ref.at[slot, b, n], job_sem.at[slot, b, n]) for b in range(n_batch) for n, q in enumerate(quarters)]

        def job(chip, quarters, read, add):
            part = CORES * seq
            lhs = [at2_ref[:, pl.ds(pl.multiple_of(b * n_seq + q * part, part), part)] for b in range(n_batch) for q in quarters]
            rhs = [read(b, n, q).reshape(part, cols) for b in range(n_batch) for n, q in enumerate(quarters)]
            y = dot(jnp.concatenate(lhs, axis=1), jnp.concatenate(rhs, axis=0))
            for j in range(group):
                v = y[:, j * head_dim:(j + 1) * head_dim]
                dwq_ref[chip * group + j] = dwq_ref[chip * group + j] + v if add else v
            for j, ref in enumerate((dwk_ref, dwv_ref)):
                v = y[:, (group + j) * head_dim:(group + j + 1) * head_dim]
                rows = pl.ds(chip, half, stride=chips)
                ref[rows, :] = ref[rows, :] + v if add else v

        def near_pair(quarters, add):
            for slot, step in enumerate(steps):
                for copy in job_in(at.ring(step), quarters, slot):
                    copy.start()

            @pl.loop(0, 2)
            def _(slot):
                chip = at.ring(1 - 2 * slot)
                for copy in job_in(chip, quarters, slot):
                    copy.wait()
                job(chip, quarters, lambda b, n, q: job_ref[slot, b, n], add)

        halves = [[at.ring(q) for q in half_of] for half_of in ((0, 1), (2, 3))]
        for slot in range(2):
            for copy in job_in(at.chip, [at.ring(2 * slot), at.ring(2 * slot + 1)], slot):
                copy.start()
        with jax.named_scope('own_dh'):
            grow_near(0)
        with jax.named_scope('own_job'):
            for slot in range(2):
                quarters = [at.ring(2 * slot), at.ring(2 * slot + 1)]
                for copy in job_in(at.chip, quarters, slot):
                    copy.wait()
                job(at.chip, quarters, lambda b, n, q: job_ref[slot, b, n], slot == 1)

        with jax.named_scope('d01_wait'):
            for q in range(2):
                for i in range(2):
                    direct[i][q].wait_recv()
                for i in range(2):
                    onward[i][q].start()
                    near_across[i][q].start()
        with jax.named_scope('d01_across'):
            for q in range(2):
                for i in range(2):
                    near_across[i][q].wait_recv()
        with jax.named_scope('near_dh'):
            @pl.loop(1, chips - 1)
            def _(i):
                grow_near(i)

        with jax.named_scope('near_a'):
            near_pair(halves[0], False)
        with jax.named_scope('hat'):
            @pl.loop(0, n_tok // (2 * ROWS))
            def _(step):
                for i in range(2):
                    sl = block(2 * step + i, ROWS)
                    hat, inv = layer_norm(dx_ref[sl, :].astype(F32))
                    hat_ref[sl, :] = hat
                    inv_ref[sl, :] = jnp.broadcast_to(inv, (ROWS, 128))

        with jax.named_scope('d23_wait'):
            for q in range(2, chips):
                for i in range(2):
                    direct[i][q].wait_recv()
                    near_across[i][q].start()
        with jax.named_scope('d23_across'):
            for q in range(2, chips):
                for i in range(2):
                    near_across[i][q].wait_recv()

        with jax.named_scope('near_b'):
            near_pair(halves[1], True)
        far_chip = at.ring(2)
        with jax.named_scope('far0_wait'):
            for i in range(2):
                onward[i][0].wait_recv()
                end_across[i][0].start()
        with jax.named_scope('far0_across'):
            for i in range(2):
                end_across[i][0].wait_recv()
        with jax.named_scope('far_dh'):
            grow(chips - 1, lambda b: far_ref[b, me])
        for copy in dy_back:
            copy.wait()
        part_ref[...] = jnp.zeros_like(part_ref)

        with jax.named_scope('norm_back'):
            @pl.loop(0, n_tok // (2 * ROWS))
            def _(step):
                for i in range(2):
                    sl = block(2 * step + i, ROWS)
                    hat, inv = hat_ref[sl, :], inv_ref[sl, 0:1]
                    dh = acc_ref[sl, :]
                    dg = dh * hat
                    gh = dh * gain
                    one = jnp.mean(gh, axis=-1, keepdims=True)
                    two = jnp.mean(dg * gain, axis=-1, keepdims=True)
                    dx_ref[sl, :] = (h_ref[sl, :].astype(F32) + inv * (gh - one - hat * two)).astype(BF16)
                    part_ref[0] += dg[0:8] + dg[8:16]
                    part_ref[1] += dh[0:8] + dh[8:16]

        all_ref[me, 0:1, :] = jnp.sum(part_ref[0], axis=0, keepdims=True)
        all_ref[me, 1:2, :] = jnp.sum(part_ref[1], axis=0, keepdims=True)
        read_far = lambda b, n, q: far_ref[b, span_of(q)]
        for copy in sums:
            copy.start()
        with jax.named_scope('far_a'):
            job(far_chip, [ends[0][0], ends[1][0]], read_far, False)
        with jax.named_scope('far1_wait'):
            for i in range(2):
                onward[i][1].wait_recv()
                end_across[i][1].start()
        with jax.named_scope('far1_across'):
            for i in range(2):
                end_across[i][1].wait_recv()
        with jax.named_scope('far_b'):
            job(far_chip, [ends[0][1], ends[1][1]], read_far, True)

    pl.run_scoped(
        weight_grads,
        pltpu.VMEM((W_SLOTS, group, W_ROWS, head_dim), BF16), pltpu.VMEM((W_SLOTS, W_ROWS, 2 * head_dim), BF16), pltpu.VMEM((n_tok, width), F32),
        pltpu.VMEM((n_tok, width), F32), pltpu.VMEM((n_tok, 128), F32), pltpu.VMEM((2, n_batch, 2, CORES, seq, cols), BF16), pltpu.VMEM((n_batch, seq, cols), BF16),
    )

    with jax.named_scope('sums'):
        for j in range(1, n_dev):
            source = lax.rem(me + j, n_dev)
            send(all_ref.at[me], all_ref.at[source], s_ssem.at[0], s_rsem.at[source], at.partner).wait_recv()
        total = all_ref[0]
        for d in range(1, n_dev):
            total = total + all_ref[d]
        dgain_ref[...] = total[0:1].reshape(width)
        dbias_ref[...] = total[1:2].reshape(width)
    done = dys.sent() + [heads_across] + spots
    done += direct[0] + direct[1] + onward[0] + onward[1] + [g_across] + near_across[0] + near_across[1] + end_across[0] + end_across[1] + sums
    with jax.named_scope('done'):
        for copy in done:
            copy.wait_send()
        hcols.wait_send()


def whole_block(n_dev, x, gain, bias, positions, freq, dy, wq, wk, wv, wo):
    n_batch, seq, width = dy.shape
    n_tok = n_batch * seq
    head_dim = wq.shape[2]
    chips = n_dev // CORES
    group = wq.shape[0] // chips
    cols = (group + 2) * head_dim
    n_rows = group * head_dim
    half = n_rows // CORES
    n_seq = n_dev * seq
    quarter = head_dim // 4
    dma = pltpu.SemaphoreType.DMA
    vm = pltpu.VMEM
    shapes = [((n_tok, width), BF16)] * 2 + [((chips * group, half, head_dim), F32)] + [((chips * half, head_dim), F32)] * 2 + [((half, width), F32), ((width,), F32), ((width,), F32)]
    held = [((n_dev, n_batch, seq, width), BF16), ((n_dev, half, n_tok), BF16), ((n_dev, n_dev, seq, cols), BF16), ((chips, width, 2 * head_dim), BF16)]
    return pl.pallas_call(
        functools.partial(block_body, n_dev, group),
        out_shape=tuple(pltpu.VMEM(*t) for t in shapes) + tuple(sds(*t) for t in held),
        in_specs=[VM] * 4 + [HBM] * 6,
        out_specs=(VM,) * len(shapes) + (HBM,) * len(held),
        scratch_shapes=[
            vm((n_tok, width), BF16), vm((width, n_tok), BF16), vm((n_dev, seq, cols), BF16), vm((n_dev, seq, n_rows), BF16),
            vm((n_rows, n_seq), BF16), vm((half, n_batch * n_seq), BF16), vm((n_seq, n_rows), BF16),
            vm((head_dim, n_seq), BF16), vm((head_dim, n_seq), BF16), vm((n_seq, head_dim), F32), vm((n_seq, head_dim), F32),
            vm((quarter, n_seq), F32), vm((quarter, n_seq), F32), vm((3, n_tok, head_dim), F32), vm((n_dev, n_batch, seq), jnp.int32),
            vm((2, seq, n_rows), BF16), vm((2, half, n_tok), BF16),
            vm((n_batch, n_dev, seq, cols), BF16), vm((2, 8, width), F32), vm((n_dev, 2, width), F32),
            dma((13,)), dma((13,)), dma((13,)), dma((13,)), dma((9,)), dma((n_dev + 2,)), dma((9,)), dma((n_dev + 2,)), dma((n_dev,)), dma((n_dev,)), dma((2,)),
            dma((2, chips)), dma((2, chips)), dma((2, 2)), dma((2, 2)), dma((1 + 4 * chips,)), dma((1 + 4 * chips,)), dma((n_dev,)), dma((n_dev,)),
            dma((1 + n_dev,)), dma((3,)), dma((n_batch * n_dev,)), dma((W_SLOTS, 2)), dma((3, n_batch, 2)),
        ],
        compiler_params=pltpu.CompilerParams(collective_id=0, has_side_effects=True, vmem_limit_bytes=VMEM_LIMIT),
        cost_estimate=pl.CostEstimate(flops=10 ** 11, bytes_accessed=10 ** 8, transcendentals=0),
        name='block',
    )(gain, bias, positions, freq, x.reshape(n_tok, width), dy, wq, wk, wv, wo)[:len(shapes)]


def settle_body(n, *refs):
    sems = refs[2 * n]
    copies = []
    for i in range(n):
        src, dst = refs[i], refs[n + i]
        pieces = SETTLE if len(src.shape) > 1 else 1
        size = src.shape[0] // pieces
        for p in range(pieces):
            copies.append(pltpu.make_async_copy(src.at[pl.ds(p * size, size)], dst.at[pl.ds(p * size, size)], sems.at[i, p]))
    for copy in copies:
        copy.start()
    for copy in copies:
        copy.wait()


def settle(arrays):
    n = len(arrays)
    return pl.pallas_call(
        functools.partial(settle_body, n),
        out_shape=tuple(sds(t.shape, t.dtype) for t in arrays),
        in_specs=[ANY] * n,
        out_specs=(HBM,) * n,
        scratch_shapes=[pltpu.SemaphoreType.DMA((n, SETTLE))],
        compiler_params=pltpu.CompilerParams(vmem_limit_bytes=1024 * 1024),
        name='settle',
    )(*arrays)


def solution(mesh):
    n_dev = mesh.shape['cp']

    def device_step(x_act, d_out, positions, ln_gain, ln_bias, w_query, w_key, w_value, w_out):
        n_batch, seq, width = x_act.shape
        q_heads, (kv_heads, head_dim) = w_query.shape[1], w_key.shape[1:]
        group = q_heads // kv_heads
        quarter = head_dim // 4
        assert n_batch == CORES and n_dev // CORES == kv_heads == 4 and q_heads * head_dim == width

        freq = np.exp(np.arange(quarter) * (-2.0 * math.log(ROPE_BASE) / (head_dim // 2))).astype(np.float32).reshape(quarter, 1)
        by_head = lambda t: jnp.transpose(t, (1, 0, 2))
        by_row = lambda t: t.reshape(width * kv_heads, head_dim)
        wq = by_head(w_query)

        results = whole_block(n_dev, x_act, ln_gain, ln_bias, positions, jnp.asarray(freq), d_out, wq, by_row(w_key), by_row(w_value), w_out)
        out, dx, dwq, dwk, dwv, dwo, dgain, dbias = settle(results)
        kv_rows = lambda t: t.reshape(width // n_dev, kv_heads, head_dim)
        return (out.reshape(x_act.shape), dx.reshape(x_act.shape), by_head(dwq), kv_rows(dwk), kv_rows(dwv), dwo, dgain, dbias)

    return jax.shard_map(device_step, mesh=mesh, in_specs=(P('dp', 'cp', None), P('dp', 'cp', None), P('dp', 'cp'), P(None), P(None), P(None, None, None), P(None, None, None), P(None, None, None), P(None, None)), out_specs=(P('dp', 'cp', None), P('dp', 'cp', None), P(('dp', 'cp'), None, None), P(('dp', 'cp'), None, None), P(('dp', 'cp'), None, None), P(('dp', 'cp'), None), P('dp'), P('dp')), check_vma=False)
```

```python
import functools
import math
import jax
import jax.numpy as jnp
import numpy as np
from jax import lax
from jax.experimental import pallas as pl
from jax.experimental.pallas import tpu as pltpu
from jax.sharding import PartitionSpec as P

EPS = 1e-5
ROPE_BASE = 10000.0
BF16 = jnp.bfloat16
F32 = jnp.float32
VMEM_LIMIT = 46 * 1024 * 1024
NT = (((1,), (1,)), ((), ()))
ANY = pl.BlockSpec(memory_space=pl.ANY)
VM = pl.BlockSpec(memory_space=pltpu.VMEM)
HBM = pl.BlockSpec(memory_space=pltpu.HBM)
CORES = 2
COL_TILE = 512
ROWS = 16
W_SLOTS = 4
W_ROWS = 512
SETTLE = 4


def dot(a, b):
    return jnp.dot(a, b, preferred_element_type=F32)


def dot_nt(a, b):
    return lax.dot_general(a, b, NT, preferred_element_type=F32)


def sds(shape, dtype):
    return jax.ShapeDtypeStruct(shape, dtype)


def block(i, size):
    return pl.ds(pl.multiple_of(i * size, size), size)


class Place:
    def __init__(self, n_dev):
        self.n_dev = n_dev
        self.chips = n_dev // CORES
        self.me = lax.axis_index('cp')
        self.chip = self.me // CORES
        self.core = self.me % CORES
        self.partner = self.chip * CORES + 1 - self.core

    def ring(self, step):
        return lax.rem(self.chip + self.chips + step, self.chips)

    def dev(self, step, core):
        return self.ring(step) * CORES + core

    def peers(self, far):
        near = [self.partner] + [self.dev(s, c) for s in (1, -1) for c in range(CORES)]
        return near + ([self.dev(2, c) for c in range(CORES)] if far else [])


def send(src, dst, ssem, rsem, to):
    return pltpu.make_async_remote_copy(src_ref=src, dst_ref=dst, send_sem=ssem, recv_sem=rsem, device_id={'cp': to}, device_id_type=pl.DeviceIdType.MESH)


def meet(peers):
    barrier = pltpu.get_barrier_semaphore()
    for peer in peers:
        pl.semaphore_signal(barrier, inc=1, device_id={'cp': peer}, device_id_type=pl.DeviceIdType.MESH)
    pl.semaphore_wait(barrier, len(peers))


class Ring:
    def __init__(self, n, slots, copies):
        self.n, self.slots, self.copies = n, slots, copies

    def prime(self):
        for s in range(self.slots):
            for copy in self.copies(s, s):
                copy.start()

    def run(self, use):
        @pl.loop(0, self.n)
        def _(s):
            slot = lax.rem(s, self.slots)
            for copy in self.copies(s, slot):
                copy.wait()
            use(s, slot)

            @pl.when(s + self.slots < self.n)
            def _():
                for copy in self.copies(s + self.slots, slot):
                    copy.start()


class Gather:
    def __init__(self, at, own, piece, both, ssem, rsem):
        steps = (1, -1)
        origin = [at.dev(-1, at.core), at.dev(1, at.core)]
        far = at.dev(2, at.core)
        link = lambda i, src, dst, to: send(src, dst, ssem.at[i], rsem.at[i], to)
        self.first = [link(b, own(b), piece(at.me, b), at.dev(steps[b], at.core)) for b in range(2)]
        self.second = [link(2 + b, own(1 - b), piece(at.me, 1 - b), at.dev(steps[b], at.core)) for b in range(2)]
        self.again = [link(4 + b, piece(origin[b], b), piece(origin[b], b), at.dev(steps[b], at.core)) for b in range(2)]
        self.own_across = link(6, both(None), both(at.me), at.partner)
        self.first_across = [link(7 + b, piece(origin[b], b), piece(origin[b], b), at.partner) for b in range(2)]
        self.second_across = [link(9 + b, piece(origin[b], 1 - b), piece(origin[b], 1 - b), at.partner) for b in range(2)]
        self.far_across = [link(11 + b, piece(far, b), piece(far, b), at.partner) for b in range(2)]

    def start_first(self):
        for copy in self.first + [self.own_across]:
            copy.start()

    def start_second(self):
        for copy in self.second:
            copy.start()

    def pass_on(self):
        for copy, again, across in zip(self.first, self.again, self.first_across):
            copy.wait_recv()
            again.start()
            across.start()

    def share_second(self):
        for copy, across in zip(self.second, self.second_across):
            copy.wait_recv()
            across.start()

    def share_far(self):
        for copy, across in zip(self.again, self.far_across):
            copy.wait_recv()
            across.start()

    def wait_near(self):
        for copy in self.first_across + self.second_across:
            copy.wait_recv()

    def wait_far(self):
        for copy in self.far_across:
            copy.wait_recv()

    def sent(self):
        return self.first + self.second + self.again + [self.own_across] + self.first_across + self.second_across + self.far_across


class Exchange:
    def __init__(self, at, src, dst, relay, ssem, rsem):
        self.at, self.src, self.dst, self.relay, self.ssem, self.rsem = at, src, dst, relay, ssem, rsem
        near = [(0, 1 - at.core)] + [(s, c) for s in (1, -1) for c in range(CORES)]
        n = at.n_dev
        self.near = [send(src(at.dev(s, c)), dst(at.me), ssem.at[i], rsem.at[at.me], at.dev(s, c)) for i, (s, c) in enumerate(near)]
        self.far = [send(src(at.dev(2, i)), relay.at[i], ssem.at[5 + i], rsem.at[n + i], at.dev(step, at.core)) for i, step in enumerate((1, -1))]
        self.on = [send(relay.at[i], dst(at.dev(-step, at.core)), ssem.at[7 + i], rsem.at[at.dev(-step, at.core)], at.dev(step, i)) for i, step in enumerate((1, -1))]

    def start(self):
        for copy in self.far + self.near:
            copy.start()

    def pass_on(self):
        for far, on in zip(self.far, self.on):
            far.wait_recv()
            on.start()

    def wait_recv(self):
        at = self.at
        for j in range(1, at.n_dev):
            origin = lax.rem(at.me + j, at.n_dev)
            send(self.src(at.me), self.dst(origin), self.ssem.at[0], self.rsem.at[origin], at.partner).wait_recv()

    def wait_send(self):
        for copy in self.far + self.near + self.on:
            copy.wait_send()


def layer_norm(x):
    cen = x - jnp.mean(x, axis=-1, keepdims=True)
    inv = lax.rsqrt(jnp.mean(cen * cen, axis=-1, keepdims=True) + EPS)
    return cen * inv, inv


def block_body(n_dev, group, gain_ref, bias_ref, pos_ref, freq_ref, x_hbm, dy_ref, wq_ref, wk_ref, wv_ref, wo_ref,
               out_ref, dx_ref, dwq_ref, dwk_ref, dwv_ref, dwo_ref, dgain_ref, dbias_ref, dy_all, ht_all, g_all, wkv_all,
               h_ref, ht_ref, g_ref, q_ref, at_ref, at2_ref, da_ref, kt_ref, vt_ref, dk_ref, dv_ref,
               cost_ref, sint_ref, tab_ref, spot_ref, relay_q, relay_h, far_ref, part_ref, all_ref,
               dy_ssem, dy_rsem, kv_ssem, kv_rsem, q_ssem, q_rsem, h_ssem, h_rsem, p_ssem, p_rsem, t_sem,
               g_ssem, g_rsem, r_ssem, r_rsem, x_ssem, x_rsem, s_ssem, s_rsem, loc_sem, mix_sem, lhs_sem, w_sem, job_sem):
    at = Place(n_dev)
    n_batch, seq, width = dy_ref.shape
    n_tok = n_batch * seq
    head_dim = wq_ref.shape[2]
    cols = (group + 2) * head_dim
    n_rows = group * head_dim
    half = n_rows // CORES
    n_seq = n_dev * seq
    quarter = head_dim // 4
    scale = head_dim ** -0.5
    chips = at.chips
    tile = CORES * seq
    core, me = at.core, at.me
    steps = (1, -1)
    origin = [at.dev(-1, core), at.dev(1, core)]
    far_dev = at.dev(2, core)
    scope = jax.named_scope

    with scope('meet'):
        meet(at.peers(True))

    kv_cols = 2 * head_dim * chips
    kv_piece = lambda d, b: far_ref.at[b, d, :, pl.ds(0, kv_cols)]
    kv_both = lambda d: far_ref.at[:, me if d is None else d, :, pl.ds(0, kv_cols)]
    dys = Gather(at, lambda b: dy_ref.at[b], lambda d, b: dy_all.at[d, b], lambda d: dy_ref if d is None else dy_all.at[d], dy_ssem, dy_rsem)
    kvs = Gather(at, lambda b: kv_piece(me, b), kv_piece, kv_both, kv_ssem, kv_rsem)
    q_part = pl.ds(0, n_rows)
    queries = Exchange(at, lambda d: g_ref.at[d, :, q_part], lambda d: q_ref.at[d], relay_q, q_ssem, q_rsem)
    hcols = Exchange(at, lambda d: ht_ref.at[block(d, half)], lambda d: ht_all.at[d], relay_h, h_ssem, h_rsem)
    heads_across = send(at_ref.at[block(1 - core, half)], at2_ref.at[:, block(core, n_seq)], t_sem.at[0], t_sem.at[1], at.partner)
    spots = [send(pos_ref, spot_ref.at[me], p_ssem.at[j], p_rsem.at[me], peer) for j, peer in enumerate(at.peers(True))]

    dys.start_first()
    x_in = pltpu.make_async_copy(x_hbm, dx_ref, loc_sem.at[1])
    x_in.start()
    for copy in spots:
        copy.start()
    spot_ref[me] = pos_ref[...]

    freq = freq_ref[...]
    for b in range(n_batch):
        angle = freq * pos_ref[b:b + 1, :].astype(F32)
        cos, sin, none = jnp.cos(angle), jnp.sin(angle), jnp.zeros((quarter, seq), F32)
        rest = jnp.zeros((head_dim - 2 * quarter, seq), F32)
        for i, rows in enumerate(([cos, cos, rest + 1.0], [-sin, none, rest], [none, sin, rest])):
            tab_ref[i, b * seq:(b + 1) * seq, :] = jnp.concatenate(rows, axis=0).T

    gain = (1.0 + gain_ref[...]).reshape(1, width)
    bias = bias_ref[...].reshape(1, width)

    def project_all(wkv_ref, raw_ref, wq_vm, raw_sem, wq_sem, stage_sem):
        pieces = [(b, i) for b in range(n_batch) for i in range(width // n_rows)]
        there = lambda n: da_ref.at[pl.ds(n * seq, seq)]
        dy_in = [pltpu.make_async_copy(dy_ref.at[b, :, pl.ds(i * n_rows, n_rows)], there(n), stage_sem.at[n]) for n, (b, i) in enumerate(pieces)]
        dy_keep = [pltpu.make_async_copy(there(n), dy_all.at[me, b, :, pl.ds(i * n_rows, n_rows)], stage_sem.at[n]) for n, (b, i) in enumerate(pieces)]
        span = 64 * chips
        batch = raw_ref.shape[2] // span
        row = lax.broadcasted_iota(jnp.int32, (span, span), 0)
        col = lax.broadcasted_iota(jnp.int32, (span, span), 1)
        pick = jnp.where(col == lax.rem(row, 64) * chips + lax.div(row, 64), 1.0, 0.0).astype(BF16)

        def raw_in(s, slot):
            return [pltpu.make_async_copy(w.at[block(s, span * batch)], raw_ref.at[slot, i], raw_sem.at[slot, i]) for i, w in enumerate((wk_ref, wv_ref))]

        def wq_in(s, slot):
            return [pltpu.make_async_copy(wq_ref.at[block(s, 2)], wq_vm.at[slot], wq_sem.at[slot])]

        def part_heads(s, slot):
            for i in range(batch):
                sl = slice(i * span, (i + 1) * span)
                rows = dot(pick, jnp.concatenate([raw_ref[slot, 0, sl, :], raw_ref[slot, 1, sl, :]], axis=1)).astype(BF16)
                for n in range(chips):
                    wkv_ref[n, block(s * batch + i, 64), :] = rows[n * 64:(n + 1) * 64]

        def turned(v):
            return v * tab_ref[0] + pltpu.roll(v, head_dim - quarter, 1) * tab_ref[1] + pltpu.roll(v, quarter, 1) * tab_ref[2]

        def project(s, slot):
            y = dot(h_ref[...], jnp.concatenate([wq_vm[slot, 0], wq_vm[slot, 1]], axis=1))
            for i in range(2):
                head = s * 2 + i
                v = turned(y[:, i * head_dim:(i + 1) * head_dim]).astype(BF16)
                for b in range(n_batch):
                    g_ref[lax.div(head, group) * n_batch + b, :, block(lax.rem(head, group), head_dim)] = v[b * seq:(b + 1) * seq]

        kv_ring = Ring(width // (64 * batch), raw_ref.shape[0], raw_in)
        q_ring = Ring(chips * group // 2, wq_vm.shape[0], wq_in)
        kv_ring.prime()
        q_ring.prime()
        for copy in dy_in:
            copy.start()
        x_in.wait()
        with scope('norm'):
            @pl.loop(0, n_tok // (2 * ROWS))
            def _(step):
                for i in range(2):
                    sl = block(2 * step + i, ROWS)
                    hat, _ = layer_norm(dx_ref[sl, :].astype(F32))
                    h_ref[sl, :] = (hat * gain + bias).astype(BF16)

        with scope('heads_kv'):
            kv_ring.run(part_heads)
        keep = pltpu.make_async_copy(wkv_ref, wkv_all, mix_sem.at[2])
        keep.start()
        for come, go in zip(dy_in, dy_keep):
            come.wait()
            go.start()
        with scope('project_kv'):
            @pl.loop(0, chips)
            def _(n):
                y = dot(h_ref[...], wkv_ref[n])
                v = jnp.concatenate([turned(y[:, :head_dim]), y[:, head_dim:]], axis=1).astype(BF16)
                for b in range(n_batch):
                    far_ref[b, me, :, block(n, 2 * head_dim)] = v[b * seq:(b + 1) * seq]

        kvs.start_first()
        kvs.start_second()
        with scope('project_q'):
            q_ring.run(project)
        keep.wait()
        for copy in dy_keep:
            copy.wait()

    pl.run_scoped(
        project_all,
        pltpu.VMEM((chips, width, 2 * head_dim), BF16),
        pltpu.VMEM((3, 2, 4 * 64 * chips, head_dim), BF16), pltpu.VMEM((4, 2, width, head_dim), BF16),
        pltpu.SemaphoreType.DMA((3, 2)), pltpu.SemaphoreType.DMA((4,)), pltpu.SemaphoreType.DMA((n_batch * width // n_rows,)),
    )

    with scope('kv_pass'):
        kvs.pass_on()
    queries.start()
    q_ref[me] = g_ref[me, :, q_part]
    with scope('turn_h'):
        @pl.loop(0, width // 128)
        def _(step):
            sl = block(step, 128)
            ht_ref[sl, :] = h_ref[:, sl].T

    with scope('kv_wait'):
        kvs.share_second()
        kvs.share_far()
        kvs.own_across.wait_recv()
        kvs.wait_near()
        kvs.wait_far()

    def chip_at(i):
        return at.ring(jnp.where(i == 0, 0, jnp.where(i == 1, 1, jnp.where(i == 2, 3, 2))))

    def soft(s, seen):
        s = s * scale
        clear = s.shape[0] - seen.shape[0]
        tail = jnp.where(seen, s[clear:], -1e30)
        s = tail if clear == 0 else jnp.concatenate([s[:clear], tail], axis=0)
        e = jnp.exp(s - jnp.max(s, axis=0, keepdims=True))
        return e * (1.0 / jnp.sum(e, axis=0, keepdims=True))

    def attend(limit, clear):
        @pl.loop(0, n_batch * chips)
        def _(i):
            @pl.when(i == 1)
            def _():
                with scope('q_pass'):
                    queries.pass_on()
                dys.start_second()
                dys.pass_on()
                hcols.start()

            b, n = lax.rem(i, n_batch), lax.div(i, n_batch)
            k = far_ref[b, 0:limit // seq, :, block(2 * n, head_dim)].reshape(limit, head_dim)
            vt = far_ref[b, 0:limit // seq, :, block(2 * n + 1, head_dim)].reshape(limit, head_dim).T
            q = jnp.concatenate([g_ref[n * n_batch + b, :, block(j, head_dim)] for j in range(group)], axis=0)
            row = lax.broadcasted_iota(jnp.int32, (limit - clear, n_rows), 0)
            col = lax.broadcasted_iota(jnp.int32, (limit - clear, n_rows), 1)
            p = soft(dot_nt(k, q), row <= lax.rem(col, seq) + (me * seq - clear))
            mixed = dot(vt, p.astype(BF16)).astype(BF16)
            for j in range(group):
                h_ref[block(b, seq), block(n * group + j, head_dim)] = mixed[:, j * seq:(j + 1) * seq].T

    with scope('attend'):
        @pl.when(at.chip == chips - 1)
        def _():
            attend(chips * tile, (chips - 1) * tile)

        @pl.when(at.chip < chips - 1)
        def _():
            attend((chips - 1) * tile, 0)

    h_keep = pltpu.make_async_copy(ht_ref.at[block(me, half)], ht_all.at[me], loc_sem.at[1])
    h_keep.start()

    k_all = lambda n: far_ref[core, 0:n, :, block(2 * at.chip, head_dim)].reshape(n * seq, head_dim)
    v_all = lambda n: far_ref[core, 0:n, :, block(2 * at.chip + 1, head_dim)].reshape(n * seq, head_dim)

    def rotate_back(t, cos, sin):
        u, w = t[:quarter], t[quarter:2 * quarter]
        return jnp.concatenate([u * cos + w * sin, w * cos - u * sin, t[2 * quarter:]], axis=0)

    def by_dev(t):
        return t.astype(BF16).reshape(t.shape[0] // seq, seq, head_dim)

    def attend_back(t):
        limit = (t + 1) * tile
        sl = slice(t * tile, limit)
        devs = slice(t * CORES, (t + 1) * CORES)

        def heads(first, count):
            each = range(count)
            q = jnp.concatenate([q_ref[devs, :, block(first + j, head_dim)].reshape(tile, head_dim) for j in each], axis=0)
            da = jnp.concatenate([da_ref[sl, block(first + j, head_dim)] for j in each], axis=0)
            k, v = k_all(limit // seq), v_all(limit // seq)
            row = lax.broadcasted_iota(jnp.int32, (tile, count * tile), 0)
            col = lax.broadcasted_iota(jnp.int32, (tile, count * tile), 1)
            p = soft(dot_nt(k, q), row <= lax.rem(col, tile))
            p_low = p.astype(BF16)
            mixed = dot(vt_ref[:, :limit], p_low).astype(BF16)
            dp = dot_nt(v, da)
            row_dot = jnp.sum(p * dp, axis=0, keepdims=True)
            ds = (p * (dp - row_dot) * scale).astype(BF16)
            dv_ref[:limit, :] += dot(p_low, da)
            dk_ref[:limit, :] += dot(ds, q)
            back = dot(kt_ref[:, :limit], ds)
            for j in each:
                part = slice(j * tile, (j + 1) * tile)
                at_ref[block(first + j, head_dim), sl] = mixed[:, part]
                g_ref[devs, :, block(first + j, head_dim)] = by_dev(rotate_back(back[:, part], cost_ref[:, sl], sint_ref[:, sl]).T)

        @pl.loop(0, group // 2)
        def _(j):
            heads(2 * j, 2)

        heads(group - 1, 1)

    def middle(wo_vm, dyk):
        wo_in = pltpu.make_async_copy(wo_ref.at[block(at.chip, n_rows)], wo_vm, mix_sem.at[2])
        wo_in.start()
        for j in range(1, n_dev):
            source = lax.rem(me + j, n_dev)
            send(pos_ref, spot_ref.at[source], p_ssem.at[0], p_rsem.at[source], at.partner).wait_recv()
        for d in range(n_dev):
            angle = freq * spot_ref[d, pl.ds(core, 1), :].astype(F32)
            cost_ref[:, d * seq:(d + 1) * seq] = jnp.cos(angle)
            sint_ref[:, d * seq:(d + 1) * seq] = jnp.sin(angle)
        with scope('q_wait'):
            queries.wait_recv()
            queries.wait_send()
            for copy in kvs.sent():
                copy.wait_send()
        kt_ref[...] = k_all(n_dev).T
        vt_ref[...] = v_all(n_dev).T
        dk_ref[...] = jnp.zeros_like(dk_ref)
        dv_ref[...] = jnp.zeros_like(dv_ref)
        dys.own_across.wait_recv()

        def fetch(i, slot):
            return pltpu.make_async_copy(dy_all.at[block(chip_at(i), CORES), core], dyk.at[slot], mix_sem.at[slot])

        with scope('wo_wait'):
            fetch(0, 0).start()
            wo_in.wait()

        @pl.loop(0, chips)
        def _(i):
            slot = lax.rem(i, 2)

            @pl.when(i == 1)
            def _():
                with scope('dy_wait'):
                    dys.share_second()
                    dys.wait_near()
                fetch(i, slot).start()

            @pl.when(i == chips - 1)
            def _():
                with scope('dy_far'):
                    dys.share_far()
                with scope('dy_far2'):
                    dys.wait_far()
                fetch(i, slot).start()
                with scope('h_pass'):
                    hcols.pass_on()

            fetch(i, slot).wait()

            @pl.when((i > 0) & (i < chips - 2))
            def _():
                fetch(i + 1, 1 - slot).start()

            chip = chip_at(i)
            with scope('da'):
                da_ref[block(chip, tile), :] = dot_nt(dyk[slot].reshape(tile, width), wo_vm[...]).astype(BF16)
            with scope('attend_back'):
                for t in range(chips):
                    @pl.when(chip == t)
                    def _(t=t):
                        attend_back(t)

    pl.run_scoped(middle, pltpu.VMEM((n_rows, width), BF16), pltpu.VMEM((2, CORES, seq, width), BF16))
    g_ref[:, :, n_rows:n_rows + head_dim] = by_dev(rotate_back(dk_ref[...].T, cost_ref[...], sint_ref[...]).T)
    g_ref[:, :, n_rows + head_dim:] = by_dev(dv_ref[...])

    def span_of(q):
        return block(q, CORES)

    turn = [[at.ring(q) for q in (2, 1, 3, 0)], [at.ring(q) for q in (3, 0, 1, 2)]]
    direct = [[send(g_ref.at[span_of(turn[i][q])], g_all.at[me, span_of(turn[i][q])], g_ssem.at[i, q], g_rsem.at[i, q], at.dev(steps[i], core)) for q in range(chips)] for i in range(2)]
    came = [[at.ring(q) for q in (1, 0, 2, 3)], [at.ring(q) for q in (0, 1, 2, 3)]]
    onward = [[send(g_all.at[origin[i], span_of(came[i][q])], far_ref.at[core, span_of(came[i][q])], r_ssem.at[i, q], r_rsem.at[i, q], at.dev(steps[i], core)) for q in range(2)] for i in range(2)]
    ends = [[at.ring(q) for q in (0, 3)], [at.ring(q) for q in (1, 2)]]
    g_across = send(g_ref, g_all.at[me], x_ssem.at[0], x_rsem.at[0], at.partner)
    near_across = [[send(g_all.at[origin[i], span_of(came[i][q])], g_all.at[origin[i], span_of(came[i][q])], x_ssem.at[1 + i * chips + q], x_rsem.at[1 + i * chips + q], at.partner) for q in range(chips)] for i in range(2)]
    end_across = [[send(far_ref.at[core, span_of(ends[i][q])], far_ref.at[core, span_of(ends[i][q])], x_ssem.at[1 + (2 + i) * chips + q], x_rsem.at[1 + (2 + i) * chips + q], at.partner) for q in range(2)] for i in range(2)]
    for q in range(chips):
        for i in range(2):
            direct[i][q].start()
    g_across.start()
    g_keep = pltpu.make_async_copy(g_ref, g_all.at[me], loc_sem.at[0])
    g_keep.start()
    heads_across.start()
    at2_ref[:, block(core, n_seq)] = at_ref[block(core, half), :]

    def out_tile(wo):
        sl = block(pl.program_id(0), COL_TILE)
        out_ref[:, sl] = (dx_ref[:, sl].astype(F32) + dot(h_ref[...], wo[...])).astype(BF16)

    with scope('output'):
        pltpu.emit_pipeline(out_tile, grid=(width // COL_TILE,), in_specs=[pl.BlockSpec((width, COL_TILE), lambda i: (0, i))], out_specs=[])(wo_ref)

    dy_back = [pltpu.make_async_copy(dy_ref.at[b], h_ref.at[pl.ds(b * seq, seq)], loc_sem.at[2 + b]) for b in range(n_batch)]
    for copy in dy_back:
        copy.start()

    with jax.named_scope('heads_wait'):
        heads_across.wait_recv()

    def wo_tile(dy):
        pieces = [dy[d, b] for b in range(n_batch) for d in range(n_dev)]
        dwo_ref[:, block(pl.program_id(0), COL_TILE)] = dot(at2_ref[...], jnp.concatenate(pieces, axis=0))

    with jax.named_scope('grad_wo'):
        pltpu.emit_pipeline(wo_tile, grid=(width // COL_TILE,), in_specs=[pl.BlockSpec((n_dev, n_batch, seq, COL_TILE), lambda i: (0, 0, 0, i))], out_specs=[])(dy_all)

    with scope('h_wait'):
        hcols.wait_recv()
    h_keep.wait()
    lhs_in = [pltpu.make_async_copy(ht_all.at[d, :, pl.ds(b * seq, seq)], at2_ref.at[:, pl.ds((b * n_dev + d) * seq, seq)], lhs_sem.at[b * n_dev + d]) for d in range(n_dev) for b in range(n_batch)]
    for copy in lhs_in:
        copy.start()
    with jax.named_scope('own_wait'):
        for copy in lhs_in:
            copy.wait()
        g_keep.wait()
        g_across.wait_recv()
    sums = [send(all_ref.at[me], all_ref.at[me], s_ssem.at[j], s_rsem.at[me], peer) for j, peer in enumerate(at.peers(True))]

    def weight_grads(wq_vm, wkv_vm, acc_ref, hat_ref, inv_ref, job_ref, mine_ref):
        n_slots = wq_vm.shape[0]
        chunk = wq_vm.shape[2]
        n_chunks = width // chunk
        total = n_chunks * chips

        def weights(s):
            slot = lax.rem(s, n_slots)
            chip = chip_at(lax.div(s, n_chunks))
            rows = block(lax.rem(s, n_chunks), chunk)
            return [
                pltpu.make_async_copy(wq_ref.at[block(chip, group), rows], wq_vm.at[slot], w_sem.at[slot, 0]),
                pltpu.make_async_copy(wkv_all.at[chip, rows], wkv_vm.at[slot], w_sem.at[slot, 1]),
            ]

        for s in range(n_slots):
            for copy in weights(s):
                copy.start()

        def grow(i, read):
            @pl.loop(0, n_chunks)
            def _(n):
                s = i * n_chunks + n
                slot = lax.rem(s, n_slots)
                for copy in weights(s):
                    copy.wait()
                rows = jnp.concatenate([read(b) for b in range(n_batch)], axis=0)
                part = dot_nt(rows, jnp.concatenate([wq_vm[slot, j] for j in range(group)] + [wkv_vm[slot]], axis=1))
                sl = block(n, chunk)

                @pl.when(i == 0)
                def _():
                    acc_ref[:, sl] = part

                @pl.when(i > 0)
                def _():
                    acc_ref[:, sl] += part

                @pl.when(s + n_slots < total)
                def _():
                    for copy in weights(s + n_slots):
                        copy.start()

        def mine_in(chip):
            return [pltpu.make_async_copy(g_all.at[chip * CORES + b, me], mine_ref.at[b], job_sem.at[2, b, 0]) for b in range(n_batch)]

        def grow_near(i):
            copies = mine_in(chip_at(i))
            for copy in copies:
                copy.start()
            for copy in copies:
                copy.wait()
            grow(i, lambda b: mine_ref[b])

        def job_in(chip, quarters, slot):
            return [pltpu.make_async_copy(g_all.at[chip * CORES + b, span_of(q)], job_ref.at[slot, b, n], job_sem.at[slot, b, n]) for b in range(n_batch) for n, q in enumerate(quarters)]

        def job(chip, quarters, read, add):
            part = CORES * seq
            lhs = [at2_ref[:, pl.ds(pl.multiple_of(b * n_seq + q * part, part), part)] for b in range(n_batch) for q in quarters]
            rhs = [read(b, n, q).reshape(part, cols) for b in range(n_batch) for n, q in enumerate(quarters)]
            y = dot(jnp.concatenate(lhs, axis=1), jnp.concatenate(rhs, axis=0))
            for j in range(group):
                v = y[:, j * head_dim:(j + 1) * head_dim]
                dwq_ref[chip * group + j] = dwq_ref[chip * group + j] + v if add else v
            for j, ref in enumerate((dwk_ref, dwv_ref)):
                v = y[:, (group + j) * head_dim:(group + j + 1) * head_dim]
                rows = pl.ds(chip, half, stride=chips)
                ref[rows, :] = ref[rows, :] + v if add else v

        def near_pair(quarters, add):
            for slot, step in enumerate(steps):
                for copy in job_in(at.ring(step), quarters, slot):
                    copy.start()

            @pl.loop(0, 2)
            def _(slot):
                chip = at.ring(1 - 2 * slot)
                for copy in job_in(chip, quarters, slot):
                    copy.wait()
                job(chip, quarters, lambda b, n, q: job_ref[slot, b, n], add)

        halves = [[at.ring(q) for q in half_of] for half_of in ((0, 1), (2, 3))]
        for slot in range(2):
            for copy in job_in(at.chip, [at.ring(2 * slot), at.ring(2 * slot + 1)], slot):
                copy.start()
        with jax.named_scope('own_job'):
            for slot in range(2):
                quarters = [at.ring(2 * slot), at.ring(2 * slot + 1)]
                for copy in job_in(at.chip, quarters, slot):
                    copy.wait()
                job(at.chip, quarters, lambda b, n, q: job_ref[slot, b, n], slot == 1)

        with jax.named_scope('own_dh'):
            grow_near(0)

        with jax.named_scope('d01_wait'):
            for q in range(2):
                for i in range(2):
                    direct[i][q].wait_recv()
                for i in range(2):
                    onward[i][q].start()
                    near_across[i][q].start()
        with jax.named_scope('d01_across'):
            for q in range(2):
                for i in range(2):
                    near_across[i][q].wait_recv()
        with jax.named_scope('near_dh'):
            @pl.loop(1, chips - 1)
            def _(i):
                grow_near(i)

        with jax.named_scope('near_a'):
            near_pair(halves[0], False)
        with jax.named_scope('hat'):
            @pl.loop(0, n_tok // (2 * ROWS))
            def _(step):
                for i in range(2):
                    sl = block(2 * step + i, ROWS)
                    hat, inv = layer_norm(dx_ref[sl, :].astype(F32))
                    hat_ref[sl, :] = hat
                    inv_ref[sl, :] = jnp.broadcast_to(inv, (ROWS, 128))

        with jax.named_scope('d23_wait'):
            for q in range(2, chips):
                for i in range(2):
                    direct[i][q].wait_recv()
                    near_across[i][q].start()
        with jax.named_scope('d23_across'):
            for q in range(2, chips):
                for i in range(2):
                    near_across[i][q].wait_recv()

        with jax.named_scope('near_b'):
            near_pair(halves[1], True)
        far_chip = at.ring(2)
        with jax.named_scope('far0_wait'):
            for i in range(2):
                onward[i][0].wait_recv()
                end_across[i][0].start()
        with jax.named_scope('far0_across'):
            for i in range(2):
                end_across[i][0].wait_recv()
        with jax.named_scope('far_dh'):
            grow(chips - 1, lambda b: far_ref[b, me])
        for copy in dy_back:
            copy.wait()
        part_ref[...] = jnp.zeros_like(part_ref)

        with jax.named_scope('norm_back'):
            @pl.loop(0, n_tok // (2 * ROWS))
            def _(step):
                for i in range(2):
                    sl = block(2 * step + i, ROWS)
                    hat, inv = hat_ref[sl, :], inv_ref[sl, 0:1]
                    dh = acc_ref[sl, :]
                    dg = dh * hat
                    gh = dh * gain
                    one = jnp.mean(gh, axis=-1, keepdims=True)
                    two = jnp.mean(dg * gain, axis=-1, keepdims=True)
                    dx_ref[sl, :] = (h_ref[sl, :].astype(F32) + inv * (gh - one - hat * two)).astype(BF16)
                    part_ref[0] += dg[0:8] + dg[8:16]
                    part_ref[1] += dh[0:8] + dh[8:16]

        all_ref[me, 0:1, :] = jnp.sum(part_ref[0], axis=0, keepdims=True)
        all_ref[me, 1:2, :] = jnp.sum(part_ref[1], axis=0, keepdims=True)
        read_far = lambda b, n, q: far_ref[b, span_of(q)]
        for copy in sums:
            copy.start()
        with jax.named_scope('far_a'):
            job(far_chip, [ends[0][0], ends[1][0]], read_far, False)
        with jax.named_scope('far1_wait'):
            for i in range(2):
                onward[i][1].wait_recv()
                end_across[i][1].start()
        with jax.named_scope('far1_across'):
            for i in range(2):
                end_across[i][1].wait_recv()
        with jax.named_scope('far_b'):
            job(far_chip, [ends[0][1], ends[1][1]], read_far, True)

    pl.run_scoped(
        weight_grads,
        pltpu.VMEM((W_SLOTS, group, W_ROWS, head_dim), BF16), pltpu.VMEM((W_SLOTS, W_ROWS, 2 * head_dim), BF16), pltpu.VMEM((n_tok, width), F32),
        pltpu.VMEM((n_tok, width), F32), pltpu.VMEM((n_tok, 128), F32), pltpu.VMEM((2, n_batch, 2, CORES, seq, cols), BF16), pltpu.VMEM((n_batch, seq, cols), BF16),
    )

    with jax.named_scope('sums'):
        for j in range(1, n_dev):
            source = lax.rem(me + j, n_dev)
            send(all_ref.at[me], all_ref.at[source], s_ssem.at[0], s_rsem.at[source], at.partner).wait_recv()
        total = all_ref[0]
        for d in range(1, n_dev):
            total = total + all_ref[d]
        dgain_ref[...] = total[0:1].reshape(width)
        dbias_ref[...] = total[1:2].reshape(width)
    done = dys.sent() + [heads_across] + spots
    done += direct[0] + direct[1] + onward[0] + onward[1] + [g_across] + near_across[0] + near_across[1] + end_across[0] + end_across[1] + sums
    with jax.named_scope('done'):
        for copy in done:
            copy.wait_send()
        hcols.wait_send()


def whole_block(n_dev, x, gain, bias, positions, freq, dy, wq, wk, wv, wo):
    n_batch, seq, width = dy.shape
    n_tok = n_batch * seq
    head_dim = wq.shape[2]
    chips = n_dev // CORES
    group = wq.shape[0] // chips
    cols = (group + 2) * head_dim
    n_rows = group * head_dim
    half = n_rows // CORES
    n_seq = n_dev * seq
    quarter = head_dim // 4
    dma = pltpu.SemaphoreType.DMA
    vm = pltpu.VMEM
    shapes = [((n_tok, width), BF16)] * 2 + [((chips * group, half, head_dim), F32)] + [((chips * half, head_dim), F32)] * 2 + [((half, width), F32), ((width,), F32), ((width,), F32)]
    held = [((n_dev, n_batch, seq, width), BF16), ((n_dev, half, n_tok), BF16), ((n_dev, n_dev, seq, cols), BF16), ((chips, width, 2 * head_dim), BF16)]
    return pl.pallas_call(
        functools.partial(block_body, n_dev, group),
        out_shape=tuple(pltpu.VMEM(*t) for t in shapes) + tuple(sds(*t) for t in held),
        in_specs=[VM] * 4 + [HBM] * 6,
        out_specs=(VM,) * len(shapes) + (HBM,) * len(held),
        scratch_shapes=[
            vm((n_tok, width), BF16), vm((width, n_tok), BF16), vm((n_dev, seq, cols), BF16), vm((n_dev, seq, n_rows), BF16),
            vm((n_rows, n_seq), BF16), vm((half, n_batch * n_seq), BF16), vm((n_seq, n_rows), BF16),
            vm((head_dim, n_seq), BF16), vm((head_dim, n_seq), BF16), vm((n_seq, head_dim), F32), vm((n_seq, head_dim), F32),
            vm((quarter, n_seq), F32), vm((quarter, n_seq), F32), vm((3, n_tok, head_dim), F32), vm((n_dev, n_batch, seq), jnp.int32),
            vm((2, seq, n_rows), BF16), vm((2, half, n_tok), BF16),
            vm((n_batch, n_dev, seq, cols), BF16), vm((2, 8, width), F32), vm((n_dev, 2, width), F32),
            dma((13,)), dma((13,)), dma((13,)), dma((13,)), dma((9,)), dma((n_dev + 2,)), dma((9,)), dma((n_dev + 2,)), dma((n_dev,)), dma((n_dev,)), dma((2,)),
            dma((2, chips)), dma((2, chips)), dma((2, 2)), dma((2, 2)), dma((1 + 4 * chips,)), dma((1 + 4 * chips,)), dma((n_dev,)), dma((n_dev,)),
            dma((1 + n_dev,)), dma((3,)), dma((n_batch * n_dev,)), dma((W_SLOTS, 2)), dma((3, n_batch, 2)),
        ],
        compiler_params=pltpu.CompilerParams(collective_id=0, has_side_effects=True, vmem_limit_bytes=VMEM_LIMIT),
        cost_estimate=pl.CostEstimate(flops=10 ** 11, bytes_accessed=10 ** 8, transcendentals=0),
        name='block',
    )(gain, bias, positions, freq, x.reshape(n_tok, width), dy, wq, wk, wv, wo)[:len(shapes)]


def settle_body(n, *refs):
    sems = refs[2 * n]
    copies = []
    for i in range(n):
        src, dst = refs[i], refs[n + i]
        pieces = SETTLE if len(src.shape) > 1 else 1
        size = src.shape[0] // pieces
        for p in range(pieces):
            copies.append(pltpu.make_async_copy(src.at[pl.ds(p * size, size)], dst.at[pl.ds(p * size, size)], sems.at[i, p]))
    for copy in copies:
        copy.start()
    for copy in copies:
        copy.wait()


def settle(arrays):
    n = len(arrays)
    return pl.pallas_call(
        functools.partial(settle_body, n),
        out_shape=tuple(sds(t.shape, t.dtype) for t in arrays),
        in_specs=[ANY] * n,
        out_specs=(HBM,) * n,
        scratch_shapes=[pltpu.SemaphoreType.DMA((n, SETTLE))],
        compiler_params=pltpu.CompilerParams(vmem_limit_bytes=1024 * 1024),
        name='settle',
    )(*arrays)


def solution(mesh):
    n_dev = mesh.shape['cp']

    def device_step(x_act, d_out, positions, ln_gain, ln_bias, w_query, w_key, w_value, w_out):
        n_batch, seq, width = x_act.shape
        q_heads, (kv_heads, head_dim) = w_query.shape[1], w_key.shape[1:]
        group = q_heads // kv_heads
        quarter = head_dim // 4
        assert n_batch == CORES and n_dev // CORES == kv_heads == 4 and q_heads * head_dim == width

        freq = np.exp(np.arange(quarter) * (-2.0 * math.log(ROPE_BASE) / (head_dim // 2))).astype(np.float32).reshape(quarter, 1)
        by_head = lambda t: jnp.transpose(t, (1, 0, 2))
        by_row = lambda t: t.reshape(width * kv_heads, head_dim)
        wq = by_head(w_query)

        results = whole_block(n_dev, x_act, ln_gain, ln_bias, positions, jnp.asarray(freq), d_out, wq, by_row(w_key), by_row(w_value), w_out)
        out, dx, dwq, dwk, dwv, dwo, dgain, dbias = settle(results)
        kv_rows = lambda t: t.reshape(width // n_dev, kv_heads, head_dim)
        return (out.reshape(x_act.shape), dx.reshape(x_act.shape), by_head(dwq), kv_rows(dwk), kv_rows(dwv), dwo, dgain, dbias)

    return jax.shard_map(device_step, mesh=mesh, in_specs=(P('dp', 'cp', None), P('dp', 'cp', None), P('dp', 'cp'), P(None), P(None), P(None, None, None), P(None, None, None), P(None, None, None), P(None, None)), out_specs=(P('dp', 'cp', None), P('dp', 'cp', None), P(('dp', 'cp'), None, None), P(('dp', 'cp'), None, None), P(('dp', 'cp'), None, None), P(('dp', 'cp'), None), P('dp'), P('dp')), check_vma=False)
```

```python
import functools
import math
import jax
import jax.numpy as jnp
import numpy as np
from jax import lax
from jax.experimental import pallas as pl
from jax.experimental.pallas import tpu as pltpu
from jax.sharding import PartitionSpec as P

EPS = 1e-5
ROPE_BASE = 10000.0
BF16 = jnp.bfloat16
F32 = jnp.float32
VMEM_LIMIT = 46 * 1024 * 1024
NT = (((1,), (1,)), ((), ()))
ANY = pl.BlockSpec(memory_space=pl.ANY)
VM = pl.BlockSpec(memory_space=pltpu.VMEM)
HBM = pl.BlockSpec(memory_space=pltpu.HBM)
CORES = 2
COL_TILE = 512
OUT_TILE = 256
ROWS = 16
W_SLOTS = 4
W_ROWS = 512
SETTLE = 8


def dot(a, b):
    return jnp.dot(a, b, preferred_element_type=F32)


def dot_nt(a, b):
    return lax.dot_general(a, b, NT, preferred_element_type=F32)


def sds(shape, dtype):
    return jax.ShapeDtypeStruct(shape, dtype)


def block(i, size):
    return pl.ds(pl.multiple_of(i * size, size), size)


class Place:
    def __init__(self, n_dev):
        self.n_dev = n_dev
        self.chips = n_dev // CORES
        self.me = lax.axis_index('cp')
        self.chip = self.me // CORES
        self.core = self.me % CORES
        self.partner = self.chip * CORES + 1 - self.core

    def ring(self, step):
        return lax.rem(self.chip + self.chips + step, self.chips)

    def dev(self, step, core):
        return self.ring(step) * CORES + core

    def peers(self, far):
        near = [self.partner] + [self.dev(s, c) for s in (1, -1) for c in range(CORES)]
        return near + ([self.dev(2, c) for c in range(CORES)] if far else [])


def send(src, dst, ssem, rsem, to):
    return pltpu.make_async_remote_copy(src_ref=src, dst_ref=dst, send_sem=ssem, recv_sem=rsem, device_id={'cp': to}, device_id_type=pl.DeviceIdType.MESH)


def meet(peers):
    barrier = pltpu.get_barrier_semaphore()
    for peer in peers:
        pl.semaphore_signal(barrier, inc=1, device_id={'cp': peer}, device_id_type=pl.DeviceIdType.MESH)
    pl.semaphore_wait(barrier, len(peers))


class Ring:
    def __init__(self, n, slots, copies):
        self.n, self.slots, self.copies = n, slots, copies

    def prime(self):
        for s in range(self.slots):
            for copy in self.copies(s, s):
                copy.start()

    def run(self, use):
        @pl.loop(0, self.n)
        def _(s):
            slot = lax.rem(s, self.slots)
            for copy in self.copies(s, slot):
                copy.wait()
            use(s, slot)

            @pl.when(s + self.slots < self.n)
            def _():
                for copy in self.copies(s + self.slots, slot):
                    copy.start()


class Gather:
    def __init__(self, at, own, piece, both, ssem, rsem):
        steps = (1, -1)
        origin = [at.dev(-1, at.core), at.dev(1, at.core)]
        far = at.dev(2, at.core)
        link = lambda i, src, dst, to: send(src, dst, ssem.at[i], rsem.at[i], to)
        self.first = [link(b, own(b), piece(at.me, b), at.dev(steps[b], at.core)) for b in range(2)]
        self.second = [link(2 + b, own(1 - b), piece(at.me, 1 - b), at.dev(steps[b], at.core)) for b in range(2)]
        self.again = [link(4 + b, piece(origin[b], b), piece(origin[b], b), at.dev(steps[b], at.core)) for b in range(2)]
        self.own_across = link(6, both(None), both(at.me), at.partner)
        self.first_across = [link(7 + b, piece(origin[b], b), piece(origin[b], b), at.partner) for b in range(2)]
        self.second_across = [link(9 + b, piece(origin[b], 1 - b), piece(origin[b], 1 - b), at.partner) for b in range(2)]
        self.far_across = [link(11 + b, piece(far, b), piece(far, b), at.partner) for b in range(2)]

    def start_first(self):
        for copy in self.first + [self.own_across]:
            copy.start()

    def start_second(self):
        for copy in self.second:
            copy.start()

    def pass_on(self):
        for copy, again, across in zip(self.first, self.again, self.first_across):
            copy.wait_recv()
            again.start()
            across.start()

    def share_second(self):
        for copy, across in zip(self.second, self.second_across):
            copy.wait_recv()
            across.start()

    def share_far(self):
        for copy, across in zip(self.again, self.far_across):
            copy.wait_recv()
            across.start()

    def wait_near(self):
        for copy in self.first_across + self.second_across:
            copy.wait_recv()

    def wait_far(self):
        for copy in self.far_across:
            copy.wait_recv()

    def sent(self):
        return self.first + self.second + self.again + [self.own_across] + self.first_across + self.second_across + self.far_across


class Exchange:
    def __init__(self, at, src, dst, relay, ssem, rsem):
        self.at, self.src, self.dst, self.relay, self.ssem, self.rsem = at, src, dst, relay, ssem, rsem
        near = [(0, 1 - at.core)] + [(s, c) for s in (1, -1) for c in range(CORES)]
        n = at.n_dev
        self.near = [send(src(at.dev(s, c)), dst(at.me), ssem.at[i], rsem.at[at.me], at.dev(s, c)) for i, (s, c) in enumerate(near)]
        self.far = [send(src(at.dev(2, i)), relay.at[i], ssem.at[5 + i], rsem.at[n + i], at.dev(step, at.core)) for i, step in enumerate((1, -1))]
        self.on = [send(relay.at[i], dst(at.dev(-step, at.core)), ssem.at[7 + i], rsem.at[at.dev(-step, at.core)], at.dev(step, i)) for i, step in enumerate((1, -1))]

    def start(self):
        for copy in self.far + self.near:
            copy.start()

    def pass_on(self):
        for far, on in zip(self.far, self.on):
            far.wait_recv()
            on.start()

    def wait_recv(self):
        at = self.at
        for j in range(1, at.n_dev):
            origin = lax.rem(at.me + j, at.n_dev)
            send(self.src(at.me), self.dst(origin), self.ssem.at[0], self.rsem.at[origin], at.partner).wait_recv()

    def wait_send(self):
        for copy in self.far + self.near + self.on:
            copy.wait_send()


def layer_norm(x):
    cen = x - jnp.mean(x, axis=-1, keepdims=True)
    inv = lax.rsqrt(jnp.mean(cen * cen, axis=-1, keepdims=True) + EPS)
    return cen * inv, inv


def block_body(n_dev, group, gain_ref, bias_ref, pos_ref, freq_ref, x_hbm, dy_ref, wq_ref, wk_ref, wv_ref, wo_ref,
               out_ref, dx_ref, dwq_ref, dwk_ref, dwv_ref, dwo_ref, dgain_ref, dbias_ref, dy_all, ht_all, g_all, wkv_all,
               h_ref, ht_ref, g_ref, q_ref, at_ref, at2_ref, da_ref, kt_ref, vt_ref, dk_ref, dv_ref,
               cost_ref, sint_ref, tab_ref, spot_ref, relay_q, relay_h, far_ref, part_ref, all_ref,
               dy_ssem, dy_rsem, kv_ssem, kv_rsem, q_ssem, q_rsem, h_ssem, h_rsem, p_ssem, p_rsem, t_sem,
               g_ssem, g_rsem, r_ssem, r_rsem, x_ssem, x_rsem, s_ssem, s_rsem, loc_sem, mix_sem, lhs_sem, w_sem, job_sem):
    at = Place(n_dev)
    n_batch, seq, width = dy_ref.shape
    n_tok = n_batch * seq
    head_dim = wq_ref.shape[2]
    cols = (group + 2) * head_dim
    n_rows = group * head_dim
    half = n_rows // CORES
    n_seq = n_dev * seq
    quarter = head_dim // 4
    scale = head_dim ** -0.5
    chips = at.chips
    tile = CORES * seq
    core, me = at.core, at.me
    steps = (1, -1)
    origin = [at.dev(-1, core), at.dev(1, core)]
    far_dev = at.dev(2, core)
    scope = jax.named_scope

    with scope('meet'):
        meet(at.peers(True))

    kv_cols = 2 * head_dim * chips
    kv_piece = lambda d, b: far_ref.at[b, d, :, pl.ds(0, kv_cols)]
    kv_both = lambda d: far_ref.at[:, me if d is None else d, :, pl.ds(0, kv_cols)]
    dys = Gather(at, lambda b: dy_ref.at[b], lambda d, b: dy_all.at[d, b], lambda d: dy_ref if d is None else dy_all.at[d], dy_ssem, dy_rsem)
    kvs = Gather(at, lambda b: kv_piece(me, b), kv_piece, kv_both, kv_ssem, kv_rsem)
    q_part = pl.ds(0, n_rows)
    queries = Exchange(at, lambda d: g_ref.at[d, :, q_part], lambda d: q_ref.at[d], relay_q, q_ssem, q_rsem)
    hcols = Exchange(at, lambda d: ht_ref.at[block(d, half)], lambda d: ht_all.at[d], relay_h, h_ssem, h_rsem)
    heads_across = send(at_ref.at[block(1 - core, half)], at2_ref.at[:, block(core, n_seq)], t_sem.at[0], t_sem.at[1], at.partner)
    spots = [send(pos_ref, spot_ref.at[me], p_ssem.at[j], p_rsem.at[me], peer) for j, peer in enumerate(at.peers(True))]

    dys.start_first()
    x_in = pltpu.make_async_copy(x_hbm, dx_ref, loc_sem.at[1])
    x_in.start()
    for copy in spots:
        copy.start()
    spot_ref[me] = pos_ref[...]

    freq = freq_ref[...]
    for b in range(n_batch):
        angle = freq * pos_ref[b:b + 1, :].astype(F32)
        cos, sin, none = jnp.cos(angle), jnp.sin(angle), jnp.zeros((quarter, seq), F32)
        rest = jnp.zeros((head_dim - 2 * quarter, seq), F32)
        for i, rows in enumerate(([cos, cos, rest + 1.0], [-sin, none, rest], [none, sin, rest])):
            tab_ref[i, b * seq:(b + 1) * seq, :] = jnp.concatenate(rows, axis=0).T

    gain = (1.0 + gain_ref[...]).reshape(1, width)
    bias = bias_ref[...].reshape(1, width)

    def project_all(wkv_ref, raw_ref, wq_vm, raw_sem, wq_sem, stage_sem):
        pieces = [(b, i) for b in range(n_batch) for i in range(width // n_rows)]
        there = lambda n: da_ref.at[pl.ds(n * seq, seq)]
        dy_in = [pltpu.make_async_copy(dy_ref.at[b, :, pl.ds(i * n_rows, n_rows)], there(n), stage_sem.at[n]) for n, (b, i) in enumerate(pieces)]
        dy_keep = [pltpu.make_async_copy(there(n), dy_all.at[me, b, :, pl.ds(i * n_rows, n_rows)], stage_sem.at[n]) for n, (b, i) in enumerate(pieces)]
        span = 64 * chips
        batch = raw_ref.shape[2] // span
        row = lax.broadcasted_iota(jnp.int32, (span, span), 0)
        col = lax.broadcasted_iota(jnp.int32, (span, span), 1)
        pick = jnp.where(col == lax.rem(row, 64) * chips + lax.div(row, 64), 1.0, 0.0).astype(BF16)

        def raw_in(s, slot):
            return [pltpu.make_async_copy(w.at[block(s, span * batch)], raw_ref.at[slot, i], raw_sem.at[slot, i]) for i, w in enumerate((wk_ref, wv_ref))]

        def wq_in(s, slot):
            return [pltpu.make_async_copy(wq_ref.at[block(s, 2)], wq_vm.at[slot], wq_sem.at[slot])]

        def part_heads(s, slot):
            for i in range(batch):
                sl = slice(i * span, (i + 1) * span)
                rows = dot(pick, jnp.concatenate([raw_ref[slot, 0, sl, :], raw_ref[slot, 1, sl, :]], axis=1)).astype(BF16)
                for n in range(chips):
                    wkv_ref[n, block(s * batch + i, 64), :] = rows[n * 64:(n + 1) * 64]

        def turned(v):
            return v * tab_ref[0] + pltpu.roll(v, head_dim - quarter, 1) * tab_ref[1] + pltpu.roll(v, quarter, 1) * tab_ref[2]

        def project(s, slot):
            y = dot(h_ref[...], jnp.concatenate([wq_vm[slot, 0], wq_vm[slot, 1]], axis=1))
            for i in range(2):
                head = s * 2 + i
                v = turned(y[:, i * head_dim:(i + 1) * head_dim]).astype(BF16)
                for b in range(n_batch):
                    g_ref[lax.div(head, group) * n_batch + b, :, block(lax.rem(head, group), head_dim)] = v[b * seq:(b + 1) * seq]

        kv_ring = Ring(width // (64 * batch), raw_ref.shape[0], raw_in)
        q_ring = Ring(chips * group // 2, wq_vm.shape[0], wq_in)
        kv_ring.prime()
        q_ring.prime()
        for copy in dy_in:
            copy.start()
        x_in.wait()
        with scope('norm'):
            @pl.loop(0, n_tok // (2 * ROWS))
            def _(step):
                for i in range(2):
                    sl = block(2 * step + i, ROWS)
                    hat, _ = layer_norm(dx_ref[sl, :].astype(F32))
                    h_ref[sl, :] = (hat * gain + bias).astype(BF16)

        with scope('heads_kv'):
            kv_ring.run(part_heads)
        keep = pltpu.make_async_copy(wkv_ref, wkv_all, mix_sem.at[2])
        keep.start()
        for come, go in zip(dy_in, dy_keep):
            come.wait()
            go.start()
        with scope('project_kv'):
            @pl.loop(0, chips)
            def _(n):
                y = dot(h_ref[...], wkv_ref[n])
                v = jnp.concatenate([turned(y[:, :head_dim]), y[:, head_dim:]], axis=1).astype(BF16)
                for b in range(n_batch):
                    far_ref[b, me, :, block(n, 2 * head_dim)] = v[b * seq:(b + 1) * seq]

        kvs.start_first()
        kvs.start_second()
        with scope('project_q'):
            q_ring.run(project)
        keep.wait()
        for copy in dy_keep:
            copy.wait()

    pl.run_scoped(
        project_all,
        pltpu.VMEM((chips, width, 2 * head_dim), BF16),
        pltpu.VMEM((3, 2, 4 * 64 * chips, head_dim), BF16), pltpu.VMEM((4, 2, width, head_dim), BF16),
        pltpu.SemaphoreType.DMA((3, 2)), pltpu.SemaphoreType.DMA((4,)), pltpu.SemaphoreType.DMA((n_batch * width // n_rows,)),
    )

    with scope('kv_pass'):
        kvs.pass_on()
    queries.start()
    q_ref[me] = g_ref[me, :, q_part]
    with scope('turn_h'):
        @pl.loop(0, width // 128)
        def _(step):
            sl = block(step, 128)
            ht_ref[sl, :] = h_ref[:, sl].T

    with scope('kv_wait'):
        kvs.share_second()
        kvs.share_far()
        kvs.own_across.wait_recv()
        kvs.wait_near()
        kvs.wait_far()

    def chip_at(i):
        return at.ring(jnp.where(i == 0, 0, jnp.where(i == 1, 1, jnp.where(i == 2, 3, 2))))

    def soft(s, seen):
        s = s * scale
        clear = s.shape[0] - seen.shape[0]
        tail = jnp.where(seen, s[clear:], -1e30)
        s = tail if clear == 0 else jnp.concatenate([s[:clear], tail], axis=0)
        e = jnp.exp(s - jnp.max(s, axis=0, keepdims=True))
        return e * (1.0 / jnp.sum(e, axis=0, keepdims=True))

    def attend(limit, clear):
        @pl.loop(0, n_batch * chips)
        def _(i):
            @pl.when(i == 1)
            def _():
                with scope('q_pass'):
                    queries.pass_on()
                dys.start_second()
                dys.pass_on()
                hcols.start()

            b, n = lax.rem(i, n_batch), lax.div(i, n_batch)
            k = far_ref[b, 0:limit // seq, :, block(2 * n, head_dim)].reshape(limit, head_dim)
            vt = far_ref[b, 0:limit // seq, :, block(2 * n + 1, head_dim)].reshape(limit, head_dim).T
            q = jnp.concatenate([g_ref[n * n_batch + b, :, block(j, head_dim)] for j in range(group)], axis=0)
            row = lax.broadcasted_iota(jnp.int32, (limit - clear, n_rows), 0)
            col = lax.broadcasted_iota(jnp.int32, (limit - clear, n_rows), 1)
            p = soft(dot_nt(k, q), row <= lax.rem(col, seq) + (me * seq - clear))
            mixed = dot(vt, p.astype(BF16)).astype(BF16)
            for j in range(group):
                h_ref[block(b, seq), block(n * group + j, head_dim)] = mixed[:, j * seq:(j + 1) * seq].T

    with scope('attend'):
        @pl.when(at.chip == chips - 1)
        def _():
            attend(chips * tile, (chips - 1) * tile)

        @pl.when(at.chip < chips - 1)
        def _():
            attend((chips - 1) * tile, 0)

    h_keep = pltpu.make_async_copy(ht_ref.at[block(me, half)], ht_all.at[me], loc_sem.at[1])
    h_keep.start()

    def block_out():
        def stream(wo_vm, sem):
            def wo_in(s, slot):
                return [pltpu.make_async_copy(wo_ref.at[:, block(s, OUT_TILE)], wo_vm.at[slot], sem.at[slot])]

            def out_tile(s, slot):
                sl = block(s, OUT_TILE)
                out_ref[:, sl] = (dx_ref[:, sl].astype(F32) + dot(h_ref[...], wo_vm[slot])).astype(BF16)

            ring = Ring(width // OUT_TILE, wo_vm.shape[0], wo_in)
            ring.prime()
            ring.run(out_tile)

        with scope('output'):
            pl.run_scoped(stream, pltpu.VMEM((4, width, OUT_TILE), BF16), pltpu.SemaphoreType.DMA((4,)))

    k_all = lambda n: far_ref[core, 0:n, :, block(2 * at.chip, head_dim)].reshape(n * seq, head_dim)
    v_all = lambda n: far_ref[core, 0:n, :, block(2 * at.chip + 1, head_dim)].reshape(n * seq, head_dim)

    def rotate_back(t, cos, sin):
        u, w = t[:quarter], t[quarter:2 * quarter]
        return jnp.concatenate([u * cos + w * sin, w * cos - u * sin, t[2 * quarter:]], axis=0)

    def by_dev(t):
        return t.astype(BF16).reshape(t.shape[0] // seq, seq, head_dim)

    def attend_back(t):
        limit = (t + 1) * tile
        sl = slice(t * tile, limit)
        devs = slice(t * CORES, (t + 1) * CORES)

        def heads(first, count):
            each = range(count)
            q = jnp.concatenate([q_ref[devs, :, block(first + j, head_dim)].reshape(tile, head_dim) for j in each], axis=0)
            da = jnp.concatenate([da_ref[sl, block(first + j, head_dim)] for j in each], axis=0)
            k, v = k_all(limit // seq), v_all(limit // seq)
            row = lax.broadcasted_iota(jnp.int32, (tile, count * tile), 0)
            col = lax.broadcasted_iota(jnp.int32, (tile, count * tile), 1)
            p = soft(dot_nt(k, q), row <= lax.rem(col, tile))
            p_low = p.astype(BF16)
            mixed = dot(vt_ref[:, :limit], p_low).astype(BF16)
            dp = dot_nt(v, da)
            row_dot = jnp.sum(p * dp, axis=0, keepdims=True)
            ds = (p * (dp - row_dot) * scale).astype(BF16)
            dv_ref[:limit, :] += dot(p_low, da)
            dk_ref[:limit, :] += dot(ds, q)
            back = dot(kt_ref[:, :limit], ds)
            for j in each:
                part = slice(j * tile, (j + 1) * tile)
                at_ref[block(first + j, head_dim), sl] = mixed[:, part]
                g_ref[devs, :, block(first + j, head_dim)] = by_dev(rotate_back(back[:, part], cost_ref[:, sl], sint_ref[:, sl]).T)

        @pl.loop(0, group // 2)
        def _(j):
            heads(2 * j, 2)

        heads(group - 1, 1)

    def middle(wo_vm, dyk):
        wo_in = pltpu.make_async_copy(wo_ref.at[block(at.chip, n_rows)], wo_vm, mix_sem.at[2])
        wo_in.start()
        for j in range(1, n_dev):
            source = lax.rem(me + j, n_dev)
            send(pos_ref, spot_ref.at[source], p_ssem.at[0], p_rsem.at[source], at.partner).wait_recv()
        for d in range(n_dev):
            angle = freq * spot_ref[d, pl.ds(core, 1), :].astype(F32)
            cost_ref[:, d * seq:(d + 1) * seq] = jnp.cos(angle)
            sint_ref[:, d * seq:(d + 1) * seq] = jnp.sin(angle)
        with scope('q_wait'):
            queries.wait_recv()
            queries.wait_send()
            for copy in kvs.sent():
                copy.wait_send()
        kt_ref[...] = k_all(n_dev).T
        vt_ref[...] = v_all(n_dev).T
        dk_ref[...] = jnp.zeros_like(dk_ref)
        dv_ref[...] = jnp.zeros_like(dv_ref)
        dys.own_across.wait_recv()

        def fetch(i, slot):
            return pltpu.make_async_copy(dy_all.at[block(chip_at(i), CORES), core], dyk.at[slot], mix_sem.at[slot])

        with scope('wo_wait'):
            fetch(0, 0).start()
            wo_in.wait()

        @pl.loop(0, chips)
        def _(i):
            slot = lax.rem(i, 2)

            @pl.when((i == 1) & (at.chip < chips - 1))
            def _():
                block_out()

            @pl.when(i == 1)
            def _():
                with scope('dy_wait'):
                    dys.share_second()
                    dys.wait_near()
                fetch(i, slot).start()

            @pl.when(i == chips - 1)
            def _():
                with scope('dy_far'):
                    dys.share_far()
                with scope('dy_far2'):
                    dys.wait_far()
                fetch(i, slot).start()
                with scope('h_pass'):
                    hcols.pass_on()

            fetch(i, slot).wait()

            @pl.when((i > 0) & (i < chips - 2))
            def _():
                fetch(i + 1, 1 - slot).start()

            chip = chip_at(i)
            with scope('da'):
                da_ref[block(chip, tile), :] = dot_nt(dyk[slot].reshape(tile, width), wo_vm[...]).astype(BF16)
            with scope('attend_back'):
                for t in range(chips):
                    @pl.when(chip == t)
                    def _(t=t):
                        attend_back(t)

    pl.run_scoped(middle, pltpu.VMEM((n_rows, width), BF16), pltpu.VMEM((2, CORES, seq, width), BF16))
    g_ref[:, :, n_rows:n_rows + head_dim] = by_dev(rotate_back(dk_ref[...].T, cost_ref[...], sint_ref[...]).T)
    g_ref[:, :, n_rows + head_dim:] = by_dev(dv_ref[...])

    def span_of(q):
        return block(q, CORES)

    turn = [[at.ring(q) for q in (2, 1, 3, 0)], [at.ring(q) for q in (3, 0, 1, 2)]]
    direct = [[send(g_ref.at[span_of(turn[i][q])], g_all.at[me, span_of(turn[i][q])], g_ssem.at[i, q], g_rsem.at[i, q], at.dev(steps[i], core)) for q in range(chips)] for i in range(2)]
    came = [[at.ring(q) for q in (1, 0, 2, 3)], [at.ring(q) for q in (0, 1, 2, 3)]]
    def halves_of(quarters):
        return [span_of(quarters[0])] + [pl.ds(quarters[1] * CORES + c, 1) for c in range(CORES)]

    onward = [[send(g_all.at[origin[i], sl], far_ref.at[core, sl], r_ssem.at[i, q], r_rsem.at[i, q], at.dev(steps[i], core)) for q, sl in enumerate(halves_of(came[i]))] for i in range(2)]
    ends = [[at.ring(q) for q in (0, 3)], [at.ring(q) for q in (1, 2)]]
    g_across = send(g_ref, g_all.at[me], x_ssem.at[0], x_rsem.at[0], at.partner)
    near_across = [[send(g_all.at[origin[i], span_of(came[i][q])], g_all.at[origin[i], span_of(came[i][q])], x_ssem.at[1 + i * chips + q], x_rsem.at[1 + i * chips + q], at.partner) for q in range(chips)] for i in range(2)]
    end_across = [[send(far_ref.at[core, sl], far_ref.at[core, sl], x_ssem.at[1 + (2 + i) * chips + q], x_rsem.at[1 + (2 + i) * chips + q], at.partner) for q, sl in enumerate(halves_of(ends[i]))] for i in range(2)]
    for q in range(chips):
        for i in range(2):
            direct[i][q].start()
    g_across.start()
    g_keep = pltpu.make_async_copy(g_ref, g_all.at[me], loc_sem.at[0])
    g_keep.start()
    heads_across.start()
    at2_ref[:, block(core, n_seq)] = at_ref[block(core, half), :]

    @pl.when(at.chip == chips - 1)
    def _():
        block_out()

    dy_back = [pltpu.make_async_copy(dy_ref.at[b], h_ref.at[pl.ds(b * seq, seq)], loc_sem.at[2 + b]) for b in range(n_batch)]
    for copy in dy_back:
        copy.start()

    def wo_rows(dy_vm, sem):
        def dy_tile(s, slot):
            return [pltpu.make_async_copy(dy_all.at[:, :, :, block(s, COL_TILE)], dy_vm.at[slot], sem.at[slot])]

        def wo_tile(s, slot):
            pieces = [dy_vm[slot, d, b] for b in range(n_batch) for d in range(n_dev)]
            dwo_ref[:, block(s, COL_TILE)] = dot(at2_ref[...], jnp.concatenate(pieces, axis=0))

        ring = Ring(width // COL_TILE, dy_vm.shape[0], dy_tile)
        ring.prime()
        with scope('heads_wait'):
            heads_across.wait_recv()
        with scope('grad_wo'):
            ring.run(wo_tile)

    pl.run_scoped(wo_rows, pltpu.VMEM((4, n_dev, n_batch, seq, COL_TILE), BF16), pltpu.SemaphoreType.DMA((4,)))

    with scope('h_wait'):
        hcols.wait_recv()
    h_keep.wait()
    lhs_in = [pltpu.make_async_copy(ht_all.at[d, :, pl.ds(b * seq, seq)], at2_ref.at[:, pl.ds((b * n_dev + d) * seq, seq)], lhs_sem.at[b * n_dev + d]) for d in range(n_dev) for b in range(n_batch)]
    for copy in lhs_in:
        copy.start()
    with jax.named_scope('own_wait'):
        for copy in lhs_in:
            copy.wait()
        g_keep.wait()
        g_across.wait_recv()
    sums = [send(all_ref.at[me], all_ref.at[me], s_ssem.at[j], s_rsem.at[me], peer) for j, peer in enumerate(at.peers(True))]

    def weight_grads(wq_vm, wkv_vm, acc_ref, hat_ref, inv_ref, job_ref, mine_ref):
        n_slots = wq_vm.shape[0]
        chunk = wq_vm.shape[2]
        n_chunks = width // chunk
        total = n_chunks * chips

        def weights(s):
            slot = lax.rem(s, n_slots)
            chip = chip_at(lax.div(s, n_chunks))
            rows = block(lax.rem(s, n_chunks), chunk)
            return [
                pltpu.make_async_copy(wq_ref.at[block(chip, group), rows], wq_vm.at[slot], w_sem.at[slot, 0]),
                pltpu.make_async_copy(wkv_all.at[chip, rows], wkv_vm.at[slot], w_sem.at[slot, 1]),
            ]

        for s in range(n_slots):
            for copy in weights(s):
                copy.start()

        def grow(i, read):
            @pl.loop(0, n_chunks)
            def _(n):
                s = i * n_chunks + n
                slot = lax.rem(s, n_slots)
                for copy in weights(s):
                    copy.wait()
                rows = jnp.concatenate([read(b) for b in range(n_batch)], axis=0)
                part = dot_nt(rows, jnp.concatenate([wq_vm[slot, j] for j in range(group)] + [wkv_vm[slot]], axis=1))
                sl = block(n, chunk)

                @pl.when(i == 0)
                def _():
                    acc_ref[:, sl] = part

                @pl.when(i > 0)
                def _():
                    acc_ref[:, sl] += part

                @pl.when(s + n_slots < total)
                def _():
                    for copy in weights(s + n_slots):
                        copy.start()

        def mine_in(i):
            return [pltpu.make_async_copy(g_all.at[chip_at(i) * CORES + b, me], mine_ref.at[lax.rem(i, 2), b], job_sem.at[2 + lax.rem(i, 2), b, 0]) for b in range(n_batch)]

        def grow_near(i):
            for copy in mine_in(i):
                copy.wait()
            grow(i, lambda b: mine_ref[lax.rem(i, 2), b])

        def job_in(chip, quarters, slot):
            return [pltpu.make_async_copy(g_all.at[chip * CORES + b, span_of(q)], job_ref.at[slot, b, n], job_sem.at[slot, b, n]) for b in range(n_batch) for n, q in enumerate(quarters)]

        def job(chip, pieces, read, add):
            lhs = [at2_ref[:, pl.ds(pl.multiple_of(b * n_seq + d * seq, seq), seq)] for b in range(n_batch) for d in pieces]
            rhs = [read(b, n) for b in range(n_batch) for n in range(len(pieces))]
            y = dot(jnp.concatenate(lhs, axis=1), jnp.concatenate(rhs, axis=0))
            for j in range(group):
                v = y[:, j * head_dim:(j + 1) * head_dim]
                dwq_ref[chip * group + j] = dwq_ref[chip * group + j] + v if add else v
            for j, ref in enumerate((dwk_ref, dwv_ref)):
                v = y[:, (group + j) * head_dim:(group + j + 1) * head_dim]
                rows = pl.ds(chip, half, stride=chips)
                ref[rows, :] = ref[rows, :] + v if add else v

        def devs_of(quarters):
            return [q * CORES + c for q in quarters for c in range(CORES)]

        def near_pair(quarters, add):
            for slot, step in enumerate(steps):
                for copy in job_in(at.ring(step), quarters, slot):
                    copy.start()

            @pl.loop(0, 2)
            def _(slot):
                chip = at.ring(1 - 2 * slot)
                for copy in job_in(chip, quarters, slot):
                    copy.wait()
                job(chip, devs_of(quarters), lambda b, n: job_ref[slot, b, n // CORES, n % CORES], add)

        halves = [[at.ring(q) for q in half_of] for half_of in ((0, 1), (2, 3))]
        for slot in range(2):
            for copy in job_in(at.chip, [at.ring(2 * slot), at.ring(2 * slot + 1)], slot):
                copy.start()
        for copy in mine_in(0):
            copy.start()
        with jax.named_scope('own_job'):
            for slot in range(2):
                quarters = [at.ring(2 * slot), at.ring(2 * slot + 1)]
                for copy in job_in(at.chip, quarters, slot):
                    copy.wait()
                job(at.chip, devs_of(quarters), lambda b, n: job_ref[slot, b, n // CORES, n % CORES], slot == 1)

        with jax.named_scope('own_dh'):
            grow_near(0)

        with jax.named_scope('d01_wait'):
            for q in range(2):
                for i in range(2):
                    direct[i][q].wait_recv()
                for i in range(2):
                    for copy in onward[i][:1] if q == 0 else onward[i][1:]:
                        copy.start()
                    near_across[i][q].start()
        with jax.named_scope('d01_across'):
            for q in range(2):
                for i in range(2):
                    near_across[i][q].wait_recv()
        for i in (1, 2):
            for copy in mine_in(i):
                copy.start()
        with scope('near_dh'):
            @pl.loop(1, chips - 1)
            def _(i):
                grow_near(i)

        with jax.named_scope('near_a'):
            near_pair(halves[0], False)
        with scope('d2_wait'):
            for i in range(2):
                direct[i][2].wait_recv()
                near_across[i][2].start()
        with jax.named_scope('hat'):
            @pl.loop(0, n_tok // (2 * ROWS))
            def _(step):
                for i in range(2):
                    sl = block(2 * step + i, ROWS)
                    hat, inv = layer_norm(dx_ref[sl, :].astype(F32))
                    hat_ref[sl, :] = hat
                    inv_ref[sl, :] = jnp.broadcast_to(inv, (ROWS, 128))

        with scope('d3_wait'):
            for i in range(2):
                direct[i][3].wait_recv()
                near_across[i][3].start()
        with jax.named_scope('d23_across'):
            for q in range(2, chips):
                for i in range(2):
                    near_across[i][q].wait_recv()

        with jax.named_scope('near_b'):
            near_pair(halves[1], True)
        far_chip = at.ring(2)
        with jax.named_scope('far0_wait'):
            for i in range(2):
                onward[i][0].wait_recv()
                end_across[i][0].start()
        with jax.named_scope('far0_across'):
            for i in range(2):
                end_across[i][0].wait_recv()
        with jax.named_scope('far_dh'):
            grow(chips - 1, lambda b: far_ref[b, me])
        for copy in dy_back:
            copy.wait()
        part_ref[...] = jnp.zeros_like(part_ref)

        with jax.named_scope('norm_back'):
            @pl.loop(0, n_tok // (2 * ROWS))
            def _(step):
                for i in range(2):
                    sl = block(2 * step + i, ROWS)
                    hat, inv = hat_ref[sl, :], inv_ref[sl, 0:1]
                    dh = acc_ref[sl, :]
                    dg = dh * hat
                    gh = dh * gain
                    one = jnp.mean(gh, axis=-1, keepdims=True)
                    two = jnp.mean(dg * gain, axis=-1, keepdims=True)
                    dx_ref[sl, :] = (h_ref[sl, :].astype(F32) + inv * (gh - one - hat * two)).astype(BF16)
                    part_ref[0] += dg[0:8] + dg[8:16]
                    part_ref[1] += dh[0:8] + dh[8:16]

        all_ref[me, 0:1, :] = jnp.sum(part_ref[0], axis=0, keepdims=True)
        all_ref[me, 1:2, :] = jnp.sum(part_ref[1], axis=0, keepdims=True)
        for copy in sums:
            copy.start()
        with scope('far_a'):
            first_devs = devs_of([ends[0][0], ends[1][0]])
            job(far_chip, first_devs, lambda b, n: far_ref[b, first_devs[n]], False)
        for c in range(CORES):
            with scope('far1_wait'):
                for i in range(2):
                    onward[i][1 + c].wait_recv()
                    end_across[i][1 + c].start()
            with scope('far1_across'):
                for i in range(2):
                    end_across[i][1 + c].wait_recv()
            with scope('far_b'):
                last_devs = [ends[i][1] * CORES + c for i in range(2)]
                job(far_chip, last_devs, lambda b, n: far_ref[b, last_devs[n]], True)

    pl.run_scoped(
        weight_grads,
        pltpu.VMEM((W_SLOTS, group, W_ROWS, head_dim), BF16), pltpu.VMEM((W_SLOTS, W_ROWS, 2 * head_dim), BF16), pltpu.VMEM((n_tok, width), F32),
        pltpu.VMEM((n_tok, width), F32), pltpu.VMEM((n_tok, 128), F32), pltpu.VMEM((2, n_batch, 2, CORES, seq, cols), BF16), pltpu.VMEM((2, n_batch, seq, cols), BF16),
    )

    with jax.named_scope('sums'):
        for j in range(1, n_dev):
            source = lax.rem(me + j, n_dev)
            send(all_ref.at[me], all_ref.at[source], s_ssem.at[0], s_rsem.at[source], at.partner).wait_recv()
        total = all_ref[0]
        for d in range(1, n_dev):
            total = total + all_ref[d]
        dgain_ref[...] = total[0:1].reshape(width)
        dbias_ref[...] = total[1:2].reshape(width)
    done = dys.sent() + [heads_across] + spots
    done += direct[0] + direct[1] + onward[0] + onward[1] + [g_across] + near_across[0] + near_across[1] + end_across[0] + end_across[1] + sums
    with jax.named_scope('done'):
        for copy in done:
            copy.wait_send()
        hcols.wait_send()


def whole_block(n_dev, x, gain, bias, positions, freq, dy, wq, wk, wv, wo):
    n_batch, seq, width = dy.shape
    n_tok = n_batch * seq
    head_dim = wq.shape[2]
    chips = n_dev // CORES
    group = wq.shape[0] // chips
    cols = (group + 2) * head_dim
    n_rows = group * head_dim
    half = n_rows // CORES
    n_seq = n_dev * seq
    quarter = head_dim // 4
    dma = pltpu.SemaphoreType.DMA
    vm = pltpu.VMEM
    shapes = [((n_tok, width), BF16)] * 2 + [((chips * group, half, head_dim), F32)] + [((chips * half, head_dim), F32)] * 2 + [((half, width), F32), ((width,), F32), ((width,), F32)]
    held = [((n_dev, n_batch, seq, width), BF16), ((n_dev, half, n_tok), BF16), ((n_dev, n_dev, seq, cols), BF16), ((chips, width, 2 * head_dim), BF16)]
    return pl.pallas_call(
        functools.partial(block_body, n_dev, group),
        out_shape=tuple(pltpu.VMEM(*t) for t in shapes) + tuple(sds(*t) for t in held),
        in_specs=[VM] * 4 + [HBM] * 6,
        out_specs=(VM,) * len(shapes) + (HBM,) * len(held),
        scratch_shapes=[
            vm((n_tok, width), BF16), vm((width, n_tok), BF16), vm((n_dev, seq, cols), BF16), vm((n_dev, seq, n_rows), BF16),
            vm((n_rows, n_seq), BF16), vm((half, n_batch * n_seq), BF16), vm((n_seq, n_rows), BF16),
            vm((head_dim, n_seq), BF16), vm((head_dim, n_seq), BF16), vm((n_seq, head_dim), F32), vm((n_seq, head_dim), F32),
            vm((quarter, n_seq), F32), vm((quarter, n_seq), F32), vm((3, n_tok, head_dim), F32), vm((n_dev, n_batch, seq), jnp.int32),
            vm((2, seq, n_rows), BF16), vm((2, half, n_tok), BF16),
            vm((n_batch, n_dev, seq, cols), BF16), vm((2, 8, width), F32), vm((n_dev, 2, width), F32),
            dma((13,)), dma((13,)), dma((13,)), dma((13,)), dma((9,)), dma((n_dev + 2,)), dma((9,)), dma((n_dev + 2,)), dma((n_dev,)), dma((n_dev,)), dma((2,)),
            dma((2, chips)), dma((2, chips)), dma((2, 3)), dma((2, 3)), dma((1 + 4 * chips,)), dma((1 + 4 * chips,)), dma((n_dev,)), dma((n_dev,)),
            dma((1 + n_dev,)), dma((3,)), dma((n_batch * n_dev,)), dma((W_SLOTS, 2)), dma((4, n_batch, 2)),
        ],
        compiler_params=pltpu.CompilerParams(collective_id=0, has_side_effects=True, vmem_limit_bytes=VMEM_LIMIT),
        cost_estimate=pl.CostEstimate(flops=10 ** 11, bytes_accessed=10 ** 8, transcendentals=0),
        name='block',
    )(gain, bias, positions, freq, x.reshape(n_tok, width), dy, wq, wk, wv, wo)[:len(shapes)]


def settle_body(n, *refs):
    sems = refs[2 * n]
    copies = []
    for i in range(n):
        src, dst = refs[i], refs[n + i]
        pieces = max(p for p in range(1, SETTLE + 1) if src.shape[0] % p == 0) if len(src.shape) > 1 else 1
        size = src.shape[0] // pieces
        for p in range(pieces):
            copies.append(pltpu.make_async_copy(src.at[pl.ds(p * size, size)], dst.at[pl.ds(p * size, size)], sems.at[i, p]))
    for copy in copies:
        copy.start()
    for copy in copies:
        copy.wait()


def settle(arrays):
    n = len(arrays)
    return pl.pallas_call(
        functools.partial(settle_body, n),
        out_shape=tuple(sds(t.shape, t.dtype) for t in arrays),
        in_specs=[ANY] * n,
        out_specs=(HBM,) * n,
        scratch_shapes=[pltpu.SemaphoreType.DMA((n, SETTLE))],
        compiler_params=pltpu.CompilerParams(vmem_limit_bytes=1024 * 1024),
        name='settle',
    )(*arrays)


def solution(mesh):
    n_dev = mesh.shape['cp']

    def device_step(x_act, d_out, positions, ln_gain, ln_bias, w_query, w_key, w_value, w_out):
        n_batch, seq, width = x_act.shape
        q_heads, (kv_heads, head_dim) = w_query.shape[1], w_key.shape[1:]
        group = q_heads // kv_heads
        quarter = head_dim // 4
        assert n_batch == CORES and n_dev // CORES == kv_heads == 4 and q_heads * head_dim == width

        freq = np.exp(np.arange(quarter) * (-2.0 * math.log(ROPE_BASE) / (head_dim // 2))).astype(np.float32).reshape(quarter, 1)
        by_head = lambda t: jnp.transpose(t, (1, 0, 2))
        by_row = lambda t: t.reshape(width * kv_heads, head_dim)
        wq = by_head(w_query)

        results = whole_block(n_dev, x_act, ln_gain, ln_bias, positions, jnp.asarray(freq), d_out, wq, by_row(w_key), by_row(w_value), w_out)
        out, dx, dwq, dwk, dwv, dwo, dgain, dbias = settle(results)
        kv_rows = lambda t: t.reshape(width // n_dev, kv_heads, head_dim)
        return (out.reshape(x_act.shape), dx.reshape(x_act.shape), by_head(dwq), kv_rows(dwk), kv_rows(dwv), dwo, dgain, dbias)

    return jax.shard_map(device_step, mesh=mesh, in_specs=(P('dp', 'cp', None), P('dp', 'cp', None), P('dp', 'cp'), P(None), P(None), P(None, None, None), P(None, None, None), P(None, None, None), P(None, None)), out_specs=(P('dp', 'cp', None), P('dp', 'cp', None), P(('dp', 'cp'), None, None), P(('dp', 'cp'), None, None), P(('dp', 'cp'), None, None), P(('dp', 'cp'), None), P('dp'), P('dp')), check_vma=False)
```

```python
import functools
import math
import jax
import jax.numpy as jnp
import numpy as np
from jax import lax
from jax.experimental import pallas as pl
from jax.experimental.pallas import tpu as pltpu
from jax.sharding import PartitionSpec as P

EPS = 1e-5
ROPE_BASE = 10000.0
BF16 = jnp.bfloat16
F32 = jnp.float32
VMEM_LIMIT = 46 * 1024 * 1024
NT = (((1,), (1,)), ((), ()))
ANY = pl.BlockSpec(memory_space=pl.ANY)
VM = pl.BlockSpec(memory_space=pltpu.VMEM)
HBM = pl.BlockSpec(memory_space=pltpu.HBM)
CORES = 2
COL_TILE = 512
OUT_TILE = 256
ROWS = 16
W_SLOTS = 4
W_ROWS = 512
SETTLE = 4


def dot(a, b):
    return jnp.dot(a, b, preferred_element_type=F32)


def dot_nt(a, b):
    return lax.dot_general(a, b, NT, preferred_element_type=F32)


def sds(shape, dtype):
    return jax.ShapeDtypeStruct(shape, dtype)


def block(i, size):
    return pl.ds(pl.multiple_of(i * size, size), size)


class Place:
    def __init__(self, n_dev):
        self.n_dev = n_dev
        self.chips = n_dev // CORES
        self.me = lax.axis_index('cp')
        self.chip = self.me // CORES
        self.core = self.me % CORES
        self.partner = self.chip * CORES + 1 - self.core

    def ring(self, step):
        return lax.rem(self.chip + self.chips + step, self.chips)

    def dev(self, step, core):
        return self.ring(step) * CORES + core

    def peers(self, far):
        near = [self.partner] + [self.dev(s, c) for s in (1, -1) for c in range(CORES)]
        return near + ([self.dev(2, c) for c in range(CORES)] if far else [])


def send(src, dst, ssem, rsem, to):
    return pltpu.make_async_remote_copy(src_ref=src, dst_ref=dst, send_sem=ssem, recv_sem=rsem, device_id={'cp': to}, device_id_type=pl.DeviceIdType.MESH)


def meet(peers):
    barrier = pltpu.get_barrier_semaphore()
    for peer in peers:
        pl.semaphore_signal(barrier, inc=1, device_id={'cp': peer}, device_id_type=pl.DeviceIdType.MESH)
    pl.semaphore_wait(barrier, len(peers))


class Ring:
    def __init__(self, n, slots, copies):
        self.n, self.slots, self.copies = n, slots, copies

    def prime(self):
        for s in range(self.slots):
            for copy in self.copies(s, s):
                copy.start()

    def run(self, use):
        @pl.loop(0, self.n)
        def _(s):
            slot = lax.rem(s, self.slots)
            for copy in self.copies(s, slot):
                copy.wait()
            use(s, slot)

            @pl.when(s + self.slots < self.n)
            def _():
                for copy in self.copies(s + self.slots, slot):
                    copy.start()


class Gather:
    def __init__(self, at, own, piece, both, ssem, rsem):
        steps = (1, -1)
        origin = [at.dev(-1, at.core), at.dev(1, at.core)]
        far = at.dev(2, at.core)
        link = lambda i, src, dst, to: send(src, dst, ssem.at[i], rsem.at[i], to)
        self.first = [link(b, own(b), piece(at.me, b), at.dev(steps[b], at.core)) for b in range(2)]
        self.second = [link(2 + b, own(1 - b), piece(at.me, 1 - b), at.dev(steps[b], at.core)) for b in range(2)]
        self.again = [link(4 + b, piece(origin[b], b), piece(origin[b], b), at.dev(steps[b], at.core)) for b in range(2)]
        self.own_across = link(6, both(None), both(at.me), at.partner)
        self.first_across = [link(7 + b, piece(origin[b], b), piece(origin[b], b), at.partner) for b in range(2)]
        self.second_across = [link(9 + b, piece(origin[b], 1 - b), piece(origin[b], 1 - b), at.partner) for b in range(2)]
        self.far_across = [link(11 + b, piece(far, b), piece(far, b), at.partner) for b in range(2)]

    def start_first(self):
        for copy in self.first + [self.own_across]:
            copy.start()

    def start_second(self):
        for copy in self.second:
            copy.start()

    def pass_on(self):
        for copy, again, across in zip(self.first, self.again, self.first_across):
            copy.wait_recv()
            again.start()
            across.start()

    def share_second(self):
        for copy, across in zip(self.second, self.second_across):
            copy.wait_recv()
            across.start()

    def share_far(self):
        for copy, across in zip(self.again, self.far_across):
            copy.wait_recv()
            across.start()

    def wait_near(self):
        for copy in self.first_across + self.second_across:
            copy.wait_recv()

    def wait_far(self):
        for copy in self.far_across:
            copy.wait_recv()

    def sent(self):
        return self.first + self.second + self.again + [self.own_across] + self.first_across + self.second_across + self.far_across


class Exchange:
    def __init__(self, at, src, dst, relay, ssem, rsem):
        self.at, self.src, self.dst, self.relay, self.ssem, self.rsem = at, src, dst, relay, ssem, rsem
        near = [(0, 1 - at.core)] + [(s, c) for s in (1, -1) for c in range(CORES)]
        n = at.n_dev
        self.near = [send(src(at.dev(s, c)), dst(at.me), ssem.at[i], rsem.at[at.me], at.dev(s, c)) for i, (s, c) in enumerate(near)]
        self.far = [send(src(at.dev(2, i)), relay.at[i], ssem.at[5 + i], rsem.at[n + i], at.dev(step, at.core)) for i, step in enumerate((1, -1))]
        self.on = [send(relay.at[i], dst(at.dev(-step, at.core)), ssem.at[7 + i], rsem.at[at.dev(-step, at.core)], at.dev(step, i)) for i, step in enumerate((1, -1))]

    def start(self):
        for copy in self.far + self.near:
            copy.start()

    def pass_on(self):
        for far, on in zip(self.far, self.on):
            far.wait_recv()
            on.start()

    def wait_recv(self):
        at = self.at
        for j in range(1, at.n_dev):
            origin = lax.rem(at.me + j, at.n_dev)
            send(self.src(at.me), self.dst(origin), self.ssem.at[0], self.rsem.at[origin], at.partner).wait_recv()

    def wait_send(self):
        for copy in self.far + self.near + self.on:
            copy.wait_send()


def layer_norm(x):
    cen = x - jnp.mean(x, axis=-1, keepdims=True)
    inv = lax.rsqrt(jnp.mean(cen * cen, axis=-1, keepdims=True) + EPS)
    return cen * inv, inv


def block_body(n_dev, group, gain_hbm, bias_hbm, pos_hbm, freq_hbm, x_hbm, dy_ref, wq_ref, wk_ref, wv_ref, wo_ref,
               out_ref, dx_ref, dwq_ref, dwk_ref, dwv_ref, dwo_ref, dgain_ref, dbias_ref, dy_all, ht_all, g_all, wkv_all,
               h_ref, ht_ref, g_ref, q_ref, at_ref, at2_ref, da_ref, kt_ref, vt_ref, dk_ref, dv_ref,
               cost_ref, sint_ref, tab_ref, spot_ref, gain_ref, bias_ref, freq_ref, relay_q, relay_h, far_ref, part_ref, all_ref,
               dy_ssem, dy_rsem, kv_ssem, kv_rsem, q_ssem, q_rsem, h_ssem, h_rsem, p_ssem, p_rsem, t_sem,
               x_ssem, x_rsem, loc_sem, mix_sem, lhs_sem, w_sem, job_sem):
    at = Place(n_dev)
    n_batch, seq, width = dy_ref.shape
    n_tok = n_batch * seq
    head_dim = wq_ref.shape[2]
    cols = (group + 2) * head_dim
    n_rows = group * head_dim
    half = n_rows // CORES
    n_seq = n_dev * seq
    quarter = head_dim // 4
    scale = head_dim ** -0.5
    chips = at.chips
    tile = CORES * seq
    core, me = at.core, at.me
    steps = (1, -1)
    origin = [at.dev(-1, core), at.dev(1, core)]
    far_dev = at.dev(2, core)
    scope = jax.named_scope

    with scope('meet'):
        meet(at.peers(True))

    kv_cols = 2 * head_dim * chips
    kv_piece = lambda d, b: far_ref.at[b, d, :, pl.ds(0, kv_cols)]
    kv_both = lambda d: far_ref.at[:, me if d is None else d, :, pl.ds(0, kv_cols)]
    dys = Gather(at, lambda b: dy_ref.at[b], lambda d, b: dy_all.at[d, b], lambda d: dy_ref if d is None else dy_all.at[d], dy_ssem, dy_rsem)
    kvs = Gather(at, lambda b: kv_piece(me, b), kv_piece, kv_both, kv_ssem, kv_rsem)
    q_part = pl.ds(0, n_rows)
    queries = Exchange(at, lambda d: g_ref.at[d, :, q_part], lambda d: q_ref.at[d], relay_q, q_ssem, q_rsem)
    hcols = Exchange(at, lambda d: ht_ref.at[block(d, half)], lambda d: ht_all.at[d], relay_h, h_ssem, h_rsem)
    heads_across = send(at_ref.at[block(1 - core, half)], at2_ref.at[:, block(core, n_seq)], t_sem.at[0], t_sem.at[1], at.partner)
    spots = [send(pos_hbm, spot_ref.at[me], p_ssem.at[j], p_rsem.at[me], peer) for j, peer in enumerate(at.peers(True))]

    dys.start_first()
    x_in = pltpu.make_async_copy(x_hbm, dx_ref, loc_sem.at[1])
    x_in.start()
    for copy in spots:
        copy.start()
    small = [pltpu.make_async_copy(src, dst, loc_sem.at[2 + n]) for n, (src, dst) in enumerate(((gain_hbm, gain_ref), (bias_hbm, bias_ref), (freq_hbm, freq_ref), (pos_hbm, spot_ref.at[me])))]
    for copy in small:
        copy.start()
    for copy in small:
        copy.wait()

    freq = freq_ref[...]
    for b in range(n_batch):
        angle = freq * spot_ref[me, b:b + 1, :].astype(F32)
        cos, sin, none = jnp.cos(angle), jnp.sin(angle), jnp.zeros((quarter, seq), F32)
        rest = jnp.zeros((head_dim - 2 * quarter, seq), F32)
        for i, rows in enumerate(([cos, cos, rest + 1.0], [-sin, none, rest], [none, sin, rest])):
            tab_ref[i, b * seq:(b + 1) * seq, :] = jnp.concatenate(rows, axis=0).T

    gain = (1.0 + gain_ref[...]).reshape(1, width)
    bias = bias_ref[...].reshape(1, width)

    def project_all(wkv_ref, raw_ref, wq_vm, raw_sem, wq_sem, stage_sem):
        pieces = [(b, i) for b in range(n_batch) for i in range(width // n_rows)]
        there = lambda n: da_ref.at[pl.ds(n * seq, seq)]
        dy_in = [pltpu.make_async_copy(dy_ref.at[b, :, pl.ds(i * n_rows, n_rows)], there(n), stage_sem.at[n]) for n, (b, i) in enumerate(pieces)]
        dy_keep = [pltpu.make_async_copy(there(n), dy_all.at[me, b, :, pl.ds(i * n_rows, n_rows)], stage_sem.at[n]) for n, (b, i) in enumerate(pieces)]
        span = 64 * chips
        batch = raw_ref.shape[2] // span
        row = lax.broadcasted_iota(jnp.int32, (span, span), 0)
        col = lax.broadcasted_iota(jnp.int32, (span, span), 1)
        pick = jnp.where(col == lax.rem(row, 64) * chips + lax.div(row, 64), 1.0, 0.0).astype(BF16)

        def raw_in(s, slot):
            return [pltpu.make_async_copy(w.at[block(s, span * batch)], raw_ref.at[slot, i], raw_sem.at[slot, i]) for i, w in enumerate((wk_ref, wv_ref))]

        def wq_in(s, slot):
            return [pltpu.make_async_copy(wq_ref.at[block(s, 2)], wq_vm.at[slot], wq_sem.at[slot])]

        def part_heads(s, slot):
            for i in range(batch):
                sl = slice(i * span, (i + 1) * span)
                rows = dot(pick, jnp.concatenate([raw_ref[slot, 0, sl, :], raw_ref[slot, 1, sl, :]], axis=1)).astype(BF16)
                for n in range(chips):
                    wkv_ref[n, block(s * batch + i, 64), :] = rows[n * 64:(n + 1) * 64]

        def turned(v):
            return v * tab_ref[0] + pltpu.roll(v, head_dim - quarter, 1) * tab_ref[1] + pltpu.roll(v, quarter, 1) * tab_ref[2]

        def project(s, slot):
            y = dot(h_ref[...], jnp.concatenate([wq_vm[slot, 0], wq_vm[slot, 1]], axis=1))
            for i in range(2):
                head = s * 2 + i
                v = turned(y[:, i * head_dim:(i + 1) * head_dim]).astype(BF16)
                for b in range(n_batch):
                    g_ref[lax.div(head, group) * n_batch + b, :, block(lax.rem(head, group), head_dim)] = v[b * seq:(b + 1) * seq]

        kv_ring = Ring(width // (64 * batch), raw_ref.shape[0], raw_in)
        q_ring = Ring(chips * group // 2, wq_vm.shape[0], wq_in)
        kv_ring.prime()
        q_ring.prime()
        for copy in dy_in:
            copy.start()
        x_in.wait()
        with scope('norm'):
            @pl.loop(0, n_tok // (2 * ROWS))
            def _(step):
                for i in range(2):
                    sl = block(2 * step + i, ROWS)
                    hat, _ = layer_norm(dx_ref[sl, :].astype(F32))
                    h_ref[sl, :] = (hat * gain + bias).astype(BF16)

        with scope('heads_kv'):
            kv_ring.run(part_heads)
        keep = pltpu.make_async_copy(wkv_ref, wkv_all, mix_sem.at[2])
        keep.start()
        for come, go in zip(dy_in, dy_keep):
            come.wait()
            go.start()
        with scope('project_kv'):
            @pl.loop(0, chips)
            def _(n):
                y = dot(h_ref[...], wkv_ref[n])
                v = jnp.concatenate([turned(y[:, :head_dim]), y[:, head_dim:]], axis=1).astype(BF16)
                for b in range(n_batch):
                    far_ref[b, me, :, block(n, 2 * head_dim)] = v[b * seq:(b + 1) * seq]

        kvs.start_first()
        kvs.start_second()
        with scope('project_q'):
            q_ring.run(project)
        keep.wait()
        for copy in dy_keep:
            copy.wait()

    pl.run_scoped(
        project_all,
        pltpu.VMEM((chips, width, 2 * head_dim), BF16),
        pltpu.VMEM((3, 2, 4 * 64 * chips, head_dim), BF16), pltpu.VMEM((4, 2, width, head_dim), BF16),
        pltpu.SemaphoreType.DMA((3, 2)), pltpu.SemaphoreType.DMA((4,)), pltpu.SemaphoreType.DMA((n_batch * width // n_rows,)),
    )

    with scope('kv_pass'):
        kvs.pass_on()
    queries.start()
    q_ref[me] = g_ref[me, :, q_part]
    with scope('turn_h'):
        @pl.loop(0, width // 128)
        def _(step):
            sl = block(step, 128)
            ht_ref[sl, :] = h_ref[:, sl].T

    with scope('kv_wait'):
        kvs.share_second()
        kvs.share_far()
        kvs.own_across.wait_recv()
        kvs.wait_near()
        kvs.wait_far()

    def chip_at(i):
        return at.ring(jnp.where(i == 0, 0, jnp.where(i == 1, 1, jnp.where(i == 2, 3, 2))))

    def soft(s, seen):
        s = s * scale
        clear = s.shape[0] - seen.shape[0]
        tail = jnp.where(seen, s[clear:], -1e30)
        s = tail if clear == 0 else jnp.concatenate([s[:clear], tail], axis=0)
        e = jnp.exp(s - jnp.max(s, axis=0, keepdims=True))
        return e * (1.0 / jnp.sum(e, axis=0, keepdims=True))

    def attend(limit, clear):
        @pl.loop(0, n_batch * chips)
        def _(i):
            @pl.when(i == 1)
            def _():
                with scope('q_pass'):
                    queries.pass_on()
                dys.start_second()
                dys.pass_on()
                hcols.start()

            b, n = lax.rem(i, n_batch), lax.div(i, n_batch)
            k = far_ref[b, 0:limit // seq, :, block(2 * n, head_dim)].reshape(limit, head_dim)
            vt = far_ref[b, 0:limit // seq, :, block(2 * n + 1, head_dim)].reshape(limit, head_dim).T
            q = jnp.concatenate([g_ref[n * n_batch + b, :, block(j, head_dim)] for j in range(group)], axis=0)
            row = lax.broadcasted_iota(jnp.int32, (limit - clear, n_rows), 0)
            col = lax.broadcasted_iota(jnp.int32, (limit - clear, n_rows), 1)
            p = soft(dot_nt(k, q), row <= lax.rem(col, seq) + (me * seq - clear))
            mixed = dot(vt, p.astype(BF16)).astype(BF16)
            for j in range(group):
                h_ref[block(b, seq), block(n * group + j, head_dim)] = mixed[:, j * seq:(j + 1) * seq].T

    with scope('attend'):
        @pl.when(at.chip == chips - 1)
        def _():
            attend(chips * tile, (chips - 1) * tile)

        @pl.when(at.chip < chips - 1)
        def _():
            attend((chips - 1) * tile, 0)

    h_keep = pltpu.make_async_copy(ht_ref.at[block(me, half)], ht_all.at[me], loc_sem.at[1])
    h_keep.start()

    def block_out():
        def stream(wo_vm, sem):
            def wo_in(s, slot):
                return [pltpu.make_async_copy(wo_ref.at[:, block(s, OUT_TILE)], wo_vm.at[slot], sem.at[slot])]

            def out_tile(s, slot):
                sl = block(s, OUT_TILE)
                out_ref[:, sl] = (dx_ref[:, sl].astype(F32) + dot(h_ref[...], wo_vm[slot])).astype(BF16)

            ring = Ring(width // OUT_TILE, wo_vm.shape[0], wo_in)
            ring.prime()
            ring.run(out_tile)

        with scope('output'):
            pl.run_scoped(stream, pltpu.VMEM((4, width, OUT_TILE), BF16), pltpu.SemaphoreType.DMA((4,)))

    k_all = lambda n: far_ref[core, 0:n, :, block(2 * at.chip, head_dim)].reshape(n * seq, head_dim)
    v_all = lambda n: far_ref[core, 0:n, :, block(2 * at.chip + 1, head_dim)].reshape(n * seq, head_dim)

    def rotate_back(t, cos, sin):
        u, w = t[:quarter], t[quarter:2 * quarter]
        return jnp.concatenate([u * cos + w * sin, w * cos - u * sin, t[2 * quarter:]], axis=0)

    def by_dev(t):
        return t.astype(BF16).reshape(t.shape[0] // seq, seq, head_dim)

    def attend_back(t, i):
        limit = (t + 1) * tile
        sl = slice(t * tile, limit)
        devs = slice(t * CORES, (t + 1) * CORES)

        def heads(first, count):
            each = range(count)
            q = jnp.concatenate([q_ref[devs, :, block(first + j, head_dim)].reshape(tile, head_dim) for j in each], axis=0)
            da = jnp.concatenate([da_ref[sl, block(first + j, head_dim)] for j in each], axis=0)
            k, v = k_all(limit // seq), v_all(limit // seq)
            row = lax.broadcasted_iota(jnp.int32, (tile, count * tile), 0)
            col = lax.broadcasted_iota(jnp.int32, (tile, count * tile), 1)
            p = soft(dot_nt(k, q), row <= lax.rem(col, tile))
            p_low = p.astype(BF16)
            mixed = dot(vt_ref[:, :limit], p_low).astype(BF16)
            dp = dot_nt(v, da)
            row_dot = jnp.sum(p * dp, axis=0, keepdims=True)
            ds = (p * (dp - row_dot) * scale).astype(BF16)
            dv_ref[:limit, :] += dot(p_low, da)
            dk_ref[:limit, :] += dot(ds, q)
            back = dot(kt_ref[:, :limit], ds)
            for j in each:
                part = slice(j * tile, (j + 1) * tile)
                at_ref[block(first + j, head_dim), sl] = mixed[:, part]
                g_ref[devs, :, block(first + j, head_dim)] = by_dev(rotate_back(back[:, part], cost_ref[:, sl], sint_ref[:, sl]).T)

        @pl.loop(0, group // 2)
        def _(j):
            heads(2 * j, 2)

        @pl.when(i == chips - 2)
        def _():
            with scope('dy_far'):
                dys.share_far()

        heads(group - 1, 1)

    def middle(wo_vm, dyk):
        wo_in = pltpu.make_async_copy(wo_ref.at[block(at.chip, n_rows)], wo_vm, mix_sem.at[2])
        wo_in.start()
        for j in range(1, n_dev):
            source = lax.rem(me + j, n_dev)
            send(pos_hbm, spot_ref.at[source], p_ssem.at[0], p_rsem.at[source], at.partner).wait_recv()
        for d in range(n_dev):
            angle = freq * spot_ref[d, pl.ds(core, 1), :].astype(F32)
            cost_ref[:, d * seq:(d + 1) * seq] = jnp.cos(angle)
            sint_ref[:, d * seq:(d + 1) * seq] = jnp.sin(angle)
        with scope('q_wait'):
            queries.wait_recv()
            queries.wait_send()
            for copy in kvs.sent() + spots:
                copy.wait_send()
        kt_ref[...] = k_all(n_dev).T
        vt_ref[...] = v_all(n_dev).T
        dk_ref[...] = jnp.zeros_like(dk_ref)
        dv_ref[...] = jnp.zeros_like(dv_ref)
        dys.own_across.wait_recv()

        def fetch(i, slot):
            return pltpu.make_async_copy(dy_all.at[block(chip_at(i), CORES), core], dyk.at[slot], mix_sem.at[slot])

        with scope('wo_wait'):
            fetch(0, 0).start()
            wo_in.wait()

        @pl.loop(0, chips)
        def _(i):
            slot = lax.rem(i, 2)

            @pl.when((i == 1) & (at.chip < chips - 1))
            def _():
                block_out()

            @pl.when(i == 1)
            def _():
                with scope('dy_wait'):
                    dys.share_second()
                    dys.wait_near()
                fetch(i, slot).start()

            @pl.when(i == chips - 1)
            def _():
                with scope('dy_far2'):
                    dys.wait_far()
                fetch(i, slot).start()
                with scope('h_pass'):
                    hcols.pass_on()

            fetch(i, slot).wait()

            @pl.when((i > 0) & (i < chips - 2))
            def _():
                fetch(i + 1, 1 - slot).start()

            chip = chip_at(i)
            with scope('da'):
                da_ref[block(chip, tile), :] = dot_nt(dyk[slot].reshape(tile, width), wo_vm[...]).astype(BF16)
            with scope('attend_back'):
                for t in range(chips):
                    @pl.when(chip == t)
                    def _(t=t):
                        attend_back(t, i)

    pl.run_scoped(middle, pltpu.VMEM((n_rows, width), BF16), pltpu.VMEM((2, CORES, seq, width), BF16))
    heads_across.start()
    g_ref[:, :, n_rows:n_rows + head_dim] = by_dev(rotate_back(dk_ref[...].T, cost_ref[...], sint_ref[...]).T)
    g_ref[:, :, n_rows + head_dim:] = by_dev(dv_ref[...])

    def span_of(q):
        return block(q, CORES)

    turn = [[at.ring(q) for q in (2, 1, 3, 0)], [at.ring(q) for q in (3, 0, 1, 2)]]
    direct = [[send(g_ref.at[span_of(turn[i][q])], g_all.at[me, span_of(turn[i][q])], kv_ssem.at[i * chips + q], kv_rsem.at[i * chips + q], at.dev(steps[i], core)) for q in range(chips)] for i in range(2)]
    came = [[at.ring(q) for q in (1, 0, 2, 3)], [at.ring(q) for q in (0, 1, 2, 3)]]
    def halves_of(quarters):
        return [span_of(quarters[0])] + [pl.ds(quarters[1] * CORES + c, 1) for c in range(CORES)]

    onward = [[send(g_all.at[origin[i], sl], far_ref.at[core, sl], q_ssem.at[3 * i + q], q_rsem.at[3 * i + q], at.dev(steps[i], core)) for q, sl in enumerate(halves_of(came[i]))] for i in range(2)]
    ends = [[at.ring(q) for q in (0, 3)], [at.ring(q) for q in (1, 2)]]
    g_across = send(g_ref, g_all.at[me], x_ssem.at[0], x_rsem.at[0], at.partner)
    near_across = [[send(g_all.at[origin[i], span_of(came[i][q])], g_all.at[origin[i], span_of(came[i][q])], x_ssem.at[1 + i * chips + q], x_rsem.at[1 + i * chips + q], at.partner) for q in range(chips)] for i in range(2)]
    end_across = [[send(far_ref.at[core, sl], far_ref.at[core, sl], x_ssem.at[1 + 2 * chips + 3 * i + q], x_rsem.at[1 + 2 * chips + 3 * i + q], at.partner) for q, sl in enumerate(halves_of(ends[i]))] for i in range(2)]
    for q in range(chips):
        for i in range(2):
            direct[i][q].start()
    g_across.start()
    g_keep = pltpu.make_async_copy(g_ref, g_all.at[me], loc_sem.at[0])
    g_keep.start()
    at2_ref[:, block(core, n_seq)] = at_ref[block(core, half), :]

    @pl.when(at.chip == chips - 1)
    def _():
        block_out()

    dy_back = [pltpu.make_async_copy(dy_ref.at[b], h_ref.at[pl.ds(b * seq, seq)], loc_sem.at[2 + b]) for b in range(n_batch)]
    for copy in dy_back:
        copy.start()

    def wo_rows(dy_vm, sem):
        def dy_tile(s, slot):
            return [pltpu.make_async_copy(dy_all.at[:, :, :, block(s, COL_TILE)], dy_vm.at[slot], sem.at[slot])]

        def wo_tile(s, slot):
            pieces = [dy_vm[slot, d, b] for b in range(n_batch) for d in range(n_dev)]
            dwo_ref[:, block(s, COL_TILE)] = dot(at2_ref[...], jnp.concatenate(pieces, axis=0))

        ring = Ring(width // COL_TILE, dy_vm.shape[0], dy_tile)
        ring.prime()
        with scope('heads_wait'):
            heads_across.wait_recv()
        with scope('grad_wo'):
            ring.run(wo_tile)

    pl.run_scoped(wo_rows, pltpu.VMEM((4, n_dev, n_batch, seq, COL_TILE), BF16), pltpu.SemaphoreType.DMA((4,)))

    with scope('h_wait'):
        hcols.wait_recv()
    h_keep.wait()
    lhs_in = [pltpu.make_async_copy(ht_all.at[d, :, pl.ds(b * seq, seq)], at2_ref.at[:, pl.ds((b * n_dev + d) * seq, seq)], lhs_sem.at[0]) for d in range(n_dev) for b in range(n_batch)]
    for copy in lhs_in:
        copy.start()
    with jax.named_scope('own_wait'):
        pltpu.make_async_copy(at2_ref, at2_ref, lhs_sem.at[0]).wait()
        g_keep.wait()
        g_across.wait_recv()
    sums = [send(all_ref.at[me], all_ref.at[me], p_ssem.at[j], p_rsem.at[me], peer) for j, peer in enumerate(at.peers(True))]

    def weight_grads(wq_vm, wkv_vm, acc_ref, hat_ref, inv_ref, job_ref, mine_ref):
        n_slots = wq_vm.shape[0]
        chunk = wq_vm.shape[2]
        n_chunks = width // chunk
        total = n_chunks * chips

        def weights(s):
            slot = lax.rem(s, n_slots)
            chip = chip_at(lax.div(s, n_chunks))
            rows = block(lax.rem(s, n_chunks), chunk)
            return [
                pltpu.make_async_copy(wq_ref.at[block(chip, group), rows], wq_vm.at[slot], w_sem.at[slot, 0]),
                pltpu.make_async_copy(wkv_all.at[chip, rows], wkv_vm.at[slot], w_sem.at[slot, 1]),
            ]

        for s in range(n_slots):
            for copy in weights(s):
                copy.start()

        def grow(i, read):
            @pl.loop(0, n_chunks)
            def _(n):
                s = i * n_chunks + n
                slot = lax.rem(s, n_slots)
                for copy in weights(s):
                    copy.wait()
                rows = jnp.concatenate([read(b) for b in range(n_batch)], axis=0)
                part = dot_nt(rows, jnp.concatenate([wq_vm[slot, j] for j in range(group)] + [wkv_vm[slot]], axis=1))
                sl = block(n, chunk)

                @pl.when(i == 0)
                def _():
                    acc_ref[:, sl] = part

                @pl.when(i > 0)
                def _():
                    acc_ref[:, sl] += part

                @pl.when(s + n_slots < total)
                def _():
                    for copy in weights(s + n_slots):
                        copy.start()

        def mine_in(i):
            return [pltpu.make_async_copy(g_all.at[chip_at(i) * CORES + b, me], mine_ref.at[lax.rem(i, 2), b], job_sem.at[2 + lax.rem(i, 2)]) for b in range(n_batch)]

        def grow_near(i):
            here = mine_ref.at[lax.rem(i, 2)]
            pltpu.make_async_copy(here, here, job_sem.at[2 + lax.rem(i, 2)]).wait()
            grow(i, lambda b: mine_ref[lax.rem(i, 2), b])

        def job_in(chip, quarters, slot):
            return [pltpu.make_async_copy(g_all.at[chip * CORES + b, span_of(q)], job_ref.at[slot, b, n], job_sem.at[slot]) for b in range(n_batch) for n, q in enumerate(quarters)]

        def job(chip, pieces, read, add):
            lhs = [at2_ref[:, pl.ds(pl.multiple_of(b * n_seq + d * seq, seq), seq)] for b in range(n_batch) for d in pieces]
            rhs = [read(b, n) for b in range(n_batch) for n in range(len(pieces))]
            y = dot(jnp.concatenate(lhs, axis=1), jnp.concatenate(rhs, axis=0))
            for j in range(group):
                v = y[:, j * head_dim:(j + 1) * head_dim]
                dwq_ref[chip * group + j] = dwq_ref[chip * group + j] + v if add else v
            for j, ref in enumerate((dwk_ref, dwv_ref)):
                v = y[:, (group + j) * head_dim:(group + j + 1) * head_dim]
                rows = pl.ds(chip, half, stride=chips)
                ref[rows, :] = ref[rows, :] + v if add else v

        def devs_of(quarters):
            return [q * CORES + c for q in quarters for c in range(CORES)]

        def near_pair(quarters, add):
            for slot, step in enumerate(steps):
                for copy in job_in(at.ring(step), quarters, slot):
                    copy.start()

            @pl.loop(0, 2)
            def _(slot):
                chip = at.ring(1 - 2 * slot)
                pltpu.make_async_copy(job_ref.at[slot], job_ref.at[slot], job_sem.at[slot]).wait()
                job(chip, devs_of(quarters), lambda b, n: job_ref[slot, b, n // CORES, n % CORES], add)

        halves = [[at.ring(q) for q in half_of] for half_of in ((0, 1), (2, 3))]
        for slot in range(2):
            for copy in job_in(at.chip, [at.ring(2 * slot), at.ring(2 * slot + 1)], slot):
                copy.start()
        for copy in mine_in(0):
            copy.start()
        with jax.named_scope('own_job'):
            for slot in range(2):
                quarters = [at.ring(2 * slot), at.ring(2 * slot + 1)]
                pltpu.make_async_copy(job_ref.at[slot], job_ref.at[slot], job_sem.at[slot]).wait()
                job(at.chip, devs_of(quarters), lambda b, n: job_ref[slot, b, n // CORES, n % CORES], slot == 1)

        with jax.named_scope('own_dh'):
            grow_near(0)

        with jax.named_scope('d01_wait'):
            for q in range(2):
                for i in range(2):
                    direct[i][q].wait_recv()
                for i in range(2):
                    for copy in onward[i][:1] if q == 0 else onward[i][1:]:
                        copy.start()
                    near_across[i][q].start()
        with jax.named_scope('d01_across'):
            for q in range(2):
                for i in range(2):
                    near_across[i][q].wait_recv()
        for i in (1, 2):
            for copy in mine_in(i):
                copy.start()
        with scope('near_dh'):
            @pl.loop(1, chips - 1)
            def _(i):
                grow_near(i)

        with jax.named_scope('near_a'):
            near_pair(halves[0], False)
        with scope('d2_wait'):
            for i in range(2):
                direct[i][2].wait_recv()
                near_across[i][2].start()
        with jax.named_scope('hat'):
            @pl.loop(0, n_tok // (2 * ROWS))
            def _(step):
                for i in range(2):
                    sl = block(2 * step + i, ROWS)
                    hat, inv = layer_norm(dx_ref[sl, :].astype(F32))
                    hat_ref[sl, :] = hat
                    inv_ref[sl, :] = jnp.broadcast_to(inv, (ROWS, 128))

        with scope('d3_wait'):
            for i in range(2):
                direct[i][3].wait_recv()
                near_across[i][3].start()
        with jax.named_scope('d23_across'):
            for q in range(2, chips):
                for i in range(2):
                    near_across[i][q].wait_recv()

        with jax.named_scope('near_b'):
            near_pair(halves[1], True)
        far_chip = at.ring(2)
        with jax.named_scope('far0_wait'):
            for i in range(2):
                onward[i][0].wait_recv()
                end_across[i][0].start()
        with jax.named_scope('far0_across'):
            for i in range(2):
                end_across[i][0].wait_recv()
        with jax.named_scope('far_dh'):
            grow(chips - 1, lambda b: far_ref[b, me])
        for copy in dy_back:
            copy.wait()
        part_ref[...] = jnp.zeros_like(part_ref)

        with jax.named_scope('norm_back'):
            @pl.loop(0, n_tok // (2 * ROWS))
            def _(step):
                for i in range(2):
                    sl = block(2 * step + i, ROWS)
                    hat, inv = hat_ref[sl, :], inv_ref[sl, 0:1]
                    dh = acc_ref[sl, :]
                    dg = dh * hat
                    gh = dh * gain
                    one = jnp.mean(gh, axis=-1, keepdims=True)
                    two = jnp.mean(dg * gain, axis=-1, keepdims=True)
                    dx_ref[sl, :] = (h_ref[sl, :].astype(F32) + inv * (gh - one - hat * two)).astype(BF16)
                    part_ref[0] += dg[0:8] + dg[8:16]
                    part_ref[1] += dh[0:8] + dh[8:16]

        all_ref[me, 0:1, :] = jnp.sum(part_ref[0], axis=0, keepdims=True)
        all_ref[me, 1:2, :] = jnp.sum(part_ref[1], axis=0, keepdims=True)
        for copy in sums:
            copy.start()
        def hand_on(c):
            with scope('far1_wait'):
                for i in range(2):
                    onward[i][1 + c].wait_recv()
                    end_across[i][1 + c].start()

        hand_on(0)
        with scope('far_a'):
            first_devs = devs_of([ends[0][0], ends[1][0]])
            job(far_chip, first_devs, lambda b, n: far_ref[b, first_devs[n]], False)
        for c in range(CORES):
            if c > 0:
                hand_on(c)
            with scope('far1_across'):
                for i in range(2):
                    end_across[i][1 + c].wait_recv()
            with scope('far_b'):
                last_devs = [ends[i][1] * CORES + c for i in range(2)]
                job(far_chip, last_devs, lambda b, n: far_ref[b, last_devs[n]], True)

    pl.run_scoped(
        weight_grads,
        pltpu.VMEM((W_SLOTS, group, W_ROWS, head_dim), BF16), pltpu.VMEM((W_SLOTS, W_ROWS, 2 * head_dim), BF16), pltpu.VMEM((n_tok, width), F32),
        pltpu.VMEM((n_tok, width), F32), pltpu.VMEM((n_tok, 128), F32), pltpu.VMEM((2, n_batch, 2, CORES, seq, cols), BF16), pltpu.VMEM((2, n_batch, seq, cols), BF16),
    )

    with jax.named_scope('sums'):
        for j in range(1, n_dev):
            source = lax.rem(me + j, n_dev)
            send(all_ref.at[me], all_ref.at[source], p_ssem.at[0], p_rsem.at[source], at.partner).wait_recv()
        total = all_ref[0]
        for d in range(1, n_dev):
            total = total + all_ref[d]
        dgain_ref[...] = total[0:1].reshape(width)
        dbias_ref[...] = total[1:2].reshape(width)
    done = dys.sent() + [heads_across]
    done += direct[0] + direct[1] + onward[0] + onward[1] + [g_across] + near_across[0] + near_across[1] + end_across[0] + end_across[1] + sums
    with jax.named_scope('done'):
        for copy in done:
            copy.wait_send()
        hcols.wait_send()


def whole_block(n_dev, x, gain, bias, positions, freq, dy, wq, wk, wv, wo):
    n_batch, seq, width = dy.shape
    n_tok = n_batch * seq
    head_dim = wq.shape[2]
    chips = n_dev // CORES
    group = wq.shape[0] // chips
    cols = (group + 2) * head_dim
    n_rows = group * head_dim
    half = n_rows // CORES
    n_seq = n_dev * seq
    quarter = head_dim // 4
    dma = pltpu.SemaphoreType.DMA
    vm = pltpu.VMEM
    shapes = [((n_tok, width), BF16)] * 2 + [((chips * group, half, head_dim), F32)] + [((chips * half, head_dim), F32)] * 2 + [((half, width), F32), ((width,), F32), ((width,), F32)]
    held = [((n_dev, n_batch, seq, width), BF16), ((n_dev, half, n_tok), BF16), ((n_dev, n_dev, seq, cols), BF16), ((chips, width, 2 * head_dim), BF16)]
    return pl.pallas_call(
        functools.partial(block_body, n_dev, group),
        out_shape=tuple(pltpu.VMEM(*t) for t in shapes) + tuple(sds(*t) for t in held),
        in_specs=[HBM] * 10,
        out_specs=(VM,) * len(shapes) + (HBM,) * len(held),
        scratch_shapes=[
            vm((n_tok, width), BF16), vm((width, n_tok), BF16), vm((n_dev, seq, cols), BF16), vm((n_dev, seq, n_rows), BF16),
            vm((n_rows, n_seq), BF16), vm((half, n_batch * n_seq), BF16), vm((n_seq, n_rows), BF16),
            vm((head_dim, n_seq), BF16), vm((head_dim, n_seq), BF16), vm((n_seq, head_dim), F32), vm((n_seq, head_dim), F32),
            vm((quarter, n_seq), F32), vm((quarter, n_seq), F32), vm((3, n_tok, head_dim), F32), vm((n_dev, n_batch, seq), jnp.int32), vm((width,), F32), vm((width,), F32), vm((quarter, 1), F32),
            vm((2, seq, n_rows), BF16), vm((2, half, n_tok), BF16),
            vm((n_batch, n_dev, seq, cols), BF16), vm((2, 8, width), F32), vm((n_dev, 2, width), F32),
            dma((13,)), dma((13,)), dma((13,)), dma((13,)), dma((9,)), dma((n_dev + 2,)), dma((9,)), dma((n_dev + 2,)), dma((n_dev,)), dma((n_dev,)), dma((2,)),
            dma((7 + 2 * chips,)), dma((7 + 2 * chips,)),
            dma((1 + n_dev,)), dma((3,)), dma((1,)), dma((W_SLOTS, 2)), dma((4,)),
        ],
        compiler_params=pltpu.CompilerParams(collective_id=0, has_side_effects=True, vmem_limit_bytes=VMEM_LIMIT),
        cost_estimate=pl.CostEstimate(flops=10 ** 11, bytes_accessed=10 ** 8, transcendentals=0),
        name='block',
    )(gain, bias, positions, freq, x.reshape(n_tok, width), dy, wq, wk, wv, wo)[:len(shapes)]


def settle_body(n, *refs):
    sems = refs[2 * n]
    copies = []
    for i in range(n):
        src, dst = refs[i], refs[n + i]
        pieces = max(p for p in range(1, SETTLE + 1) if src.shape[0] % p == 0) if len(src.shape) > 1 else 1
        size = src.shape[0] // pieces
        for p in range(pieces):
            copies.append(pltpu.make_async_copy(src.at[pl.ds(p * size, size)], dst.at[pl.ds(p * size, size)], sems.at[i, p]))
    for copy in copies:
        copy.start()
    for copy in copies:
        copy.wait()


def settle(arrays):
    n = len(arrays)
    return pl.pallas_call(
        functools.partial(settle_body, n),
        out_shape=tuple(sds(t.shape, t.dtype) for t in arrays),
        in_specs=[ANY] * n,
        out_specs=(HBM,) * n,
        scratch_shapes=[pltpu.SemaphoreType.DMA((n, SETTLE))],
        compiler_params=pltpu.CompilerParams(vmem_limit_bytes=1024 * 1024),
        name='settle',
    )(*arrays)


def solution(mesh):
    n_dev = mesh.shape['cp']

    def device_step(x_act, d_out, positions, ln_gain, ln_bias, w_query, w_key, w_value, w_out):
        n_batch, seq, width = x_act.shape
        q_heads, (kv_heads, head_dim) = w_query.shape[1], w_key.shape[1:]
        group = q_heads // kv_heads
        quarter = head_dim // 4
        assert n_batch == CORES and n_dev // CORES == kv_heads == 4 and q_heads * head_dim == width

        freq = np.exp(np.arange(quarter) * (-2.0 * math.log(ROPE_BASE) / (head_dim // 2))).astype(np.float32).reshape(quarter, 1)
        by_head = lambda t: jnp.transpose(t, (1, 0, 2))
        by_row = lambda t: t.reshape(width * kv_heads, head_dim)
        wq = by_head(w_query)

        results = whole_block(n_dev, x_act, ln_gain, ln_bias, positions, jnp.asarray(freq), d_out, wq, by_row(w_key), by_row(w_value), w_out)
        out, dx, dwq, dwk, dwv, dwo, dgain, dbias = settle(results)
        kv_rows = lambda t: t.reshape(width // n_dev, kv_heads, head_dim)
        return (out.reshape(x_act.shape), dx.reshape(x_act.shape), by_head(dwq), kv_rows(dwk), kv_rows(dwv), dwo, dgain, dbias)

    return jax.shard_map(device_step, mesh=mesh, in_specs=(P('dp', 'cp', None), P('dp', 'cp', None), P('dp', 'cp'), P(None), P(None), P(None, None, None), P(None, None, None), P(None, None, None), P(None, None)), out_specs=(P('dp', 'cp', None), P('dp', 'cp', None), P(('dp', 'cp'), None, None), P(('dp', 'cp'), None, None), P(('dp', 'cp'), None, None), P(('dp', 'cp'), None), P('dp'), P('dp')), check_vma=False)
```

```python
import functools
import math
import jax
import jax.numpy as jnp
import numpy as np
from jax import lax
from jax.experimental import pallas as pl
from jax.experimental.pallas import tpu as pltpu
from jax.sharding import PartitionSpec as P

EPS = 1e-5
ROPE_BASE = 10000.0
BF16 = jnp.bfloat16
F32 = jnp.float32
VMEM_LIMIT = 46 * 1024 * 1024
NT = (((1,), (1,)), ((), ()))
ANY = pl.BlockSpec(memory_space=pl.ANY)
VM = pl.BlockSpec(memory_space=pltpu.VMEM)
HBM = pl.BlockSpec(memory_space=pltpu.HBM)
CORES = 2
COL_TILE = 512
OUT_TILE = 256
ROWS = 16
W_SLOTS = 4
W_ROWS = 512
SETTLE = 4


def dot(a, b):
    return jnp.dot(a, b, preferred_element_type=F32)


def dot_nt(a, b):
    return lax.dot_general(a, b, NT, preferred_element_type=F32)


def sds(shape, dtype):
    return jax.ShapeDtypeStruct(shape, dtype)


def block(i, size):
    return pl.ds(pl.multiple_of(i * size, size), size)


class Place:
    def __init__(self, n_dev):
        self.n_dev = n_dev
        self.chips = n_dev // CORES
        self.me = lax.axis_index('cp')
        self.chip = self.me // CORES
        self.core = self.me % CORES
        self.partner = self.chip * CORES + 1 - self.core

    def ring(self, step):
        return lax.rem(self.chip + self.chips + step, self.chips)

    def dev(self, step, core):
        return self.ring(step) * CORES + core

    def peers(self, far):
        near = [self.partner] + [self.dev(s, c) for s in (1, -1) for c in range(CORES)]
        return near + ([self.dev(2, c) for c in range(CORES)] if far else [])


def send(src, dst, ssem, rsem, to):
    return pltpu.make_async_remote_copy(src_ref=src, dst_ref=dst, send_sem=ssem, recv_sem=rsem, device_id={'cp': to}, device_id_type=pl.DeviceIdType.MESH)


def all_sent(total, ssem, to):
    send(total, total, ssem, ssem, to).wait_send()


def meet(peers):
    barrier = pltpu.get_barrier_semaphore()
    for peer in peers:
        pl.semaphore_signal(barrier, inc=1, device_id={'cp': peer}, device_id_type=pl.DeviceIdType.MESH)
    pl.semaphore_wait(barrier, len(peers))


class Ring:
    def __init__(self, n, slots, copies):
        self.n, self.slots, self.copies = n, slots, copies

    def prime(self):
        for s in range(self.slots):
            for copy in self.copies(s, s):
                copy.start()

    def run(self, use):
        @pl.loop(0, self.n)
        def _(s):
            slot = lax.rem(s, self.slots)
            for copy in self.copies(s, slot):
                copy.wait()
            use(s, slot)

            @pl.when(s + self.slots < self.n)
            def _():
                for copy in self.copies(s + self.slots, slot):
                    copy.start()


class Gather:
    def __init__(self, at, own, piece, both, ssem, rsem):
        steps = (1, -1)
        origin = [at.dev(-1, at.core), at.dev(1, at.core)]
        far = at.dev(2, at.core)
        link = lambda i, src, dst, to: send(src, dst, ssem, rsem.at[i], to)
        self.first = [link(b, own(b), piece(at.me, b), at.dev(steps[b], at.core)) for b in range(2)]
        self.second = [link(2 + b, own(1 - b), piece(at.me, 1 - b), at.dev(steps[b], at.core)) for b in range(2)]
        self.again = [link(4 + b, piece(origin[b], b), piece(origin[b], b), at.dev(steps[b], at.core)) for b in range(2)]
        self.own_across = link(6, both(None), both(at.me), at.partner)
        self.first_across = [link(7 + b, piece(origin[b], b), piece(origin[b], b), at.partner) for b in range(2)]
        self.second_across = [link(9 + b, piece(origin[b], 1 - b), piece(origin[b], 1 - b), at.partner) for b in range(2)]
        self.far_across = [link(11 + b, piece(far, b), piece(far, b), at.partner) for b in range(2)]

    def start_first(self):
        for copy in self.first + [self.own_across]:
            copy.start()

    def start_second(self):
        for copy in self.second:
            copy.start()

    def pass_on(self):
        for copy, again, across in zip(self.first, self.again, self.first_across):
            copy.wait_recv()
            again.start()
            across.start()

    def share_second(self):
        for copy, across in zip(self.second, self.second_across):
            copy.wait_recv()
            across.start()

    def share_far(self):
        for copy, across in zip(self.again, self.far_across):
            copy.wait_recv()
            across.start()

    def wait_near(self):
        for copy in self.first_across + self.second_across:
            copy.wait_recv()

    def wait_far(self):
        for copy in self.far_across:
            copy.wait_recv()


class Exchange:
    def __init__(self, at, src, dst, relay, ssem, rsem):
        self.at, self.src, self.dst, self.relay, self.ssem, self.rsem = at, src, dst, relay, ssem, rsem
        near = [(0, 1 - at.core)] + [(s, c) for s in (1, -1) for c in range(CORES)]
        n = at.n_dev
        self.near = [send(src(at.dev(s, c)), dst(at.me), ssem, rsem.at[at.me], at.dev(s, c)) for s, c in near]
        self.far = [send(src(at.dev(2, i)), relay.at[i], ssem, rsem.at[n + i], at.dev(step, at.core)) for i, step in enumerate((1, -1))]
        self.on = [send(relay.at[i], dst(at.dev(-step, at.core)), ssem, rsem.at[at.dev(-step, at.core)], at.dev(step, i)) for i, step in enumerate((1, -1))]

    def start(self):
        for copy in self.far + self.near:
            copy.start()

    def pass_on(self):
        for far, on in zip(self.far, self.on):
            far.wait_recv()
            on.start()

    def wait_recv(self):
        at = self.at
        for j in range(1, at.n_dev):
            origin = lax.rem(at.me + j, at.n_dev)
            send(self.src(at.me), self.dst(origin), self.ssem, self.rsem.at[origin], at.partner).wait_recv()


def layer_norm(x):
    cen = x - jnp.mean(x, axis=-1, keepdims=True)
    inv = lax.rsqrt(jnp.mean(cen * cen, axis=-1, keepdims=True) + EPS)
    return cen * inv, inv


def block_body(n_dev, group, gain_hbm, bias_hbm, pos_hbm, freq_hbm, x_hbm, dy_ref, wq_ref, wk_ref, wv_ref, wo_ref,
               out_ref, dx_ref, dwq_ref, dwk_ref, dwv_ref, dwo_ref, dgain_ref, dbias_ref, dy_all, ht_all, g_all, wkv_all,
               h_ref, ht_ref, g_ref, q_ref, at_ref, at2_ref, da_ref, kt_ref, vt_ref, dk_ref, dv_ref,
               cost_ref, sint_ref, tab_ref, spot_ref, gain_ref, bias_ref, freq_ref, relay_q, relay_h, far_ref, part_ref, all_ref,
               s_sem, dy_rsem, kv_rsem, q_rsem, h_rsem, p_rsem, t_sem, loc_sem, mix_sem, lhs_sem, w_sem, job_sem):
    at = Place(n_dev)
    n_batch, seq, width = dy_ref.shape
    n_tok = n_batch * seq
    head_dim = wq_ref.shape[2]
    cols = (group + 2) * head_dim
    n_rows = group * head_dim
    half = n_rows // CORES
    n_seq = n_dev * seq
    quarter = head_dim // 4
    scale = head_dim ** -0.5
    chips = at.chips
    tile = CORES * seq
    core, me = at.core, at.me
    steps = (1, -1)
    origin = [at.dev(-1, core), at.dev(1, core)]
    far_dev = at.dev(2, core)
    scope = jax.named_scope

    dy_ssem, kv_ssem, q_ssem, h_ssem, p_ssem, x_ssem = [s_sem.at[i] for i in range(6)]
    assert (n_dev + 1) * n_rows == (n_dev - 1) * cols
    block_total = far_ref.at[0, pl.ds(0, n_dev - 1)]

    with scope('meet'):
        meet(at.peers(True))

    kv_cols = 2 * head_dim * chips
    kv_piece = lambda d, b: far_ref.at[b, d, :, pl.ds(0, kv_cols)]
    kv_both = lambda d: far_ref.at[:, me if d is None else d, :, pl.ds(0, kv_cols)]
    dys = Gather(at, lambda b: dy_ref.at[b], lambda d, b: dy_all.at[d, b], lambda d: dy_ref if d is None else dy_all.at[d], dy_ssem, dy_rsem)
    kvs = Gather(at, lambda b: kv_piece(me, b), kv_piece, kv_both, kv_ssem, kv_rsem)
    q_part = pl.ds(0, n_rows)
    queries = Exchange(at, lambda d: g_ref.at[d, :, q_part], lambda d: q_ref.at[d], relay_q, q_ssem, q_rsem)
    hcols = Exchange(at, lambda d: ht_ref.at[block(d, half)], lambda d: ht_all.at[d], relay_h, h_ssem, h_rsem)
    heads_across = send(at_ref.at[block(1 - core, half)], at2_ref.at[:, block(core, n_seq)], t_sem.at[0], t_sem.at[1], at.partner)
    spots = [send(pos_hbm, spot_ref.at[me], p_ssem, p_rsem.at[me], peer) for peer in at.peers(True)]

    dys.start_first()
    x_in = pltpu.make_async_copy(x_hbm, dx_ref, loc_sem.at[1])
    x_in.start()
    for copy in spots:
        copy.start()
    small = [pltpu.make_async_copy(src, dst, loc_sem.at[2 + n]) for n, (src, dst) in enumerate(((gain_hbm, gain_ref), (bias_hbm, bias_ref), (freq_hbm, freq_ref), (pos_hbm, spot_ref.at[me])))]
    for copy in small:
        copy.start()
    for copy in small:
        copy.wait()

    freq = freq_ref[...]
    for b in range(n_batch):
        angle = freq * spot_ref[me, b:b + 1, :].astype(F32)
        cos, sin, none = jnp.cos(angle), jnp.sin(angle), jnp.zeros((quarter, seq), F32)
        rest = jnp.zeros((head_dim - 2 * quarter, seq), F32)
        for i, rows in enumerate(([cos, cos, rest + 1.0], [-sin, none, rest], [none, sin, rest])):
            tab_ref[i, b * seq:(b + 1) * seq, :] = jnp.concatenate(rows, axis=0).T

    gain = (1.0 + gain_ref[...]).reshape(1, width)
    bias = bias_ref[...].reshape(1, width)

    def project_all(wkv_ref, raw_ref, wq_vm, raw_sem, wq_sem, stage_sem):
        pieces = [(b, i) for b in range(n_batch) for i in range(width // n_rows)]
        there = lambda n: da_ref.at[pl.ds(n * seq, seq)]
        dy_in = [pltpu.make_async_copy(dy_ref.at[b, :, pl.ds(i * n_rows, n_rows)], there(n), stage_sem.at[n]) for n, (b, i) in enumerate(pieces)]
        dy_keep = [pltpu.make_async_copy(there(n), dy_all.at[me, b, :, pl.ds(i * n_rows, n_rows)], stage_sem.at[n]) for n, (b, i) in enumerate(pieces)]
        span = 64 * chips
        batch = raw_ref.shape[2] // span
        row = lax.broadcasted_iota(jnp.int32, (span, span), 0)
        col = lax.broadcasted_iota(jnp.int32, (span, span), 1)
        pick = jnp.where(col == lax.rem(row, 64) * chips + lax.div(row, 64), 1.0, 0.0).astype(BF16)

        def raw_in(s, slot):
            return [pltpu.make_async_copy(w.at[block(s, span * batch)], raw_ref.at[slot, i], raw_sem.at[slot, i]) for i, w in enumerate((wk_ref, wv_ref))]

        def wq_in(s, slot):
            return [pltpu.make_async_copy(wq_ref.at[block(s, 2)], wq_vm.at[slot], wq_sem.at[slot])]

        def part_heads(s, slot):
            for i in range(batch):
                sl = slice(i * span, (i + 1) * span)
                rows = dot(pick, jnp.concatenate([raw_ref[slot, 0, sl, :], raw_ref[slot, 1, sl, :]], axis=1)).astype(BF16)
                for n in range(chips):
                    wkv_ref[n, block(s * batch + i, 64), :] = rows[n * 64:(n + 1) * 64]

        def turned(v):
            return v * tab_ref[0] + pltpu.roll(v, head_dim - quarter, 1) * tab_ref[1] + pltpu.roll(v, quarter, 1) * tab_ref[2]

        def project(s, slot):
            y = dot(h_ref[...], jnp.concatenate([wq_vm[slot, 0], wq_vm[slot, 1]], axis=1))
            for i in range(2):
                head = s * 2 + i
                v = turned(y[:, i * head_dim:(i + 1) * head_dim]).astype(BF16)
                for b in range(n_batch):
                    g_ref[lax.div(head, group) * n_batch + b, :, block(lax.rem(head, group), head_dim)] = v[b * seq:(b + 1) * seq]

        kv_ring = Ring(width // (64 * batch), raw_ref.shape[0], raw_in)
        q_ring = Ring(chips * group // 2, wq_vm.shape[0], wq_in)
        kv_ring.prime()
        q_ring.prime()
        for copy in dy_in:
            copy.start()
        x_in.wait()
        with scope('norm'):
            @pl.loop(0, n_tok // (2 * ROWS))
            def _(step):
                for i in range(2):
                    sl = block(2 * step + i, ROWS)
                    hat, _ = layer_norm(dx_ref[sl, :].astype(F32))
                    h_ref[sl, :] = (hat * gain + bias).astype(BF16)

        with scope('heads_kv'):
            kv_ring.run(part_heads)
        keep = pltpu.make_async_copy(wkv_ref, wkv_all, mix_sem.at[2])
        keep.start()
        for come, go in zip(dy_in, dy_keep):
            come.wait()
            go.start()
        with scope('project_kv'):
            @pl.loop(0, chips)
            def _(n):
                y = dot(h_ref[...], wkv_ref[n])
                v = jnp.concatenate([turned(y[:, :head_dim]), y[:, head_dim:]], axis=1).astype(BF16)
                for b in range(n_batch):
                    far_ref[b, me, :, block(n, 2 * head_dim)] = v[b * seq:(b + 1) * seq]

        kvs.start_first()
        kvs.start_second()
        with scope('project_q'):
            q_ring.run(project)
        keep.wait()
        for copy in dy_keep:
            copy.wait()

    pl.run_scoped(
        project_all,
        pltpu.VMEM((chips, width, 2 * head_dim), BF16),
        pltpu.VMEM((3, 2, 4 * 64 * chips, head_dim), BF16), pltpu.VMEM((4, 2, width, head_dim), BF16),
        pltpu.SemaphoreType.DMA((3, 2)), pltpu.SemaphoreType.DMA((4,)), pltpu.SemaphoreType.DMA((n_batch * width // n_rows,)),
    )

    with scope('kv_pass'):
        kvs.pass_on()
    queries.start()
    q_ref[me] = g_ref[me, :, q_part]
    with scope('turn_h'):
        @pl.loop(0, width // 128)
        def _(step):
            sl = block(step, 128)
            ht_ref[sl, :] = h_ref[:, sl].T

    with scope('kv_wait'):
        kvs.share_second()
        kvs.share_far()
        kvs.own_across.wait_recv()
        kvs.wait_near()
        kvs.wait_far()

    def chip_at(i):
        return at.ring(jnp.where(i == 0, 0, jnp.where(i == 1, 1, jnp.where(i == 2, 3, 2))))

    def soft(s, seen):
        s = s * scale
        clear = s.shape[0] - seen.shape[0]
        tail = jnp.where(seen, s[clear:], -1e30)
        s = tail if clear == 0 else jnp.concatenate([s[:clear], tail], axis=0)
        e = jnp.exp(s - jnp.max(s, axis=0, keepdims=True))
        return e * (1.0 / jnp.sum(e, axis=0, keepdims=True))

    def attend(limit, clear):
        @pl.loop(0, n_batch * chips)
        def _(i):
            @pl.when(i == 1)
            def _():
                with scope('q_pass'):
                    queries.pass_on()
                dys.start_second()
                dys.pass_on()
                hcols.start()

            b, n = lax.rem(i, n_batch), lax.div(i, n_batch)
            k = far_ref[b, 0:limit // seq, :, block(2 * n, head_dim)].reshape(limit, head_dim)
            vt = far_ref[b, 0:limit // seq, :, block(2 * n + 1, head_dim)].reshape(limit, head_dim).T
            q = jnp.concatenate([g_ref[n * n_batch + b, :, block(j, head_dim)] for j in range(group)], axis=0)
            row = lax.broadcasted_iota(jnp.int32, (limit - clear, n_rows), 0)
            col = lax.broadcasted_iota(jnp.int32, (limit - clear, n_rows), 1)
            p = soft(dot_nt(k, q), row <= lax.rem(col, seq) + (me * seq - clear))
            mixed = dot(vt, p.astype(BF16)).astype(BF16)
            for j in range(group):
                h_ref[block(b, seq), block(n * group + j, head_dim)] = mixed[:, j * seq:(j + 1) * seq].T

    with scope('attend'):
        @pl.when(at.chip == chips - 1)
        def _():
            attend(chips * tile, (chips - 1) * tile)

        @pl.when(at.chip < chips - 1)
        def _():
            attend((chips - 1) * tile, 0)

    h_keep = pltpu.make_async_copy(ht_ref.at[block(me, half)], ht_all.at[me], loc_sem.at[1])
    h_keep.start()

    def block_out():
        def stream(wo_vm, sem):
            def wo_in(s, slot):
                return [pltpu.make_async_copy(wo_ref.at[:, block(s, OUT_TILE)], wo_vm.at[slot], sem.at[slot])]

            def out_tile(s, slot):
                sl = block(s, OUT_TILE)
                out_ref[:, sl] = (dx_ref[:, sl].astype(F32) + dot(h_ref[...], wo_vm[slot])).astype(BF16)

            ring = Ring(width // OUT_TILE, wo_vm.shape[0], wo_in)
            ring.prime()
            ring.run(out_tile)

        with scope('output'):
            pl.run_scoped(stream, pltpu.VMEM((4, width, OUT_TILE), BF16), pltpu.SemaphoreType.DMA((4,)))

    k_all = lambda n: far_ref[core, 0:n, :, block(2 * at.chip, head_dim)].reshape(n * seq, head_dim)
    v_all = lambda n: far_ref[core, 0:n, :, block(2 * at.chip + 1, head_dim)].reshape(n * seq, head_dim)

    def rotate_back(t, cos, sin):
        u, w = t[:quarter], t[quarter:2 * quarter]
        return jnp.concatenate([u * cos + w * sin, w * cos - u * sin, t[2 * quarter:]], axis=0)

    def by_dev(t):
        return t.astype(BF16).reshape(t.shape[0] // seq, seq, head_dim)

    def attend_back(t, i):
        limit = (t + 1) * tile
        sl = slice(t * tile, limit)
        devs = slice(t * CORES, (t + 1) * CORES)

        def heads(first, count):
            each = range(count)
            q = jnp.concatenate([q_ref[devs, :, block(first + j, head_dim)].reshape(tile, head_dim) for j in each], axis=0)
            da = jnp.concatenate([da_ref[sl, block(first + j, head_dim)] for j in each], axis=0)
            k, v = k_all(limit // seq), v_all(limit // seq)
            row = lax.broadcasted_iota(jnp.int32, (tile, count * tile), 0)
            col = lax.broadcasted_iota(jnp.int32, (tile, count * tile), 1)
            p = soft(dot_nt(k, q), row <= lax.rem(col, tile))
            p_low = p.astype(BF16)
            mixed = dot(vt_ref[:, :limit], p_low).astype(BF16)
            dp = dot_nt(v, da)
            row_dot = jnp.sum(p * dp, axis=0, keepdims=True)
            ds = (p * (dp - row_dot) * scale).astype(BF16)
            dv_ref[:limit, :] += dot(p_low, da)
            dk_ref[:limit, :] += dot(ds, q)
            back = dot(kt_ref[:, :limit], ds)
            for j in each:
                part = slice(j * tile, (j + 1) * tile)
                at_ref[block(first + j, head_dim), sl] = mixed[:, part]
                g_ref[devs, :, block(first + j, head_dim)] = by_dev(rotate_back(back[:, part], cost_ref[:, sl], sint_ref[:, sl]).T)

        @pl.loop(0, group // 2)
        def _(j):
            heads(2 * j, 2)

        @pl.when(i == chips - 2)
        def _():
            with scope('dy_far'):
                dys.share_far()

        heads(group - 1, 1)

    def middle(wo_vm, dyk):
        wo_in = pltpu.make_async_copy(wo_ref.at[block(at.chip, n_rows)], wo_vm, mix_sem.at[2])
        wo_in.start()
        for j in range(1, n_dev):
            source = lax.rem(me + j, n_dev)
            send(pos_hbm, spot_ref.at[source], p_ssem, p_rsem.at[source], at.partner).wait_recv()
        for d in range(n_dev):
            angle = freq * spot_ref[d, pl.ds(core, 1), :].astype(F32)
            cost_ref[:, d * seq:(d + 1) * seq] = jnp.cos(angle)
            sint_ref[:, d * seq:(d + 1) * seq] = jnp.sin(angle)
        with scope('q_wait'):
            queries.wait_recv()
            all_sent(block_total, q_ssem, at.partner)
            all_sent(far_ref.at[:, pl.ds(0, n_dev - 1), :, pl.ds(0, kv_cols)], kv_ssem, at.partner)
            all_sent(spot_ref.at[pl.ds(0, n_dev - 1)], p_ssem, at.partner)
        kt_ref[...] = k_all(n_dev).T
        vt_ref[...] = v_all(n_dev).T
        dk_ref[...] = jnp.zeros_like(dk_ref)
        dv_ref[...] = jnp.zeros_like(dv_ref)
        dys.own_across.wait_recv()

        def fetch(i, slot):
            return pltpu.make_async_copy(dy_all.at[block(chip_at(i), CORES), core], dyk.at[slot], mix_sem.at[slot])

        with scope('wo_wait'):
            fetch(0, 0).start()
            wo_in.wait()

        @pl.loop(0, chips)
        def _(i):
            slot = lax.rem(i, 2)

            @pl.when((i == 1) & (at.chip < chips - 1))
            def _():
                block_out()

            @pl.when(i == 1)
            def _():
                with scope('dy_wait'):
                    dys.share_second()
                    dys.wait_near()
                fetch(i, slot).start()

            @pl.when(i == chips - 1)
            def _():
                with scope('dy_far2'):
                    dys.wait_far()
                fetch(i, slot).start()
                with scope('h_pass'):
                    hcols.pass_on()

            fetch(i, slot).wait()

            @pl.when((i > 0) & (i < chips - 2))
            def _():
                fetch(i + 1, 1 - slot).start()

            chip = chip_at(i)
            with scope('da'):
                da_ref[block(chip, tile), :] = dot_nt(dyk[slot].reshape(tile, width), wo_vm[...]).astype(BF16)
            with scope('attend_back'):
                for t in range(chips):
                    @pl.when(chip == t)
                    def _(t=t):
                        attend_back(t, i)

    pl.run_scoped(middle, pltpu.VMEM((n_rows, width), BF16), pltpu.VMEM((2, CORES, seq, width), BF16))
    all_sent(dy_all.at[pl.ds(0, n_dev - 1)], dy_ssem, at.partner)
    heads_across.start()
    g_ref[:, :, n_rows:n_rows + head_dim] = by_dev(rotate_back(dk_ref[...].T, cost_ref[...], sint_ref[...]).T)
    g_ref[:, :, n_rows + head_dim:] = by_dev(dv_ref[...])

    def span_of(q):
        return block(q, CORES)

    turn = [[at.ring(q) for q in (2, 1, 3, 0)], [at.ring(q) for q in (3, 0, 1, 2)]]
    direct = [[send(g_ref.at[span_of(turn[i][q])], g_all.at[me, span_of(turn[i][q])], kv_ssem, kv_rsem.at[i * chips + q], at.dev(steps[i], core)) for q in range(chips)] for i in range(2)]
    came = [[at.ring(q) for q in (1, 0, 2, 3)], [at.ring(q) for q in (0, 1, 2, 3)]]
    def halves_of(quarters):
        return [span_of(quarters[0])] + [pl.ds(quarters[1] * CORES + c, 1) for c in range(CORES)]

    onward = [[send(g_all.at[origin[i], sl], far_ref.at[core, sl], q_ssem, q_rsem.at[3 * i + q], at.dev(steps[i], core)) for q, sl in enumerate(halves_of(came[i]))] for i in range(2)]
    ends = [[at.ring(q) for q in (0, 3)], [at.ring(q) for q in (1, 2)]]
    g_across = send(g_ref, g_all.at[me], x_ssem, dy_rsem.at[0], at.partner)
    near_across = [[send(g_all.at[origin[i], span_of(came[i][q])], g_all.at[origin[i], span_of(came[i][q])], x_ssem, dy_rsem.at[1 + i * chips + q], at.partner) for q in range(chips)] for i in range(2)]
    end_across = [[send(far_ref.at[core, sl], far_ref.at[core, sl], x_ssem, dy_rsem.at[1 + 2 * chips + 3 * i + q], at.partner) for q, sl in enumerate(halves_of(ends[i]))] for i in range(2)]
    for q in range(chips):
        for i in range(2):
            direct[i][q].start()
    g_across.start()
    g_keep = pltpu.make_async_copy(g_ref, g_all.at[me], loc_sem.at[0])
    g_keep.start()
    at2_ref[:, block(core, n_seq)] = at_ref[block(core, half), :]

    @pl.when(at.chip == chips - 1)
    def _():
        block_out()

    dy_back = [pltpu.make_async_copy(dy_ref.at[b], h_ref.at[pl.ds(b * seq, seq)], loc_sem.at[2 + b]) for b in range(n_batch)]
    for copy in dy_back:
        copy.start()

    def wo_rows(dy_vm, sem):
        def dy_tile(s, slot):
            return [pltpu.make_async_copy(dy_all.at[:, :, :, block(s, COL_TILE)], dy_vm.at[slot], sem.at[slot])]

        def wo_tile(s, slot):
            pieces = [dy_vm[slot, d, b] for b in range(n_batch) for d in range(n_dev)]
            dwo_ref[:, block(s, COL_TILE)] = dot(at2_ref[...], jnp.concatenate(pieces, axis=0))

        ring = Ring(width // COL_TILE, dy_vm.shape[0], dy_tile)
        ring.prime()
        with scope('heads_wait'):
            heads_across.wait_recv()
        with scope('grad_wo'):
            ring.run(wo_tile)

    pl.run_scoped(wo_rows, pltpu.VMEM((4, n_dev, n_batch, seq, COL_TILE), BF16), pltpu.SemaphoreType.DMA((4,)))

    with scope('h_wait'):
        hcols.wait_recv()
        all_sent(block_total, h_ssem, at.partner)
    h_keep.wait()
    lhs_in = [pltpu.make_async_copy(ht_all.at[d, :, pl.ds(b * seq, seq)], at2_ref.at[:, pl.ds((b * n_dev + d) * seq, seq)], lhs_sem.at[0]) for d in range(n_dev) for b in range(n_batch)]
    for copy in lhs_in:
        copy.start()
    with jax.named_scope('own_wait'):
        pltpu.make_async_copy(at2_ref, at2_ref, lhs_sem.at[0]).wait()
        g_keep.wait()
        g_across.wait_recv()
    sums = [send(all_ref.at[me], all_ref.at[me], p_ssem, p_rsem.at[me], peer) for peer in at.peers(True)]

    def weight_grads(wq_vm, wkv_vm, acc_ref, hat_ref, inv_ref, job_ref, mine_ref):
        n_slots = wq_vm.shape[0]
        chunk = wq_vm.shape[2]
        n_chunks = width // chunk
        total = n_chunks * chips

        def weights(s):
            slot = lax.rem(s, n_slots)
            chip = chip_at(lax.div(s, n_chunks))
            rows = block(lax.rem(s, n_chunks), chunk)
            return [
                pltpu.make_async_copy(wq_ref.at[block(chip, group), rows], wq_vm.at[slot], w_sem.at[slot, 0]),
                pltpu.make_async_copy(wkv_all.at[chip, rows], wkv_vm.at[slot], w_sem.at[slot, 1]),
            ]

        for s in range(n_slots):
            for copy in weights(s):
                copy.start()

        def grow(i, read):
            @pl.loop(0, n_chunks)
            def _(n):
                s = i * n_chunks + n
                slot = lax.rem(s, n_slots)
                for copy in weights(s):
                    copy.wait()
                rows = jnp.concatenate([read(b) for b in range(n_batch)], axis=0)
                part = dot_nt(rows, jnp.concatenate([wq_vm[slot, j] for j in range(group)] + [wkv_vm[slot]], axis=1))
                sl = block(n, chunk)

                @pl.when(i == 0)
                def _():
                    acc_ref[:, sl] = part

                @pl.when(i > 0)
                def _():
                    acc_ref[:, sl] += part

                @pl.when(s + n_slots < total)
                def _():
                    for copy in weights(s + n_slots):
                        copy.start()

        def mine_in(i):
            return [pltpu.make_async_copy(g_all.at[chip_at(i) * CORES + b, me], mine_ref.at[lax.rem(i, 2), b], job_sem.at[2 + lax.rem(i, 2)]) for b in range(n_batch)]

        def grow_near(i):
            here = mine_ref.at[lax.rem(i, 2)]
            pltpu.make_async_copy(here, here, job_sem.at[2 + lax.rem(i, 2)]).wait()
            grow(i, lambda b: mine_ref[lax.rem(i, 2), b])

        def job_in(chip, quarters, slot):
            return [pltpu.make_async_copy(g_all.at[chip * CORES + b, span_of(q)], job_ref.at[slot, b, n], job_sem.at[slot]) for b in range(n_batch) for n, q in enumerate(quarters)]

        def job(chip, pieces, read, add):
            lhs = [at2_ref[:, pl.ds(pl.multiple_of(b * n_seq + d * seq, seq), seq)] for b in range(n_batch) for d in pieces]
            rhs = [read(b, n) for b in range(n_batch) for n in range(len(pieces))]
            y = dot(jnp.concatenate(lhs, axis=1), jnp.concatenate(rhs, axis=0))
            for j in range(group):
                v = y[:, j * head_dim:(j + 1) * head_dim]
                dwq_ref[chip * group + j] = dwq_ref[chip * group + j] + v if add else v
            for j, ref in enumerate((dwk_ref, dwv_ref)):
                v = y[:, (group + j) * head_dim:(group + j + 1) * head_dim]
                rows = pl.ds(chip, half, stride=chips)
                ref[rows, :] = ref[rows, :] + v if add else v

        def devs_of(quarters):
            return [q * CORES + c for q in quarters for c in range(CORES)]

        def near_pair(quarters, add):
            for slot, step in enumerate(steps):
                for copy in job_in(at.ring(step), quarters, slot):
                    copy.start()

            @pl.loop(0, 2)
            def _(slot):
                chip = at.ring(1 - 2 * slot)
                pltpu.make_async_copy(job_ref.at[slot], job_ref.at[slot], job_sem.at[slot]).wait()
                job(chip, devs_of(quarters), lambda b, n: job_ref[slot, b, n // CORES, n % CORES], add)

        halves = [[at.ring(q) for q in half_of] for half_of in ((0, 1), (2, 3))]
        for slot in range(2):
            for copy in job_in(at.chip, [at.ring(2 * slot), at.ring(2 * slot + 1)], slot):
                copy.start()
        for copy in mine_in(0):
            copy.start()
        with jax.named_scope('own_job'):
            for slot in range(2):
                quarters = [at.ring(2 * slot), at.ring(2 * slot + 1)]
                pltpu.make_async_copy(job_ref.at[slot], job_ref.at[slot], job_sem.at[slot]).wait()
                job(at.chip, devs_of(quarters), lambda b, n: job_ref[slot, b, n // CORES, n % CORES], slot == 1)

        with jax.named_scope('own_dh'):
            grow_near(0)

        with jax.named_scope('d01_wait'):
            for q in range(2):
                for i in range(2):
                    direct[i][q].wait_recv()
                for i in range(2):
                    for copy in onward[i][:1] if q == 0 else onward[i][1:]:
                        copy.start()
                    near_across[i][q].start()
        with jax.named_scope('d01_across'):
            for q in range(2):
                for i in range(2):
                    near_across[i][q].wait_recv()
        for i in (1, 2):
            for copy in mine_in(i):
                copy.start()
        with scope('near_dh'):
            @pl.loop(1, chips - 1)
            def _(i):
                grow_near(i)

        with jax.named_scope('near_a'):
            near_pair(halves[0], False)
        with scope('d2_wait'):
            for i in range(2):
                direct[i][2].wait_recv()
                near_across[i][2].start()
        with jax.named_scope('hat'):
            @pl.loop(0, n_tok // (2 * ROWS))
            def _(step):
                for i in range(2):
                    sl = block(2 * step + i, ROWS)
                    hat, inv = layer_norm(dx_ref[sl, :].astype(F32))
                    hat_ref[sl, :] = hat
                    inv_ref[sl, :] = jnp.broadcast_to(inv, (ROWS, 128))

        with scope('d3_wait'):
            for i in range(2):
                direct[i][3].wait_recv()
                near_across[i][3].start()
        with jax.named_scope('d23_across'):
            for q in range(2, chips):
                for i in range(2):
                    near_across[i][q].wait_recv()

        with jax.named_scope('near_b'):
            near_pair(halves[1], True)
        far_chip = at.ring(2)
        with jax.named_scope('far0_wait'):
            for i in range(2):
                onward[i][0].wait_recv()
                end_across[i][0].start()
        with jax.named_scope('far0_across'):
            for i in range(2):
                end_across[i][0].wait_recv()
        with jax.named_scope('far_dh'):
            grow(chips - 1, lambda b: far_ref[b, me])
        for copy in dy_back:
            copy.wait()
        part_ref[...] = jnp.zeros_like(part_ref)

        with jax.named_scope('norm_back'):
            @pl.loop(0, n_tok // (2 * ROWS))
            def _(step):
                for i in range(2):
                    sl = block(2 * step + i, ROWS)
                    hat, inv = hat_ref[sl, :], inv_ref[sl, 0:1]
                    dh = acc_ref[sl, :]
                    dg = dh * hat
                    gh = dh * gain
                    one = jnp.mean(gh, axis=-1, keepdims=True)
                    two = jnp.mean(dg * gain, axis=-1, keepdims=True)
                    dx_ref[sl, :] = (h_ref[sl, :].astype(F32) + inv * (gh - one - hat * two)).astype(BF16)
                    part_ref[0] += dg[0:8] + dg[8:16]
                    part_ref[1] += dh[0:8] + dh[8:16]

        all_ref[me, 0:1, :] = jnp.sum(part_ref[0], axis=0, keepdims=True)
        all_ref[me, 1:2, :] = jnp.sum(part_ref[1], axis=0, keepdims=True)
        for copy in sums:
            copy.start()
        def hand_on(c):
            with scope('far1_wait'):
                for i in range(2):
                    onward[i][1 + c].wait_recv()
                    end_across[i][1 + c].start()

        hand_on(0)
        with scope('far_a'):
            first_devs = devs_of([ends[0][0], ends[1][0]])
            job(far_chip, first_devs, lambda b, n: far_ref[b, first_devs[n]], False)
        for c in range(CORES):
            if c > 0:
                hand_on(c)
            with scope('far1_across'):
                for i in range(2):
                    end_across[i][1 + c].wait_recv()
            with scope('far_b'):
                last_devs = [ends[i][1] * CORES + c for i in range(2)]
                job(far_chip, last_devs, lambda b, n: far_ref[b, last_devs[n]], True)

    pl.run_scoped(
        weight_grads,
        pltpu.VMEM((W_SLOTS, group, W_ROWS, head_dim), BF16), pltpu.VMEM((W_SLOTS, W_ROWS, 2 * head_dim), BF16), pltpu.VMEM((n_tok, width), F32),
        pltpu.VMEM((n_tok, width), F32), pltpu.VMEM((n_tok, 128), F32), pltpu.VMEM((2, n_batch, 2, CORES, seq, cols), BF16), pltpu.VMEM((2, n_batch, seq, cols), BF16),
    )

    with jax.named_scope('sums'):
        for j in range(1, n_dev):
            source = lax.rem(me + j, n_dev)
            send(all_ref.at[me], all_ref.at[source], p_ssem, p_rsem.at[source], at.partner).wait_recv()
        total = all_ref[0]
        for d in range(1, n_dev):
            total = total + all_ref[d]
        dgain_ref[...] = total[0:1].reshape(width)
        dbias_ref[...] = total[1:2].reshape(width)
    with scope('done'):
        heads_across.wait_send()
        all_sent(far_ref, kv_ssem, at.partner)
        all_sent(g_ref, q_ssem, at.partner)
        all_sent(g_all.at[pl.ds(0, chips)], x_ssem, at.partner)
        all_sent(all_ref.at[pl.ds(0, n_dev - 1)], p_ssem, at.partner)


def whole_block(n_dev, x, gain, bias, positions, freq, dy, wq, wk, wv, wo):
    n_batch, seq, width = dy.shape
    n_tok = n_batch * seq
    head_dim = wq.shape[2]
    chips = n_dev // CORES
    group = wq.shape[0] // chips
    cols = (group + 2) * head_dim
    n_rows = group * head_dim
    half = n_rows // CORES
    n_seq = n_dev * seq
    quarter = head_dim // 4
    dma = pltpu.SemaphoreType.DMA
    vm = pltpu.VMEM
    shapes = [((n_tok, width), BF16)] * 2 + [((chips * group, half, head_dim), F32)] + [((chips * half, head_dim), F32)] * 2 + [((half, width), F32), ((width,), F32), ((width,), F32)]
    held = [((n_dev, n_batch, seq, width), BF16), ((n_dev, half, n_tok), BF16), ((n_dev, n_dev, seq, cols), BF16), ((chips, width, 2 * head_dim), BF16)]
    return pl.pallas_call(
        functools.partial(block_body, n_dev, group),
        out_shape=tuple(pltpu.VMEM(*t) for t in shapes) + tuple(sds(*t) for t in held),
        in_specs=[HBM] * 10,
        out_specs=(VM,) * len(shapes) + (HBM,) * len(held),
        scratch_shapes=[
            vm((n_tok, width), BF16), vm((width, n_tok), BF16), vm((n_dev, seq, cols), BF16), vm((n_dev, seq, n_rows), BF16),
            vm((n_rows, n_seq), BF16), vm((half, n_batch * n_seq), BF16), vm((n_seq, n_rows), BF16),
            vm((head_dim, n_seq), BF16), vm((head_dim, n_seq), BF16), vm((n_seq, head_dim), F32), vm((n_seq, head_dim), F32),
            vm((quarter, n_seq), F32), vm((quarter, n_seq), F32), vm((3, n_tok, head_dim), F32), vm((n_dev, n_batch, seq), jnp.int32), vm((width,), F32), vm((width,), F32), vm((quarter, 1), F32),
            vm((2, seq, n_rows), BF16), vm((2, half, n_tok), BF16),
            vm((n_batch, n_dev, seq, cols), BF16), vm((2, 8, width), F32), vm((n_dev, 2, width), F32),
            dma((6,)), dma((7 + 2 * chips,)), dma((13,)), dma((n_dev + 2,)), dma((n_dev + 2,)), dma((n_dev,)), dma((2,)),
            dma((6,)), dma((3,)), dma((1,)), dma((W_SLOTS, 2)), dma((4,)),
        ],
        compiler_params=pltpu.CompilerParams(collective_id=0, has_side_effects=True, vmem_limit_bytes=VMEM_LIMIT),
        cost_estimate=pl.CostEstimate(flops=10 ** 11, bytes_accessed=10 ** 8, transcendentals=0),
        name='block',
    )(gain, bias, positions, freq, x.reshape(n_tok, width), dy, wq, wk, wv, wo)[:len(shapes)]


def settle_body(n, *refs):
    sems = refs[2 * n]
    copies = []
    for i in range(n):
        src, dst = refs[i], refs[n + i]
        pieces = max(p for p in range(1, SETTLE + 1) if src.shape[0] % p == 0) if len(src.shape) > 1 else 1
        size = src.shape[0] // pieces
        for p in range(pieces):
            copies.append(pltpu.make_async_copy(src.at[pl.ds(p * size, size)], dst.at[pl.ds(p * size, size)], sems.at[i, p]))
    for copy in copies:
        copy.start()
    for copy in copies:
        copy.wait()


def settle(arrays):
    n = len(arrays)
    return pl.pallas_call(
        functools.partial(settle_body, n),
        out_shape=tuple(sds(t.shape, t.dtype) for t in arrays),
        in_specs=[ANY] * n,
        out_specs=(HBM,) * n,
        scratch_shapes=[pltpu.SemaphoreType.DMA((n, SETTLE))],
        compiler_params=pltpu.CompilerParams(vmem_limit_bytes=1024 * 1024),
        name='settle',
    )(*arrays)


def solution(mesh):
    n_dev = mesh.shape['cp']

    def device_step(x_act, d_out, positions, ln_gain, ln_bias, w_query, w_key, w_value, w_out):
        n_batch, seq, width = x_act.shape
        q_heads, (kv_heads, head_dim) = w_query.shape[1], w_key.shape[1:]
        group = q_heads // kv_heads
        quarter = head_dim // 4
        assert n_batch == CORES and n_dev // CORES == kv_heads == 4 and q_heads * head_dim == width

        freq = np.exp(np.arange(quarter) * (-2.0 * math.log(ROPE_BASE) / (head_dim // 2))).astype(np.float32).reshape(quarter, 1)
        by_head = lambda t: jnp.transpose(t, (1, 0, 2))
        by_row = lambda t: t.reshape(width * kv_heads, head_dim)
        wq = by_head(w_query)

        results = whole_block(n_dev, x_act, ln_gain, ln_bias, positions, jnp.asarray(freq), d_out, wq, by_row(w_key), by_row(w_value), w_out)
        out, dx, dwq, dwk, dwv, dwo, dgain, dbias = settle(results)
        kv_rows = lambda t: t.reshape(width // n_dev, kv_heads, head_dim)
        return (out.reshape(x_act.shape), dx.reshape(x_act.shape), by_head(dwq), kv_rows(dwk), kv_rows(dwv), dwo, dgain, dbias)

    return jax.shard_map(device_step, mesh=mesh, in_specs=(P('dp', 'cp', None), P('dp', 'cp', None), P('dp', 'cp'), P(None), P(None), P(None, None, None), P(None, None, None), P(None, None, None), P(None, None)), out_specs=(P('dp', 'cp', None), P('dp', 'cp', None), P(('dp', 'cp'), None, None), P(('dp', 'cp'), None, None), P(('dp', 'cp'), None, None), P(('dp', 'cp'), None), P('dp'), P('dp')), check_vma=False)
```

```python
import functools
import math
import jax
import jax.numpy as jnp
import numpy as np
from jax import lax
from jax.experimental import pallas as pl
from jax.experimental.pallas import tpu as pltpu
from jax.sharding import PartitionSpec as P

EPS = 1e-5
ROPE_BASE = 10000.0
BF16 = jnp.bfloat16
F32 = jnp.float32
VMEM_LIMIT = 46 * 1024 * 1024
NT = (((1,), (1,)), ((), ()))
ANY = pl.BlockSpec(memory_space=pl.ANY)
VM = pl.BlockSpec(memory_space=pltpu.VMEM)
HBM = pl.BlockSpec(memory_space=pltpu.HBM)
CORES = 2
COL_TILE = 512
OUT_TILE = 256
ROWS = 16
W_SLOTS = 4
W_ROWS = 512
SETTLE = 4


def dot(a, b):
    return jnp.dot(a, b, preferred_element_type=F32)


def dot_nt(a, b):
    return lax.dot_general(a, b, NT, preferred_element_type=F32)


def sds(shape, dtype):
    return jax.ShapeDtypeStruct(shape, dtype)


def block(i, size):
    return pl.ds(pl.multiple_of(i * size, size), size)


class Place:
    def __init__(self, n_dev):
        self.n_dev = n_dev
        self.chips = n_dev // CORES
        self.me = lax.axis_index('cp')
        self.chip = self.me // CORES
        self.core = self.me % CORES
        self.partner = self.chip * CORES + 1 - self.core

    def ring(self, step):
        return lax.rem(self.chip + self.chips + step, self.chips)

    def dev(self, step, core):
        return self.ring(step) * CORES + core

    def peers(self, far):
        near = [self.partner] + [self.dev(s, c) for s in (1, -1) for c in range(CORES)]
        return near + ([self.dev(2, c) for c in range(CORES)] if far else [])


def send(src, dst, ssem, rsem, to):
    return pltpu.make_async_remote_copy(src_ref=src, dst_ref=dst, send_sem=ssem, recv_sem=rsem, device_id={'cp': to}, device_id_type=pl.DeviceIdType.MESH)


def all_sent(total, ssem, to):
    send(total, total, ssem, ssem, to).wait_send()


def all_came(total, rsem, to):
    send(total, total, rsem, rsem, to).wait_recv()


def meet(peers):
    barrier = pltpu.get_barrier_semaphore()
    for peer in peers:
        pl.semaphore_signal(barrier, inc=1, device_id={'cp': peer}, device_id_type=pl.DeviceIdType.MESH)
    pl.semaphore_wait(barrier, len(peers))


class Ring:
    def __init__(self, n, slots, copies):
        self.n, self.slots, self.copies = n, slots, copies

    def prime(self):
        for s in range(self.slots):
            for copy in self.copies(s, s):
                copy.start()

    def run(self, use):
        @pl.loop(0, self.n)
        def _(s):
            slot = lax.rem(s, self.slots)
            for copy in self.copies(s, slot):
                copy.wait()
            use(s, slot)

            @pl.when(s + self.slots < self.n)
            def _():
                for copy in self.copies(s + self.slots, slot):
                    copy.start()


class Gather:
    def __init__(self, at, own, piece, both, ssem, rsem, across):
        steps = (1, -1)
        origin = [at.dev(-1, at.core), at.dev(1, at.core)]
        far = at.dev(2, at.core)
        link = lambda i, src, dst, to: send(src, dst, ssem, rsem.at[i], to)
        self.first = [link(b, own(b), piece(at.me, b), at.dev(steps[b], at.core)) for b in range(2)]
        self.second = [link(2 + b, own(1 - b), piece(at.me, 1 - b), at.dev(steps[b], at.core)) for b in range(2)]
        self.again = [link(4 + b, piece(origin[b], b), piece(origin[b], b), at.dev(steps[b], at.core)) for b in range(2)]
        self.own_across = link(across[0], both(None), both(at.me), at.partner)
        self.first_across = [link(across[1], piece(origin[b], b), piece(origin[b], b), at.partner) for b in range(2)]
        self.second_across = [link(across[1], piece(origin[b], 1 - b), piece(origin[b], 1 - b), at.partner) for b in range(2)]
        self.far_across = [link(across[2], piece(far, b), piece(far, b), at.partner) for b in range(2)]

    def start_first(self):
        for copy in self.first + [self.own_across]:
            copy.start()

    def start_second(self):
        for copy in self.second:
            copy.start()

    def pass_on(self):
        for copy, again, across in zip(self.first, self.again, self.first_across):
            copy.wait_recv()
            again.start()
            across.start()

    def share_second(self):
        for copy, across in zip(self.second, self.second_across):
            copy.wait_recv()
            across.start()

    def share_far(self):
        for copy, across in zip(self.again, self.far_across):
            copy.wait_recv()
            across.start()


class Exchange:
    def __init__(self, at, src, dst, relay, ssem, rsem):
        near = [(0, 1 - at.core)] + [(s, c) for s in (1, -1) for c in range(CORES)]
        self.near = [send(src(at.dev(s, c)), dst(at.me), ssem, rsem.at[0], at.dev(s, c)) for s, c in near]
        self.far = [send(src(at.dev(2, i)), relay.at[i], ssem, rsem.at[1 + i], at.dev(step, at.core)) for i, step in enumerate((1, -1))]
        self.on = [send(relay.at[i], dst(at.dev(-step, at.core)), ssem, rsem.at[0], at.dev(step, i)) for i, step in enumerate((1, -1))]

    def start(self):
        for copy in self.far + self.near:
            copy.start()

    def pass_on(self):
        for far, on in zip(self.far, self.on):
            far.wait_recv()
            on.start()


def layer_norm(x):
    cen = x - jnp.mean(x, axis=-1, keepdims=True)
    inv = lax.rsqrt(jnp.mean(cen * cen, axis=-1, keepdims=True) + EPS)
    return cen * inv, inv


def block_body(n_dev, group, gain_hbm, bias_hbm, pos_hbm, freq_hbm, x_hbm, dy_ref, wq_ref, wk_ref, wv_ref, wo_ref,
               out_ref, dx_ref, dwq_ref, dwk_ref, dwv_ref, dwo_ref, dgain_ref, dbias_ref, dy_all, ht_all, g_all, wkv_all,
               h_ref, ht_ref, g_ref, q_ref, at_ref, at2_ref, da_ref, kt_ref, vt_ref, dk_ref, dv_ref,
               cost_ref, sint_ref, tab_ref, spot_ref, gain_ref, bias_ref, freq_ref, relay_q, relay_h, far_ref, part_ref, pair_ref, row_ref, total_ref,
               s_sem, dy_rsem, kv_rsem, q_rsem, h_rsem, p_rsem, t_sem, loc_sem, mix_sem, lhs_sem, w_sem, job_sem):
    at = Place(n_dev)
    n_batch, seq, width = dy_ref.shape
    n_tok = n_batch * seq
    head_dim = wq_ref.shape[2]
    cols = (group + 2) * head_dim
    n_rows = group * head_dim
    half = n_rows // CORES
    n_seq = n_dev * seq
    quarter = head_dim // 4
    scale = head_dim ** -0.5
    chips = at.chips
    tile = CORES * seq
    core, me = at.core, at.me
    steps = (1, -1)
    origin = [at.dev(-1, core), at.dev(1, core)]
    far_dev = at.dev(2, core)
    scope = jax.named_scope

    dy_ssem, kv_ssem, q_ssem, h_ssem, p_ssem, x_ssem = [s_sem.at[i] for i in range(6)]
    assert (n_dev + 1) * n_rows == (n_dev - 1) * cols
    block_total = far_ref.at[0, pl.ds(0, n_dev - 1)]

    with scope('meet'):
        meet(at.peers(True))

    kv_cols = 2 * head_dim * chips
    kv_piece = lambda d, b: far_ref.at[b, d, :, pl.ds(0, kv_cols)]
    kv_both = lambda d: far_ref.at[:, me if d is None else d, :, pl.ds(0, kv_cols)]
    dys = Gather(at, lambda b: dy_ref.at[b], lambda d, b: dy_all.at[d, b], lambda d: dy_ref if d is None else dy_all.at[d], dy_ssem, dy_rsem, (6, 7, 8))
    kvs = Gather(at, lambda b: kv_piece(me, b), kv_piece, kv_both, kv_ssem, kv_rsem, (6, 6, 6))
    q_part = pl.ds(0, n_rows)
    queries = Exchange(at, lambda d: g_ref.at[d, :, q_part], lambda d: q_ref.at[d], relay_q, q_ssem, q_rsem)
    hcols = Exchange(at, lambda d: ht_ref.at[block(d, half)], lambda d: ht_all.at[d], relay_h, h_ssem, h_rsem)
    heads_across = send(at_ref.at[block(1 - core, half)], at2_ref.at[:, block(core, n_seq)], t_sem.at[0], t_sem.at[1], at.partner)
    spots = [send(pos_hbm, spot_ref.at[me], p_ssem, p_rsem.at[0], peer) for peer in at.peers(True)]

    dys.start_first()
    x_in = pltpu.make_async_copy(x_hbm, dx_ref, loc_sem.at[1])
    x_in.start()
    for copy in spots:
        copy.start()
    small = [pltpu.make_async_copy(src, dst, loc_sem.at[2 + n]) for n, (src, dst) in enumerate(((gain_hbm, gain_ref), (bias_hbm, bias_ref), (freq_hbm, freq_ref), (pos_hbm, spot_ref.at[me])))]
    for copy in small:
        copy.start()
    for copy in small:
        copy.wait()

    freq = freq_ref[...]
    for b in range(n_batch):
        angle = freq * spot_ref[me, b:b + 1, :].astype(F32)
        cos, sin, none = jnp.cos(angle), jnp.sin(angle), jnp.zeros((quarter, seq), F32)
        rest = jnp.zeros((head_dim - 2 * quarter, seq), F32)
        for i, rows in enumerate(([cos, cos, rest + 1.0], [-sin, none, rest], [none, sin, rest])):
            tab_ref[i, b * seq:(b + 1) * seq, :] = jnp.concatenate(rows, axis=0).T

    gain = (1.0 + gain_ref[...]).reshape(1, width)
    bias = bias_ref[...].reshape(1, width)

    def project_all(wkv_ref, raw_ref, wq_vm, raw_sem, wq_sem, stage_sem):
        pieces = [(b, i) for b in range(n_batch) for i in range(width // n_rows)]
        there = lambda n: da_ref.at[pl.ds(n * seq, seq)]
        dy_in = [pltpu.make_async_copy(dy_ref.at[b, :, pl.ds(i * n_rows, n_rows)], there(n), stage_sem.at[n]) for n, (b, i) in enumerate(pieces)]
        dy_keep = [pltpu.make_async_copy(there(n), dy_all.at[me, b, :, pl.ds(i * n_rows, n_rows)], stage_sem.at[n]) for n, (b, i) in enumerate(pieces)]
        span = 64 * chips
        batch = raw_ref.shape[2] // span
        row = lax.broadcasted_iota(jnp.int32, (span, span), 0)
        col = lax.broadcasted_iota(jnp.int32, (span, span), 1)
        pick = jnp.where(col == lax.rem(row, 64) * chips + lax.div(row, 64), 1.0, 0.0).astype(BF16)

        def raw_in(s, slot):
            return [pltpu.make_async_copy(w.at[block(s, span * batch)], raw_ref.at[slot, i], raw_sem.at[slot, i]) for i, w in enumerate((wk_ref, wv_ref))]

        def wq_in(s, slot):
            return [pltpu.make_async_copy(wq_ref.at[block(s, 2)], wq_vm.at[slot], wq_sem.at[slot])]

        def part_heads(s, slot):
            for i in range(batch):
                sl = slice(i * span, (i + 1) * span)
                rows = dot(pick, jnp.concatenate([raw_ref[slot, 0, sl, :], raw_ref[slot, 1, sl, :]], axis=1)).astype(BF16)
                for n in range(chips):
                    wkv_ref[n, block(s * batch + i, 64), :] = rows[n * 64:(n + 1) * 64]

        def turned(v):
            return v * tab_ref[0] + pltpu.roll(v, head_dim - quarter, 1) * tab_ref[1] + pltpu.roll(v, quarter, 1) * tab_ref[2]

        def project(s, slot):
            y = dot(h_ref[...], jnp.concatenate([wq_vm[slot, 0], wq_vm[slot, 1]], axis=1))
            for i in range(2):
                head = s * 2 + i
                v = turned(y[:, i * head_dim:(i + 1) * head_dim]).astype(BF16)
                for b in range(n_batch):
                    g_ref[lax.div(head, group) * n_batch + b, :, block(lax.rem(head, group), head_dim)] = v[b * seq:(b + 1) * seq]

        kv_ring = Ring(width // (64 * batch), raw_ref.shape[0], raw_in)
        q_ring = Ring(chips * group // 2, wq_vm.shape[0], wq_in)
        kv_ring.prime()
        q_ring.prime()
        for copy in dy_in:
            copy.start()
        x_in.wait()
        with scope('norm'):
            @pl.loop(0, n_tok // (2 * ROWS))
            def _(step):
                for i in range(2):
                    sl = block(2 * step + i, ROWS)
                    hat, _ = layer_norm(dx_ref[sl, :].astype(F32))
                    h_ref[sl, :] = (hat * gain + bias).astype(BF16)

        with scope('heads_kv'):
            kv_ring.run(part_heads)
        keep = pltpu.make_async_copy(wkv_ref, wkv_all, mix_sem.at[2])
        keep.start()
        for come, go in zip(dy_in, dy_keep):
            come.wait()
            go.start()
        with scope('project_kv'):
            @pl.loop(0, chips)
            def _(n):
                y = dot(h_ref[...], wkv_ref[n])
                v = jnp.concatenate([turned(y[:, :head_dim]), y[:, head_dim:]], axis=1).astype(BF16)
                for b in range(n_batch):
                    far_ref[b, me, :, block(n, 2 * head_dim)] = v[b * seq:(b + 1) * seq]

        kvs.start_first()
        kvs.start_second()
        with scope('project_q'):
            q_ring.run(project)
        keep.wait()
        for copy in dy_keep:
            copy.wait()

    pl.run_scoped(
        project_all,
        pltpu.VMEM((chips, width, 2 * head_dim), BF16),
        pltpu.VMEM((3, 2, 4 * 64 * chips, head_dim), BF16), pltpu.VMEM((4, 2, width, head_dim), BF16),
        pltpu.SemaphoreType.DMA((3, 2)), pltpu.SemaphoreType.DMA((4,)), pltpu.SemaphoreType.DMA((n_batch * width // n_rows,)),
    )

    with scope('kv_pass'):
        kvs.pass_on()
    queries.start()
    q_ref[me] = g_ref[me, :, q_part]
    with scope('turn_h'):
        @pl.loop(0, width // 128)
        def _(step):
            sl = block(step, 128)
            ht_ref[sl, :] = h_ref[:, sl].T

    with scope('kv_wait'):
        kvs.share_second()
        kvs.share_far()
        all_came(far_ref.at[:, pl.ds(0, chips), :, pl.ds(0, kv_cols)], kv_rsem.at[6], at.partner)

    def chip_at(i):
        return at.ring(jnp.where(i == 0, 0, jnp.where(i == 1, 1, jnp.where(i == 2, 3, 2))))

    def soft(s, seen):
        s = s * scale
        clear = s.shape[0] - seen.shape[0]
        tail = jnp.where(seen, s[clear:], -1e30)
        s = tail if clear == 0 else jnp.concatenate([s[:clear], tail], axis=0)
        e = jnp.exp(s - jnp.max(s, axis=0, keepdims=True))
        return e * (1.0 / jnp.sum(e, axis=0, keepdims=True))

    def attend(limit, clear):
        @pl.loop(0, n_batch * chips)
        def _(i):
            @pl.when(i == 1)
            def _():
                with scope('q_pass'):
                    queries.pass_on()
                dys.start_second()
                dys.pass_on()
                hcols.start()

            b, n = lax.rem(i, n_batch), lax.div(i, n_batch)
            k = far_ref[b, 0:limit // seq, :, block(2 * n, head_dim)].reshape(limit, head_dim)
            vt = far_ref[b, 0:limit // seq, :, block(2 * n + 1, head_dim)].reshape(limit, head_dim).T
            q = jnp.concatenate([g_ref[n * n_batch + b, :, block(j, head_dim)] for j in range(group)], axis=0)
            row = lax.broadcasted_iota(jnp.int32, (limit - clear, n_rows), 0)
            col = lax.broadcasted_iota(jnp.int32, (limit - clear, n_rows), 1)
            p = soft(dot_nt(k, q), row <= lax.rem(col, seq) + (me * seq - clear))
            mixed = dot(vt, p.astype(BF16)).astype(BF16)
            for j in range(group):
                h_ref[block(b, seq), block(n * group + j, head_dim)] = mixed[:, j * seq:(j + 1) * seq].T

    with scope('attend'):
        @pl.when(at.chip == chips - 1)
        def _():
            attend(chips * tile, (chips - 1) * tile)

        @pl.when(at.chip < chips - 1)
        def _():
            attend((chips - 1) * tile, 0)

    h_keep = pltpu.make_async_copy(ht_ref.at[block(me, half)], ht_all.at[me], loc_sem.at[1])
    h_keep.start()

    def block_out():
        def stream(wo_vm, sem):
            def wo_in(s, slot):
                return [pltpu.make_async_copy(wo_ref.at[:, block(s, OUT_TILE)], wo_vm.at[slot], sem.at[slot])]

            def out_tile(s, slot):
                sl = block(s, OUT_TILE)
                out_ref[:, sl] = (dx_ref[:, sl].astype(F32) + dot(h_ref[...], wo_vm[slot])).astype(BF16)

            ring = Ring(width // OUT_TILE, wo_vm.shape[0], wo_in)
            ring.prime()
            ring.run(out_tile)

        with scope('output'):
            pl.run_scoped(stream, pltpu.VMEM((4, width, OUT_TILE), BF16), pltpu.SemaphoreType.DMA((4,)))

    k_all = lambda n: far_ref[core, 0:n, :, block(2 * at.chip, head_dim)].reshape(n * seq, head_dim)
    v_all = lambda n: far_ref[core, 0:n, :, block(2 * at.chip + 1, head_dim)].reshape(n * seq, head_dim)

    def rotate_back(t, cos, sin):
        u, w = t[:quarter], t[quarter:2 * quarter]
        return jnp.concatenate([u * cos + w * sin, w * cos - u * sin, t[2 * quarter:]], axis=0)

    def by_dev(t):
        return t.astype(BF16).reshape(t.shape[0] // seq, seq, head_dim)

    def attend_back(t, i):
        limit = (t + 1) * tile
        sl = slice(t * tile, limit)
        devs = slice(t * CORES, (t + 1) * CORES)

        def heads(first, count):
            each = range(count)
            q = jnp.concatenate([q_ref[devs, :, block(first + j, head_dim)].reshape(tile, head_dim) for j in each], axis=0)
            da = jnp.concatenate([da_ref[sl, block(first + j, head_dim)] for j in each], axis=0)
            k, v = k_all(limit // seq), v_all(limit // seq)
            row = lax.broadcasted_iota(jnp.int32, (tile, count * tile), 0)
            col = lax.broadcasted_iota(jnp.int32, (tile, count * tile), 1)
            p = soft(dot_nt(k, q), row <= lax.rem(col, tile))
            p_low = p.astype(BF16)
            mixed = dot(vt_ref[:, :limit], p_low).astype(BF16)
            dp = dot_nt(v, da)
            row_dot = jnp.sum(p * dp, axis=0, keepdims=True)
            ds = (p * (dp - row_dot) * scale).astype(BF16)
            dv_ref[:limit, :] += dot(p_low, da)
            dk_ref[:limit, :] += dot(ds, q)
            back = dot(kt_ref[:, :limit], ds)
            for j in each:
                part = slice(j * tile, (j + 1) * tile)
                at_ref[block(first + j, head_dim), sl] = mixed[:, part]
                g_ref[devs, :, block(first + j, head_dim)] = by_dev(rotate_back(back[:, part], cost_ref[:, sl], sint_ref[:, sl]).T)

        @pl.loop(0, group // 2)
        def _(j):
            heads(2 * j, 2)

        @pl.when(i == chips - 2)
        def _():
            with scope('dy_far'):
                dys.share_far()

        heads(group - 1, 1)

    def middle(wo_vm, dyk):
        wo_in = pltpu.make_async_copy(wo_ref.at[block(at.chip, n_rows)], wo_vm, mix_sem.at[2])
        wo_in.start()
        all_came(spot_ref.at[pl.ds(0, n_dev - 1)], p_rsem.at[0], at.partner)
        for d in range(n_dev):
            angle = freq * spot_ref[d, pl.ds(core, 1), :].astype(F32)
            cost_ref[:, d * seq:(d + 1) * seq] = jnp.cos(angle)
            sint_ref[:, d * seq:(d + 1) * seq] = jnp.sin(angle)
        with scope('q_wait'):
            all_came(q_ref.at[pl.ds(0, n_dev - 1)], q_rsem.at[0], at.partner)
            all_sent(block_total, q_ssem, at.partner)
            all_sent(far_ref.at[:, pl.ds(0, n_dev - 1), :, pl.ds(0, kv_cols)], kv_ssem, at.partner)
            all_sent(spot_ref.at[pl.ds(0, n_dev - 1)], p_ssem, at.partner)
        kt_ref[...] = k_all(n_dev).T
        vt_ref[...] = v_all(n_dev).T
        dk_ref[...] = jnp.zeros_like(dk_ref)
        dv_ref[...] = jnp.zeros_like(dv_ref)
        dys.own_across.wait_recv()

        def fetch(i, slot):
            return pltpu.make_async_copy(dy_all.at[block(chip_at(i), CORES), core], dyk.at[slot], mix_sem.at[slot])

        with scope('wo_wait'):
            fetch(0, 0).start()
            wo_in.wait()

        @pl.loop(0, chips)
        def _(i):
            slot = lax.rem(i, 2)

            @pl.when((i == 1) & (at.chip < chips - 1))
            def _():
                block_out()

            @pl.when(i == 1)
            def _():
                with scope('dy_wait'):
                    dys.share_second()
                    all_came(dy_all.at[pl.ds(0, 2)], dy_rsem.at[7], at.partner)
                fetch(i, slot).start()

            @pl.when(i == chips - 1)
            def _():
                with scope('dy_far2'):
                    all_came(dy_all.at[0], dy_rsem.at[8], at.partner)
                fetch(i, slot).start()
                with scope('h_pass'):
                    hcols.pass_on()

            fetch(i, slot).wait()

            @pl.when((i > 0) & (i < chips - 2))
            def _():
                fetch(i + 1, 1 - slot).start()

            chip = chip_at(i)
            with scope('da'):
                da_ref[block(chip, tile), :] = dot_nt(dyk[slot].reshape(tile, width), wo_vm[...]).astype(BF16)
            with scope('attend_back'):
                for t in range(chips):
                    @pl.when(chip == t)
                    def _(t=t):
                        attend_back(t, i)

    pl.run_scoped(middle, pltpu.VMEM((n_rows, width), BF16), pltpu.VMEM((2, CORES, seq, width), BF16))
    all_sent(dy_all.at[pl.ds(0, n_dev - 1)], dy_ssem, at.partner)
    heads_across.start()
    g_ref[:, :, n_rows:n_rows + head_dim] = by_dev(rotate_back(dk_ref[...].T, cost_ref[...], sint_ref[...]).T)
    g_ref[:, :, n_rows + head_dim:] = by_dev(dv_ref[...])

    def span_of(q):
        return block(q, CORES)

    turn = [[at.ring(q) for q in (2, 1, 3, 0)], [at.ring(q) for q in (3, 0, 1, 2)]]
    direct = [[send(g_ref.at[span_of(turn[i][q])], g_all.at[me, span_of(turn[i][q])], kv_ssem, kv_rsem.at[i * chips + q], at.dev(steps[i], core)) for q in range(chips)] for i in range(2)]
    came = [[at.ring(q) for q in (1, 0, 2, 3)], [at.ring(q) for q in (0, 1, 2, 3)]]
    def halves_of(quarters):
        return [span_of(quarters[0])] + [pl.ds(quarters[1] * CORES + c, 1) for c in range(CORES)]

    onward = [[send(g_all.at[origin[i], sl], far_ref.at[core, sl], q_ssem, q_rsem.at[3 * i + q], at.dev(steps[i], core)) for q, sl in enumerate(halves_of(came[i]))] for i in range(2)]
    ends = [[at.ring(q) for q in (0, 3)], [at.ring(q) for q in (1, 2)]]
    g_across = send(g_ref, g_all.at[me], x_ssem, dy_rsem.at[0], at.partner)
    near_across = [[send(g_all.at[origin[i], span_of(came[i][q])], g_all.at[origin[i], span_of(came[i][q])], x_ssem, dy_rsem.at[1 + q // 2], at.partner) for q in range(chips)] for i in range(2)]
    end_across = [[send(far_ref.at[core, sl], far_ref.at[core, sl], x_ssem, dy_rsem.at[3 + q], at.partner) for q, sl in enumerate(halves_of(ends[i]))] for i in range(2)]
    for q in range(chips):
        for i in range(2):
            direct[i][q].start()
    g_across.start()
    g_keep = pltpu.make_async_copy(g_ref, g_all.at[me], loc_sem.at[0])
    g_keep.start()
    at2_ref[:, block(core, n_seq)] = at_ref[block(core, half), :]

    @pl.when(at.chip == chips - 1)
    def _():
        block_out()

    dy_back = [pltpu.make_async_copy(dy_ref.at[b], h_ref.at[pl.ds(b * seq, seq)], loc_sem.at[2 + b]) for b in range(n_batch)]
    for copy in dy_back:
        copy.start()

    def wo_rows(dy_vm, sem):
        def dy_tile(s, slot):
            return [pltpu.make_async_copy(dy_all.at[:, :, :, block(s, COL_TILE)], dy_vm.at[slot], sem.at[slot])]

        def wo_tile(s, slot):
            pieces = [dy_vm[slot, d, b] for b in range(n_batch) for d in range(n_dev)]
            dwo_ref[:, block(s, COL_TILE)] = dot(at2_ref[...], jnp.concatenate(pieces, axis=0))

        ring = Ring(width // COL_TILE, dy_vm.shape[0], dy_tile)
        ring.prime()
        with scope('heads_wait'):
            heads_across.wait_recv()
        with scope('grad_wo'):
            ring.run(wo_tile)

    pl.run_scoped(wo_rows, pltpu.VMEM((4, n_dev, n_batch, seq, COL_TILE), BF16), pltpu.SemaphoreType.DMA((4,)))

    with scope('h_wait'):
        all_came(ht_all.at[pl.ds(0, n_dev - 1)], h_rsem.at[0], at.partner)
        all_sent(block_total, h_ssem, at.partner)
    h_keep.wait()
    lhs_in = [pltpu.make_async_copy(ht_all.at[d, :, pl.ds(b * seq, seq)], at2_ref.at[:, pl.ds((b * n_dev + d) * seq, seq)], lhs_sem.at[0]) for d in range(n_dev) for b in range(n_batch)]
    for copy in lhs_in:
        copy.start()
    with jax.named_scope('own_wait'):
        pltpu.make_async_copy(at2_ref, at2_ref, lhs_sem.at[0]).wait()
        g_keep.wait()
        g_across.wait_recv()
    pair_across = send(pair_ref.at[core], pair_ref.at[core], p_ssem, p_rsem.at[1], at.partner)
    rows_out = [send(row_ref.at[at.chip], row_ref.at[at.chip], p_ssem, p_rsem.at[2], at.dev(step, core)) for step in (1, -1, 2)]
    total_across = send(total_ref.at[core], total_ref.at[core], p_ssem, p_rsem.at[3], at.partner)

    def weight_grads(wq_vm, wkv_vm, acc_ref, hat_ref, inv_ref, job_ref, mine_ref):
        n_slots = wq_vm.shape[0]
        chunk = wq_vm.shape[2]
        n_chunks = width // chunk
        total = n_chunks * chips

        def weights(s):
            slot = lax.rem(s, n_slots)
            chip = chip_at(lax.div(s, n_chunks))
            rows = block(lax.rem(s, n_chunks), chunk)
            return [
                pltpu.make_async_copy(wq_ref.at[block(chip, group), rows], wq_vm.at[slot], w_sem.at[slot, 0]),
                pltpu.make_async_copy(wkv_all.at[chip, rows], wkv_vm.at[slot], w_sem.at[slot, 1]),
            ]

        for s in range(n_slots):
            for copy in weights(s):
                copy.start()

        def grow(i, read):
            @pl.loop(0, n_chunks)
            def _(n):
                s = i * n_chunks + n
                slot = lax.rem(s, n_slots)
                for copy in weights(s):
                    copy.wait()
                rows = jnp.concatenate([read(b) for b in range(n_batch)], axis=0)
                part = dot_nt(rows, jnp.concatenate([wq_vm[slot, j] for j in range(group)] + [wkv_vm[slot]], axis=1))
                sl = block(n, chunk)

                @pl.when(i == 0)
                def _():
                    acc_ref[:, sl] = part

                @pl.when(i > 0)
                def _():
                    acc_ref[:, sl] += part

                @pl.when(s + n_slots < total)
                def _():
                    for copy in weights(s + n_slots):
                        copy.start()

        def mine_in(i):
            return [pltpu.make_async_copy(g_all.at[chip_at(i) * CORES + b, me], mine_ref.at[lax.rem(i, 2), b], job_sem.at[2 + lax.rem(i, 2)]) for b in range(n_batch)]

        def grow_near(i):
            here = mine_ref.at[lax.rem(i, 2)]
            pltpu.make_async_copy(here, here, job_sem.at[2 + lax.rem(i, 2)]).wait()
            grow(i, lambda b: mine_ref[lax.rem(i, 2), b])

        def job_in(chip, quarters, slot):
            return [pltpu.make_async_copy(g_all.at[chip * CORES + b, span_of(q)], job_ref.at[slot, b, n], job_sem.at[slot]) for b in range(n_batch) for n, q in enumerate(quarters)]

        def job(chip, pieces, read, add):
            lhs = [at2_ref[:, pl.ds(pl.multiple_of(b * n_seq + d * seq, seq), seq)] for b in range(n_batch) for d in pieces]
            rhs = [read(b, n) for b in range(n_batch) for n in range(len(pieces))]
            y = dot(jnp.concatenate(lhs, axis=1), jnp.concatenate(rhs, axis=0))
            for j in range(group):
                v = y[:, j * head_dim:(j + 1) * head_dim]
                dwq_ref[chip * group + j] = dwq_ref[chip * group + j] + v if add else v
            for j, ref in enumerate((dwk_ref, dwv_ref)):
                v = y[:, (group + j) * head_dim:(group + j + 1) * head_dim]
                rows = pl.ds(chip, half, stride=chips)
                ref[rows, :] = ref[rows, :] + v if add else v

        def devs_of(quarters):
            return [q * CORES + c for q in quarters for c in range(CORES)]

        def near_pair(quarters, add):
            for slot, step in enumerate(steps):
                for copy in job_in(at.ring(step), quarters, slot):
                    copy.start()

            @pl.loop(0, 2)
            def _(slot):
                chip = at.ring(1 - 2 * slot)
                pltpu.make_async_copy(job_ref.at[slot], job_ref.at[slot], job_sem.at[slot]).wait()
                job(chip, devs_of(quarters), lambda b, n: job_ref[slot, b, n // CORES, n % CORES], add)

        halves = [[at.ring(q) for q in half_of] for half_of in ((0, 1), (2, 3))]
        for slot in range(2):
            for copy in job_in(at.chip, [at.ring(2 * slot), at.ring(2 * slot + 1)], slot):
                copy.start()
        for copy in mine_in(0):
            copy.start()
        with jax.named_scope('own_job'):
            for slot in range(2):
                quarters = [at.ring(2 * slot), at.ring(2 * slot + 1)]
                pltpu.make_async_copy(job_ref.at[slot], job_ref.at[slot], job_sem.at[slot]).wait()
                job(at.chip, devs_of(quarters), lambda b, n: job_ref[slot, b, n // CORES, n % CORES], slot == 1)

        with jax.named_scope('own_dh'):
            grow_near(0)

        with jax.named_scope('d01_wait'):
            for q in range(2):
                for i in range(2):
                    direct[i][q].wait_recv()
                for i in range(2):
                    for copy in onward[i][:1] if q == 0 else onward[i][1:]:
                        copy.start()
                    near_across[i][q].start()
        with scope('d01_across'):
            all_came(g_all.at[0], dy_rsem.at[1], at.partner)
        for i in (1, 2):
            for copy in mine_in(i):
                copy.start()
        with scope('near_dh'):
            @pl.loop(1, chips - 1)
            def _(i):
                grow_near(i)

        with jax.named_scope('near_a'):
            near_pair(halves[0], False)
        with scope('d2_wait'):
            for i in range(2):
                direct[i][2].wait_recv()
                near_across[i][2].start()
        with jax.named_scope('hat'):
            @pl.loop(0, n_tok // (2 * ROWS))
            def _(step):
                for i in range(2):
                    sl = block(2 * step + i, ROWS)
                    hat, inv = layer_norm(dx_ref[sl, :].astype(F32))
                    hat_ref[sl, :] = hat
                    inv_ref[sl, :] = jnp.broadcast_to(inv, (ROWS, 128))

        with scope('d3_wait'):
            for i in range(2):
                direct[i][3].wait_recv()
                near_across[i][3].start()
        with scope('d23_across'):
            all_came(g_all.at[0], dy_rsem.at[2], at.partner)
        with jax.named_scope('near_b'):
            near_pair(halves[1], True)
        far_chip = at.ring(2)
        with jax.named_scope('far0_wait'):
            for i in range(2):
                onward[i][0].wait_recv()
                end_across[i][0].start()
        with scope('far0_across'):
            all_came(g_all.at[0, pl.ds(0, chips)], dy_rsem.at[3], at.partner)
        with jax.named_scope('far_dh'):
            grow(chips - 1, lambda b: far_ref[b, me])
        for copy in dy_back:
            copy.wait()
        part_ref[...] = jnp.zeros_like(part_ref)

        with jax.named_scope('norm_back'):
            @pl.loop(0, n_tok // (2 * ROWS))
            def _(step):
                for i in range(2):
                    sl = block(2 * step + i, ROWS)
                    hat, inv = hat_ref[sl, :], inv_ref[sl, 0:1]
                    dh = acc_ref[sl, :]
                    dg = dh * hat
                    gh = dh * gain
                    one = jnp.mean(gh, axis=-1, keepdims=True)
                    two = jnp.mean(dg * gain, axis=-1, keepdims=True)
                    dx_ref[sl, :] = (h_ref[sl, :].astype(F32) + inv * (gh - one - hat * two)).astype(BF16)
                    part_ref[0] += dg[0:8] + dg[8:16]
                    part_ref[1] += dh[0:8] + dh[8:16]

        for i in range(2):
            pair_ref[core, i:i + 1, :] = jnp.sum(part_ref[i], axis=0, keepdims=True)
        pair_across.start()

        def hand_on(c):
            with scope('far1_wait'):
                for i in range(2):
                    onward[i][1 + c].wait_recv()
                    end_across[i][1 + c].start()

        hand_on(0)
        with scope('far_a'):
            first_devs = devs_of([ends[0][0], ends[1][0]])
            job(far_chip, first_devs, lambda b, n: far_ref[b, first_devs[n]], False)
        with scope('rows'):
            all_came(pair_ref.at[0], p_rsem.at[1], at.partner)
            all_sent(pair_ref.at[0], p_ssem, at.partner)
            row_ref[at.chip] = pair_ref[0, pl.ds(core, 1), :] + pair_ref[1, pl.ds(core, 1), :]
            for copy in rows_out:
                copy.start()
        for c in range(CORES):
            if c > 0:
                hand_on(c)
                with scope('total'):
                    all_came(row_ref.at[pl.ds(0, chips - 1)], p_rsem.at[2], at.partner)
                    all_sent(row_ref.at[pl.ds(0, chips - 1)], p_ssem, at.partner)
                    total = row_ref[0]
                    for n in range(1, chips):
                        total = total + row_ref[n]
                    total_ref[core] = total
                    total_across.start()
            with scope('far1_across'):
                all_came(g_all.at[0, pl.ds(0, CORES)], dy_rsem.at[4 + c], at.partner)
            with scope('far_b'):
                last_devs = [ends[i][1] * CORES + c for i in range(2)]
                job(far_chip, last_devs, lambda b, n: far_ref[b, last_devs[n]], True)

    pl.run_scoped(
        weight_grads,
        pltpu.VMEM((W_SLOTS, group, W_ROWS, head_dim), BF16), pltpu.VMEM((W_SLOTS, W_ROWS, 2 * head_dim), BF16), pltpu.VMEM((n_tok, width), F32),
        pltpu.VMEM((n_tok, width), F32), pltpu.VMEM((n_tok, 128), F32), pltpu.VMEM((2, n_batch, 2, CORES, seq, cols), BF16), pltpu.VMEM((2, n_batch, seq, cols), BF16),
    )

    with scope('sums'):
        all_came(total_ref.at[0], p_rsem.at[3], at.partner)
        dgain_ref[...] = total_ref[0].reshape(width)
        dbias_ref[...] = total_ref[1].reshape(width)
    with scope('done'):
        heads_across.wait_send()
        all_sent(far_ref, kv_ssem, at.partner)
        all_sent(g_ref, q_ssem, at.partner)
        all_sent(g_all.at[pl.ds(0, chips)], x_ssem, at.partner)
        all_sent(total_ref.at[0], p_ssem, at.partner)


def whole_block(n_dev, x, gain, bias, positions, freq, dy, wq, wk, wv, wo):
    n_batch, seq, width = dy.shape
    n_tok = n_batch * seq
    head_dim = wq.shape[2]
    chips = n_dev // CORES
    group = wq.shape[0] // chips
    cols = (group + 2) * head_dim
    n_rows = group * head_dim
    half = n_rows // CORES
    n_seq = n_dev * seq
    quarter = head_dim // 4
    dma = pltpu.SemaphoreType.DMA
    vm = pltpu.VMEM
    shapes = [((n_tok, width), BF16)] * 2 + [((chips * group, half, head_dim), F32)] + [((chips * half, head_dim), F32)] * 2 + [((half, width), F32), ((width,), F32), ((width,), F32)]
    held = [((n_dev, n_batch, seq, width), BF16), ((n_dev, half, n_tok), BF16), ((n_dev, n_dev, seq, cols), BF16), ((chips, width, 2 * head_dim), BF16)]
    return pl.pallas_call(
        functools.partial(block_body, n_dev, group),
        out_shape=tuple(pltpu.VMEM(*t) for t in shapes) + tuple(sds(*t) for t in held),
        in_specs=[HBM] * 10,
        out_specs=(VM,) * len(shapes) + (HBM,) * len(held),
        scratch_shapes=[
            vm((n_tok, width), BF16), vm((width, n_tok), BF16), vm((n_dev, seq, cols), BF16), vm((n_dev, seq, n_rows), BF16),
            vm((n_rows, n_seq), BF16), vm((half, n_batch * n_seq), BF16), vm((n_seq, n_rows), BF16),
            vm((head_dim, n_seq), BF16), vm((head_dim, n_seq), BF16), vm((n_seq, head_dim), F32), vm((n_seq, head_dim), F32),
            vm((quarter, n_seq), F32), vm((quarter, n_seq), F32), vm((3, n_tok, head_dim), F32), vm((n_dev, n_batch, seq), jnp.int32), vm((width,), F32), vm((width,), F32), vm((quarter, 1), F32),
            vm((2, seq, n_rows), BF16), vm((2, half, n_tok), BF16),
            vm((n_batch, n_dev, seq, cols), BF16), vm((2, 8, width), F32), vm((CORES, 2, width), F32), vm((chips, 1, width), F32), vm((CORES, 1, width), F32),
            dma((6,)), dma((9,)), dma((8,)), dma((6,)), dma((3,)), dma((4,)), dma((2,)),
            dma((6,)), dma((3,)), dma((1,)), dma((W_SLOTS, 2)), dma((4,)),
        ],
        compiler_params=pltpu.CompilerParams(collective_id=0, has_side_effects=True, vmem_limit_bytes=VMEM_LIMIT),
        cost_estimate=pl.CostEstimate(flops=10 ** 11, bytes_accessed=10 ** 8, transcendentals=0),
        name='block',
    )(gain, bias, positions, freq, x.reshape(n_tok, width), dy, wq, wk, wv, wo)[:len(shapes)]


def settle_body(n, *refs):
    sem = refs[2 * n]
    copies = []
    for src, dst in zip(refs[:n], refs[n:2 * n]):
        pieces = SETTLE if len(src.shape) > 1 else 1
        size = src.shape[0] // pieces
        copies += [pltpu.make_async_copy(src.at[pl.ds(p * size, size)], dst.at[pl.ds(p * size, size)], sem) for p in range(pieces)]
    for copy in copies:
        copy.start()
    for copy in copies:
        copy.wait()


def settle(arrays):
    n = len(arrays)
    return pl.pallas_call(
        functools.partial(settle_body, n),
        out_shape=tuple(sds(t.shape, t.dtype) for t in arrays),
        in_specs=[ANY] * n,
        out_specs=(HBM,) * n,
        scratch_shapes=[pltpu.SemaphoreType.DMA],
        compiler_params=pltpu.CompilerParams(vmem_limit_bytes=1024 * 1024),
        name='settle',
    )(*arrays)


def solution(mesh):
    n_dev = mesh.shape['cp']

    def device_step(x_act, d_out, positions, ln_gain, ln_bias, w_query, w_key, w_value, w_out):
        n_batch, seq, width = x_act.shape
        q_heads, (kv_heads, head_dim) = w_query.shape[1], w_key.shape[1:]
        group = q_heads // kv_heads
        quarter = head_dim // 4
        assert n_batch == CORES and n_dev // CORES == kv_heads == 4 and q_heads * head_dim == width

        freq = np.exp(np.arange(quarter) * (-2.0 * math.log(ROPE_BASE) / (head_dim // 2))).astype(np.float32).reshape(quarter, 1)
        by_head = lambda t: jnp.transpose(t, (1, 0, 2))
        by_row = lambda t: t.reshape(width * kv_heads, head_dim)
        wq = by_head(w_query)

        results = whole_block(n_dev, x_act, ln_gain, ln_bias, positions, jnp.asarray(freq), d_out, wq, by_row(w_key), by_row(w_value), w_out)
        out, dx, dwq, dwk, dwv, dwo, dgain, dbias = settle(results)
        kv_rows = lambda t: t.reshape(width // n_dev, kv_heads, head_dim)
        return (out.reshape(x_act.shape), dx.reshape(x_act.shape), by_head(dwq), kv_rows(dwk), kv_rows(dwv), dwo, dgain, dbias)

    return jax.shard_map(device_step, mesh=mesh, in_specs=(P('dp', 'cp', None), P('dp', 'cp', None), P('dp', 'cp'), P(None), P(None), P(None, None, None), P(None, None, None), P(None, None, None), P(None, None)), out_specs=(P('dp', 'cp', None), P('dp', 'cp', None), P(('dp', 'cp'), None, None), P(('dp', 'cp'), None, None), P(('dp', 'cp'), None, None), P(('dp', 'cp'), None), P('dp'), P('dp')), check_vma=False)
```

```python
import functools
import math
import jax
import jax.numpy as jnp
import numpy as np
from jax import lax
from jax.experimental import pallas as pl
from jax.experimental.pallas import tpu as pltpu
from jax.sharding import PartitionSpec as P

EPS = 1e-5
ROPE_BASE = 10000.0
BF16 = jnp.bfloat16
F32 = jnp.float32
VMEM_LIMIT = 46 * 1024 * 1024
NT = (((1,), (1,)), ((), ()))
ANY = pl.BlockSpec(memory_space=pl.ANY)
VM = pl.BlockSpec(memory_space=pltpu.VMEM)
HBM = pl.BlockSpec(memory_space=pltpu.HBM)
CORES = 2
PAIR = range(2)
STEPS = (1, -1)
COL_TILE = 512
OUT_TILE = 256
ROWS = 16
W_SLOTS = 4
W_ROWS = 512
SETTLE = 4


def dot(a, b):
    return jnp.dot(a, b, preferred_element_type=F32)


def dot_nt(a, b):
    return lax.dot_general(a, b, NT, preferred_element_type=F32)


def sds(shape, dtype):
    return jax.ShapeDtypeStruct(shape, dtype)


def block(i, size):
    return pl.ds(pl.multiple_of(i * size, size), size)


class Place:
    def __init__(self, n_dev):
        self.n_dev = n_dev
        self.chips = n_dev // CORES
        self.me = lax.axis_index('cp')
        self.chip = self.me // CORES
        self.core = self.me % CORES
        self.partner = self.chip * CORES + 1 - self.core

    def ring(self, step):
        return lax.rem(self.chip + self.chips + step, self.chips)

    def dev(self, step, core):
        return self.ring(step) * CORES + core

    def peers(self, far):
        near = [self.partner] + [self.dev(s, c) for s in STEPS for c in range(CORES)]
        return near + ([self.dev(2, c) for c in range(CORES)] if far else [])


def send(src, dst, ssem, rsem, to):
    return pltpu.make_async_remote_copy(src_ref=src, dst_ref=dst, send_sem=ssem, recv_sem=rsem, device_id={'cp': to}, device_id_type=pl.DeviceIdType.MESH)


def all_sent(total, ssem, to):
    send(total, total, ssem, ssem, to).wait_send()


def all_came(total, rsem, to):
    send(total, total, rsem, rsem, to).wait_recv()


def meet(peers):
    barrier = pltpu.get_barrier_semaphore()
    for peer in peers:
        pl.semaphore_signal(barrier, inc=1, device_id={'cp': peer}, device_id_type=pl.DeviceIdType.MESH)
    pl.semaphore_wait(barrier, len(peers))


class Ring:
    def __init__(self, n, slots, copies):
        self.n, self.slots, self.copies = n, slots, copies

    def prime(self):
        for s in range(self.slots):
            for copy in self.copies(s, s):
                copy.start()

    def run(self, use):
        @pl.loop(0, self.n)
        def _(s):
            slot = lax.rem(s, self.slots)
            for copy in self.copies(s, slot):
                copy.wait()
            use(s, slot)

            @pl.when(s + self.slots < self.n)
            def _():
                for copy in self.copies(s + self.slots, slot):
                    copy.start()


class Gather:
    def __init__(self, at, own, piece, both, ssem, rsem, across):
        steps = STEPS
        origin = [at.dev(-1, at.core), at.dev(1, at.core)]
        far = at.dev(2, at.core)
        link = lambda i, src, dst, to: send(src, dst, ssem, rsem.at[i], to)
        self.first = [link(b, own(b), piece(at.me, b), at.dev(steps[b], at.core)) for b in PAIR]
        self.second = [link(2 + b, own(1 - b), piece(at.me, 1 - b), at.dev(steps[b], at.core)) for b in PAIR]
        self.again = [link(4 + b, piece(origin[b], b), piece(origin[b], b), at.dev(steps[b], at.core)) for b in PAIR]
        self.own_across = link(across[0], both(None), both(at.me), at.partner)
        self.first_across = [link(across[1], piece(origin[b], b), piece(origin[b], b), at.partner) for b in PAIR]
        self.second_across = [link(across[1], piece(origin[b], 1 - b), piece(origin[b], 1 - b), at.partner) for b in PAIR]
        self.far_across = [link(across[2], piece(far, b), piece(far, b), at.partner) for b in PAIR]

    def start_first(self):
        for copy in self.first + [self.own_across]:
            copy.start()

    def start_second(self):
        for copy in self.second:
            copy.start()

    def pass_on(self):
        for copy, again, across in zip(self.first, self.again, self.first_across):
            copy.wait_recv()
            again.start()
            across.start()

    def share_second(self):
        for copy, across in zip(self.second, self.second_across):
            copy.wait_recv()
            across.start()

    def share_far(self):
        for copy, across in zip(self.again, self.far_across):
            copy.wait_recv()
            across.start()


class Exchange:
    def __init__(self, at, src, dst, relay, ssem, rsem):
        near = [(0, 1 - at.core)] + [(s, c) for s in STEPS for c in range(CORES)]
        self.near = [send(src(at.dev(s, c)), dst(at.me), ssem, rsem.at[0], at.dev(s, c)) for s, c in near]
        self.far = [send(src(at.dev(2, i)), relay.at[i], ssem, rsem.at[1 + i], at.dev(step, at.core)) for i, step in enumerate(STEPS)]
        self.on = [send(relay.at[i], dst(at.dev(-step, at.core)), ssem, rsem.at[0], at.dev(step, i)) for i, step in enumerate(STEPS)]

    def start(self):
        for copy in self.far + self.near:
            copy.start()

    def pass_on(self):
        for far, on in zip(self.far, self.on):
            far.wait_recv()
            on.start()


def layer_norm(x):
    cen = x - jnp.mean(x, axis=-1, keepdims=True)
    inv = lax.rsqrt(jnp.mean(cen * cen, axis=-1, keepdims=True) + EPS)
    return cen * inv, inv


def block_body(n_dev, group, gain_hbm, bias_hbm, pos_hbm, freq_hbm, x_hbm, dy_ref, wq_ref, wk_ref, wv_ref, wo_ref,
               out_ref, dx_ref, dwq_ref, dwk_ref, dwv_ref, dwo_ref, dgain_ref, dbias_ref, dy_all, ht_all, g_all, wkv_all,
               h_ref, ht_ref, g_ref, q_ref, at_ref, at2_ref, da_ref, kt_ref, vt_ref, dk_ref, dv_ref,
               cost_ref, sint_ref, tab_ref, spot_ref, gain_ref, bias_ref, freq_ref, relay_q, relay_h, far_ref, part_ref, row_ref, total_ref,
               s_sem, dy_rsem, kv_rsem, q_rsem, h_rsem, p_rsem, t_sem, loc_sem, mix_sem, lhs_sem, w_sem, job_sem):
    at = Place(n_dev)
    n_batch, seq, width = dy_ref.shape
    n_tok = n_batch * seq
    head_dim = wq_ref.shape[2]
    cols = (group + 2) * head_dim
    n_rows = group * head_dim
    half = n_rows // CORES
    n_seq = n_dev * seq
    quarter = head_dim // 4
    scale = head_dim ** -0.5
    chips = at.chips
    tile = CORES * seq
    core, me = at.core, at.me
    steps = STEPS
    origin = [at.dev(-1, core), at.dev(1, core)]
    far_dev = at.dev(2, core)
    scope = jax.named_scope

    dy_ssem, kv_ssem, q_ssem, h_ssem, p_ssem, x_ssem = [s_sem.at[i] for i in range(6)]
    assert (n_dev + 1) * n_rows == (n_dev - 1) * cols
    block_total = far_ref.at[0, pl.ds(0, n_dev - 1)]

    with scope('meet'):
        meet(at.peers(True))

    kv_cols = 2 * head_dim * chips
    kv_piece = lambda d, b: far_ref.at[b, d, :, pl.ds(0, kv_cols)]
    kv_both = lambda d: far_ref.at[:, me if d is None else d, :, pl.ds(0, kv_cols)]
    dys = Gather(at, lambda b: dy_ref.at[b], lambda d, b: dy_all.at[d, b], lambda d: dy_ref if d is None else dy_all.at[d], dy_ssem, dy_rsem, (6, 7, 8))
    kvs = Gather(at, lambda b: kv_piece(me, b), kv_piece, kv_both, kv_ssem, kv_rsem, (6, 6, 6))
    q_part = pl.ds(0, n_rows)
    queries = Exchange(at, lambda d: g_ref.at[d, :, q_part], lambda d: q_ref.at[d], relay_q, q_ssem, q_rsem)
    hcols = Exchange(at, lambda d: ht_ref.at[block(d, half)], lambda d: ht_all.at[d], relay_h, h_ssem, h_rsem)
    heads_across = send(at_ref.at[block(1 - core, half)], at2_ref.at[:, block(core, n_seq)], t_sem.at[0], t_sem.at[1], at.partner)
    spots = [send(pos_hbm, spot_ref.at[me], p_ssem, p_rsem.at[0], peer) for peer in at.peers(True)]

    dys.start_first()
    x_in = pltpu.make_async_copy(x_hbm, dx_ref, loc_sem.at[1])
    x_in.start()
    for copy in spots:
        copy.start()
    small = [pltpu.make_async_copy(src, dst, loc_sem.at[2 + n]) for n, (src, dst) in enumerate(((gain_hbm, gain_ref), (bias_hbm, bias_ref), (freq_hbm, freq_ref), (pos_hbm, spot_ref.at[me])))]
    for copy in small:
        copy.start()
    for copy in small:
        copy.wait()

    freq = freq_ref[...]
    for b in range(n_batch):
        angle = freq * spot_ref[me, b:b + 1, :].astype(F32)
        cos, sin, none = jnp.cos(angle), jnp.sin(angle), jnp.zeros((quarter, seq), F32)
        rest = jnp.zeros((head_dim - 2 * quarter, seq), F32)
        for i, rows in enumerate(([cos, cos, rest + 1.0], [-sin, none, rest], [none, sin, rest])):
            tab_ref[i, b * seq:(b + 1) * seq, :] = jnp.concatenate(rows, axis=0).T

    gain = (1.0 + gain_ref[...]).reshape(1, width)
    bias = bias_ref[...].reshape(1, width)

    def project_all(wkv_ref, raw_ref, wq_vm, raw_sem, wq_sem, stage_sem):
        pieces = [(b, i) for b in range(n_batch) for i in range(width // n_rows)]
        there = lambda n: da_ref.at[pl.ds(n * seq, seq)]
        dy_in = [pltpu.make_async_copy(dy_ref.at[b, :, pl.ds(i * n_rows, n_rows)], there(n), stage_sem.at[n]) for n, (b, i) in enumerate(pieces)]
        dy_keep = [pltpu.make_async_copy(there(n), dy_all.at[me, b, :, pl.ds(i * n_rows, n_rows)], stage_sem.at[n]) for n, (b, i) in enumerate(pieces)]
        span = 64 * chips
        batch = raw_ref.shape[2] // span
        row = lax.broadcasted_iota(jnp.int32, (span, span), 0)
        col = lax.broadcasted_iota(jnp.int32, (span, span), 1)
        pick = jnp.where(col == lax.rem(row, 64) * chips + lax.div(row, 64), 1.0, 0.0).astype(BF16)

        def raw_in(s, slot):
            return [pltpu.make_async_copy(w.at[block(s, span * batch)], raw_ref.at[slot, i], raw_sem.at[slot, i]) for i, w in enumerate((wk_ref, wv_ref))]

        def wq_in(s, slot):
            return [pltpu.make_async_copy(wq_ref.at[block(s, 2)], wq_vm.at[slot], wq_sem.at[slot])]

        def part_heads(s, slot):
            for i in range(batch):
                sl = slice(i * span, (i + 1) * span)
                rows = dot(pick, jnp.concatenate([raw_ref[slot, 0, sl, :], raw_ref[slot, 1, sl, :]], axis=1)).astype(BF16)
                for n in range(chips):
                    wkv_ref[n, block(s * batch + i, 64), :] = rows[n * 64:(n + 1) * 64]

        def turned(v):
            return v * tab_ref[0] + pltpu.roll(v, head_dim - quarter, 1) * tab_ref[1] + pltpu.roll(v, quarter, 1) * tab_ref[2]

        def project(s, slot):
            y = dot(h_ref[...], jnp.concatenate([wq_vm[slot, 0], wq_vm[slot, 1]], axis=1))
            for i in PAIR:
                head = s * 2 + i
                v = turned(y[:, i * head_dim:(i + 1) * head_dim]).astype(BF16)
                for b in range(n_batch):
                    g_ref[lax.div(head, group) * n_batch + b, :, block(lax.rem(head, group), head_dim)] = v[b * seq:(b + 1) * seq]

        kv_ring = Ring(width // (64 * batch), raw_ref.shape[0], raw_in)
        q_ring = Ring(chips * group // 2, wq_vm.shape[0], wq_in)
        kv_ring.prime()
        q_ring.prime()
        for copy in dy_in:
            copy.start()
        x_in.wait()
        with scope('norm'):
            @pl.loop(0, n_tok // (2 * ROWS))
            def _(step):
                for i in PAIR:
                    sl = block(2 * step + i, ROWS)
                    hat, _ = layer_norm(dx_ref[sl, :].astype(F32))
                    h_ref[sl, :] = (hat * gain + bias).astype(BF16)

        with scope('heads_kv'):
            kv_ring.run(part_heads)
        keep = pltpu.make_async_copy(wkv_ref, wkv_all, mix_sem.at[2])
        keep.start()
        for come, go in zip(dy_in, dy_keep):
            come.wait()
            go.start()
        with scope('project_kv'):
            @pl.loop(0, chips)
            def _(n):
                y = dot(h_ref[...], wkv_ref[n])
                v = jnp.concatenate([turned(y[:, :head_dim]), y[:, head_dim:]], axis=1).astype(BF16)
                for b in range(n_batch):
                    far_ref[b, me, :, block(n, 2 * head_dim)] = v[b * seq:(b + 1) * seq]

        kvs.start_first()
        kvs.start_second()
        with scope('project_q'):
            q_ring.run(project)
        keep.wait()
        for copy in dy_keep:
            copy.wait()

    pl.run_scoped(
        project_all,
        pltpu.VMEM((chips, width, 2 * head_dim), BF16),
        pltpu.VMEM((3, 2, 4 * 64 * chips, head_dim), BF16), pltpu.VMEM((4, 2, width, head_dim), BF16),
        pltpu.SemaphoreType.DMA((3, 2)), pltpu.SemaphoreType.DMA((4,)), pltpu.SemaphoreType.DMA((n_batch * width // n_rows,)),
    )

    with scope('kv_pass'):
        kvs.pass_on()
    queries.start()
    q_ref[me] = g_ref[me, :, q_part]
    with scope('turn_h'):
        @pl.loop(0, width // 128)
        def _(step):
            sl = block(step, 128)
            ht_ref[sl, :] = h_ref[:, sl].T

    with scope('kv_wait'):
        kvs.share_second()
        kvs.share_far()
        all_came(far_ref.at[:, pl.ds(0, chips), :, pl.ds(0, kv_cols)], kv_rsem.at[6], at.partner)

    def chip_at(i):
        return at.ring(jnp.where(i == 0, 0, jnp.where(i == 1, 1, jnp.where(i == 2, 3, 2))))

    def soft(s, seen):
        s = s * scale
        clear = s.shape[0] - seen.shape[0]
        tail = jnp.where(seen, s[clear:], -1e30)
        s = tail if clear == 0 else jnp.concatenate([s[:clear], tail], axis=0)
        e = jnp.exp(s - jnp.max(s, axis=0, keepdims=True))
        return e * (1.0 / jnp.sum(e, axis=0, keepdims=True))

    def attend(limit, clear):
        @pl.loop(0, n_batch * chips)
        def _(i):
            @pl.when(i == 1)
            def _():
                with scope('q_pass'):
                    queries.pass_on()
                dys.start_second()
                dys.pass_on()
                hcols.start()

            b, n = lax.rem(i, n_batch), lax.div(i, n_batch)
            k = far_ref[b, 0:limit // seq, :, block(2 * n, head_dim)].reshape(limit, head_dim)
            vt = far_ref[b, 0:limit // seq, :, block(2 * n + 1, head_dim)].reshape(limit, head_dim).T
            q = jnp.concatenate([g_ref[n * n_batch + b, :, block(j, head_dim)] for j in range(group)], axis=0)
            row = lax.broadcasted_iota(jnp.int32, (limit - clear, n_rows), 0)
            col = lax.broadcasted_iota(jnp.int32, (limit - clear, n_rows), 1)
            p = soft(dot_nt(k, q), row <= lax.rem(col, seq) + (me * seq - clear))
            mixed = dot(vt, p.astype(BF16)).astype(BF16)
            for j in range(group):
                h_ref[block(b, seq), block(n * group + j, head_dim)] = mixed[:, j * seq:(j + 1) * seq].T

    with scope('attend'):
        @pl.when(at.chip == chips - 1)
        def _():
            attend(chips * tile, (chips - 1) * tile)

        @pl.when(at.chip < chips - 1)
        def _():
            attend((chips - 1) * tile, 0)

    h_keep = pltpu.make_async_copy(ht_ref.at[block(me, half)], ht_all.at[me], loc_sem.at[1])
    h_keep.start()

    def block_out():
        def stream(wo_vm, sem):
            def wo_in(s, slot):
                return [pltpu.make_async_copy(wo_ref.at[:, block(s, OUT_TILE)], wo_vm.at[slot], sem.at[slot])]

            def out_tile(s, slot):
                sl = block(s, OUT_TILE)
                out_ref[:, sl] = (dx_ref[:, sl].astype(F32) + dot(h_ref[...], wo_vm[slot])).astype(BF16)

            ring = Ring(width // OUT_TILE, wo_vm.shape[0], wo_in)
            ring.prime()
            ring.run(out_tile)

        with scope('output'):
            pl.run_scoped(stream, pltpu.VMEM((4, width, OUT_TILE), BF16), pltpu.SemaphoreType.DMA((4,)))

    k_all = lambda n: far_ref[core, 0:n, :, block(2 * at.chip, head_dim)].reshape(n * seq, head_dim)
    v_all = lambda n: far_ref[core, 0:n, :, block(2 * at.chip + 1, head_dim)].reshape(n * seq, head_dim)

    def rotate_back(t, cos, sin):
        u, w = t[:quarter], t[quarter:2 * quarter]
        return jnp.concatenate([u * cos + w * sin, w * cos - u * sin, t[2 * quarter:]], axis=0)

    def by_dev(t):
        return t.astype(BF16).reshape(t.shape[0] // seq, seq, head_dim)

    def attend_back(t, i):
        limit = (t + 1) * tile
        sl = slice(t * tile, limit)
        devs = slice(t * CORES, (t + 1) * CORES)

        def heads(first, count):
            each = range(count)
            q = jnp.concatenate([q_ref[devs, :, block(first + j, head_dim)].reshape(tile, head_dim) for j in each], axis=0)
            da = jnp.concatenate([da_ref[sl, block(first + j, head_dim)] for j in each], axis=0)
            k, v = k_all(limit // seq), v_all(limit // seq)
            row = lax.broadcasted_iota(jnp.int32, (tile, count * tile), 0)
            col = lax.broadcasted_iota(jnp.int32, (tile, count * tile), 1)
            p = soft(dot_nt(k, q), row <= lax.rem(col, tile))
            p_low = p.astype(BF16)
            mixed = dot(vt_ref[:, :limit], p_low).astype(BF16)
            dp = dot_nt(v, da)
            row_dot = jnp.sum(p * dp, axis=0, keepdims=True)
            ds = (p * (dp - row_dot) * scale).astype(BF16)
            dv_ref[:limit, :] += dot(p_low, da)
            dk_ref[:limit, :] += dot(ds, q)
            back = dot(kt_ref[:, :limit], ds)
            for j in each:
                part = slice(j * tile, (j + 1) * tile)
                at_ref[block(first + j, head_dim), sl] = mixed[:, part]
                g_ref[devs, :, block(first + j, head_dim)] = by_dev(rotate_back(back[:, part], cost_ref[:, sl], sint_ref[:, sl]).T)

        @pl.loop(0, group // 2)
        def _(j):
            heads(2 * j, 2)

        @pl.when(i == chips - 2)
        def _():
            with scope('dy_far'):
                dys.share_far()

        heads(group - 1, 1)

    def middle(wo_vm, dyk):
        wo_in = pltpu.make_async_copy(wo_ref.at[block(at.chip, n_rows)], wo_vm, mix_sem.at[2])
        wo_in.start()
        all_came(spot_ref.at[pl.ds(0, n_dev - 1)], p_rsem.at[0], at.partner)
        for d in range(n_dev):
            angle = freq * spot_ref[d, pl.ds(core, 1), :].astype(F32)
            cost_ref[:, d * seq:(d + 1) * seq] = jnp.cos(angle)
            sint_ref[:, d * seq:(d + 1) * seq] = jnp.sin(angle)
        with scope('q_wait'):
            all_came(q_ref.at[pl.ds(0, n_dev - 1)], q_rsem.at[0], at.partner)
            all_sent(block_total, q_ssem, at.partner)
            all_sent(far_ref.at[:, pl.ds(0, n_dev - 1), :, pl.ds(0, kv_cols)], kv_ssem, at.partner)
            all_sent(spot_ref.at[pl.ds(0, n_dev - 1)], p_ssem, at.partner)
        kt_ref[...] = k_all(n_dev).T
        vt_ref[...] = v_all(n_dev).T
        dk_ref[...] = jnp.zeros_like(dk_ref)
        dv_ref[...] = jnp.zeros_like(dv_ref)
        dys.own_across.wait_recv()

        def fetch(i, slot):
            return pltpu.make_async_copy(dy_all.at[block(chip_at(i), CORES), core], dyk.at[slot], mix_sem.at[slot])

        with scope('wo_wait'):
            fetch(0, 0).start()
            wo_in.wait()

        @pl.loop(0, chips)
        def _(i):
            slot = lax.rem(i, 2)

            @pl.when((i == 1) & (at.chip < chips - 1))
            def _():
                block_out()

            @pl.when(i == 1)
            def _():
                with scope('dy_wait'):
                    dys.share_second()
                    all_came(dy_all.at[pl.ds(0, 2)], dy_rsem.at[7], at.partner)
                fetch(i, slot).start()

            @pl.when(i == chips - 1)
            def _():
                with scope('dy_far2'):
                    all_came(dy_all.at[0], dy_rsem.at[8], at.partner)
                fetch(i, slot).start()
                with scope('h_pass'):
                    hcols.pass_on()

            fetch(i, slot).wait()

            @pl.when((i > 0) & (i < chips - 2))
            def _():
                fetch(i + 1, 1 - slot).start()

            chip = chip_at(i)
            with scope('da'):
                da_ref[block(chip, tile), :] = dot_nt(dyk[slot].reshape(tile, width), wo_vm[...]).astype(BF16)
            with scope('attend_back'):
                for t in range(chips):
                    @pl.when(chip == t)
                    def _(t=t):
                        attend_back(t, i)

    pl.run_scoped(middle, pltpu.VMEM((n_rows, width), BF16), pltpu.VMEM((2, CORES, seq, width), BF16))
    all_sent(dy_all.at[pl.ds(0, n_dev - 1)], dy_ssem, at.partner)
    heads_across.start()
    g_ref[:, :, n_rows:n_rows + head_dim] = by_dev(rotate_back(dk_ref[...].T, cost_ref[...], sint_ref[...]).T)
    g_ref[:, :, n_rows + head_dim:] = by_dev(dv_ref[...])

    def span_of(q):
        return block(q, CORES)

    turn = [[at.ring(q) for q in (2, 1, 3, 0)], [at.ring(q) for q in (3, 0, 1, 2)]]
    direct = [[send(g_ref.at[span_of(turn[i][q])], g_all.at[me, span_of(turn[i][q])], kv_ssem, kv_rsem.at[i * chips + q], at.dev(steps[i], core)) for q in range(chips)] for i in PAIR]
    came = [[at.ring(q) for q in (1, 0, 2, 3)], [at.ring(q) for q in (0, 1, 2, 3)]]
    def halves_of(quarters):
        return [span_of(quarters[0])] + [pl.ds(quarters[1] * CORES + c, 1) for c in range(CORES)]

    onward = [[send(g_all.at[origin[i], sl], far_ref.at[core, sl], q_ssem, q_rsem.at[3 * i + q], at.dev(steps[i], core)) for q, sl in enumerate(halves_of(came[i]))] for i in PAIR]
    ends = [[at.ring(q) for q in (0, 3)], [at.ring(q) for q in (1, 2)]]
    g_across = send(g_ref, g_all.at[me], x_ssem, dy_rsem.at[0], at.partner)
    near_across = [[send(g_all.at[origin[i], span_of(came[i][q])], g_all.at[origin[i], span_of(came[i][q])], x_ssem, dy_rsem.at[1 + q // 2], at.partner) for q in range(chips)] for i in PAIR]
    end_across = [[send(far_ref.at[core, sl], far_ref.at[core, sl], x_ssem, dy_rsem.at[3 + (q or 3 * i)], at.partner) for q, sl in enumerate(halves_of(ends[i]))] for i in PAIR]
    for q in range(chips):
        for i in PAIR:
            direct[i][q].start()
    g_across.start()
    g_keep = pltpu.make_async_copy(g_ref, g_all.at[me], loc_sem.at[0])
    g_keep.start()
    at2_ref[:, block(core, n_seq)] = at_ref[block(core, half), :]

    @pl.when(at.chip == chips - 1)
    def _():
        block_out()

    dy_back = [pltpu.make_async_copy(dy_ref.at[b], h_ref.at[pl.ds(b * seq, seq)], loc_sem.at[2 + b]) for b in range(n_batch)]
    for copy in dy_back:
        copy.start()

    def wo_rows(dy_vm, sem):
        def dy_tile(s, slot):
            return [pltpu.make_async_copy(dy_all.at[:, :, :, block(s, COL_TILE)], dy_vm.at[slot], sem.at[slot])]

        def wo_tile(s, slot):
            pieces = [dy_vm[slot, d, b] for b in range(n_batch) for d in range(n_dev)]
            dwo_ref[:, block(s, COL_TILE)] = dot(at2_ref[...], jnp.concatenate(pieces, axis=0))

        ring = Ring(width // COL_TILE, dy_vm.shape[0], dy_tile)
        ring.prime()
        with scope('heads_wait'):
            heads_across.wait_recv()
        with scope('grad_wo'):
            ring.run(wo_tile)

    pl.run_scoped(wo_rows, pltpu.VMEM((4, n_dev, n_batch, seq, COL_TILE), BF16), pltpu.SemaphoreType.DMA((4,)))

    with scope('h_wait'):
        all_came(ht_all.at[pl.ds(0, n_dev - 1)], h_rsem.at[0], at.partner)
        all_sent(block_total, h_ssem, at.partner)
    h_keep.wait()
    lhs_in = [pltpu.make_async_copy(ht_all.at[d, :, pl.ds(b * seq, seq)], at2_ref.at[:, pl.ds((b * n_dev + d) * seq, seq)], lhs_sem.at[0]) for d in range(n_dev) for b in range(n_batch)]
    for copy in lhs_in:
        copy.start()
    with jax.named_scope('own_wait'):
        pltpu.make_async_copy(at2_ref, at2_ref, lhs_sem.at[0]).wait()
        g_keep.wait()
        g_across.wait_recv()
    rows_out = [send(row_ref.at[at.chip], row_ref.at[at.chip], p_ssem, p_rsem.at[1], at.dev(step, core)) for step in (1, -1, 2)]
    total_across = send(total_ref.at[core], total_ref.at[core], p_ssem, p_rsem.at[2], at.partner)

    def weight_grads(wq_vm, wkv_vm, acc_ref, hat_ref, inv_ref, job_ref, mine_ref):
        n_slots = wq_vm.shape[0]
        chunk = wq_vm.shape[2]
        n_chunks = width // chunk
        total = n_chunks * chips

        def weights(s):
            slot = lax.rem(s, n_slots)
            chip = chip_at(lax.div(s, n_chunks))
            rows = block(lax.rem(s, n_chunks), chunk)
            return [
                pltpu.make_async_copy(wq_ref.at[block(chip, group), rows], wq_vm.at[slot], w_sem.at[slot, 0]),
                pltpu.make_async_copy(wkv_all.at[chip, rows], wkv_vm.at[slot], w_sem.at[slot, 1]),
            ]

        for s in range(n_slots):
            for copy in weights(s):
                copy.start()

        def grow(i, read):
            @pl.loop(0, n_chunks)
            def _(n):
                s = i * n_chunks + n
                slot = lax.rem(s, n_slots)
                for copy in weights(s):
                    copy.wait()
                rows = jnp.concatenate([read(b) for b in range(n_batch)], axis=0)
                part = dot_nt(rows, jnp.concatenate([wq_vm[slot, j] for j in range(group)] + [wkv_vm[slot]], axis=1))
                sl = block(n, chunk)

                @pl.when(i == 0)
                def _():
                    acc_ref[:, sl] = part

                @pl.when(i > 0)
                def _():
                    acc_ref[:, sl] += part

                @pl.when(s + n_slots < total)
                def _():
                    for copy in weights(s + n_slots):
                        copy.start()

        def mine_in(i):
            return [pltpu.make_async_copy(g_all.at[chip_at(i) * CORES + b, me], mine_ref.at[lax.rem(i, 2), b], job_sem.at[2 + lax.rem(i, 2)]) for b in range(n_batch)]

        def grow_near(i):
            here = mine_ref.at[lax.rem(i, 2)]
            pltpu.make_async_copy(here, here, job_sem.at[2 + lax.rem(i, 2)]).wait()
            grow(i, lambda b: mine_ref[lax.rem(i, 2), b])

        def job_in(chip, quarters, slot):
            return [pltpu.make_async_copy(g_all.at[chip * CORES + b, span_of(q)], job_ref.at[slot, b, n], job_sem.at[slot]) for b in range(n_batch) for n, q in enumerate(quarters)]

        def job(chip, pieces, read, add):
            lhs = [at2_ref[:, pl.ds(pl.multiple_of(b * n_seq + d * seq, seq), seq)] for b in range(n_batch) for d in pieces]
            rhs = [read(b, n) for b in range(n_batch) for n in range(len(pieces))]
            y = dot(jnp.concatenate(lhs, axis=1), jnp.concatenate(rhs, axis=0))
            for j in range(group):
                v = y[:, j * head_dim:(j + 1) * head_dim]
                dwq_ref[chip * group + j] = dwq_ref[chip * group + j] + v if add else v
            for j, ref in enumerate((dwk_ref, dwv_ref)):
                v = y[:, (group + j) * head_dim:(group + j + 1) * head_dim]
                rows = pl.ds(chip, half, stride=chips)
                ref[rows, :] = ref[rows, :] + v if add else v

        def devs_of(quarters):
            return [q * CORES + c for q in quarters for c in range(CORES)]

        def near_pair(quarters, add):
            for slot, step in enumerate(steps):
                for copy in job_in(at.ring(step), quarters, slot):
                    copy.start()

            @pl.loop(0, 2)
            def _(slot):
                chip = at.ring(1 - 2 * slot)
                pltpu.make_async_copy(job_ref.at[slot], job_ref.at[slot], job_sem.at[slot]).wait()
                job(chip, devs_of(quarters), lambda b, n: job_ref[slot, b, n // CORES, n % CORES], add)

        halves = [[at.ring(q) for q in half_of] for half_of in ((0, 1), (2, 3))]
        for slot in PAIR:
            for copy in job_in(at.chip, [at.ring(2 * slot), at.ring(2 * slot + 1)], slot):
                copy.start()
        for copy in mine_in(0):
            copy.start()
        with jax.named_scope('own_job'):
            for slot in PAIR:
                quarters = [at.ring(2 * slot), at.ring(2 * slot + 1)]
                pltpu.make_async_copy(job_ref.at[slot], job_ref.at[slot], job_sem.at[slot]).wait()
                job(at.chip, devs_of(quarters), lambda b, n: job_ref[slot, b, n // CORES, n % CORES], slot == 1)

        with jax.named_scope('own_dh'):
            grow_near(0)

        with jax.named_scope('d01_wait'):
            for q in PAIR:
                for i in PAIR:
                    direct[i][q].wait_recv()
                for i in PAIR:
                    for copy in onward[i][:1] if q == 0 else onward[i][1:]:
                        copy.start()
                    near_across[i][q].start()
        with scope('d01_across'):
            all_came(g_all.at[0], dy_rsem.at[1], at.partner)
        for i in (1, 2):
            for copy in mine_in(i):
                copy.start()
        with scope('near_dh'):
            @pl.loop(1, chips - 1)
            def _(i):
                grow_near(i)

        with jax.named_scope('near_a'):
            near_pair(halves[0], False)
        with scope('d2_wait'):
            for i in PAIR:
                direct[i][2].wait_recv()
                near_across[i][2].start()
        with jax.named_scope('hat'):
            @pl.loop(0, n_tok // (2 * ROWS))
            def _(step):
                for i in PAIR:
                    sl = block(2 * step + i, ROWS)
                    hat, inv = layer_norm(dx_ref[sl, :].astype(F32))
                    hat_ref[sl, :] = hat
                    inv_ref[sl, :] = jnp.broadcast_to(inv, (ROWS, 128))

        with scope('d3_wait'):
            for i in PAIR:
                direct[i][3].wait_recv()
                near_across[i][3].start()
        with scope('d23_across'):
            all_came(g_all.at[0], dy_rsem.at[2], at.partner)
        with jax.named_scope('near_b'):
            near_pair(halves[1], True)
        far_chip = at.ring(2)
        end_total = g_all.at[0, pl.ds(0, CORES)]
        with jax.named_scope('far0_wait'):
            for i in PAIR:
                onward[i][0].wait_recv()
                end_across[i][0].start()
        with scope('far0_across'):
            all_came(end_total, dy_rsem.at[3], at.partner)
        with jax.named_scope('far_dh'):
            grow(chips - 1, lambda b: far_ref[b, me])
        for copy in dy_back:
            copy.wait()
        part_ref[...] = jnp.zeros_like(part_ref)

        with jax.named_scope('norm_back'):
            @pl.loop(0, n_tok // (2 * ROWS))
            def _(step):
                for i in PAIR:
                    sl = block(2 * step + i, ROWS)
                    hat, inv = hat_ref[sl, :], inv_ref[sl, 0:1]
                    dh = acc_ref[sl, :]
                    dg = dh * hat
                    gh = dh * gain
                    one = jnp.mean(gh, axis=-1, keepdims=True)
                    two = jnp.mean(dg * gain, axis=-1, keepdims=True)
                    dx_ref[sl, :] = (h_ref[sl, :].astype(F32) + inv * (gh - one - hat * two)).astype(BF16)
                    part_ref[0] += dg[0:8] + dg[8:16]
                    part_ref[1] += dh[0:8] + dh[8:16]

        for i in PAIR:
            row_ref[at.chip, i:i + 1, :] = jnp.sum(part_ref[i], axis=0, keepdims=True)
        for copy in rows_out:
            copy.start()

        def hand_on(c):
            with scope('far1_wait'):
                for i in PAIR:
                    onward[i][1 + c].wait_recv()
                    end_across[i][1 + c].start()

        def far_rows(devs, add):
            job(far_chip, devs, lambda b, n: far_ref[b, devs[n]], add)

        def last_half(c):
            with scope('far1_across'):
                all_came(end_total, dy_rsem.at[4 + c], at.partner)
            with scope('far_b'):
                far_rows([ends[i][1] * CORES + c for i in PAIR], True)

        hand_on(0)
        with scope('far_a'):
            all_came(end_total, dy_rsem.at[6], at.partner)
            far_rows(devs_of([ends[0][0], ends[1][0]]), False)
        hand_on(1)
        last_half(0)
        with scope('total'):
            all_came(row_ref.at[pl.ds(0, chips - 1)], p_rsem.at[1], at.partner)
            all_sent(row_ref.at[pl.ds(0, chips - 1)], p_ssem, at.partner)
            total = row_ref[0]
            for n in range(1, chips):
                total = total + row_ref[n]
            total_ref[core] = total
            total_across.start()
        last_half(1)

    pl.run_scoped(
        weight_grads,
        pltpu.VMEM((W_SLOTS, group, W_ROWS, head_dim), BF16), pltpu.VMEM((W_SLOTS, W_ROWS, 2 * head_dim), BF16), pltpu.VMEM((n_tok, width), F32),
        pltpu.VMEM((n_tok, width), F32), pltpu.VMEM((n_tok, 128), F32), pltpu.VMEM((2, n_batch, 2, CORES, seq, cols), BF16), pltpu.VMEM((2, n_batch, seq, cols), BF16),
    )

    with scope('sums'):
        all_came(total_ref.at[0], p_rsem.at[2], at.partner)
        total = total_ref[0] + total_ref[1]
        dgain_ref[...] = total[0:1].reshape(width)
        dbias_ref[...] = total[1:2].reshape(width)
    with scope('done'):
        heads_across.wait_send()
        all_sent(far_ref, kv_ssem, at.partner)
        all_sent(g_ref, q_ssem, at.partner)
        all_sent(g_all.at[pl.ds(0, chips)], x_ssem, at.partner)
        all_sent(total_ref.at[0], p_ssem, at.partner)


def whole_block(n_dev, x, gain, bias, positions, freq, dy, wq, wk, wv, wo):
    n_batch, seq, width = dy.shape
    n_tok = n_batch * seq
    head_dim = wq.shape[2]
    chips = n_dev // CORES
    group = wq.shape[0] // chips
    cols = (group + 2) * head_dim
    n_rows = group * head_dim
    half = n_rows // CORES
    n_seq = n_dev * seq
    quarter = head_dim // 4
    dma = pltpu.SemaphoreType.DMA
    vm = pltpu.VMEM
    shapes = [((n_tok, width), BF16)] * 2 + [((chips * group, half, head_dim), F32)] + [((chips * half, head_dim), F32)] * 2 + [((half, width), F32), ((width,), F32), ((width,), F32)]
    held = [((n_dev, n_batch, seq, width), BF16), ((n_dev, half, n_tok), BF16), ((n_dev, n_dev, seq, cols), BF16), ((chips, width, 2 * head_dim), BF16)]
    return pl.pallas_call(
        functools.partial(block_body, n_dev, group),
        out_shape=tuple(pltpu.VMEM(*t) for t in shapes) + tuple(sds(*t) for t in held),
        in_specs=[HBM] * 10,
        out_specs=(VM,) * len(shapes) + (HBM,) * len(held),
        scratch_shapes=[
            vm((n_tok, width), BF16), vm((width, n_tok), BF16), vm((n_dev, seq, cols), BF16), vm((n_dev, seq, n_rows), BF16),
            vm((n_rows, n_seq), BF16), vm((half, n_batch * n_seq), BF16), vm((n_seq, n_rows), BF16),
            vm((head_dim, n_seq), BF16), vm((head_dim, n_seq), BF16), vm((n_seq, head_dim), F32), vm((n_seq, head_dim), F32),
            vm((quarter, n_seq), F32), vm((quarter, n_seq), F32), vm((3, n_tok, head_dim), F32), vm((n_dev, n_batch, seq), jnp.int32), vm((width,), F32), vm((width,), F32), vm((quarter, 1), F32),
            vm((2, seq, n_rows), BF16), vm((2, half, n_tok), BF16),
            vm((n_batch, n_dev, seq, cols), BF16), vm((2, 8, width), F32), vm((chips, 2, width), F32), vm((CORES, 2, width), F32),
            dma((6,)), dma((9,)), dma((8,)), dma((6,)), dma((3,)), dma((3,)), dma((2,)),
            dma((6,)), dma((3,)), dma((1,)), dma((W_SLOTS, 2)), dma((4,)),
        ],
        compiler_params=pltpu.CompilerParams(collective_id=0, has_side_effects=True, vmem_limit_bytes=VMEM_LIMIT),
        cost_estimate=pl.CostEstimate(flops=10 ** 11, bytes_accessed=10 ** 8, transcendentals=0),
        name='block',
    )(gain, bias, positions, freq, x.reshape(n_tok, width), dy, wq, wk, wv, wo)[:len(shapes)]


def settle_body(n, *refs):
    sem = refs[2 * n]
    copies = []
    for src, dst in zip(refs[:n], refs[n:2 * n]):
        pieces = SETTLE if len(src.shape) > 1 else 1
        size = src.shape[0] // pieces
        copies += [pltpu.make_async_copy(src.at[pl.ds(p * size, size)], dst.at[pl.ds(p * size, size)], sem) for p in range(pieces)]
    for copy in copies:
        copy.start()
    for copy in copies:
        copy.wait()


def settle(arrays):
    n = len(arrays)
    return pl.pallas_call(
        functools.partial(settle_body, n),
        out_shape=tuple(sds(t.shape, t.dtype) for t in arrays),
        in_specs=[ANY] * n,
        out_specs=(HBM,) * n,
        scratch_shapes=[pltpu.SemaphoreType.DMA],
        compiler_params=pltpu.CompilerParams(vmem_limit_bytes=1024 * 1024),
        name='settle',
    )(*arrays)


def solution(mesh):
    n_dev = mesh.shape['cp']

    def device_step(x_act, d_out, positions, ln_gain, ln_bias, w_query, w_key, w_value, w_out):
        n_batch, seq, width = x_act.shape
        q_heads, (kv_heads, head_dim) = w_query.shape[1], w_key.shape[1:]
        group = q_heads // kv_heads
        quarter = head_dim // 4
        assert n_batch == CORES and n_dev // CORES == kv_heads == 4 and q_heads * head_dim == width

        freq = np.exp(np.arange(quarter) * (-2.0 * math.log(ROPE_BASE) / (head_dim // 2))).astype(np.float32).reshape(quarter, 1)
        by_head = lambda t: jnp.transpose(t, (1, 0, 2))
        by_row = lambda t: t.reshape(width * kv_heads, head_dim)
        wq = by_head(w_query)

        results = whole_block(n_dev, x_act, ln_gain, ln_bias, positions, jnp.asarray(freq), d_out, wq, by_row(w_key), by_row(w_value), w_out)
        out, dx, dwq, dwk, dwv, dwo, dgain, dbias = settle(results)
        kv_rows = lambda t: t.reshape(width // n_dev, kv_heads, head_dim)
        return (out.reshape(x_act.shape), dx.reshape(x_act.shape), by_head(dwq), kv_rows(dwk), kv_rows(dwv), dwo, dgain, dbias)

    return jax.shard_map(device_step, mesh=mesh, in_specs=(P('dp', 'cp', None), P('dp', 'cp', None), P('dp', 'cp'), P(None), P(None), P(None, None, None), P(None, None, None), P(None, None, None), P(None, None)), out_specs=(P('dp', 'cp', None), P('dp', 'cp', None), P(('dp', 'cp'), None, None), P(('dp', 'cp'), None, None), P(('dp', 'cp'), None, None), P(('dp', 'cp'), None), P('dp'), P('dp')), check_vma=False)
```

```python
import functools
import math
import jax
import jax.numpy as jnp
import numpy as np
from jax import lax
from jax.experimental import pallas as pl
from jax.experimental.pallas import tpu as pltpu
from jax.sharding import PartitionSpec as P

EPS = 1e-5
ROPE_BASE = 10000.0
BF16 = jnp.bfloat16
F32 = jnp.float32
VMEM_LIMIT = 46 * 1024 * 1024
NT = (((1,), (1,)), ((), ()))
ANY = pl.BlockSpec(memory_space=pl.ANY)
VM = pl.BlockSpec(memory_space=pltpu.VMEM)
HBM = pl.BlockSpec(memory_space=pltpu.HBM)
CORES = 2
PAIR = range(2)
STEPS = (1, -1)
COL_TILE = 512
OUT_TILE = 256
ROWS = 16
W_SLOTS = 4
W_ROWS = 512
SETTLE = 4


def dot(a, b):
    return jnp.dot(a, b, preferred_element_type=F32)


def dot_nt(a, b):
    return lax.dot_general(a, b, NT, preferred_element_type=F32)


def sds(shape, dtype):
    return jax.ShapeDtypeStruct(shape, dtype)


def head(size):
    return pl.ds(0, size)


def block(i, size):
    return pl.ds(pl.multiple_of(i * size, size), size)


class Place:
    def __init__(self, n_dev):
        self.n_dev = n_dev
        self.chips = n_dev // CORES
        self.me = lax.axis_index('cp')
        self.chip = self.me // CORES
        self.core = self.me % CORES
        self.partner = self.chip * CORES + 1 - self.core

    def ring(self, step):
        return lax.rem(self.chip + self.chips + step, self.chips)

    def dev(self, step, core):
        return self.ring(step) * CORES + core

    def peers(self, far):
        near = [self.partner] + [self.dev(s, c) for s in STEPS for c in range(CORES)]
        return near + ([self.dev(2, c) for c in range(CORES)] if far else [])


def send(src, dst, ssem, rsem, to):
    return pltpu.make_async_remote_copy(src_ref=src, dst_ref=dst, send_sem=ssem, recv_sem=rsem, device_id={'cp': to}, device_id_type=pl.DeviceIdType.MESH)


def all_sent(total, ssem, to):
    send(total, total, ssem, ssem, to).wait_send()


def all_came(total, rsem, to):
    send(total, total, rsem, rsem, to).wait_recv()


def meet(peers):
    barrier = pltpu.get_barrier_semaphore()
    for peer in peers:
        pl.semaphore_signal(barrier, inc=1, device_id={'cp': peer}, device_id_type=pl.DeviceIdType.MESH)
    pl.semaphore_wait(barrier, len(peers))


class Ring:
    def __init__(self, n, slots, copies):
        self.n, self.slots, self.copies = n, slots, copies

    def prime(self):
        for s in range(self.slots):
            for copy in self.copies(s, s):
                copy.start()

    def run(self, use):
        @pl.loop(0, self.n)
        def _(s):
            slot = lax.rem(s, self.slots)
            for copy in self.copies(s, slot):
                copy.wait()
            use(s, slot)

            @pl.when(s + self.slots < self.n)
            def _():
                for copy in self.copies(s + self.slots, slot):
                    copy.start()


class Gather:
    def __init__(self, at, own, piece, both, ssem, rsem, across):
        steps = STEPS
        origin = [at.dev(-1, at.core), at.dev(1, at.core)]
        far = at.dev(2, at.core)
        link = lambda i, src, dst, to: send(src, dst, ssem, rsem.at[i], to)
        self.first = [link(b, own(b), piece(at.me, b), at.dev(steps[b], at.core)) for b in PAIR]
        self.second = [link(2 + b, own(1 - b), piece(at.me, 1 - b), at.dev(steps[b], at.core)) for b in PAIR]
        self.again = [link(4 + b, piece(origin[b], b), piece(origin[b], b), at.dev(steps[b], at.core)) for b in PAIR]
        self.own_across = link(across[0], both(None), both(at.me), at.partner)
        self.first_across = [link(across[1], piece(origin[b], b), piece(origin[b], b), at.partner) for b in PAIR]
        self.second_across = [link(across[1], piece(origin[b], 1 - b), piece(origin[b], 1 - b), at.partner) for b in PAIR]
        self.far_across = [link(across[2], piece(far, b), piece(far, b), at.partner) for b in PAIR]

    def start_first(self):
        for copy in self.first + [self.own_across]:
            copy.start()

    def start_second(self):
        for copy in self.second:
            copy.start()

    def pass_on(self):
        for copy, again, across in zip(self.first, self.again, self.first_across):
            copy.wait_recv()
            again.start()
            across.start()

    def share_second(self):
        for copy, across in zip(self.second, self.second_across):
            copy.wait_recv()
            across.start()

    def share_far(self):
        for copy, across in zip(self.again, self.far_across):
            copy.wait_recv()
            across.start()


class Exchange:
    def __init__(self, at, src, dst, relay, ssem, rsem):
        near = [(0, 1 - at.core)] + [(s, c) for s in STEPS for c in range(CORES)]
        self.near = [send(src(at.dev(s, c)), dst(at.me), ssem, rsem.at[0], at.dev(s, c)) for s, c in near]
        self.far = [send(src(at.dev(2, i)), relay.at[i], ssem, rsem.at[1 + i], at.dev(step, at.core)) for i, step in enumerate(STEPS)]
        self.on = [send(relay.at[i], dst(at.dev(-step, at.core)), ssem, rsem.at[0], at.dev(step, i)) for i, step in enumerate(STEPS)]

    def start(self):
        for copy in self.far + self.near:
            copy.start()

    def pass_on(self):
        for far, on in zip(self.far, self.on):
            far.wait_recv()
            on.start()


def layer_norm(x):
    cen = x - jnp.mean(x, axis=-1, keepdims=True)
    inv = lax.rsqrt(jnp.mean(cen * cen, axis=-1, keepdims=True) + EPS)
    return cen * inv, inv


def block_body(n_dev, group, gain_hbm, bias_hbm, pos_hbm, freq_hbm, x_hbm, dy_ref, wq_ref, wk_ref, wv_ref, wo_ref,
               out_ref, dx_ref, dwq_ref, dwk_ref, dwv_ref, dwo_ref, dgain_ref, dbias_ref, dy_all, ht_all, g_all, wkv_all,
               h_ref, ht_ref, g_ref, q_ref, at_ref, at2_ref, da_ref, kt_ref, vt_ref, dk_ref, dv_ref,
               cost_ref, sint_ref, tab_ref, spot_ref, gain_ref, bias_ref, freq_ref, relay_q, relay_h, far_ref, part_ref, row_ref, total_ref,
               s_sem, dy_rsem, kv_rsem, q_rsem, h_rsem, p_rsem, t_sem, loc_sem, mix_sem, lhs_sem, w_sem, job_sem):
    at = Place(n_dev)
    n_batch, seq, width = dy_ref.shape
    n_tok = n_batch * seq
    head_dim = wq_ref.shape[2]
    cols = (group + 2) * head_dim
    n_rows = group * head_dim
    half = n_rows // CORES
    n_seq = n_dev * seq
    quarter = head_dim // 4
    scale = head_dim ** -0.5
    chips = at.chips
    tile = CORES * seq
    core, me = at.core, at.me
    steps = STEPS
    origin = [at.dev(-1, core), at.dev(1, core)]
    far_dev = at.dev(2, core)
    scope = jax.named_scope

    dy_ssem, kv_ssem, q_ssem, h_ssem, p_ssem, x_ssem = [s_sem.at[i] for i in range(6)]
    assert (n_dev + 1) * n_rows == (n_dev - 1) * cols
    block_total = far_ref.at[0, head(n_dev - 1)]

    with scope('meet'):
        meet(at.peers(True))

    kv_cols = 2 * head_dim * chips
    kv_piece = lambda d, b: far_ref.at[b, d, :, head(kv_cols)]
    kv_both = lambda d: far_ref.at[:, me if d is None else d, :, head(kv_cols)]
    dys = Gather(at, lambda b: dy_ref.at[b], lambda d, b: dy_all.at[d, b], lambda d: dy_ref if d is None else dy_all.at[d], dy_ssem, dy_rsem, (6, 7, 8))
    kvs = Gather(at, lambda b: kv_piece(me, b), kv_piece, kv_both, kv_ssem, kv_rsem, (6, 6, 6))
    q_part = head(n_rows)
    queries = Exchange(at, lambda d: g_ref.at[d, :, q_part], lambda d: q_ref.at[d], relay_q, q_ssem, q_rsem)
    hcols = Exchange(at, lambda d: ht_ref.at[block(d, half)], lambda d: ht_all.at[d], relay_h, h_ssem, h_rsem)
    heads_across = send(at_ref.at[block(1 - core, half)], at2_ref.at[:, block(core, n_seq)], t_sem.at[0], t_sem.at[1], at.partner)
    spots = [send(pos_hbm, spot_ref.at[me], p_ssem, p_rsem.at[0], peer) for peer in at.peers(True)]

    dys.start_first()
    x_in = pltpu.make_async_copy(x_hbm, dx_ref, loc_sem.at[1])
    x_in.start()
    for copy in spots:
        copy.start()
    small = [pltpu.make_async_copy(src, dst, loc_sem.at[2 + n]) for n, (src, dst) in enumerate(((gain_hbm, gain_ref), (bias_hbm, bias_ref), (freq_hbm, freq_ref), (pos_hbm, spot_ref.at[me])))]
    for copy in small:
        copy.start()
    for copy in small:
        copy.wait()

    freq = freq_ref[...]
    for b in range(n_batch):
        angle = freq * spot_ref[me, b:b + 1, :].astype(F32)
        cos, sin, none = jnp.cos(angle), jnp.sin(angle), jnp.zeros((quarter, seq), F32)
        rest = jnp.zeros((head_dim - 2 * quarter, seq), F32)
        for i, rows in enumerate(([cos, cos, rest + 1.0], [-sin, none, rest], [none, sin, rest])):
            tab_ref[i, b * seq:(b + 1) * seq, :] = jnp.concatenate(rows, axis=0).T

    gain = (1.0 + gain_ref[...]).reshape(1, width)
    bias = bias_ref[...].reshape(1, width)

    def project_all(wkv_ref, raw_ref, wq_vm, raw_sem, wq_sem, stage_sem):
        pieces = [(b, i) for b in range(n_batch) for i in range(width // n_rows)]
        there = lambda n: da_ref.at[pl.ds(n * seq, seq)]
        dy_in = [pltpu.make_async_copy(dy_ref.at[b, :, pl.ds(i * n_rows, n_rows)], there(n), stage_sem.at[n]) for n, (b, i) in enumerate(pieces)]
        dy_keep = [pltpu.make_async_copy(there(n), dy_all.at[me, b, :, pl.ds(i * n_rows, n_rows)], stage_sem.at[n]) for n, (b, i) in enumerate(pieces)]
        span = 64 * chips
        batch = raw_ref.shape[2] // span
        row = lax.broadcasted_iota(jnp.int32, (span, span), 0)
        col = lax.broadcasted_iota(jnp.int32, (span, span), 1)
        pick = jnp.where(col == lax.rem(row, 64) * chips + lax.div(row, 64), 1.0, 0.0).astype(BF16)

        def raw_in(s, slot):
            return [pltpu.make_async_copy(w.at[block(s, span * batch)], raw_ref.at[slot, i], raw_sem.at[slot, i]) for i, w in enumerate((wk_ref, wv_ref))]

        def wq_in(s, slot):
            return [pltpu.make_async_copy(wq_ref.at[block(s, 2)], wq_vm.at[slot], wq_sem.at[slot])]

        def part_heads(s, slot):
            for i in range(batch):
                sl = slice(i * span, (i + 1) * span)
                rows = dot(pick, jnp.concatenate([raw_ref[slot, 0, sl, :], raw_ref[slot, 1, sl, :]], axis=1)).astype(BF16)
                for n in range(chips):
                    wkv_ref[n, block(s * batch + i, 64), :] = rows[n * 64:(n + 1) * 64]

        def turned(v):
            return v * tab_ref[0] + pltpu.roll(v, head_dim - quarter, 1) * tab_ref[1] + pltpu.roll(v, quarter, 1) * tab_ref[2]

        def project(s, slot):
            y = dot(h_ref[...], jnp.concatenate([wq_vm[slot, 0], wq_vm[slot, 1]], axis=1))
            for i in PAIR:
                head = s * 2 + i
                v = turned(y[:, i * head_dim:(i + 1) * head_dim]).astype(BF16)
                for b in range(n_batch):
                    g_ref[lax.div(head, group) * n_batch + b, :, block(lax.rem(head, group), head_dim)] = v[b * seq:(b + 1) * seq]

        kv_ring = Ring(width // (64 * batch), raw_ref.shape[0], raw_in)
        q_ring = Ring(chips * group // 2, wq_vm.shape[0], wq_in)
        kv_ring.prime()
        q_ring.prime()
        for copy in dy_in:
            copy.start()
        x_in.wait()
        with scope('norm'):
            @pl.loop(0, n_tok // (2 * ROWS))
            def _(step):
                for i in PAIR:
                    sl = block(2 * step + i, ROWS)
                    hat, _ = layer_norm(dx_ref[sl, :].astype(F32))
                    h_ref[sl, :] = (hat * gain + bias).astype(BF16)

        with scope('heads_kv'):
            kv_ring.run(part_heads)
        keep = pltpu.make_async_copy(wkv_ref, wkv_all, mix_sem.at[2])
        keep.start()
        for come, go in zip(dy_in, dy_keep):
            come.wait()
            go.start()
        with scope('project_kv'):
            @pl.loop(0, chips)
            def _(n):
                y = dot(h_ref[...], wkv_ref[n])
                v = jnp.concatenate([turned(y[:, :head_dim]), y[:, head_dim:]], axis=1).astype(BF16)
                for b in range(n_batch):
                    far_ref[b, me, :, block(n, 2 * head_dim)] = v[b * seq:(b + 1) * seq]

        kvs.start_first()
        kvs.start_second()
        with scope('project_q'):
            q_ring.run(project)
        keep.wait()
        for copy in dy_keep:
            copy.wait()

    pl.run_scoped(
        project_all,
        pltpu.VMEM((chips, width, 2 * head_dim), BF16),
        pltpu.VMEM((3, 2, 4 * 64 * chips, head_dim), BF16), pltpu.VMEM((4, 2, width, head_dim), BF16),
        pltpu.SemaphoreType.DMA((3, 2)), pltpu.SemaphoreType.DMA((4,)), pltpu.SemaphoreType.DMA((n_batch * width // n_rows,)),
    )

    with scope('kv_pass'):
        kvs.pass_on()
    queries.start()
    q_ref[me] = g_ref[me, :, q_part]
    with scope('turn_h'):
        @pl.loop(0, width // 128)
        def _(step):
            sl = block(step, 128)
            ht_ref[sl, :] = h_ref[:, sl].T

    with scope('kv_wait'):
        kvs.share_second()
        kvs.share_far()
        all_came(far_ref.at[:, head(chips), :, head(kv_cols)], kv_rsem.at[6], at.partner)

    def chip_at(i):
        return at.ring(jnp.where(i == 0, 0, jnp.where(i == 1, 1, jnp.where(i == 2, 3, 2))))

    def soft(s, seen):
        s = s * scale
        clear = s.shape[0] - seen.shape[0]
        tail = jnp.where(seen, s[clear:], -1e30)
        s = tail if clear == 0 else jnp.concatenate([s[:clear], tail], axis=0)
        e = jnp.exp(s - jnp.max(s, axis=0, keepdims=True))
        return e * (1.0 / jnp.sum(e, axis=0, keepdims=True))

    def attend(limit, clear):
        @pl.loop(0, n_batch * chips)
        def _(i):
            @pl.when(i == 1)
            def _():
                with scope('q_pass'):
                    queries.pass_on()
                dys.start_second()
                dys.pass_on()
                hcols.start()

            b, n = lax.rem(i, n_batch), lax.div(i, n_batch)
            k = far_ref[b, 0:limit // seq, :, block(2 * n, head_dim)].reshape(limit, head_dim)
            vt = far_ref[b, 0:limit // seq, :, block(2 * n + 1, head_dim)].reshape(limit, head_dim).T
            q = jnp.concatenate([g_ref[n * n_batch + b, :, block(j, head_dim)] for j in range(group)], axis=0)
            row = lax.broadcasted_iota(jnp.int32, (limit - clear, n_rows), 0)
            col = lax.broadcasted_iota(jnp.int32, (limit - clear, n_rows), 1)
            p = soft(dot_nt(k, q), row <= lax.rem(col, seq) + (me * seq - clear))
            mixed = dot(vt, p.astype(BF16)).astype(BF16)
            for j in range(group):
                h_ref[block(b, seq), block(n * group + j, head_dim)] = mixed[:, j * seq:(j + 1) * seq].T

    with scope('attend'):
        @pl.when(at.chip == chips - 1)
        def _():
            attend(chips * tile, (chips - 1) * tile)

        @pl.when(at.chip < chips - 1)
        def _():
            attend((chips - 1) * tile, 0)

    h_keep = pltpu.make_async_copy(ht_ref.at[block(me, half)], ht_all.at[me], loc_sem.at[1])
    h_keep.start()

    def block_out():
        def stream(wo_vm, sem):
            def wo_in(s, slot):
                return [pltpu.make_async_copy(wo_ref.at[:, block(s, OUT_TILE)], wo_vm.at[slot], sem.at[slot])]

            def out_tile(s, slot):
                sl = block(s, OUT_TILE)
                out_ref[:, sl] = (dx_ref[:, sl].astype(F32) + dot(h_ref[...], wo_vm[slot])).astype(BF16)

            ring = Ring(width // OUT_TILE, wo_vm.shape[0], wo_in)
            ring.prime()
            ring.run(out_tile)

        with scope('output'):
            pl.run_scoped(stream, pltpu.VMEM((4, width, OUT_TILE), BF16), pltpu.SemaphoreType.DMA((4,)))

    k_all = lambda n: far_ref[core, 0:n, :, block(2 * at.chip, head_dim)].reshape(n * seq, head_dim)
    v_all = lambda n: far_ref[core, 0:n, :, block(2 * at.chip + 1, head_dim)].reshape(n * seq, head_dim)

    def rotate_back(t, cos, sin):
        u, w = t[:quarter], t[quarter:2 * quarter]
        return jnp.concatenate([u * cos + w * sin, w * cos - u * sin, t[2 * quarter:]], axis=0)

    def by_dev(t):
        return t.astype(BF16).reshape(t.shape[0] // seq, seq, head_dim)

    def attend_back(t, i):
        limit = (t + 1) * tile
        sl = slice(t * tile, limit)
        devs = slice(t * CORES, (t + 1) * CORES)

        def heads(first, count):
            each = range(count)
            q = jnp.concatenate([q_ref[devs, :, block(first + j, head_dim)].reshape(tile, head_dim) for j in each], axis=0)
            da = jnp.concatenate([da_ref[sl, block(first + j, head_dim)] for j in each], axis=0)
            k, v = k_all(limit // seq), v_all(limit // seq)
            row = lax.broadcasted_iota(jnp.int32, (tile, count * tile), 0)
            col = lax.broadcasted_iota(jnp.int32, (tile, count * tile), 1)
            p = soft(dot_nt(k, q), row <= lax.rem(col, tile))
            p_low = p.astype(BF16)
            mixed = dot(vt_ref[:, :limit], p_low).astype(BF16)
            dp = dot_nt(v, da)
            row_dot = jnp.sum(p * dp, axis=0, keepdims=True)
            ds = (p * (dp - row_dot) * scale).astype(BF16)
            dv_ref[:limit, :] += dot(p_low, da)
            dk_ref[:limit, :] += dot(ds, q)
            back = dot(kt_ref[:, :limit], ds)
            for j in each:
                part = slice(j * tile, (j + 1) * tile)
                at_ref[block(first + j, head_dim), sl] = mixed[:, part]
                g_ref[devs, :, block(first + j, head_dim)] = by_dev(rotate_back(back[:, part], cost_ref[:, sl], sint_ref[:, sl]).T)

        @pl.loop(0, group // 2)
        def _(j):
            heads(2 * j, 2)

        @pl.when(i == chips - 2)
        def _():
            with scope('dy_far'):
                dys.share_far()

        heads(group - 1, 1)

    def middle(wo_vm, dyk):
        wo_in = pltpu.make_async_copy(wo_ref.at[block(at.chip, n_rows)], wo_vm, mix_sem.at[2])
        wo_in.start()
        all_came(spot_ref.at[head(n_dev - 1)], p_rsem.at[0], at.partner)
        for d in range(n_dev):
            angle = freq * spot_ref[d, pl.ds(core, 1), :].astype(F32)
            cost_ref[:, d * seq:(d + 1) * seq] = jnp.cos(angle)
            sint_ref[:, d * seq:(d + 1) * seq] = jnp.sin(angle)
        with scope('q_wait'):
            all_came(q_ref.at[head(n_dev - 1)], q_rsem.at[0], at.partner)
            all_sent(block_total, q_ssem, at.partner)
            all_sent(far_ref.at[:, head(n_dev - 1), :, head(kv_cols)], kv_ssem, at.partner)
            all_sent(spot_ref.at[head(n_dev - 1)], p_ssem, at.partner)
        kt_ref[...] = k_all(n_dev).T
        vt_ref[...] = v_all(n_dev).T
        dk_ref[...] = jnp.zeros_like(dk_ref)
        dv_ref[...] = jnp.zeros_like(dv_ref)
        dys.own_across.wait_recv()

        def fetch(i, slot):
            return pltpu.make_async_copy(dy_all.at[block(chip_at(i), CORES), core], dyk.at[slot], mix_sem.at[slot])

        with scope('wo_wait'):
            fetch(0, 0).start()
            wo_in.wait()

        @pl.loop(0, chips)
        def _(i):
            slot = lax.rem(i, 2)

            @pl.when((i == 1) & (at.chip < chips - 1))
            def _():
                block_out()

            @pl.when(i == 1)
            def _():
                with scope('dy_wait'):
                    dys.share_second()
                    all_came(dy_all.at[head(2)], dy_rsem.at[7], at.partner)
                fetch(i, slot).start()

            @pl.when(i == chips - 1)
            def _():
                with scope('dy_far2'):
                    all_came(dy_all.at[0], dy_rsem.at[8], at.partner)
                fetch(i, slot).start()
                with scope('h_pass'):
                    hcols.pass_on()

            fetch(i, slot).wait()

            @pl.when((i > 0) & (i < chips - 2))
            def _():
                fetch(i + 1, 1 - slot).start()

            chip = chip_at(i)
            with scope('da'):
                da_ref[block(chip, tile), :] = dot_nt(dyk[slot].reshape(tile, width), wo_vm[...]).astype(BF16)
            with scope('attend_back'):
                for t in range(chips):
                    @pl.when(chip == t)
                    def _(t=t):
                        attend_back(t, i)

    pl.run_scoped(middle, pltpu.VMEM((n_rows, width), BF16), pltpu.VMEM((2, CORES, seq, width), BF16))
    all_sent(dy_all.at[head(n_dev - 1)], dy_ssem, at.partner)
    heads_across.start()
    g_ref[:, :, n_rows:n_rows + head_dim] = by_dev(rotate_back(dk_ref[...].T, cost_ref[...], sint_ref[...]).T)
    g_ref[:, :, n_rows + head_dim:] = by_dev(dv_ref[...])

    def span_of(q):
        return block(q, CORES)

    turn = [[at.ring(q) for q in (2, 1, 3, 0)], [at.ring(q) for q in (3, 0, 1, 2)]]
    direct = [[send(g_ref.at[span_of(turn[i][q])], g_all.at[me, span_of(turn[i][q])], kv_ssem, kv_rsem.at[i * chips + q], at.dev(steps[i], core)) for q in range(chips)] for i in PAIR]
    came = [[at.ring(q) for q in (1, 0, 2, 3)], [at.ring(q) for q in (0, 1, 2, 3)]]
    n_heads = group + 2
    late_heads = [range(n_heads), range(n_heads // 2 + 1), range(n_heads // 2 + 1, n_heads)]

    def columns(heads):
        return pl.ds(heads[0] * head_dim, len(heads) * head_dim)

    def late(ref, quarters):
        own = [ref.at[pl.ds(quarters[1] * CORES + min(c, 1), 1), :, columns(heads)] for c, heads in enumerate(late_heads)]
        return [ref.at[span_of(quarters[0])]] + own

    onward = [[send(src, dst, q_ssem, q_rsem.at[4 * i + q], at.dev(steps[i], core)) for q, (src, dst) in enumerate(zip(late(g_all.at[origin[i]], came[i]), late(far_ref.at[core], came[i])))] for i in PAIR]
    ends = [[at.ring(q) for q in (0, 3)], [at.ring(q) for q in (1, 2)]]
    g_across = send(g_ref, g_all.at[me], x_ssem, dy_rsem.at[0], at.partner)
    near_across = [[send(g_all.at[origin[i], span_of(came[i][q])], g_all.at[origin[i], span_of(came[i][q])], x_ssem, dy_rsem.at[1 + q // 2], at.partner) for q in range(chips)] for i in PAIR]
    end_across = [[send(ref, ref, x_ssem, dy_rsem.at[3 + (q or 4 * i)], at.partner) for q, ref in enumerate(late(far_ref.at[core], ends[i]))] for i in PAIR]
    for q in range(chips):
        for i in PAIR:
            direct[i][q].start()
    g_across.start()
    g_keep = pltpu.make_async_copy(g_ref, g_all.at[me], loc_sem.at[0])
    g_keep.start()
    at2_ref[:, block(core, n_seq)] = at_ref[block(core, half), :]

    @pl.when(at.chip == chips - 1)
    def _():
        block_out()

    dy_back = [pltpu.make_async_copy(dy_ref.at[b], h_ref.at[pl.ds(b * seq, seq)], loc_sem.at[2 + b]) for b in range(n_batch)]
    for copy in dy_back:
        copy.start()

    def wo_rows(dy_vm, sem):
        def dy_tile(s, slot):
            return [pltpu.make_async_copy(dy_all.at[:, :, :, block(s, COL_TILE)], dy_vm.at[slot], sem.at[slot])]

        def wo_tile(s, slot):
            pieces = [dy_vm[slot, d, b] for b in range(n_batch) for d in range(n_dev)]
            dwo_ref[:, block(s, COL_TILE)] = dot(at2_ref[...], jnp.concatenate(pieces, axis=0))

        ring = Ring(width // COL_TILE, dy_vm.shape[0], dy_tile)
        ring.prime()
        with scope('heads_wait'):
            heads_across.wait_recv()
        with scope('grad_wo'):
            ring.run(wo_tile)

    pl.run_scoped(wo_rows, pltpu.VMEM((4, n_dev, n_batch, seq, COL_TILE), BF16), pltpu.SemaphoreType.DMA((4,)))

    with scope('h_wait'):
        all_came(ht_all.at[head(n_dev - 1)], h_rsem.at[0], at.partner)
        all_sent(block_total, h_ssem, at.partner)
    h_keep.wait()
    lhs_in = [pltpu.make_async_copy(ht_all.at[d, :, pl.ds(b * seq, seq)], at2_ref.at[:, pl.ds((b * n_dev + d) * seq, seq)], lhs_sem.at[0]) for d in range(n_dev) for b in range(n_batch)]
    for copy in lhs_in:
        copy.start()
    with jax.named_scope('own_wait'):
        pltpu.make_async_copy(at2_ref, at2_ref, lhs_sem.at[0]).wait()
        g_keep.wait()
        g_across.wait_recv()
    rows_out = [send(row_ref.at[at.chip], row_ref.at[at.chip], p_ssem, p_rsem.at[1], at.dev(step, core)) for step in (1, -1, 2)]
    total_across = send(total_ref.at[core], total_ref.at[core], p_ssem, p_rsem.at[2], at.partner)

    def weight_grads(wq_vm, wkv_vm, acc_ref, hat_ref, inv_ref, job_ref, mine_ref):
        n_slots = wq_vm.shape[0]
        chunk = wq_vm.shape[2]
        n_chunks = width // chunk
        total = n_chunks * chips

        def weights(s):
            slot = lax.rem(s, n_slots)
            chip = chip_at(lax.div(s, n_chunks))
            rows = block(lax.rem(s, n_chunks), chunk)
            return [
                pltpu.make_async_copy(wq_ref.at[block(chip, group), rows], wq_vm.at[slot], w_sem.at[slot, 0]),
                pltpu.make_async_copy(wkv_all.at[chip, rows], wkv_vm.at[slot], w_sem.at[slot, 1]),
            ]

        for s in range(n_slots):
            for copy in weights(s):
                copy.start()

        def grow(i, read):
            @pl.loop(0, n_chunks)
            def _(n):
                s = i * n_chunks + n
                slot = lax.rem(s, n_slots)
                for copy in weights(s):
                    copy.wait()
                rows = jnp.concatenate([read(b) for b in range(n_batch)], axis=0)
                part = dot_nt(rows, jnp.concatenate([wq_vm[slot, j] for j in range(group)] + [wkv_vm[slot]], axis=1))
                sl = block(n, chunk)

                @pl.when(i == 0)
                def _():
                    acc_ref[:, sl] = part

                @pl.when(i > 0)
                def _():
                    acc_ref[:, sl] += part

                @pl.when(s + n_slots < total)
                def _():
                    for copy in weights(s + n_slots):
                        copy.start()

        def mine_in(i):
            return [pltpu.make_async_copy(g_all.at[chip_at(i) * CORES + b, me], mine_ref.at[lax.rem(i, 2), b], job_sem.at[2 + lax.rem(i, 2)]) for b in range(n_batch)]

        def grow_near(i):
            here = mine_ref.at[lax.rem(i, 2)]
            pltpu.make_async_copy(here, here, job_sem.at[2 + lax.rem(i, 2)]).wait()
            grow(i, lambda b: mine_ref[lax.rem(i, 2), b])

        def job_in(chip, quarters, slot):
            return [pltpu.make_async_copy(g_all.at[chip * CORES + b, span_of(q)], job_ref.at[slot, b, n], job_sem.at[slot]) for b in range(n_batch) for n, q in enumerate(quarters)]

        def job(chip, pieces, read, add, heads=range(n_heads)):
            lhs = [at2_ref[:, pl.ds(pl.multiple_of(b * n_seq + d * seq, seq), seq)] for b in range(n_batch) for d in pieces]
            rhs = [read(b, n) for b in range(n_batch) for n in range(len(pieces))]
            y = dot(jnp.concatenate(lhs, axis=1), jnp.concatenate(rhs, axis=0))
            for n, j in enumerate(heads):
                v = y[:, n * head_dim:(n + 1) * head_dim]
                if j < group:
                    dwq_ref[chip * group + j] = dwq_ref[chip * group + j] + v if add else v
                else:
                    ref, rows = (dwk_ref, dwv_ref)[j - group], pl.ds(chip, half, stride=chips)
                    ref[rows, :] = ref[rows, :] + v if add else v

        def devs_of(quarters):
            return [q * CORES + c for q in quarters for c in range(CORES)]

        def near_pair(quarters, add):
            for slot, step in enumerate(steps):
                for copy in job_in(at.ring(step), quarters, slot):
                    copy.start()

            @pl.loop(0, 2)
            def _(slot):
                chip = at.ring(1 - 2 * slot)
                pltpu.make_async_copy(job_ref.at[slot], job_ref.at[slot], job_sem.at[slot]).wait()
                job(chip, devs_of(quarters), lambda b, n: job_ref[slot, b, n // CORES, n % CORES], add)

        halves = [[at.ring(q) for q in half_of] for half_of in ((0, 1), (2, 3))]
        for slot in PAIR:
            for copy in job_in(at.chip, [at.ring(2 * slot), at.ring(2 * slot + 1)], slot):
                copy.start()
        for copy in mine_in(0):
            copy.start()
        with jax.named_scope('own_job'):
            for slot in PAIR:
                quarters = [at.ring(2 * slot), at.ring(2 * slot + 1)]
                pltpu.make_async_copy(job_ref.at[slot], job_ref.at[slot], job_sem.at[slot]).wait()
                job(at.chip, devs_of(quarters), lambda b, n: job_ref[slot, b, n // CORES, n % CORES], slot == 1)

        with jax.named_scope('own_dh'):
            grow_near(0)

        with jax.named_scope('d01_wait'):
            for q in PAIR:
                for i in PAIR:
                    direct[i][q].wait_recv()
                for i in PAIR:
                    for copy in onward[i][:1] if q == 0 else onward[i][1:]:
                        copy.start()
                    near_across[i][q].start()
        with scope('d01_across'):
            all_came(g_all.at[0], dy_rsem.at[1], at.partner)
        for i in (1, 2):
            for copy in mine_in(i):
                copy.start()
        with scope('near_dh'):
            @pl.loop(1, chips - 1)
            def _(i):
                grow_near(i)

        with jax.named_scope('near_a'):
            near_pair(halves[0], False)
        with scope('d2_wait'):
            for i in PAIR:
                direct[i][2].wait_recv()
                near_across[i][2].start()
        with jax.named_scope('hat'):
            @pl.loop(0, n_tok // (2 * ROWS))
            def _(step):
                for i in PAIR:
                    sl = block(2 * step + i, ROWS)
                    hat, inv = layer_norm(dx_ref[sl, :].astype(F32))
                    hat_ref[sl, :] = hat
                    inv_ref[sl, :] = jnp.broadcast_to(inv, (ROWS, 128))

        with scope('d3_wait'):
            for i in PAIR:
                direct[i][3].wait_recv()
                near_across[i][3].start()
        with scope('d23_across'):
            all_came(g_all.at[0], dy_rsem.at[2], at.partner)
        with jax.named_scope('near_b'):
            near_pair(halves[1], True)
        far_chip = at.ring(2)
        end_total = [g_all.at[0, head(CORES), :, columns(heads)] for heads in late_heads]
        with jax.named_scope('far0_wait'):
            for i in PAIR:
                onward[i][0].wait_recv()
                end_across[i][0].start()
        with scope('far0_across'):
            all_came(end_total[0], dy_rsem.at[3], at.partner)
        with jax.named_scope('far_dh'):
            grow(chips - 1, lambda b: far_ref[b, me])
        for copy in dy_back:
            copy.wait()
        part_ref[...] = jnp.zeros_like(part_ref)

        with jax.named_scope('norm_back'):
            @pl.loop(0, n_tok // (2 * ROWS))
            def _(step):
                for i in PAIR:
                    sl = block(2 * step + i, ROWS)
                    hat, inv = hat_ref[sl, :], inv_ref[sl, 0:1]
                    dh = acc_ref[sl, :]
                    dg = dh * hat
                    gh = dh * gain
                    one = jnp.mean(gh, axis=-1, keepdims=True)
                    two = jnp.mean(dg * gain, axis=-1, keepdims=True)
                    dx_ref[sl, :] = (h_ref[sl, :].astype(F32) + inv * (gh - one - hat * two)).astype(BF16)
                    part_ref[0] += dg[0:8] + dg[8:16]
                    part_ref[1] += dh[0:8] + dh[8:16]

        for i in PAIR:
            row_ref[at.chip, i:i + 1, :] = jnp.sum(part_ref[i], axis=0, keepdims=True)
        for copy in rows_out:
            copy.start()

        def hand_on(c):
            with scope('far1_wait'):
                for i in PAIR:
                    onward[i][1 + c].wait_recv()
                    end_across[i][1 + c].start()

        def far_rows(devs, add, heads=range(n_heads)):
            job(far_chip, devs, lambda b, n: far_ref[b, devs[n], :, heads[0] * head_dim:(heads[-1] + 1) * head_dim], add, heads)

        def last_half(c):
            with scope('far1_across'):
                all_came(end_total[c], dy_rsem.at[4 + c], at.partner)
            with scope('far_b'):
                far_rows([ends[i][1] * CORES + min(c, 1) for i in PAIR], True, late_heads[c])

        hand_on(0)
        with scope('far_a'):
            all_came(end_total[0], dy_rsem.at[7], at.partner)
            far_rows(devs_of([ends[0][0], ends[1][0]]), False)
        hand_on(1)
        last_half(0)
        hand_on(2)
        last_half(1)
        with scope('total'):
            all_came(row_ref.at[head(chips - 1)], p_rsem.at[1], at.partner)
            all_sent(row_ref.at[head(chips - 1)], p_ssem, at.partner)
            total = row_ref[0]
            for n in range(1, chips):
                total = total + row_ref[n]
            total_ref[core] = total
            total_across.start()
        last_half(2)

    pl.run_scoped(
        weight_grads,
        pltpu.VMEM((W_SLOTS, group, W_ROWS, head_dim), BF16), pltpu.VMEM((W_SLOTS, W_ROWS, 2 * head_dim), BF16), pltpu.VMEM((n_tok, width), F32),
        pltpu.VMEM((n_tok, width), F32), pltpu.VMEM((n_tok, 128), F32), pltpu.VMEM((2, n_batch, 2, CORES, seq, cols), BF16), pltpu.VMEM((2, n_batch, seq, cols), BF16),
    )

    with scope('sums'):
        all_came(total_ref.at[0], p_rsem.at[2], at.partner)
        total = total_ref[0] + total_ref[1]
        dgain_ref[...] = total[0:1].reshape(width)
        dbias_ref[...] = total[1:2].reshape(width)
    with scope('done'):
        heads_across.wait_send()
        all_sent(far_ref, kv_ssem, at.partner)
        all_sent(g_ref, q_ssem, at.partner)
        all_sent(g_all.at[head(chips)], x_ssem, at.partner)
        all_sent(total_ref.at[0], p_ssem, at.partner)


def whole_block(n_dev, x, gain, bias, positions, freq, dy, wq, wk, wv, wo):
    n_batch, seq, width = dy.shape
    n_tok = n_batch * seq
    head_dim = wq.shape[2]
    chips = n_dev // CORES
    group = wq.shape[0] // chips
    cols = (group + 2) * head_dim
    n_rows = group * head_dim
    half = n_rows // CORES
    n_seq = n_dev * seq
    quarter = head_dim // 4
    dma = pltpu.SemaphoreType.DMA
    vm = pltpu.VMEM
    shapes = [((n_tok, width), BF16)] * 2 + [((chips * group, half, head_dim), F32)] + [((chips * half, head_dim), F32)] * 2 + [((half, width), F32), ((width,), F32), ((width,), F32)]
    held = [((n_dev, n_batch, seq, width), BF16), ((n_dev, half, n_tok), BF16), ((n_dev, n_dev, seq, cols), BF16), ((chips, width, 2 * head_dim), BF16)]
    return pl.pallas_call(
        functools.partial(block_body, n_dev, group),
        out_shape=tuple(pltpu.VMEM(*t) for t in shapes) + tuple(sds(*t) for t in held),
        in_specs=[HBM] * 10,
        out_specs=(VM,) * len(shapes) + (HBM,) * len(held),
        scratch_shapes=[
            vm((n_tok, width), BF16), vm((width, n_tok), BF16), vm((n_dev, seq, cols), BF16), vm((n_dev, seq, n_rows), BF16),
            vm((n_rows, n_seq), BF16), vm((half, n_batch * n_seq), BF16), vm((n_seq, n_rows), BF16),
            vm((head_dim, n_seq), BF16), vm((head_dim, n_seq), BF16), vm((n_seq, head_dim), F32), vm((n_seq, head_dim), F32),
            vm((quarter, n_seq), F32), vm((quarter, n_seq), F32), vm((3, n_tok, head_dim), F32), vm((n_dev, n_batch, seq), jnp.int32), vm((width,), F32), vm((width,), F32), vm((quarter, 1), F32),
            vm((2, seq, n_rows), BF16), vm((2, half, n_tok), BF16),
            vm((n_batch, n_dev, seq, cols), BF16), vm((2, 8, width), F32), vm((chips, 2, width), F32), vm((CORES, 2, width), F32),
            dma((6,)), dma((9,)), dma((8,)), dma((8,)), dma((3,)), dma((3,)), dma((2,)),
            dma((6,)), dma((3,)), dma((1,)), dma((W_SLOTS, 2)), dma((4,)),
        ],
        compiler_params=pltpu.CompilerParams(collective_id=0, has_side_effects=True, vmem_limit_bytes=VMEM_LIMIT),
        cost_estimate=pl.CostEstimate(flops=10 ** 11, bytes_accessed=10 ** 8, transcendentals=0),
        name='block',
    )(gain, bias, positions, freq, x.reshape(n_tok, width), dy, wq, wk, wv, wo)[:len(shapes)]


def settle_body(n, *refs):
    sem = refs[2 * n]
    copies = []
    for src, dst in zip(refs[:n], refs[n:2 * n]):
        pieces = SETTLE if len(src.shape) > 1 else 1
        size = src.shape[0] // pieces
        copies += [pltpu.make_async_copy(src.at[pl.ds(p * size, size)], dst.at[pl.ds(p * size, size)], sem) for p in range(pieces)]
    for copy in copies:
        copy.start()
    for copy in copies:
        copy.wait()


def settle(arrays):
    n = len(arrays)
    return pl.pallas_call(
        functools.partial(settle_body, n),
        out_shape=tuple(sds(t.shape, t.dtype) for t in arrays),
        in_specs=[ANY] * n,
        out_specs=(HBM,) * n,
        scratch_shapes=[pltpu.SemaphoreType.DMA],
        compiler_params=pltpu.CompilerParams(vmem_limit_bytes=1024 * 1024),
        name='settle',
    )(*arrays)


def solution(mesh):
    n_dev = mesh.shape['cp']

    def device_step(x_act, d_out, positions, ln_gain, ln_bias, w_query, w_key, w_value, w_out):
        n_batch, seq, width = x_act.shape
        q_heads, (kv_heads, head_dim) = w_query.shape[1], w_key.shape[1:]
        group = q_heads // kv_heads
        quarter = head_dim // 4
        assert n_batch == CORES and n_dev // CORES == kv_heads == 4 and q_heads * head_dim == width

        freq = np.exp(np.arange(quarter) * (-2.0 * math.log(ROPE_BASE) / (head_dim // 2))).astype(np.float32).reshape(quarter, 1)
        by_head = lambda t: jnp.transpose(t, (1, 0, 2))
        by_row = lambda t: t.reshape(width * kv_heads, head_dim)
        wq = by_head(w_query)

        results = whole_block(n_dev, x_act, ln_gain, ln_bias, positions, jnp.asarray(freq), d_out, wq, by_row(w_key), by_row(w_value), w_out)
        out, dx, dwq, dwk, dwv, dwo, dgain, dbias = settle(results)
        kv_rows = lambda t: t.reshape(width // n_dev, kv_heads, head_dim)
        return (out.reshape(x_act.shape), dx.reshape(x_act.shape), by_head(dwq), kv_rows(dwk), kv_rows(dwv), dwo, dgain, dbias)

    return jax.shard_map(device_step, mesh=mesh, in_specs=(P('dp', 'cp', None), P('dp', 'cp', None), P('dp', 'cp'), P(None), P(None), P(None, None, None), P(None, None, None), P(None, None, None), P(None, None)), out_specs=(P('dp', 'cp', None), P('dp', 'cp', None), P(('dp', 'cp'), None, None), P(('dp', 'cp'), None, None), P(('dp', 'cp'), None, None), P(('dp', 'cp'), None), P('dp'), P('dp')), check_vma=False)
```

```python
import functools
import math
import jax
import jax.numpy as jnp
import numpy as np
from jax import lax
from jax.experimental import pallas as pl
from jax.experimental.pallas import tpu as pltpu
from jax.sharding import PartitionSpec as P

EPS = 1e-5
ROPE_BASE = 10000.0
BF16 = jnp.bfloat16
F32 = jnp.float32
VMEM_LIMIT = 46 * 1024 * 1024
NT = (((1,), (1,)), ((), ()))
ANY = pl.BlockSpec(memory_space=pl.ANY)
VM = pl.BlockSpec(memory_space=pltpu.VMEM)
HBM = pl.BlockSpec(memory_space=pltpu.HBM)
CORES = 2
PAIR = range(2)
STEPS = (1, -1)
COL_TILE = 512
OUT_TILE = 256
ROWS = 16
W_SLOTS = 4
W_ROWS = 512
SETTLE = 4


def dot(a, b):
    return jnp.dot(a, b, preferred_element_type=F32)


def dot_nt(a, b):
    return lax.dot_general(a, b, NT, preferred_element_type=F32)


def sds(shape, dtype):
    return jax.ShapeDtypeStruct(shape, dtype)


def head(size):
    return pl.ds(0, size)


def block(i, size):
    return pl.ds(pl.multiple_of(i * size, size), size)


class Place:
    def __init__(self, n_dev):
        self.n_dev = n_dev
        self.chips = n_dev // CORES
        self.me = lax.axis_index('cp')
        self.chip = self.me // CORES
        self.core = self.me % CORES
        self.partner = self.chip * CORES + 1 - self.core

    def ring(self, step):
        return lax.rem(self.chip + self.chips + step, self.chips)

    def dev(self, step, core):
        return self.ring(step) * CORES + core

    def peers(self, far):
        near = [self.partner] + [self.dev(s, c) for s in STEPS for c in range(CORES)]
        return near + ([self.dev(2, c) for c in range(CORES)] if far else [])


def send(src, dst, ssem, rsem, to):
    return pltpu.make_async_remote_copy(src_ref=src, dst_ref=dst, send_sem=ssem, recv_sem=rsem, device_id={'cp': to}, device_id_type=pl.DeviceIdType.MESH)


def all_sent(total, ssem, to):
    send(total, total, ssem, ssem, to).wait_send()


def all_came(total, rsem, to):
    send(total, total, rsem, rsem, to).wait_recv()


def meet(peers):
    barrier = pltpu.get_barrier_semaphore()
    for peer in peers:
        pl.semaphore_signal(barrier, inc=1, device_id={'cp': peer}, device_id_type=pl.DeviceIdType.MESH)
    pl.semaphore_wait(barrier, len(peers))


class Ring:
    def __init__(self, n, slots, copies):
        self.n, self.slots, self.copies = n, slots, copies

    def prime(self):
        for s in range(self.slots):
            for copy in self.copies(s, s):
                copy.start()

    def run(self, use):
        @pl.loop(0, self.n)
        def _(s):
            slot = lax.rem(s, self.slots)
            for copy in self.copies(s, slot):
                copy.wait()
            use(s, slot)

            @pl.when(s + self.slots < self.n)
            def _():
                for copy in self.copies(s + self.slots, slot):
                    copy.start()


class Gather:
    def __init__(self, at, own, piece, both, ssem, rsem, across):
        steps = STEPS
        origin = [at.dev(-1, at.core), at.dev(1, at.core)]
        far = at.dev(2, at.core)
        link = lambda i, src, dst, to: send(src, dst, ssem, rsem.at[i], to)
        self.first = [link(b, own(b), piece(at.me, b), at.dev(steps[b], at.core)) for b in PAIR]
        self.second = [link(2 + b, own(1 - b), piece(at.me, 1 - b), at.dev(steps[b], at.core)) for b in PAIR]
        self.again = [link(4 + b, piece(origin[b], b), piece(origin[b], b), at.dev(steps[b], at.core)) for b in PAIR]
        self.own_across = link(across[0], both(None), both(at.me), at.partner)
        self.first_across = [link(across[1], piece(origin[b], b), piece(origin[b], b), at.partner) for b in PAIR]
        self.second_across = [link(across[1], piece(origin[b], 1 - b), piece(origin[b], 1 - b), at.partner) for b in PAIR]
        self.far_across = [link(across[2], piece(far, b), piece(far, b), at.partner) for b in PAIR]

    def start_first(self):
        for copy in self.first + [self.own_across]:
            copy.start()

    def start_second(self):
        for copy in self.second:
            copy.start()

    def pass_on(self):
        for copy, again, across in zip(self.first, self.again, self.first_across):
            copy.wait_recv()
            again.start()
            across.start()

    def share_second(self):
        for copy, across in zip(self.second, self.second_across):
            copy.wait_recv()
            across.start()

    def share_far(self):
        for copy, across in zip(self.again, self.far_across):
            copy.wait_recv()
            across.start()


class Exchange:
    def __init__(self, at, src, dst, relay, ssem, rsem):
        near = [(0, 1 - at.core)] + [(s, c) for s in STEPS for c in range(CORES)]
        self.near = [send(src(at.dev(s, c)), dst(at.me), ssem, rsem.at[0], at.dev(s, c)) for s, c in near]
        self.far = [send(src(at.dev(2, i)), relay.at[i], ssem, rsem.at[1 + i], at.dev(step, at.core)) for i, step in enumerate(STEPS)]
        self.on = [send(relay.at[i], dst(at.dev(-step, at.core)), ssem, rsem.at[0], at.dev(step, i)) for i, step in enumerate(STEPS)]

    def start(self):
        for copy in self.far + self.near:
            copy.start()

    def pass_on(self):
        for far, on in zip(self.far, self.on):
            far.wait_recv()
            on.start()


def layer_norm(x):
    cen = x - jnp.mean(x, axis=-1, keepdims=True)
    inv = lax.rsqrt(jnp.mean(cen * cen, axis=-1, keepdims=True) + EPS)
    return cen * inv, inv


def block_body(n_dev, group, gain_hbm, bias_hbm, pos_hbm, freq_hbm, x_hbm, dy_ref, wq_ref, wk_ref, wv_ref, wo_ref,
               out_ref, dx_ref, dwq_ref, dwk_ref, dwv_ref, dwo_ref, dgain_ref, dbias_ref, dy_all, ht_all, g_all, wkv_all,
               h_ref, ht_ref, g_ref, q_ref, at_ref, at2_ref, da_ref, kt_ref, vt_ref, dk_ref, dv_ref,
               cost_ref, sint_ref, tab_ref, spot_ref, gain_ref, bias_ref, freq_ref, relay_q, relay_h, far_ref, part_ref, row_ref, total_ref,
               s_sem, dy_rsem, kv_rsem, q_rsem, h_rsem, p_rsem, t_sem, loc_sem, mix_sem, lhs_sem, w_sem, job_sem):
    at = Place(n_dev)
    n_batch, seq, width = dy_ref.shape
    n_tok = n_batch * seq
    head_dim = wq_ref.shape[2]
    cols = (group + 2) * head_dim
    n_rows = group * head_dim
    half = n_rows // CORES
    n_seq = n_dev * seq
    quarter = head_dim // 4
    scale = head_dim ** -0.5
    chips = at.chips
    tile = CORES * seq
    core, me = at.core, at.me
    steps = STEPS
    origin = [at.dev(-1, core), at.dev(1, core)]
    far_dev = at.dev(2, core)
    scope = jax.named_scope

    dy_ssem, kv_ssem, q_ssem, h_ssem, p_ssem, x_ssem = [s_sem.at[i] for i in range(6)]
    assert (n_dev + 1) * n_rows == (n_dev - 1) * cols
    block_total = far_ref.at[0, head(n_dev - 1)]

    with scope('meet'):
        meet(at.peers(True))

    kv_cols = 2 * head_dim * chips
    kv_piece = lambda d, b: far_ref.at[b, d, :, head(kv_cols)]
    kv_both = lambda d: far_ref.at[:, me if d is None else d, :, head(kv_cols)]
    dys = Gather(at, lambda b: dy_ref.at[b], lambda d, b: dy_all.at[d, b], lambda d: dy_ref if d is None else dy_all.at[d], dy_ssem, dy_rsem, (6, 7, 8))
    kvs = Gather(at, lambda b: kv_piece(me, b), kv_piece, kv_both, kv_ssem, kv_rsem, (6, 6, 6))
    q_part = head(n_rows)
    queries = Exchange(at, lambda d: g_ref.at[d, :, q_part], lambda d: q_ref.at[d], relay_q, q_ssem, q_rsem)
    hcols = Exchange(at, lambda d: ht_ref.at[block(d, half)], lambda d: ht_all.at[d], relay_h, h_ssem, h_rsem)
    heads_across = send(at_ref.at[block(1 - core, half)], at2_ref.at[:, block(core, n_seq)], t_sem.at[0], t_sem.at[1], at.partner)
    spots = [send(pos_hbm, spot_ref.at[me], p_ssem, p_rsem.at[0], peer) for peer in at.peers(True)]

    dys.start_first()
    x_in = pltpu.make_async_copy(x_hbm, dx_ref, loc_sem.at[1])
    x_in.start()
    for copy in spots:
        copy.start()
    small = [pltpu.make_async_copy(src, dst, loc_sem.at[2 + n]) for n, (src, dst) in enumerate(((gain_hbm, gain_ref), (bias_hbm, bias_ref), (freq_hbm, freq_ref), (pos_hbm, spot_ref.at[me])))]
    for copy in small:
        copy.start()
    for copy in small:
        copy.wait()

    freq = freq_ref[...]
    for b in range(n_batch):
        angle = freq * spot_ref[me, b:b + 1, :].astype(F32)
        cos, sin, none = jnp.cos(angle), jnp.sin(angle), jnp.zeros((quarter, seq), F32)
        rest = jnp.zeros((head_dim - 2 * quarter, seq), F32)
        for i, rows in enumerate(([cos, cos, rest + 1.0], [-sin, none, rest], [none, sin, rest])):
            tab_ref[i, b * seq:(b + 1) * seq, :] = jnp.concatenate(rows, axis=0).T

    gain = (1.0 + gain_ref[...]).reshape(1, width)
    bias = bias_ref[...].reshape(1, width)

    def project_all(wkv_ref, raw_ref, wq_vm, raw_sem, wq_sem, stage_sem):
        pieces = [(b, i) for b in range(n_batch) for i in range(width // n_rows)]
        there = lambda n: da_ref.at[pl.ds(n * seq, seq)]
        dy_in = [pltpu.make_async_copy(dy_ref.at[b, :, pl.ds(i * n_rows, n_rows)], there(n), stage_sem.at[n]) for n, (b, i) in enumerate(pieces)]
        dy_keep = [pltpu.make_async_copy(there(n), dy_all.at[me, b, :, pl.ds(i * n_rows, n_rows)], stage_sem.at[n]) for n, (b, i) in enumerate(pieces)]
        span = 64 * chips
        batch = raw_ref.shape[2] // span
        row = lax.broadcasted_iota(jnp.int32, (span, span), 0)
        col = lax.broadcasted_iota(jnp.int32, (span, span), 1)
        pick = jnp.where(col == lax.rem(row, 64) * chips + lax.div(row, 64), 1.0, 0.0).astype(BF16)

        def raw_in(s, slot):
            return [pltpu.make_async_copy(w.at[block(s, span * batch)], raw_ref.at[slot, i], raw_sem.at[slot, i]) for i, w in enumerate((wk_ref, wv_ref))]

        def wq_in(s, slot):
            return [pltpu.make_async_copy(wq_ref.at[block(s, 2)], wq_vm.at[slot], wq_sem.at[slot])]

        def part_heads(s, slot):
            for i in range(batch):
                sl = slice(i * span, (i + 1) * span)
                rows = dot(pick, jnp.concatenate([raw_ref[slot, 0, sl, :], raw_ref[slot, 1, sl, :]], axis=1)).astype(BF16)
                for n in range(chips):
                    wkv_ref[n, block(s * batch + i, 64), :] = rows[n * 64:(n + 1) * 64]

        def turned(v):
            return v * tab_ref[0] + pltpu.roll(v, head_dim - quarter, 1) * tab_ref[1] + pltpu.roll(v, quarter, 1) * tab_ref[2]

        def project(s, slot):
            y = dot(h_ref[...], jnp.concatenate([wq_vm[slot, 0], wq_vm[slot, 1]], axis=1))
            for i in PAIR:
                head = s * 2 + i
                v = turned(y[:, i * head_dim:(i + 1) * head_dim]).astype(BF16)
                for b in range(n_batch):
                    g_ref[lax.div(head, group) * n_batch + b, :, block(lax.rem(head, group), head_dim)] = v[b * seq:(b + 1) * seq]

        kv_ring = Ring(width // (64 * batch), raw_ref.shape[0], raw_in)
        q_ring = Ring(chips * group // 2, wq_vm.shape[0], wq_in)
        kv_ring.prime()
        q_ring.prime()
        for copy in dy_in:
            copy.start()
        x_in.wait()
        with scope('norm'):
            @pl.loop(0, n_tok // (2 * ROWS))
            def _(step):
                for i in PAIR:
                    sl = block(2 * step + i, ROWS)
                    hat, _ = layer_norm(dx_ref[sl, :].astype(F32))
                    h_ref[sl, :] = (hat * gain + bias).astype(BF16)

        with scope('heads_kv'):
            kv_ring.run(part_heads)
        keep = pltpu.make_async_copy(wkv_ref, wkv_all, mix_sem.at[2])
        keep.start()
        for come, go in zip(dy_in, dy_keep):
            come.wait()
            go.start()
        with scope('project_kv'):
            @pl.loop(0, chips)
            def _(n):
                y = dot(h_ref[...], wkv_ref[n])
                v = jnp.concatenate([turned(y[:, :head_dim]), y[:, head_dim:]], axis=1).astype(BF16)
                for b in range(n_batch):
                    far_ref[b, me, :, block(n, 2 * head_dim)] = v[b * seq:(b + 1) * seq]

        kvs.start_first()
        kvs.start_second()
        with scope('project_q'):
            q_ring.run(project)
        keep.wait()
        for copy in dy_keep:
            copy.wait()

    pl.run_scoped(
        project_all,
        pltpu.VMEM((chips, width, 2 * head_dim), BF16),
        pltpu.VMEM((3, 2, 4 * 64 * chips, head_dim), BF16), pltpu.VMEM((4, 2, width, head_dim), BF16),
        pltpu.SemaphoreType.DMA((3, 2)), pltpu.SemaphoreType.DMA((4,)), pltpu.SemaphoreType.DMA((n_batch * width // n_rows,)),
    )

    with scope('kv_pass'):
        kvs.pass_on()
    queries.start()
    q_ref[me] = g_ref[me, :, q_part]
    with scope('turn_h'):
        @pl.loop(0, width // 128)
        def _(step):
            sl = block(step, 128)
            ht_ref[sl, :] = h_ref[:, sl].T

    with scope('kv_wait'):
        kvs.share_second()
        kvs.share_far()
        all_came(far_ref.at[:, head(chips), :, head(kv_cols)], kv_rsem.at[6], at.partner)

    def chip_at(i):
        return at.ring(jnp.where(i == 0, 0, jnp.where(i == 1, 1, jnp.where(i == 2, 3, 2))))

    def soft(s, seen):
        s = s * scale
        clear = s.shape[0] - seen.shape[0]
        tail = jnp.where(seen, s[clear:], -1e30)
        s = tail if clear == 0 else jnp.concatenate([s[:clear], tail], axis=0)
        e = jnp.exp(s - jnp.max(s, axis=0, keepdims=True))
        return e * (1.0 / jnp.sum(e, axis=0, keepdims=True))

    def attend(limit, clear):
        @pl.loop(0, n_batch * chips)
        def _(i):
            @pl.when(i == 1)
            def _():
                with scope('q_pass'):
                    queries.pass_on()
                dys.start_second()
                dys.pass_on()
                hcols.start()

            b, n = lax.rem(i, n_batch), lax.div(i, n_batch)
            k = far_ref[b, 0:limit // seq, :, block(2 * n, head_dim)].reshape(limit, head_dim)
            vt = far_ref[b, 0:limit // seq, :, block(2 * n + 1, head_dim)].reshape(limit, head_dim).T
            q = jnp.concatenate([g_ref[n * n_batch + b, :, block(j, head_dim)] for j in range(group)], axis=0)
            row = lax.broadcasted_iota(jnp.int32, (limit - clear, n_rows), 0)
            col = lax.broadcasted_iota(jnp.int32, (limit - clear, n_rows), 1)
            p = soft(dot_nt(k, q), row <= lax.rem(col, seq) + (me * seq - clear))
            mixed = dot(vt, p.astype(BF16)).astype(BF16)
            for j in range(group):
                h_ref[block(b, seq), block(n * group + j, head_dim)] = mixed[:, j * seq:(j + 1) * seq].T

    with scope('attend'):
        @pl.when(at.chip == chips - 1)
        def _():
            attend(chips * tile, (chips - 1) * tile)

        @pl.when(at.chip < chips - 1)
        def _():
            attend((chips - 1) * tile, 0)

    h_keep = pltpu.make_async_copy(ht_ref.at[block(me, half)], ht_all.at[me], loc_sem.at[1])
    h_keep.start()

    def block_out():
        def stream(wo_vm, sem):
            def wo_in(s, slot):
                return [pltpu.make_async_copy(wo_ref.at[:, block(s, OUT_TILE)], wo_vm.at[slot], sem.at[slot])]

            def out_tile(s, slot):
                sl = block(s, OUT_TILE)
                out_ref[:, sl] = (dx_ref[:, sl].astype(F32) + dot(h_ref[...], wo_vm[slot])).astype(BF16)

            ring = Ring(width // OUT_TILE, wo_vm.shape[0], wo_in)
            ring.prime()
            ring.run(out_tile)

        with scope('output'):
            pl.run_scoped(stream, pltpu.VMEM((4, width, OUT_TILE), BF16), pltpu.SemaphoreType.DMA((4,)))

    k_all = lambda n: far_ref[core, 0:n, :, block(2 * at.chip, head_dim)].reshape(n * seq, head_dim)
    v_all = lambda n: far_ref[core, 0:n, :, block(2 * at.chip + 1, head_dim)].reshape(n * seq, head_dim)

    def rotate_back(t, cos, sin):
        u, w = t[:quarter], t[quarter:2 * quarter]
        return jnp.concatenate([u * cos + w * sin, w * cos - u * sin, t[2 * quarter:]], axis=0)

    def by_dev(t):
        return t.astype(BF16).reshape(t.shape[0] // seq, seq, head_dim)

    def attend_back(t, i):
        limit = (t + 1) * tile
        sl = slice(t * tile, limit)
        devs = slice(t * CORES, (t + 1) * CORES)

        def heads(first, count):
            each = range(count)
            q = jnp.concatenate([q_ref[devs, :, block(first + j, head_dim)].reshape(tile, head_dim) for j in each], axis=0)
            da = jnp.concatenate([da_ref[sl, block(first + j, head_dim)] for j in each], axis=0)
            k, v = k_all(limit // seq), v_all(limit // seq)
            row = lax.broadcasted_iota(jnp.int32, (tile, count * tile), 0)
            col = lax.broadcasted_iota(jnp.int32, (tile, count * tile), 1)
            p = soft(dot_nt(k, q), row <= lax.rem(col, tile))
            p_low = p.astype(BF16)
            mixed = dot(vt_ref[:, :limit], p_low).astype(BF16)
            dp = dot_nt(v, da)
            row_dot = jnp.sum(p * dp, axis=0, keepdims=True)
            ds = (p * (dp - row_dot) * scale).astype(BF16)
            dv_ref[:limit, :] += dot(p_low, da)
            dk_ref[:limit, :] += dot(ds, q)
            back = dot(kt_ref[:, :limit], ds)
            for j in each:
                part = slice(j * tile, (j + 1) * tile)
                at_ref[block(first + j, head_dim), sl] = mixed[:, part]
                g_ref[devs, :, block(first + j, head_dim)] = by_dev(rotate_back(back[:, part], cost_ref[:, sl], sint_ref[:, sl]).T)

        @pl.loop(0, group // 2)
        def _(j):
            heads(2 * j, 2)

        @pl.when(i == chips - 2)
        def _():
            with scope('dy_far'):
                dys.share_far()

        heads(group - 1, 1)

    def middle(wo_vm, dyk):
        wo_in = pltpu.make_async_copy(wo_ref.at[block(at.chip, n_rows)], wo_vm, mix_sem.at[2])
        wo_in.start()
        all_came(spot_ref.at[head(n_dev - 1)], p_rsem.at[0], at.partner)
        for d in range(n_dev):
            angle = freq * spot_ref[d, pl.ds(core, 1), :].astype(F32)
            cost_ref[:, d * seq:(d + 1) * seq] = jnp.cos(angle)
            sint_ref[:, d * seq:(d + 1) * seq] = jnp.sin(angle)
        with scope('q_wait'):
            all_came(q_ref.at[head(n_dev - 1)], q_rsem.at[0], at.partner)
            all_sent(block_total, q_ssem, at.partner)
            all_sent(far_ref.at[:, head(n_dev - 1), :, head(kv_cols)], kv_ssem, at.partner)
            all_sent(spot_ref.at[head(n_dev - 1)], p_ssem, at.partner)
        kt_ref[...] = k_all(n_dev).T
        vt_ref[...] = v_all(n_dev).T
        dk_ref[...] = jnp.zeros_like(dk_ref)
        dv_ref[...] = jnp.zeros_like(dv_ref)
        dys.own_across.wait_recv()

        def fetch(i, slot):
            return pltpu.make_async_copy(dy_all.at[block(chip_at(i), CORES), core], dyk.at[slot], mix_sem.at[slot])

        with scope('wo_wait'):
            fetch(0, 0).start()
            wo_in.wait()

        @pl.loop(0, chips)
        def _(i):
            slot = lax.rem(i, 2)

            @pl.when((i == 1) & (at.chip < chips - 1))
            def _():
                block_out()

            @pl.when(i == 1)
            def _():
                with scope('dy_wait'):
                    dys.share_second()
                    all_came(dy_all.at[head(2)], dy_rsem.at[7], at.partner)
                fetch(i, slot).start()

            @pl.when(i == chips - 1)
            def _():
                with scope('dy_far2'):
                    all_came(dy_all.at[0], dy_rsem.at[8], at.partner)
                fetch(i, slot).start()
                with scope('h_pass'):
                    hcols.pass_on()

            fetch(i, slot).wait()

            @pl.when((i > 0) & (i < chips - 2))
            def _():
                fetch(i + 1, 1 - slot).start()

            chip = chip_at(i)
            with scope('da'):
                da_ref[block(chip, tile), :] = dot_nt(dyk[slot].reshape(tile, width), wo_vm[...]).astype(BF16)
            with scope('attend_back'):
                for t in range(chips):
                    @pl.when(chip == t)
                    def _(t=t):
                        attend_back(t, i)

    pl.run_scoped(middle, pltpu.VMEM((n_rows, width), BF16), pltpu.VMEM((2, CORES, seq, width), BF16))
    all_sent(dy_all.at[head(n_dev - 1)], dy_ssem, at.partner)
    heads_across.start()
    g_ref[:, :, n_rows:n_rows + head_dim] = by_dev(rotate_back(dk_ref[...].T, cost_ref[...], sint_ref[...]).T)
    g_ref[:, :, n_rows + head_dim:] = by_dev(dv_ref[...])

    def span_of(q):
        return block(q, CORES)

    turn = [[at.ring(q) for q in (2, 1, 3, 0)], [at.ring(q) for q in (3, 0, 1, 2)]]
    direct = [[send(g_ref.at[span_of(turn[i][q])], g_all.at[me, span_of(turn[i][q])], kv_ssem, kv_rsem.at[i * chips + q], at.dev(steps[i], core)) for q in range(chips)] for i in PAIR]
    came = [[at.ring(q) for q in (1, 0, 2, 3)], [at.ring(q) for q in (0, 1, 2, 3)]]
    n_heads = group + 2
    late_heads = [range(n_heads), range(n_heads // 2 + 1), range(n_heads // 2 + 1, n_heads)]

    def columns(heads):
        return pl.ds(heads[0] * head_dim, len(heads) * head_dim)

    def late(ref, quarters):
        own = [ref.at[pl.ds(quarters[1] * CORES + min(c, 1), 1), :, columns(heads)] for c, heads in enumerate(late_heads)]
        return [ref.at[span_of(quarters[0])]] + own

    onward = [[send(src, dst, q_ssem, q_rsem.at[4 * i + q], at.dev(steps[i], core)) for q, (src, dst) in enumerate(zip(late(g_all.at[origin[i]], came[i]), late(far_ref.at[core], came[i])))] for i in PAIR]
    ends = [[at.ring(q) for q in (0, 3)], [at.ring(q) for q in (1, 2)]]
    g_across = send(g_ref, g_all.at[me], x_ssem, dy_rsem.at[0], at.partner)
    near_across = [[send(g_all.at[origin[i], span_of(came[i][q])], g_all.at[origin[i], span_of(came[i][q])], x_ssem, dy_rsem.at[1 + q // 2], at.partner) for q in range(chips)] for i in PAIR]
    end_across = [[send(ref, ref, x_ssem, dy_rsem.at[3 + (q or 4 * i)], at.partner) for q, ref in enumerate(late(far_ref.at[core], ends[i]))] for i in PAIR]
    for q in range(chips):
        for i in PAIR:
            direct[i][q].start()
    g_across.start()
    g_keep = pltpu.make_async_copy(g_ref, g_all.at[me], loc_sem.at[0])
    g_keep.start()
    at2_ref[:, block(core, n_seq)] = at_ref[block(core, half), :]

    @pl.when(at.chip == chips - 1)
    def _():
        block_out()

    dy_back = [pltpu.make_async_copy(dy_ref.at[b], h_ref.at[pl.ds(b * seq, seq)], loc_sem.at[2 + b]) for b in range(n_batch)]
    for copy in dy_back:
        copy.start()

    def wo_rows(dy_vm, sem):
        def dy_tile(s, slot):
            return [pltpu.make_async_copy(dy_all.at[:, :, :, block(s, COL_TILE)], dy_vm.at[slot], sem.at[slot])]

        def wo_tile(s, slot):
            pieces = [dy_vm[slot, d, b] for b in range(n_batch) for d in range(n_dev)]
            dwo_ref[:, block(s, COL_TILE)] = dot(at2_ref[...], jnp.concatenate(pieces, axis=0))

        ring = Ring(width // COL_TILE, dy_vm.shape[0], dy_tile)
        ring.prime()
        with scope('heads_wait'):
            heads_across.wait_recv()
        with scope('grad_wo'):
            ring.run(wo_tile)

    pl.run_scoped(wo_rows, pltpu.VMEM((4, n_dev, n_batch, seq, COL_TILE), BF16), pltpu.SemaphoreType.DMA((4,)))

    with scope('h_wait'):
        all_came(ht_all.at[head(n_dev - 1)], h_rsem.at[0], at.partner)
        all_sent(block_total, h_ssem, at.partner)
    h_keep.wait()
    lhs_in = [pltpu.make_async_copy(ht_all.at[d, :, pl.ds(b * seq, seq)], at2_ref.at[:, pl.ds((b * n_dev + d) * seq, seq)], lhs_sem.at[0]) for d in range(n_dev) for b in range(n_batch)]
    for copy in lhs_in:
        copy.start()
    with jax.named_scope('own_wait'):
        pltpu.make_async_copy(at2_ref, at2_ref, lhs_sem.at[0]).wait()
        g_keep.wait()
        g_across.wait_recv()
    rows_out = [send(row_ref.at[at.chip], row_ref.at[at.chip], p_ssem, p_rsem.at[1], at.dev(step, core)) for step in (1, -1, 2)]
    total_across = send(total_ref.at[core], total_ref.at[core], p_ssem, p_rsem.at[2], at.partner)

    def weight_grads(wq_vm, wkv_vm, acc_ref, hat_ref, inv_ref, job_ref, mine_ref):
        n_slots = wq_vm.shape[0]
        chunk = wq_vm.shape[2]
        n_chunks = width // chunk
        total = n_chunks * chips

        def weights(s):
            slot = lax.rem(s, n_slots)
            chip = chip_at(lax.div(s, n_chunks))
            rows = block(lax.rem(s, n_chunks), chunk)
            return [
                pltpu.make_async_copy(wq_ref.at[block(chip, group), rows], wq_vm.at[slot], w_sem.at[slot, 0]),
                pltpu.make_async_copy(wkv_all.at[chip, rows], wkv_vm.at[slot], w_sem.at[slot, 1]),
            ]

        for s in range(n_slots):
            for copy in weights(s):
                copy.start()

        def grow(i, read):
            @pl.loop(0, n_chunks)
            def _(n):
                s = i * n_chunks + n
                slot = lax.rem(s, n_slots)
                for copy in weights(s):
                    copy.wait()
                rows = jnp.concatenate([read(b) for b in range(n_batch)], axis=0)
                part = dot_nt(rows, jnp.concatenate([wq_vm[slot, j] for j in range(group)] + [wkv_vm[slot]], axis=1))
                sl = block(n, chunk)

                @pl.when(i == 0)
                def _():
                    acc_ref[:, sl] = part

                @pl.when(i > 0)
                def _():
                    acc_ref[:, sl] += part

                @pl.when(s + n_slots < total)
                def _():
                    for copy in weights(s + n_slots):
                        copy.start()

        def mine_in(i):
            return [pltpu.make_async_copy(g_all.at[chip_at(i) * CORES + b, me], mine_ref.at[lax.rem(i, 2), b], job_sem.at[2 + lax.rem(i, 2)]) for b in range(n_batch)]

        def grow_near(i):
            here = mine_ref.at[lax.rem(i, 2)]
            pltpu.make_async_copy(here, here, job_sem.at[2 + lax.rem(i, 2)]).wait()
            grow(i, lambda b: mine_ref[lax.rem(i, 2), b])

        def job_in(chip, quarters, slot):
            return [pltpu.make_async_copy(g_all.at[chip * CORES + b, span_of(q)], job_ref.at[slot, b, n], job_sem.at[slot]) for b in range(n_batch) for n, q in enumerate(quarters)]

        def job(chip, pieces, read, add, heads=range(n_heads)):
            lhs = [at2_ref[:, pl.ds(pl.multiple_of(b * n_seq + d * seq, seq), seq)] for b in range(n_batch) for d in pieces]
            rhs = [read(b, n) for b in range(n_batch) for n in range(len(pieces))]
            y = dot(jnp.concatenate(lhs, axis=1), jnp.concatenate(rhs, axis=0))
            for n, j in enumerate(heads):
                v = y[:, n * head_dim:(n + 1) * head_dim]
                if j < group:
                    dwq_ref[chip * group + j] = dwq_ref[chip * group + j] + v if add else v
                else:
                    ref, rows = (dwk_ref, dwv_ref)[j - group], pl.ds(chip, half, stride=chips)
                    ref[rows, :] = ref[rows, :] + v if add else v

        def devs_of(quarters):
            return [q * CORES + c for q in quarters for c in range(CORES)]

        def near_pair(quarters, add):
            for slot, step in enumerate(steps):
                for copy in job_in(at.ring(step), quarters, slot):
                    copy.start()

            @pl.loop(0, 2)
            def _(slot):
                chip = at.ring(1 - 2 * slot)
                pltpu.make_async_copy(job_ref.at[slot], job_ref.at[slot], job_sem.at[slot]).wait()
                job(chip, devs_of(quarters), lambda b, n: job_ref[slot, b, n // CORES, n % CORES], add)

        halves = [[at.ring(q) for q in half_of] for half_of in ((0, 1), (2, 3))]
        for slot in PAIR:
            for copy in job_in(at.chip, [at.ring(2 * slot), at.ring(2 * slot + 1)], slot):
                copy.start()
        for copy in mine_in(0):
            copy.start()
        with jax.named_scope('own_job'):
            for slot in PAIR:
                quarters = [at.ring(2 * slot), at.ring(2 * slot + 1)]
                pltpu.make_async_copy(job_ref.at[slot], job_ref.at[slot], job_sem.at[slot]).wait()
                job(at.chip, devs_of(quarters), lambda b, n: job_ref[slot, b, n // CORES, n % CORES], slot == 1)

        with jax.named_scope('own_dh'):
            grow_near(0)

        with jax.named_scope('d01_wait'):
            for q in PAIR:
                for i in PAIR:
                    direct[i][q].wait_recv()
                for i in PAIR:
                    for copy in onward[i][:1] if q == 0 else onward[i][1:]:
                        copy.start()
                    near_across[i][q].start()
        with scope('d01_across'):
            all_came(g_all.at[0], dy_rsem.at[1], at.partner)
        for i in (1, 2):
            for copy in mine_in(i):
                copy.start()
        with scope('near_dh'):
            @pl.loop(1, chips - 1)
            def _(i):
                grow_near(i)

        with jax.named_scope('near_a'):
            near_pair(halves[0], False)
        with scope('d2_wait'):
            for i in PAIR:
                direct[i][2].wait_recv()
                near_across[i][2].start()
        with jax.named_scope('hat'):
            @pl.loop(0, n_tok // (2 * ROWS))
            def _(step):
                for i in PAIR:
                    sl = block(2 * step + i, ROWS)
                    hat, inv = layer_norm(dx_ref[sl, :].astype(F32))
                    hat_ref[sl, :] = hat
                    inv_ref[sl, :] = jnp.broadcast_to(inv, (ROWS, 128))

        with scope('d3_wait'):
            for i in PAIR:
                direct[i][3].wait_recv()
                near_across[i][3].start()
        with scope('d23_across'):
            all_came(g_all.at[0], dy_rsem.at[2], at.partner)
        with jax.named_scope('near_b'):
            near_pair(halves[1], True)
        far_chip = at.ring(2)
        end_total = [g_all.at[0, head(CORES), :, columns(heads)] for heads in late_heads]
        with jax.named_scope('far0_wait'):
            for i in PAIR:
                onward[i][0].wait_recv()
                end_across[i][0].start()
        with scope('far0_across'):
            all_came(end_total[0], dy_rsem.at[3], at.partner)
        with jax.named_scope('far_dh'):
            grow(chips - 1, lambda b: far_ref[b, me])
        for copy in dy_back:
            copy.wait()
        part_ref[...] = jnp.zeros_like(part_ref)

        with jax.named_scope('norm_back'):
            @pl.loop(0, n_tok // (2 * ROWS))
            def _(step):
                for i in PAIR:
                    sl = block(2 * step + i, ROWS)
                    hat, inv = hat_ref[sl, :], inv_ref[sl, 0:1]
                    dh = acc_ref[sl, :]
                    dg = dh * hat
                    gh = dh * gain
                    one = jnp.mean(gh, axis=-1, keepdims=True)
                    two = jnp.mean(dg * gain, axis=-1, keepdims=True)
                    dx_ref[sl, :] = (h_ref[sl, :].astype(F32) + inv * (gh - one - hat * two)).astype(BF16)
                    part_ref[0] += dg[0:8] + dg[8:16]
                    part_ref[1] += dh[0:8] + dh[8:16]

        for i in PAIR:
            row_ref[at.chip, i:i + 1, :] = jnp.sum(part_ref[i], axis=0, keepdims=True)
        for copy in rows_out:
            copy.start()

        def hand_on(c):
            with scope('far1_wait'):
                for i in PAIR:
                    onward[i][1 + c].wait_recv()
                    end_across[i][1 + c].start()

        def far_rows(devs, add, heads=range(n_heads)):
            job(far_chip, devs, lambda b, n: far_ref[b, devs[n], :, heads[0] * head_dim:(heads[-1] + 1) * head_dim], add, heads)

        def last_half(c):
            with scope('far1_across'):
                all_came(end_total[c], dy_rsem.at[4 + c], at.partner)
            with scope('far_b'):
                far_rows([ends[i][1] * CORES + min(c, 1) for i in PAIR], True, late_heads[c])

        hand_on(0)
        with scope('far_a'):
            all_came(end_total[0], dy_rsem.at[7], at.partner)
            far_rows(devs_of([ends[0][0], ends[1][0]]), False)
        hand_on(1)
        last_half(0)
        with scope('total'):
            all_came(row_ref.at[head(chips - 1)], p_rsem.at[1], at.partner)
            all_sent(row_ref.at[head(chips - 1)], p_ssem, at.partner)
            total = row_ref[0]
            for n in range(1, chips):
                total = total + row_ref[n]
            total_ref[core] = total
            total_across.start()
        hand_on(2)
        last_half(1)
        last_half(2)

    pl.run_scoped(
        weight_grads,
        pltpu.VMEM((W_SLOTS, group, W_ROWS, head_dim), BF16), pltpu.VMEM((W_SLOTS, W_ROWS, 2 * head_dim), BF16), pltpu.VMEM((n_tok, width), F32),
        pltpu.VMEM((n_tok, width), F32), pltpu.VMEM((n_tok, 128), F32), pltpu.VMEM((2, n_batch, 2, CORES, seq, cols), BF16), pltpu.VMEM((2, n_batch, seq, cols), BF16),
    )

    with scope('sums'):
        all_came(total_ref.at[0], p_rsem.at[2], at.partner)
        total = total_ref[0] + total_ref[1]
        dgain_ref[...] = total[0:1].reshape(width)
        dbias_ref[...] = total[1:2].reshape(width)
    with scope('done'):
        heads_across.wait_send()
        all_sent(far_ref, kv_ssem, at.partner)
        all_sent(g_ref, q_ssem, at.partner)
        all_sent(g_all.at[head(chips)], x_ssem, at.partner)
        all_sent(total_ref.at[0], p_ssem, at.partner)


def whole_block(n_dev, x, gain, bias, positions, freq, dy, wq, wk, wv, wo):
    n_batch, seq, width = dy.shape
    n_tok = n_batch * seq
    head_dim = wq.shape[2]
    chips = n_dev // CORES
    group = wq.shape[0] // chips
    cols = (group + 2) * head_dim
    n_rows = group * head_dim
    half = n_rows // CORES
    n_seq = n_dev * seq
    quarter = head_dim // 4
    dma = pltpu.SemaphoreType.DMA
    vm = pltpu.VMEM
    shapes = [((n_tok, width), BF16)] * 2 + [((chips * group, half, head_dim), F32)] + [((chips * half, head_dim), F32)] * 2 + [((half, width), F32), ((width,), F32), ((width,), F32)]
    held = [((n_dev, n_batch, seq, width), BF16), ((n_dev, half, n_tok), BF16), ((n_dev, n_dev, seq, cols), BF16), ((chips, width, 2 * head_dim), BF16)]
    return pl.pallas_call(
        functools.partial(block_body, n_dev, group),
        out_shape=tuple(pltpu.VMEM(*t) for t in shapes) + tuple(sds(*t) for t in held),
        in_specs=[HBM] * 10,
        out_specs=(VM,) * len(shapes) + (HBM,) * len(held),
        scratch_shapes=[
            vm((n_tok, width), BF16), vm((width, n_tok), BF16), vm((n_dev, seq, cols), BF16), vm((n_dev, seq, n_rows), BF16),
            vm((n_rows, n_seq), BF16), vm((half, n_batch * n_seq), BF16), vm((n_seq, n_rows), BF16),
            vm((head_dim, n_seq), BF16), vm((head_dim, n_seq), BF16), vm((n_seq, head_dim), F32), vm((n_seq, head_dim), F32),
            vm((quarter, n_seq), F32), vm((quarter, n_seq), F32), vm((3, n_tok, head_dim), F32), vm((n_dev, n_batch, seq), jnp.int32), vm((width,), F32), vm((width,), F32), vm((quarter, 1), F32),
            vm((2, seq, n_rows), BF16), vm((2, half, n_tok), BF16),
            vm((n_batch, n_dev, seq, cols), BF16), vm((2, 8, width), F32), vm((chips, 2, width), F32), vm((CORES, 2, width), F32),
            dma((6,)), dma((9,)), dma((8,)), dma((8,)), dma((3,)), dma((3,)), dma((2,)),
            dma((6,)), dma((3,)), dma((1,)), dma((W_SLOTS, 2)), dma((4,)),
        ],
        compiler_params=pltpu.CompilerParams(collective_id=0, has_side_effects=True, vmem_limit_bytes=VMEM_LIMIT),
        cost_estimate=pl.CostEstimate(flops=10 ** 11, bytes_accessed=10 ** 8, transcendentals=0),
        name='block',
    )(gain, bias, positions, freq, x.reshape(n_tok, width), dy, wq, wk, wv, wo)[:len(shapes)]


def settle_body(n, *refs):
    sem = refs[2 * n]
    copies = []
    for src, dst in zip(refs[:n], refs[n:2 * n]):
        pieces = SETTLE if len(src.shape) > 1 else 1
        size = src.shape[0] // pieces
        copies += [pltpu.make_async_copy(src.at[pl.ds(p * size, size)], dst.at[pl.ds(p * size, size)], sem) for p in range(pieces)]
    for copy in copies:
        copy.start()
    for copy in copies:
        copy.wait()


def settle(arrays):
    n = len(arrays)
    return pl.pallas_call(
        functools.partial(settle_body, n),
        out_shape=tuple(sds(t.shape, t.dtype) for t in arrays),
        in_specs=[ANY] * n,
        out_specs=(HBM,) * n,
        scratch_shapes=[pltpu.SemaphoreType.DMA],
        compiler_params=pltpu.CompilerParams(vmem_limit_bytes=1024 * 1024),
        name='settle',
    )(*arrays)


def solution(mesh):
    n_dev = mesh.shape['cp']

    def device_step(x_act, d_out, positions, ln_gain, ln_bias, w_query, w_key, w_value, w_out):
        n_batch, seq, width = x_act.shape
        q_heads, (kv_heads, head_dim) = w_query.shape[1], w_key.shape[1:]
        group = q_heads // kv_heads
        quarter = head_dim // 4
        assert n_batch == CORES and n_dev // CORES == kv_heads == 4 and q_heads * head_dim == width

        freq = np.exp(np.arange(quarter) * (-2.0 * math.log(ROPE_BASE) / (head_dim // 2))).astype(np.float32).reshape(quarter, 1)
        by_head = lambda t: jnp.transpose(t, (1, 0, 2))
        by_row = lambda t: t.reshape(width * kv_heads, head_dim)
        wq = by_head(w_query)

        results = whole_block(n_dev, x_act, ln_gain, ln_bias, positions, jnp.asarray(freq), d_out, wq, by_row(w_key), by_row(w_value), w_out)
        out, dx, dwq, dwk, dwv, dwo, dgain, dbias = settle(results)
        kv_rows = lambda t: t.reshape(width // n_dev, kv_heads, head_dim)
        return (out.reshape(x_act.shape), dx.reshape(x_act.shape), by_head(dwq), kv_rows(dwk), kv_rows(dwv), dwo, dgain, dbias)

    return jax.shard_map(device_step, mesh=mesh, in_specs=(P('dp', 'cp', None), P('dp', 'cp', None), P('dp', 'cp'), P(None), P(None), P(None, None, None), P(None, None, None), P(None, None, None), P(None, None)), out_specs=(P('dp', 'cp', None), P('dp', 'cp', None), P(('dp', 'cp'), None, None), P(('dp', 'cp'), None, None), P(('dp', 'cp'), None, None), P(('dp', 'cp'), None), P('dp'), P('dp')), check_vma=False)
```

```python
import functools
import math
import jax
import jax.numpy as jnp
import numpy as np
from jax import lax
from jax.experimental import pallas as pl
from jax.experimental.pallas import tpu as pltpu
from jax.sharding import PartitionSpec as P

EPS = 1e-5
ROPE_BASE = 10000.0
BF16 = jnp.bfloat16
F32 = jnp.float32
VMEM_LIMIT = 46 * 1024 * 1024
NT = (((1,), (1,)), ((), ()))
ANY = pl.BlockSpec(memory_space=pl.ANY)
VM = pl.BlockSpec(memory_space=pltpu.VMEM)
HBM = pl.BlockSpec(memory_space=pltpu.HBM)
CORES = 2
PAIR = range(2)
STEPS = (1, -1)
COL_TILE = 512
OUT_TILE = 256
ROWS = 16
W_SLOTS = 4
W_ROWS = 512
SETTLE = 4


def dot(a, b):
    return jnp.dot(a, b, preferred_element_type=F32)


def dot_nt(a, b):
    return lax.dot_general(a, b, NT, preferred_element_type=F32)


def sds(shape, dtype):
    return jax.ShapeDtypeStruct(shape, dtype)


def head(size):
    return pl.ds(0, size)


def block(i, size):
    return pl.ds(pl.multiple_of(i * size, size), size)


class Place:
    def __init__(self, n_dev):
        self.n_dev = n_dev
        self.chips = n_dev // CORES
        self.me = lax.axis_index('cp')
        self.chip = self.me // CORES
        self.core = self.me % CORES
        self.partner = self.chip * CORES + 1 - self.core

    def ring(self, step):
        return lax.rem(self.chip + self.chips + step, self.chips)

    def dev(self, step, core):
        return self.ring(step) * CORES + core

    def peers(self, far):
        near = [self.partner] + [self.dev(s, c) for s in STEPS for c in range(CORES)]
        return near + ([self.dev(2, c) for c in range(CORES)] if far else [])


def send(src, dst, ssem, rsem, to):
    return pltpu.make_async_remote_copy(src_ref=src, dst_ref=dst, send_sem=ssem, recv_sem=rsem, device_id={'cp': to}, device_id_type=pl.DeviceIdType.MESH)


def all_sent(total, ssem, to):
    send(total, total, ssem, ssem, to).wait_send()


def all_came(total, rsem, to):
    send(total, total, rsem, rsem, to).wait_recv()


def meet(peers):
    barrier = pltpu.get_barrier_semaphore()
    for peer in peers:
        pl.semaphore_signal(barrier, inc=1, device_id={'cp': peer}, device_id_type=pl.DeviceIdType.MESH)
    pl.semaphore_wait(barrier, len(peers))


class Ring:
    def __init__(self, n, slots, copies):
        self.n, self.slots, self.copies = n, slots, copies

    def prime(self):
        for s in range(self.slots):
            for copy in self.copies(s, s):
                copy.start()

    def run(self, use):
        @pl.loop(0, self.n)
        def _(s):
            slot = lax.rem(s, self.slots)
            for copy in self.copies(s, slot):
                copy.wait()
            use(s, slot)

            @pl.when(s + self.slots < self.n)
            def _():
                for copy in self.copies(s + self.slots, slot):
                    copy.start()


class Gather:
    def __init__(self, at, own, piece, both, ssem, rsem, across):
        steps = STEPS
        origin = [at.dev(-1, at.core), at.dev(1, at.core)]
        far = at.dev(2, at.core)
        link = lambda i, src, dst, to: send(src, dst, ssem, rsem.at[i], to)
        self.first = [link(b, own(b), piece(at.me, b), at.dev(steps[b], at.core)) for b in PAIR]
        self.second = [link(2 + b, own(1 - b), piece(at.me, 1 - b), at.dev(steps[b], at.core)) for b in PAIR]
        self.again = [link(4 + b, piece(origin[b], b), piece(origin[b], b), at.dev(steps[b], at.core)) for b in PAIR]
        self.own_across = link(across[0], both(None), both(at.me), at.partner)
        self.first_across = [link(across[1], piece(origin[b], b), piece(origin[b], b), at.partner) for b in PAIR]
        self.second_across = [link(across[1], piece(origin[b], 1 - b), piece(origin[b], 1 - b), at.partner) for b in PAIR]
        self.far_across = [link(across[2], piece(far, b), piece(far, b), at.partner) for b in PAIR]

    def start_first(self):
        for copy in self.first + [self.own_across]:
            copy.start()

    def start_second(self):
        for copy in self.second:
            copy.start()

    def pass_on(self):
        for copy, again, across in zip(self.first, self.again, self.first_across):
            copy.wait_recv()
            again.start()
            across.start()

    def share_second(self):
        for copy, across in zip(self.second, self.second_across):
            copy.wait_recv()
            across.start()

    def share_far(self):
        for copy, across in zip(self.again, self.far_across):
            copy.wait_recv()
            across.start()


class Exchange:
    def __init__(self, at, src, dst, relay, ssem, rsem):
        near = [(0, 1 - at.core)] + [(s, c) for s in STEPS for c in range(CORES)]
        self.near = [send(src(at.dev(s, c)), dst(at.me), ssem, rsem.at[0], at.dev(s, c)) for s, c in near]
        self.far = [send(src(at.dev(2, i)), relay.at[i], ssem, rsem.at[1 + i], at.dev(step, at.core)) for i, step in enumerate(STEPS)]
        self.on = [send(relay.at[i], dst(at.dev(-step, at.core)), ssem, rsem.at[0], at.dev(step, i)) for i, step in enumerate(STEPS)]

    def start(self):
        for copy in self.far + self.near:
            copy.start()

    def pass_on(self):
        for far, on in zip(self.far, self.on):
            far.wait_recv()
            on.start()


def layer_norm(x):
    cen = x - jnp.mean(x, axis=-1, keepdims=True)
    inv = lax.rsqrt(jnp.mean(cen * cen, axis=-1, keepdims=True) + EPS)
    return cen * inv, inv


def block_body(n_dev, group, gain_hbm, bias_hbm, pos_hbm, freq_hbm, x_hbm, dy_ref, wq_ref, wk_ref, wv_ref, wo_ref,
               out_ref, dx_ref, dwq_ref, dwk_ref, dwv_ref, dwo_ref, dgain_ref, dbias_ref, dy_all, ht_all, g_all, wkv_all,
               h_ref, ht_ref, g_ref, q_ref, at_ref, at2_ref, da_ref, kt_ref, vt_ref, dk_ref, dv_ref,
               cost_ref, sint_ref, tab_ref, spot_ref, gain_ref, bias_ref, freq_ref, relay_q, relay_h, far_ref, part_ref, pair_ref, row_ref, total_ref,
               s_sem, dy_rsem, kv_rsem, q_rsem, h_rsem, p_rsem, t_sem, loc_sem, mix_sem, lhs_sem, w_sem, job_sem):
    at = Place(n_dev)
    n_batch, seq, width = dy_ref.shape
    n_tok = n_batch * seq
    head_dim = wq_ref.shape[2]
    cols = (group + 2) * head_dim
    n_rows = group * head_dim
    half = n_rows // CORES
    n_seq = n_dev * seq
    quarter = head_dim // 4
    scale = head_dim ** -0.5
    chips = at.chips
    tile = CORES * seq
    core, me = at.core, at.me
    steps = STEPS
    origin = [at.dev(-1, core), at.dev(1, core)]
    far_dev = at.dev(2, core)
    scope = jax.named_scope

    dy_ssem, kv_ssem, q_ssem, h_ssem, p_ssem, x_ssem = [s_sem.at[i] for i in range(6)]
    assert (n_dev + 1) * n_rows == (n_dev - 1) * cols
    block_total = far_ref.at[0, head(n_dev - 1)]

    with scope('meet'):
        meet(at.peers(True))

    kv_cols = 2 * head_dim * chips
    kv_piece = lambda d, b: far_ref.at[b, d, :, head(kv_cols)]
    kv_both = lambda d: far_ref.at[:, me if d is None else d, :, head(kv_cols)]
    dys = Gather(at, lambda b: dy_ref.at[b], lambda d, b: dy_all.at[d, b], lambda d: dy_ref if d is None else dy_all.at[d], dy_ssem, dy_rsem, (6, 7, 8))
    kvs = Gather(at, lambda b: kv_piece(me, b), kv_piece, kv_both, kv_ssem, kv_rsem, (6, 6, 6))
    q_part = head(n_rows)
    queries = Exchange(at, lambda d: g_ref.at[d, :, q_part], lambda d: q_ref.at[d], relay_q, q_ssem, q_rsem)
    hcols = Exchange(at, lambda d: ht_ref.at[block(d, half)], lambda d: ht_all.at[d], relay_h, h_ssem, h_rsem)
    heads_across = send(at_ref.at[block(1 - core, half)], at2_ref.at[:, block(core, n_seq)], t_sem.at[0], t_sem.at[1], at.partner)
    spots = [send(pos_hbm, spot_ref.at[me], p_ssem, p_rsem.at[0], peer) for peer in at.peers(True)]

    dys.start_first()
    x_in = pltpu.make_async_copy(x_hbm, dx_ref, loc_sem.at[1])
    x_in.start()
    for copy in spots:
        copy.start()
    small = [pltpu.make_async_copy(src, dst, loc_sem.at[2 + n]) for n, (src, dst) in enumerate(((gain_hbm, gain_ref), (bias_hbm, bias_ref), (freq_hbm, freq_ref), (pos_hbm, spot_ref.at[me])))]
    for copy in small:
        copy.start()
    for copy in small:
        copy.wait()

    freq = freq_ref[...]
    for b in range(n_batch):
        angle = freq * spot_ref[me, b:b + 1, :].astype(F32)
        cos, sin, none = jnp.cos(angle), jnp.sin(angle), jnp.zeros((quarter, seq), F32)
        rest = jnp.zeros((head_dim - 2 * quarter, seq), F32)
        for i, rows in enumerate(([cos, cos, rest + 1.0], [-sin, none, rest], [none, sin, rest])):
            tab_ref[i, b * seq:(b + 1) * seq, :] = jnp.concatenate(rows, axis=0).T

    gain = (1.0 + gain_ref[...]).reshape(1, width)
    bias = bias_ref[...].reshape(1, width)

    def project_all(wkv_ref, raw_ref, wq_vm, raw_sem, wq_sem, stage_sem):
        pieces = [(b, i) for b in range(n_batch) for i in range(width // n_rows)]
        there = lambda n: da_ref.at[pl.ds(n * seq, seq)]
        dy_in = [pltpu.make_async_copy(dy_ref.at[b, :, pl.ds(i * n_rows, n_rows)], there(n), stage_sem.at[n]) for n, (b, i) in enumerate(pieces)]
        dy_keep = [pltpu.make_async_copy(there(n), dy_all.at[me, b, :, pl.ds(i * n_rows, n_rows)], stage_sem.at[n]) for n, (b, i) in enumerate(pieces)]
        span = 64 * chips
        batch = raw_ref.shape[2] // span
        row = lax.broadcasted_iota(jnp.int32, (span, span), 0)
        col = lax.broadcasted_iota(jnp.int32, (span, span), 1)
        pick = jnp.where(col == lax.rem(row, 64) * chips + lax.div(row, 64), 1.0, 0.0).astype(BF16)

        def raw_in(s, slot):
            return [pltpu.make_async_copy(w.at[block(s, span * batch)], raw_ref.at[slot, i], raw_sem.at[slot, i]) for i, w in enumerate((wk_ref, wv_ref))]

        def wq_in(s, slot):
            return [pltpu.make_async_copy(wq_ref.at[block(s, 2)], wq_vm.at[slot], wq_sem.at[slot])]

        def part_heads(s, slot):
            for i in range(batch):
                sl = slice(i * span, (i + 1) * span)
                rows = dot(pick, jnp.concatenate([raw_ref[slot, 0, sl, :], raw_ref[slot, 1, sl, :]], axis=1)).astype(BF16)
                for n in range(chips):
                    wkv_ref[n, block(s * batch + i, 64), :] = rows[n * 64:(n + 1) * 64]

        def turned(v):
            return v * tab_ref[0] + pltpu.roll(v, head_dim - quarter, 1) * tab_ref[1] + pltpu.roll(v, quarter, 1) * tab_ref[2]

        def project(s, slot):
            y = dot(h_ref[...], jnp.concatenate([wq_vm[slot, 0], wq_vm[slot, 1]], axis=1))
            for i in PAIR:
                head = s * 2 + i
                v = turned(y[:, i * head_dim:(i + 1) * head_dim]).astype(BF16)
                for b in range(n_batch):
                    g_ref[lax.div(head, group) * n_batch + b, :, block(lax.rem(head, group), head_dim)] = v[b * seq:(b + 1) * seq]

        kv_ring = Ring(width // (64 * batch), raw_ref.shape[0], raw_in)
        q_ring = Ring(chips * group // 2, wq_vm.shape[0], wq_in)
        kv_ring.prime()
        q_ring.prime()
        for copy in dy_in:
            copy.start()
        x_in.wait()
        with scope('norm'):
            @pl.loop(0, n_tok // (2 * ROWS))
            def _(step):
                for i in PAIR:
                    sl = block(2 * step + i, ROWS)
                    hat, _ = layer_norm(dx_ref[sl, :].astype(F32))
                    h_ref[sl, :] = (hat * gain + bias).astype(BF16)

        with scope('heads_kv'):
            kv_ring.run(part_heads)
        keep = pltpu.make_async_copy(wkv_ref, wkv_all, mix_sem.at[2])
        keep.start()
        for come, go in zip(dy_in, dy_keep):
            come.wait()
            go.start()
        with scope('project_kv'):
            @pl.loop(0, chips)
            def _(n):
                y = dot(h_ref[...], wkv_ref[n])
                v = jnp.concatenate([turned(y[:, :head_dim]), y[:, head_dim:]], axis=1).astype(BF16)
                for b in range(n_batch):
                    far_ref[b, me, :, block(n, 2 * head_dim)] = v[b * seq:(b + 1) * seq]

        kvs.start_first()
        kvs.start_second()
        with scope('project_q'):
            q_ring.run(project)
        keep.wait()
        for copy in dy_keep:
            copy.wait()

    pl.run_scoped(
        project_all,
        pltpu.VMEM((chips, width, 2 * head_dim), BF16),
        pltpu.VMEM((3, 2, 4 * 64 * chips, head_dim), BF16), pltpu.VMEM((4, 2, width, head_dim), BF16),
        pltpu.SemaphoreType.DMA((3, 2)), pltpu.SemaphoreType.DMA((4,)), pltpu.SemaphoreType.DMA((n_batch * width // n_rows,)),
    )

    with scope('kv_pass'):
        kvs.pass_on()
    queries.start()
    q_ref[me] = g_ref[me, :, q_part]
    with scope('turn_h'):
        @pl.loop(0, width // 128)
        def _(step):
            sl = block(step, 128)
            ht_ref[sl, :] = h_ref[:, sl].T

    with scope('kv_wait'):
        kvs.share_second()
        kvs.share_far()
        all_came(far_ref.at[:, head(chips), :, head(kv_cols)], kv_rsem.at[6], at.partner)

    def chip_at(i):
        return at.ring(jnp.where(i == 0, 0, jnp.where(i == 1, 1, jnp.where(i == 2, 3, 2))))

    def soft(s, seen):
        s = s * scale
        clear = s.shape[0] - seen.shape[0]
        tail = jnp.where(seen, s[clear:], -1e30)
        s = tail if clear == 0 else jnp.concatenate([s[:clear], tail], axis=0)
        e = jnp.exp(s - jnp.max(s, axis=0, keepdims=True))
        return e * (1.0 / jnp.sum(e, axis=0, keepdims=True))

    def attend(limit, clear):
        @pl.loop(0, n_batch * chips)
        def _(i):
            @pl.when(i == 1)
            def _():
                with scope('q_pass'):
                    queries.pass_on()
                dys.start_second()
                dys.pass_on()
                hcols.start()

            b, n = lax.rem(i, n_batch), lax.div(i, n_batch)
            k = far_ref[b, 0:limit // seq, :, block(2 * n, head_dim)].reshape(limit, head_dim)
            vt = far_ref[b, 0:limit // seq, :, block(2 * n + 1, head_dim)].reshape(limit, head_dim).T
            q = jnp.concatenate([g_ref[n * n_batch + b, :, block(j, head_dim)] for j in range(group)], axis=0)
            row = lax.broadcasted_iota(jnp.int32, (limit - clear, n_rows), 0)
            col = lax.broadcasted_iota(jnp.int32, (limit - clear, n_rows), 1)
            p = soft(dot_nt(k, q), row <= lax.rem(col, seq) + (me * seq - clear))
            mixed = dot(vt, p.astype(BF16)).astype(BF16)
            for j in range(group):
                h_ref[block(b, seq), block(n * group + j, head_dim)] = mixed[:, j * seq:(j + 1) * seq].T

    with scope('attend'):
        @pl.when(at.chip == chips - 1)
        def _():
            attend(chips * tile, (chips - 1) * tile)

        @pl.when(at.chip < chips - 1)
        def _():
            attend((chips - 1) * tile, 0)

    h_keep = pltpu.make_async_copy(ht_ref.at[block(me, half)], ht_all.at[me], loc_sem.at[1])
    h_keep.start()

    def block_out():
        def stream(wo_vm, sem):
            def wo_in(s, slot):
                return [pltpu.make_async_copy(wo_ref.at[:, block(s, OUT_TILE)], wo_vm.at[slot], sem.at[slot])]

            def out_tile(s, slot):
                sl = block(s, OUT_TILE)
                out_ref[:, sl] = (dx_ref[:, sl].astype(F32) + dot(h_ref[...], wo_vm[slot])).astype(BF16)

            ring = Ring(width // OUT_TILE, wo_vm.shape[0], wo_in)
            ring.prime()
            ring.run(out_tile)

        with scope('output'):
            pl.run_scoped(stream, pltpu.VMEM((4, width, OUT_TILE), BF16), pltpu.SemaphoreType.DMA((4,)))

    k_all = lambda n: far_ref[core, 0:n, :, block(2 * at.chip, head_dim)].reshape(n * seq, head_dim)
    v_all = lambda n: far_ref[core, 0:n, :, block(2 * at.chip + 1, head_dim)].reshape(n * seq, head_dim)

    def rotate_back(t, cos, sin):
        u, w = t[:quarter], t[quarter:2 * quarter]
        return jnp.concatenate([u * cos + w * sin, w * cos - u * sin, t[2 * quarter:]], axis=0)

    def by_dev(t):
        return t.astype(BF16).reshape(t.shape[0] // seq, seq, head_dim)

    def attend_back(t, i):
        limit = (t + 1) * tile
        sl = slice(t * tile, limit)
        devs = slice(t * CORES, (t + 1) * CORES)

        def heads(first, count):
            each = range(count)
            q = jnp.concatenate([q_ref[devs, :, block(first + j, head_dim)].reshape(tile, head_dim) for j in each], axis=0)
            da = jnp.concatenate([da_ref[sl, block(first + j, head_dim)] for j in each], axis=0)
            k, v = k_all(limit // seq), v_all(limit // seq)
            row = lax.broadcasted_iota(jnp.int32, (tile, count * tile), 0)
            col = lax.broadcasted_iota(jnp.int32, (tile, count * tile), 1)
            p = soft(dot_nt(k, q), row <= lax.rem(col, tile))
            p_low = p.astype(BF16)
            mixed = dot(vt_ref[:, :limit], p_low).astype(BF16)
            dp = dot_nt(v, da)
            row_dot = jnp.sum(p * dp, axis=0, keepdims=True)
            ds = (p * (dp - row_dot) * scale).astype(BF16)
            dv_ref[:limit, :] += dot(p_low, da)
            dk_ref[:limit, :] += dot(ds, q)
            back = dot(kt_ref[:, :limit], ds)
            for j in each:
                part = slice(j * tile, (j + 1) * tile)
                at_ref[block(first + j, head_dim), sl] = mixed[:, part]
                g_ref[devs, :, block(first + j, head_dim)] = by_dev(rotate_back(back[:, part], cost_ref[:, sl], sint_ref[:, sl]).T)

        @pl.loop(0, group // 2)
        def _(j):
            heads(2 * j, 2)

        @pl.when(i == chips - 2)
        def _():
            with scope('dy_far'):
                dys.share_far()

        heads(group - 1, 1)

    def middle(wo_vm, dyk):
        wo_in = pltpu.make_async_copy(wo_ref.at[block(at.chip, n_rows)], wo_vm, mix_sem.at[2])
        wo_in.start()
        all_came(spot_ref.at[head(n_dev - 1)], p_rsem.at[0], at.partner)
        for d in range(n_dev):
            angle = freq * spot_ref[d, pl.ds(core, 1), :].astype(F32)
            cost_ref[:, d * seq:(d + 1) * seq] = jnp.cos(angle)
            sint_ref[:, d * seq:(d + 1) * seq] = jnp.sin(angle)
        with scope('q_wait'):
            all_came(q_ref.at[head(n_dev - 1)], q_rsem.at[0], at.partner)
            all_sent(block_total, q_ssem, at.partner)
            all_sent(far_ref.at[:, head(n_dev - 1), :, head(kv_cols)], kv_ssem, at.partner)
            all_sent(spot_ref.at[head(n_dev - 1)], p_ssem, at.partner)
        kt_ref[...] = k_all(n_dev).T
        vt_ref[...] = v_all(n_dev).T
        dk_ref[...] = jnp.zeros_like(dk_ref)
        dv_ref[...] = jnp.zeros_like(dv_ref)
        dys.own_across.wait_recv()

        def fetch(i, slot):
            return pltpu.make_async_copy(dy_all.at[block(chip_at(i), CORES), core], dyk.at[slot], mix_sem.at[slot])

        with scope('wo_wait'):
            fetch(0, 0).start()
            wo_in.wait()

        @pl.loop(0, chips)
        def _(i):
            slot = lax.rem(i, 2)

            @pl.when((i == 1) & (at.chip < chips - 1))
            def _():
                block_out()

            @pl.when(i == 1)
            def _():
                with scope('dy_wait'):
                    dys.share_second()
                    all_came(dy_all.at[head(2)], dy_rsem.at[7], at.partner)
                fetch(i, slot).start()

            @pl.when(i == chips - 1)
            def _():
                with scope('dy_far2'):
                    all_came(dy_all.at[0], dy_rsem.at[8], at.partner)
                fetch(i, slot).start()
                with scope('h_pass'):
                    hcols.pass_on()

            fetch(i, slot).wait()

            @pl.when((i > 0) & (i < chips - 2))
            def _():
                fetch(i + 1, 1 - slot).start()

            chip = chip_at(i)
            with scope('da'):
                da_ref[block(chip, tile), :] = dot_nt(dyk[slot].reshape(tile, width), wo_vm[...]).astype(BF16)
            with scope('attend_back'):
                for t in range(chips):
                    @pl.when(chip == t)
                    def _(t=t):
                        attend_back(t, i)

    pl.run_scoped(middle, pltpu.VMEM((n_rows, width), BF16), pltpu.VMEM((2, CORES, seq, width), BF16))
    all_sent(dy_all.at[head(n_dev - 1)], dy_ssem, at.partner)
    heads_across.start()
    g_ref[:, :, n_rows:n_rows + head_dim] = by_dev(rotate_back(dk_ref[...].T, cost_ref[...], sint_ref[...]).T)
    g_ref[:, :, n_rows + head_dim:] = by_dev(dv_ref[...])

    def span_of(q):
        return block(q, CORES)

    turn = [[at.ring(q) for q in (2, 1, 3, 0)], [at.ring(q) for q in (3, 0, 1, 2)]]
    direct = [[send(g_ref.at[span_of(turn[i][q])], g_all.at[me, span_of(turn[i][q])], kv_ssem, kv_rsem.at[i * chips + q], at.dev(steps[i], core)) for q in range(chips)] for i in PAIR]
    came = [[at.ring(q) for q in (1, 0, 2, 3)], [at.ring(q) for q in (0, 1, 2, 3)]]
    n_heads = group + 2
    late_heads = [range(n_heads), range(n_heads // 2 + 1), range(n_heads // 2 + 1, n_heads)]

    def columns(heads):
        return pl.ds(heads[0] * head_dim, len(heads) * head_dim)

    def late(ref, quarters):
        own = [ref.at[pl.ds(quarters[1] * CORES + min(c, 1), 1), :, columns(heads)] for c, heads in enumerate(late_heads)]
        return [ref.at[span_of(quarters[0])]] + own

    onward = [[send(src, dst, q_ssem, q_rsem.at[4 * i + q], at.dev(steps[i], core)) for q, (src, dst) in enumerate(zip(late(g_all.at[origin[i]], came[i]), late(far_ref.at[core], came[i])))] for i in PAIR]
    ends = [[at.ring(q) for q in (0, 3)], [at.ring(q) for q in (1, 2)]]
    g_across = send(g_ref, g_all.at[me], x_ssem, dy_rsem.at[0], at.partner)
    near_across = [[send(g_all.at[origin[i], span_of(came[i][q])], g_all.at[origin[i], span_of(came[i][q])], x_ssem, dy_rsem.at[1 + q // 2], at.partner) for q in range(chips)] for i in PAIR]
    end_across = [[send(ref, ref, x_ssem, dy_rsem.at[3 + (q or 4 * i)], at.partner) for q, ref in enumerate(late(far_ref.at[core], ends[i]))] for i in PAIR]
    for q in range(chips):
        for i in PAIR:
            direct[i][q].start()
    g_across.start()
    g_keep = pltpu.make_async_copy(g_ref, g_all.at[me], loc_sem.at[0])
    g_keep.start()
    at2_ref[:, block(core, n_seq)] = at_ref[block(core, half), :]

    @pl.when(at.chip == chips - 1)
    def _():
        block_out()

    dy_back = [pltpu.make_async_copy(dy_ref.at[b], h_ref.at[pl.ds(b * seq, seq)], loc_sem.at[2 + b]) for b in range(n_batch)]
    for copy in dy_back:
        copy.start()

    def wo_rows(dy_vm, sem):
        def dy_tile(s, slot):
            return [pltpu.make_async_copy(dy_all.at[:, :, :, block(s, COL_TILE)], dy_vm.at[slot], sem.at[slot])]

        def wo_tile(s, slot):
            pieces = [dy_vm[slot, d, b] for b in range(n_batch) for d in range(n_dev)]
            dwo_ref[:, block(s, COL_TILE)] = dot(at2_ref[...], jnp.concatenate(pieces, axis=0))

        ring = Ring(width // COL_TILE, dy_vm.shape[0], dy_tile)
        ring.prime()
        with scope('heads_wait'):
            heads_across.wait_recv()
        with scope('grad_wo'):
            ring.run(wo_tile)

    pl.run_scoped(wo_rows, pltpu.VMEM((4, n_dev, n_batch, seq, COL_TILE), BF16), pltpu.SemaphoreType.DMA((4,)))

    with scope('h_wait'):
        all_came(ht_all.at[head(n_dev - 1)], h_rsem.at[0], at.partner)
        all_sent(block_total, h_ssem, at.partner)
    h_keep.wait()
    lhs_in = [pltpu.make_async_copy(ht_all.at[d, :, pl.ds(b * seq, seq)], at2_ref.at[:, pl.ds((b * n_dev + d) * seq, seq)], lhs_sem.at[0]) for d in range(n_dev) for b in range(n_batch)]
    for copy in lhs_in:
        copy.start()
    with jax.named_scope('own_wait'):
        pltpu.make_async_copy(at2_ref, at2_ref, lhs_sem.at[0]).wait()
        g_keep.wait()
        g_across.wait_recv()
    pair_across = send(pair_ref.at[core], pair_ref.at[core], p_ssem, p_rsem.at[0], at.partner)
    rows_out = [send(row_ref.at[at.chip], row_ref.at[at.chip], p_ssem, p_rsem.at[1], at.dev(step, core)) for step in (1, -1, 2)]
    total_across = send(total_ref.at[core], total_ref.at[core], p_ssem, p_rsem.at[2], at.partner)

    def weight_grads(wq_vm, wkv_vm, acc_ref, hat_ref, inv_ref, job_ref, mine_ref):
        n_slots = wq_vm.shape[0]
        chunk = wq_vm.shape[2]
        n_chunks = width // chunk
        total = n_chunks * chips

        def weights(s):
            slot = lax.rem(s, n_slots)
            chip = chip_at(lax.div(s, n_chunks))
            rows = block(lax.rem(s, n_chunks), chunk)
            return [
                pltpu.make_async_copy(wq_ref.at[block(chip, group), rows], wq_vm.at[slot], w_sem.at[slot, 0]),
                pltpu.make_async_copy(wkv_all.at[chip, rows], wkv_vm.at[slot], w_sem.at[slot, 1]),
            ]

        for s in range(n_slots):
            for copy in weights(s):
                copy.start()

        def grow(i, read):
            @pl.loop(0, n_chunks)
            def _(n):
                s = i * n_chunks + n
                slot = lax.rem(s, n_slots)
                for copy in weights(s):
                    copy.wait()
                rows = jnp.concatenate([read(b) for b in range(n_batch)], axis=0)
                part = dot_nt(rows, jnp.concatenate([wq_vm[slot, j] for j in range(group)] + [wkv_vm[slot]], axis=1))
                sl = block(n, chunk)

                @pl.when(i == 0)
                def _():
                    acc_ref[:, sl] = part

                @pl.when(i > 0)
                def _():
                    acc_ref[:, sl] += part

                @pl.when(s + n_slots < total)
                def _():
                    for copy in weights(s + n_slots):
                        copy.start()

        def mine_in(i):
            return [pltpu.make_async_copy(g_all.at[chip_at(i) * CORES + b, me], mine_ref.at[lax.rem(i, 2), b], job_sem.at[2 + lax.rem(i, 2)]) for b in range(n_batch)]

        def grow_near(i):
            here = mine_ref.at[lax.rem(i, 2)]
            pltpu.make_async_copy(here, here, job_sem.at[2 + lax.rem(i, 2)]).wait()
            grow(i, lambda b: mine_ref[lax.rem(i, 2), b])

        def job_in(chip, quarters, slot):
            return [pltpu.make_async_copy(g_all.at[chip * CORES + b, span_of(q)], job_ref.at[slot, b, n], job_sem.at[slot]) for b in range(n_batch) for n, q in enumerate(quarters)]

        def job(chip, pieces, read, add, heads=range(n_heads)):
            lhs = [at2_ref[:, pl.ds(pl.multiple_of(b * n_seq + d * seq, seq), seq)] for b in range(n_batch) for d in pieces]
            rhs = [read(b, n) for b in range(n_batch) for n in range(len(pieces))]
            y = dot(jnp.concatenate(lhs, axis=1), jnp.concatenate(rhs, axis=0))
            for n, j in enumerate(heads):
                v = y[:, n * head_dim:(n + 1) * head_dim]
                if j < group:
                    dwq_ref[chip * group + j] = dwq_ref[chip * group + j] + v if add else v
                else:
                    ref, rows = (dwk_ref, dwv_ref)[j - group], pl.ds(chip, half, stride=chips)
                    ref[rows, :] = ref[rows, :] + v if add else v

        def devs_of(quarters):
            return [q * CORES + c for q in quarters for c in range(CORES)]

        def near_pair(quarters, add):
            for slot, step in enumerate(steps):
                for copy in job_in(at.ring(step), quarters, slot):
                    copy.start()

            @pl.loop(0, 2)
            def _(slot):
                chip = at.ring(1 - 2 * slot)
                pltpu.make_async_copy(job_ref.at[slot], job_ref.at[slot], job_sem.at[slot]).wait()
                job(chip, devs_of(quarters), lambda b, n: job_ref[slot, b, n // CORES, n % CORES], add)

        halves = [[at.ring(q) for q in half_of] for half_of in ((0, 1), (2, 3))]
        for slot in PAIR:
            for copy in job_in(at.chip, [at.ring(2 * slot), at.ring(2 * slot + 1)], slot):
                copy.start()
        for copy in mine_in(0):
            copy.start()
        with jax.named_scope('own_job'):
            for slot in PAIR:
                quarters = [at.ring(2 * slot), at.ring(2 * slot + 1)]
                pltpu.make_async_copy(job_ref.at[slot], job_ref.at[slot], job_sem.at[slot]).wait()
                job(at.chip, devs_of(quarters), lambda b, n: job_ref[slot, b, n // CORES, n % CORES], slot == 1)

        with jax.named_scope('own_dh'):
            grow_near(0)

        with jax.named_scope('d01_wait'):
            for q in PAIR:
                for i in PAIR:
                    direct[i][q].wait_recv()
                for i in PAIR:
                    for copy in onward[i][:1] if q == 0 else onward[i][1:]:
                        copy.start()
                    near_across[i][q].start()
        with scope('d01_across'):
            all_came(g_all.at[0], dy_rsem.at[1], at.partner)
        for i in (1, 2):
            for copy in mine_in(i):
                copy.start()
        with scope('near_dh'):
            @pl.loop(1, chips - 1)
            def _(i):
                grow_near(i)

        with jax.named_scope('near_a'):
            near_pair(halves[0], False)
        with scope('d2_wait'):
            for i in PAIR:
                direct[i][2].wait_recv()
                near_across[i][2].start()
        with jax.named_scope('hat'):
            @pl.loop(0, n_tok // (2 * ROWS))
            def _(step):
                for i in PAIR:
                    sl = block(2 * step + i, ROWS)
                    hat, inv = layer_norm(dx_ref[sl, :].astype(F32))
                    hat_ref[sl, :] = hat
                    inv_ref[sl, :] = jnp.broadcast_to(inv, (ROWS, 128))

        with scope('d3_wait'):
            for i in PAIR:
                direct[i][3].wait_recv()
                near_across[i][3].start()
        with scope('d23_across'):
            all_came(g_all.at[0], dy_rsem.at[2], at.partner)
        with jax.named_scope('near_b'):
            near_pair(halves[1], True)
        far_chip = at.ring(2)
        end_total = [g_all.at[0, head(CORES), :, columns(heads)] for heads in late_heads]
        with jax.named_scope('far0_wait'):
            for i in PAIR:
                onward[i][0].wait_recv()
                end_across[i][0].start()
        with scope('far0_across'):
            all_came(end_total[0], dy_rsem.at[3], at.partner)
        with jax.named_scope('far_dh'):
            grow(chips - 1, lambda b: far_ref[b, me])
        for copy in dy_back:
            copy.wait()
        part_ref[...] = jnp.zeros_like(part_ref)

        with jax.named_scope('norm_back'):
            @pl.loop(0, n_tok // (2 * ROWS))
            def _(step):
                for i in PAIR:
                    sl = block(2 * step + i, ROWS)
                    hat, inv = hat_ref[sl, :], inv_ref[sl, 0:1]
                    dh = acc_ref[sl, :]
                    dg = dh * hat
                    gh = dh * gain
                    one = jnp.mean(gh, axis=-1, keepdims=True)
                    two = jnp.mean(dg * gain, axis=-1, keepdims=True)
                    dx_ref[sl, :] = (h_ref[sl, :].astype(F32) + inv * (gh - one - hat * two)).astype(BF16)
                    part_ref[0] += dg[0:8] + dg[8:16]
                    part_ref[1] += dh[0:8] + dh[8:16]

        for i in PAIR:
            pair_ref[core, i:i + 1, :] = jnp.sum(part_ref[i], axis=0, keepdims=True)
        pair_across.start()

        def hand_on(c):
            with scope('far1_wait'):
                for i in PAIR:
                    onward[i][1 + c].wait_recv()
                    end_across[i][1 + c].start()

        def far_rows(devs, add, heads=range(n_heads)):
            job(far_chip, devs, lambda b, n: far_ref[b, devs[n], :, heads[0] * head_dim:(heads[-1] + 1) * head_dim], add, heads)

        def last_half(c):
            with scope('far1_across'):
                all_came(end_total[c], dy_rsem.at[4 + c], at.partner)
            with scope('far_b'):
                far_rows([ends[i][1] * CORES + min(c, 1) for i in PAIR], True, late_heads[c])

        hand_on(0)
        with scope('far_a'):
            all_came(end_total[0], dy_rsem.at[7], at.partner)
            far_rows(devs_of([ends[0][0], ends[1][0]]), False)
        with scope('rows'):
            all_came(pair_ref.at[0], p_rsem.at[0], at.partner)
            all_sent(pair_ref.at[0], p_ssem, at.partner)
            row_ref[at.chip] = pair_ref[0, pl.ds(core, 1), :] + pair_ref[1, pl.ds(core, 1), :]
            for copy in rows_out:
                copy.start()
        hand_on(1)
        last_half(0)
        hand_on(2)
        last_half(1)
        with scope('total'):
            all_came(row_ref.at[head(chips - 1)], p_rsem.at[1], at.partner)
            all_sent(row_ref.at[head(chips - 1)], p_ssem, at.partner)
            total = row_ref[0]
            for n in range(1, chips):
                total = total + row_ref[n]
            total_ref[core] = total
            total_across.start()
        last_half(2)

    pl.run_scoped(
        weight_grads,
        pltpu.VMEM((W_SLOTS, group, W_ROWS, head_dim), BF16), pltpu.VMEM((W_SLOTS, W_ROWS, 2 * head_dim), BF16), pltpu.VMEM((n_tok, width), F32),
        pltpu.VMEM((n_tok, width), F32), pltpu.VMEM((n_tok, 128), F32), pltpu.VMEM((2, n_batch, 2, CORES, seq, cols), BF16), pltpu.VMEM((2, n_batch, seq, cols), BF16),
    )

    with scope('sums'):
        all_came(total_ref.at[0], p_rsem.at[2], at.partner)
        dgain_ref[...] = total_ref[0].reshape(width)
        dbias_ref[...] = total_ref[1].reshape(width)
    with scope('done'):
        heads_across.wait_send()
        all_sent(far_ref, kv_ssem, at.partner)
        all_sent(g_ref, q_ssem, at.partner)
        all_sent(g_all.at[head(chips)], x_ssem, at.partner)
        all_sent(total_ref.at[0], p_ssem, at.partner)


def whole_block(n_dev, x, gain, bias, positions, freq, dy, wq, wk, wv, wo):
    n_batch, seq, width = dy.shape
    n_tok = n_batch * seq
    head_dim = wq.shape[2]
    chips = n_dev // CORES
    group = wq.shape[0] // chips
    cols = (group + 2) * head_dim
    n_rows = group * head_dim
    half = n_rows // CORES
    n_seq = n_dev * seq
    quarter = head_dim // 4
    dma = pltpu.SemaphoreType.DMA
    vm = pltpu.VMEM
    shapes = [((n_tok, width), BF16)] * 2 + [((chips * group, half, head_dim), F32)] + [((chips * half, head_dim), F32)] * 2 + [((half, width), F32), ((width,), F32), ((width,), F32)]
    held = [((n_dev, n_batch, seq, width), BF16), ((n_dev, half, n_tok), BF16), ((n_dev, n_dev, seq, cols), BF16), ((chips, width, 2 * head_dim), BF16)]
    return pl.pallas_call(
        functools.partial(block_body, n_dev, group),
        out_shape=tuple(pltpu.VMEM(*t) for t in shapes) + tuple(sds(*t) for t in held),
        in_specs=[HBM] * 10,
        out_specs=(VM,) * len(shapes) + (HBM,) * len(held),
        scratch_shapes=[
            vm((n_tok, width), BF16), vm((width, n_tok), BF16), vm((n_dev, seq, cols), BF16), vm((n_dev, seq, n_rows), BF16),
            vm((n_rows, n_seq), BF16), vm((half, n_batch * n_seq), BF16), vm((n_seq, n_rows), BF16),
            vm((head_dim, n_seq), BF16), vm((head_dim, n_seq), BF16), vm((n_seq, head_dim), F32), vm((n_seq, head_dim), F32),
            vm((quarter, n_seq), F32), vm((quarter, n_seq), F32), vm((3, n_tok, head_dim), F32), vm((n_dev, n_batch, seq), jnp.int32), vm((width,), F32), vm((width,), F32), vm((quarter, 1), F32),
            vm((2, seq, n_rows), BF16), vm((2, half, n_tok), BF16),
            vm((n_batch, n_dev, seq, cols), BF16), vm((2, 8, width), F32), vm((CORES, 2, width), F32), vm((chips, 1, width), F32), vm((CORES, 1, width), F32),
            dma((6,)), dma((9,)), dma((8,)), dma((8,)), dma((3,)), dma((3,)), dma((2,)),
            dma((6,)), dma((3,)), dma((1,)), dma((W_SLOTS, 2)), dma((4,)),
        ],
        compiler_params=pltpu.CompilerParams(collective_id=0, has_side_effects=True, vmem_limit_bytes=VMEM_LIMIT),
        cost_estimate=pl.CostEstimate(flops=10 ** 11, bytes_accessed=10 ** 8, transcendentals=0),
        name='block',
    )(gain, bias, positions, freq, x.reshape(n_tok, width), dy, wq, wk, wv, wo)[:len(shapes)]


def settle_body(n, *refs):
    sem = refs[2 * n]
    copies = []
    for src, dst in zip(refs[:n], refs[n:2 * n]):
        pieces = SETTLE if len(src.shape) > 1 else 1
        size = src.shape[0] // pieces
        copies += [pltpu.make_async_copy(src.at[pl.ds(p * size, size)], dst.at[pl.ds(p * size, size)], sem) for p in range(pieces)]
    for copy in copies:
        copy.start()
    for copy in copies:
        copy.wait()


def settle(arrays):
    n = len(arrays)
    return pl.pallas_call(
        functools.partial(settle_body, n),
        out_shape=tuple(sds(t.shape, t.dtype) for t in arrays),
        in_specs=[ANY] * n,
        out_specs=(HBM,) * n,
        scratch_shapes=[pltpu.SemaphoreType.DMA],
        compiler_params=pltpu.CompilerParams(vmem_limit_bytes=1024 * 1024),
        name='settle',
    )(*arrays)


def solution(mesh):
    n_dev = mesh.shape['cp']

    def device_step(x_act, d_out, positions, ln_gain, ln_bias, w_query, w_key, w_value, w_out):
        n_batch, seq, width = x_act.shape
        q_heads, (kv_heads, head_dim) = w_query.shape[1], w_key.shape[1:]
        group = q_heads // kv_heads
        quarter = head_dim // 4
        assert n_batch == CORES and n_dev // CORES == kv_heads == 4 and q_heads * head_dim == width

        freq = np.exp(np.arange(quarter) * (-2.0 * math.log(ROPE_BASE) / (head_dim // 2))).astype(np.float32).reshape(quarter, 1)
        by_head = lambda t: jnp.transpose(t, (1, 0, 2))
        by_row = lambda t: t.reshape(width * kv_heads, head_dim)
        wq = by_head(w_query)

        results = whole_block(n_dev, x_act, ln_gain, ln_bias, positions, jnp.asarray(freq), d_out, wq, by_row(w_key), by_row(w_value), w_out)
        out, dx, dwq, dwk, dwv, dwo, dgain, dbias = settle(results)
        kv_rows = lambda t: t.reshape(width // n_dev, kv_heads, head_dim)
        return (out.reshape(x_act.shape), dx.reshape(x_act.shape), by_head(dwq), kv_rows(dwk), kv_rows(dwv), dwo, dgain, dbias)

    return jax.shard_map(device_step, mesh=mesh, in_specs=(P('dp', 'cp', None), P('dp', 'cp', None), P('dp', 'cp'), P(None), P(None), P(None, None, None), P(None, None, None), P(None, None, None), P(None, None)), out_specs=(P('dp', 'cp', None), P('dp', 'cp', None), P(('dp', 'cp'), None, None), P(('dp', 'cp'), None, None), P(('dp', 'cp'), None, None), P(('dp', 'cp'), None), P('dp'), P('dp')), check_vma=False)
```

```python
import functools
import math
import jax
import jax.numpy as jnp
import numpy as np
from jax import lax
from jax.experimental import pallas as pl
from jax.experimental.pallas import tpu as pltpu
from jax.sharding import PartitionSpec as P

EPS = 1e-5
ROPE_BASE = 10000.0
BF16 = jnp.bfloat16
F32 = jnp.float32
VMEM_LIMIT = 46 * 1024 * 1024
NT = (((1,), (1,)), ((), ()))
ANY = pl.BlockSpec(memory_space=pl.ANY)
VM = pl.BlockSpec(memory_space=pltpu.VMEM)
HBM = pl.BlockSpec(memory_space=pltpu.HBM)
CORES = 2
PAIR = range(2)
STEPS = (1, -1)
COL_TILE = 512
OUT_TILE = 256
ROWS = 16
W_SLOTS = 4
W_ROWS = 512
SETTLE = 4


def dot(a, b):
    return jnp.dot(a, b, preferred_element_type=F32)


def dot_nt(a, b):
    return lax.dot_general(a, b, NT, preferred_element_type=F32)


def sds(shape, dtype):
    return jax.ShapeDtypeStruct(shape, dtype)


def head(size):
    return pl.ds(0, size)


def block(i, size):
    return pl.ds(pl.multiple_of(i * size, size), size)


class Place:
    def __init__(self, n_dev):
        self.n_dev = n_dev
        self.chips = n_dev // CORES
        self.me = lax.axis_index('cp')
        self.chip = self.me // CORES
        self.core = self.me % CORES
        self.partner = self.chip * CORES + 1 - self.core

    def ring(self, step):
        return lax.rem(self.chip + self.chips + step, self.chips)

    def dev(self, step, core):
        return self.ring(step) * CORES + core

    def peers(self, far):
        near = [self.partner] + [self.dev(s, c) for s in STEPS for c in range(CORES)]
        return near + ([self.dev(2, c) for c in range(CORES)] if far else [])


def send(src, dst, ssem, rsem, to):
    return pltpu.make_async_remote_copy(src_ref=src, dst_ref=dst, send_sem=ssem, recv_sem=rsem, device_id={'cp': to}, device_id_type=pl.DeviceIdType.MESH)


def all_sent(total, ssem, to):
    send(total, total, ssem, ssem, to).wait_send()


def all_came(total, rsem, to):
    send(total, total, rsem, rsem, to).wait_recv()


def meet(peers):
    barrier = pltpu.get_barrier_semaphore()
    for peer in peers:
        pl.semaphore_signal(barrier, inc=1, device_id={'cp': peer}, device_id_type=pl.DeviceIdType.MESH)
    pl.semaphore_wait(barrier, len(peers))


class Ring:
    def __init__(self, n, slots, copies):
        self.n, self.slots, self.copies = n, slots, copies

    def prime(self):
        for s in range(self.slots):
            for copy in self.copies(s, s):
                copy.start()

    def run(self, use):
        @pl.loop(0, self.n)
        def _(s):
            slot = lax.rem(s, self.slots)
            for copy in self.copies(s, slot):
                copy.wait()
            use(s, slot)

            @pl.when(s + self.slots < self.n)
            def _():
                for copy in self.copies(s + self.slots, slot):
                    copy.start()


class Gather:
    def __init__(self, at, own, piece, both, ssem, rsem, across):
        steps = STEPS
        origin = [at.dev(-1, at.core), at.dev(1, at.core)]
        far = at.dev(2, at.core)
        link = lambda i, src, dst, to: send(src, dst, ssem, rsem.at[i], to)
        self.first = [link(b, own(b), piece(at.me, b), at.dev(steps[b], at.core)) for b in PAIR]
        self.second = [link(2 + b, own(1 - b), piece(at.me, 1 - b), at.dev(steps[b], at.core)) for b in PAIR]
        self.again = [link(4 + b, piece(origin[b], b), piece(origin[b], b), at.dev(steps[b], at.core)) for b in PAIR]
        self.own_across = link(across[0], both(None), both(at.me), at.partner)
        self.first_across = [link(across[1], piece(origin[b], b), piece(origin[b], b), at.partner) for b in PAIR]
        self.second_across = [link(across[1], piece(origin[b], 1 - b), piece(origin[b], 1 - b), at.partner) for b in PAIR]
        self.far_across = [link(across[2], piece(far, b), piece(far, b), at.partner) for b in PAIR]

    def start_first(self):
        for copy in self.first + [self.own_across]:
            copy.start()

    def start_second(self):
        for copy in self.second:
            copy.start()

    def pass_on(self):
        for copy, again, across in zip(self.first, self.again, self.first_across):
            copy.wait_recv()
            again.start()
            across.start()

    def share_second(self):
        for copy, across in zip(self.second, self.second_across):
            copy.wait_recv()
            across.start()

    def share_far(self):
        for copy, across in zip(self.again, self.far_across):
            copy.wait_recv()
            across.start()


class Exchange:
    def __init__(self, at, src, dst, relay, ssem, rsem):
        near = [(0, 1 - at.core)] + [(s, c) for s in STEPS for c in range(CORES)]
        self.near = [send(src(at.dev(s, c)), dst(at.me), ssem, rsem.at[0], at.dev(s, c)) for s, c in near]
        self.far = [send(src(at.dev(2, i)), relay.at[i], ssem, rsem.at[1 + i], at.dev(step, at.core)) for i, step in enumerate(STEPS)]
        self.on = [send(relay.at[i], dst(at.dev(-step, at.core)), ssem, rsem.at[0], at.dev(step, i)) for i, step in enumerate(STEPS)]

    def start(self):
        for copy in self.far + self.near:
            copy.start()

    def pass_on(self):
        for far, on in zip(self.far, self.on):
            far.wait_recv()
            on.start()


def layer_norm(x):
    cen = x - jnp.mean(x, axis=-1, keepdims=True)
    inv = lax.rsqrt(jnp.mean(cen * cen, axis=-1, keepdims=True) + EPS)
    return cen * inv, inv


def block_body(n_dev, group, gain_hbm, bias_hbm, pos_hbm, freq_hbm, x_hbm, dy_ref, wq_ref, wk_ref, wv_ref, wo_ref,
               out_ref, dx_ref, dwq_ref, dwk_ref, dwv_ref, dwo_ref, dgain_ref, dbias_ref, dy_all, ht_all, g_all, wkv_all,
               h_ref, ht_ref, g_ref, q_ref, at_ref, at2_ref, da_ref, kt_ref, vt_ref, dk_ref, dv_ref,
               cost_ref, sint_ref, tab_ref, spot_ref, gain_ref, bias_ref, freq_ref, relay_q, relay_h, far_ref, part_ref, pair_ref, row_ref,
               s_sem, dy_rsem, kv_rsem, q_rsem, h_rsem, p_rsem, t_sem, loc_sem, mix_sem, lhs_sem, w_sem, job_sem):
    at = Place(n_dev)
    n_batch, seq, width = dy_ref.shape
    n_tok = n_batch * seq
    head_dim = wq_ref.shape[2]
    cols = (group + 2) * head_dim
    n_rows = group * head_dim
    half = n_rows // CORES
    n_seq = n_dev * seq
    quarter = head_dim // 4
    scale = head_dim ** -0.5
    chips = at.chips
    tile = CORES * seq
    core, me = at.core, at.me
    steps = STEPS
    origin = [at.dev(-1, core), at.dev(1, core)]
    far_dev = at.dev(2, core)
    scope = jax.named_scope

    dy_ssem, kv_ssem, q_ssem, h_ssem, p_ssem, x_ssem = [s_sem.at[i] for i in range(6)]
    assert (n_dev + 1) * n_rows == (n_dev - 1) * cols
    block_total = far_ref.at[0, head(n_dev - 1)]

    with scope('meet'):
        meet(at.peers(True))

    kv_cols = 2 * head_dim * chips
    kv_piece = lambda d, b: far_ref.at[b, d, :, head(kv_cols)]
    kv_both = lambda d: far_ref.at[:, me if d is None else d, :, head(kv_cols)]
    dys = Gather(at, lambda b: dy_ref.at[b], lambda d, b: dy_all.at[d, b], lambda d: dy_ref if d is None else dy_all.at[d], dy_ssem, dy_rsem, (6, 7, 8))
    kvs = Gather(at, lambda b: kv_piece(me, b), kv_piece, kv_both, kv_ssem, kv_rsem, (6, 6, 6))
    q_part = head(n_rows)
    queries = Exchange(at, lambda d: g_ref.at[d, :, q_part], lambda d: q_ref.at[d], relay_q, q_ssem, q_rsem)
    hcols = Exchange(at, lambda d: ht_ref.at[block(d, half)], lambda d: ht_all.at[d], relay_h, h_ssem, h_rsem)
    heads_across = send(at_ref.at[block(1 - core, half)], at2_ref.at[:, block(core, n_seq)], t_sem.at[0], t_sem.at[1], at.partner)
    spots = [send(pos_hbm, spot_ref.at[me], p_ssem, p_rsem.at[0], peer) for peer in at.peers(True)]

    dys.start_first()
    x_in = pltpu.make_async_copy(x_hbm, dx_ref, loc_sem.at[1])
    x_in.start()
    for copy in spots:
        copy.start()
    small = [pltpu.make_async_copy(src, dst, loc_sem.at[2 + n]) for n, (src, dst) in enumerate(((gain_hbm, gain_ref), (bias_hbm, bias_ref), (freq_hbm, freq_ref), (pos_hbm, spot_ref.at[me])))]
    for copy in small:
        copy.start()
    for copy in small:
        copy.wait()

    freq = freq_ref[...]
    for b in range(n_batch):
        angle = freq * spot_ref[me, b:b + 1, :].astype(F32)
        cos, sin, none = jnp.cos(angle), jnp.sin(angle), jnp.zeros((quarter, seq), F32)
        rest = jnp.zeros((head_dim - 2 * quarter, seq), F32)
        for i, rows in enumerate(([cos, cos, rest + 1.0], [-sin, none, rest], [none, sin, rest])):
            tab_ref[i, b * seq:(b + 1) * seq, :] = jnp.concatenate(rows, axis=0).T

    gain = (1.0 + gain_ref[...]).reshape(1, width)
    bias = bias_ref[...].reshape(1, width)

    def project_all(wkv_ref, raw_ref, wq_vm, raw_sem, wq_sem, stage_sem):
        pieces = [(b, i) for b in range(n_batch) for i in range(width // n_rows)]
        there = lambda n: da_ref.at[pl.ds(n * seq, seq)]
        dy_in = [pltpu.make_async_copy(dy_ref.at[b, :, pl.ds(i * n_rows, n_rows)], there(n), stage_sem.at[n]) for n, (b, i) in enumerate(pieces)]
        dy_keep = [pltpu.make_async_copy(there(n), dy_all.at[me, b, :, pl.ds(i * n_rows, n_rows)], stage_sem.at[n]) for n, (b, i) in enumerate(pieces)]
        span = 64 * chips
        batch = raw_ref.shape[2] // span
        row = lax.broadcasted_iota(jnp.int32, (span, span), 0)
        col = lax.broadcasted_iota(jnp.int32, (span, span), 1)
        pick = jnp.where(col == lax.rem(row, 64) * chips + lax.div(row, 64), 1.0, 0.0).astype(BF16)

        def raw_in(s, slot):
            return [pltpu.make_async_copy(w.at[block(s, span * batch)], raw_ref.at[slot, i], raw_sem.at[slot, i]) for i, w in enumerate((wk_ref, wv_ref))]

        def wq_in(s, slot):
            return [pltpu.make_async_copy(wq_ref.at[block(s, 2)], wq_vm.at[slot], wq_sem.at[slot])]

        def part_heads(s, slot):
            for i in range(batch):
                sl = slice(i * span, (i + 1) * span)
                rows = dot(pick, jnp.concatenate([raw_ref[slot, 0, sl, :], raw_ref[slot, 1, sl, :]], axis=1)).astype(BF16)
                for n in range(chips):
                    wkv_ref[n, block(s * batch + i, 64), :] = rows[n * 64:(n + 1) * 64]

        def turned(v):
            return v * tab_ref[0] + pltpu.roll(v, head_dim - quarter, 1) * tab_ref[1] + pltpu.roll(v, quarter, 1) * tab_ref[2]

        def project(s, slot):
            y = dot(h_ref[...], jnp.concatenate([wq_vm[slot, 0], wq_vm[slot, 1]], axis=1))
            for i in PAIR:
                head = s * 2 + i
                v = turned(y[:, i * head_dim:(i + 1) * head_dim]).astype(BF16)
                for b in range(n_batch):
                    g_ref[lax.div(head, group) * n_batch + b, :, block(lax.rem(head, group), head_dim)] = v[b * seq:(b + 1) * seq]

        kv_ring = Ring(width // (64 * batch), raw_ref.shape[0], raw_in)
        q_ring = Ring(chips * group // 2, wq_vm.shape[0], wq_in)
        kv_ring.prime()
        q_ring.prime()
        for copy in dy_in:
            copy.start()
        x_in.wait()
        with scope('norm'):
            @pl.loop(0, n_tok // (2 * ROWS))
            def _(step):
                for i in PAIR:
                    sl = block(2 * step + i, ROWS)
                    hat, _ = layer_norm(dx_ref[sl, :].astype(F32))
                    h_ref[sl, :] = (hat * gain + bias).astype(BF16)

        with scope('heads_kv'):
            kv_ring.run(part_heads)
        keep = pltpu.make_async_copy(wkv_ref, wkv_all, mix_sem.at[2])
        keep.start()
        for come, go in zip(dy_in, dy_keep):
            come.wait()
            go.start()
        with scope('project_kv'):
            @pl.loop(0, chips)
            def _(n):
                y = dot(h_ref[...], wkv_ref[n])
                v = jnp.concatenate([turned(y[:, :head_dim]), y[:, head_dim:]], axis=1).astype(BF16)
                for b in range(n_batch):
                    far_ref[b, me, :, block(n, 2 * head_dim)] = v[b * seq:(b + 1) * seq]

        kvs.start_first()
        kvs.start_second()
        with scope('project_q'):
            q_ring.run(project)
        keep.wait()
        for copy in dy_keep:
            copy.wait()

    pl.run_scoped(
        project_all,
        pltpu.VMEM((chips, width, 2 * head_dim), BF16),
        pltpu.VMEM((3, 2, 4 * 64 * chips, head_dim), BF16), pltpu.VMEM((4, 2, width, head_dim), BF16),
        pltpu.SemaphoreType.DMA((3, 2)), pltpu.SemaphoreType.DMA((4,)), pltpu.SemaphoreType.DMA((n_batch * width // n_rows,)),
    )

    with scope('kv_pass'):
        kvs.pass_on()
    queries.start()
    q_ref[me] = g_ref[me, :, q_part]
    with scope('turn_h'):
        @pl.loop(0, width // 128)
        def _(step):
            sl = block(step, 128)
            ht_ref[sl, :] = h_ref[:, sl].T

    with scope('kv_wait'):
        kvs.share_second()
        kvs.share_far()
        all_came(far_ref.at[:, head(chips), :, head(kv_cols)], kv_rsem.at[6], at.partner)

    def chip_at(i):
        return at.ring(jnp.where(i == 0, 0, jnp.where(i == 1, 1, jnp.where(i == 2, 3, 2))))

    def soft(s, seen):
        s = s * scale
        clear = s.shape[0] - seen.shape[0]
        tail = jnp.where(seen, s[clear:], -1e30)
        s = tail if clear == 0 else jnp.concatenate([s[:clear], tail], axis=0)
        e = jnp.exp(s - jnp.max(s, axis=0, keepdims=True))
        return e * (1.0 / jnp.sum(e, axis=0, keepdims=True))

    def attend(limit, clear):
        @pl.loop(0, n_batch * chips)
        def _(i):
            @pl.when(i == 1)
            def _():
                with scope('q_pass'):
                    queries.pass_on()
                dys.start_second()
                dys.pass_on()
                hcols.start()

            b, n = lax.rem(i, n_batch), lax.div(i, n_batch)
            k = far_ref[b, 0:limit // seq, :, block(2 * n, head_dim)].reshape(limit, head_dim)
            vt = far_ref[b, 0:limit // seq, :, block(2 * n + 1, head_dim)].reshape(limit, head_dim).T
            q = jnp.concatenate([g_ref[n * n_batch + b, :, block(j, head_dim)] for j in range(group)], axis=0)
            row = lax.broadcasted_iota(jnp.int32, (limit - clear, n_rows), 0)
            col = lax.broadcasted_iota(jnp.int32, (limit - clear, n_rows), 1)
            p = soft(dot_nt(k, q), row <= lax.rem(col, seq) + (me * seq - clear))
            mixed = dot(vt, p.astype(BF16)).astype(BF16)
            for j in range(group):
                h_ref[block(b, seq), block(n * group + j, head_dim)] = mixed[:, j * seq:(j + 1) * seq].T

    with scope('attend'):
        @pl.when(at.chip == chips - 1)
        def _():
            attend(chips * tile, (chips - 1) * tile)

        @pl.when(at.chip < chips - 1)
        def _():
            attend((chips - 1) * tile, 0)

    h_keep = pltpu.make_async_copy(ht_ref.at[block(me, half)], ht_all.at[me], loc_sem.at[1])
    h_keep.start()

    def block_out():
        def stream(wo_vm, sem):
            def wo_in(s, slot):
                return [pltpu.make_async_copy(wo_ref.at[:, block(s, OUT_TILE)], wo_vm.at[slot], sem.at[slot])]

            def out_tile(s, slot):
                sl = block(s, OUT_TILE)
                out_ref[:, sl] = (dx_ref[:, sl].astype(F32) + dot(h_ref[...], wo_vm[slot])).astype(BF16)

            ring = Ring(width // OUT_TILE, wo_vm.shape[0], wo_in)
            ring.prime()
            ring.run(out_tile)

        with scope('output'):
            pl.run_scoped(stream, pltpu.VMEM((4, width, OUT_TILE), BF16), pltpu.SemaphoreType.DMA((4,)))

    k_all = lambda n: far_ref[core, 0:n, :, block(2 * at.chip, head_dim)].reshape(n * seq, head_dim)
    v_all = lambda n: far_ref[core, 0:n, :, block(2 * at.chip + 1, head_dim)].reshape(n * seq, head_dim)

    def rotate_back(t, cos, sin):
        u, w = t[:quarter], t[quarter:2 * quarter]
        return jnp.concatenate([u * cos + w * sin, w * cos - u * sin, t[2 * quarter:]], axis=0)

    def by_dev(t):
        return t.astype(BF16).reshape(t.shape[0] // seq, seq, head_dim)

    def attend_back(t, i):
        limit = (t + 1) * tile
        sl = slice(t * tile, limit)
        devs = slice(t * CORES, (t + 1) * CORES)

        def heads(first, count):
            each = range(count)
            q = jnp.concatenate([q_ref[devs, :, block(first + j, head_dim)].reshape(tile, head_dim) for j in each], axis=0)
            da = jnp.concatenate([da_ref[sl, block(first + j, head_dim)] for j in each], axis=0)
            k, v = k_all(limit // seq), v_all(limit // seq)
            row = lax.broadcasted_iota(jnp.int32, (tile, count * tile), 0)
            col = lax.broadcasted_iota(jnp.int32, (tile, count * tile), 1)
            p = soft(dot_nt(k, q), row <= lax.rem(col, tile))
            p_low = p.astype(BF16)
            mixed = dot(vt_ref[:, :limit], p_low).astype(BF16)
            dp = dot_nt(v, da)
            row_dot = jnp.sum(p * dp, axis=0, keepdims=True)
            ds = (p * (dp - row_dot) * scale).astype(BF16)
            dv_ref[:limit, :] += dot(p_low, da)
            dk_ref[:limit, :] += dot(ds, q)
            back = dot(kt_ref[:, :limit], ds)
            for j in each:
                part = slice(j * tile, (j + 1) * tile)
                at_ref[block(first + j, head_dim), sl] = mixed[:, part]
                g_ref[devs, :, block(first + j, head_dim)] = by_dev(rotate_back(back[:, part], cost_ref[:, sl], sint_ref[:, sl]).T)

        @pl.loop(0, group // 2)
        def _(j):
            heads(2 * j, 2)

        @pl.when(i == chips - 2)
        def _():
            with scope('dy_far'):
                dys.share_far()

        heads(group - 1, 1)

    def middle(wo_vm, dyk):
        wo_in = pltpu.make_async_copy(wo_ref.at[block(at.chip, n_rows)], wo_vm, mix_sem.at[2])
        wo_in.start()
        all_came(spot_ref.at[head(n_dev - 1)], p_rsem.at[0], at.partner)
        for d in range(n_dev):
            angle = freq * spot_ref[d, pl.ds(core, 1), :].astype(F32)
            cost_ref[:, d * seq:(d + 1) * seq] = jnp.cos(angle)
            sint_ref[:, d * seq:(d + 1) * seq] = jnp.sin(angle)
        with scope('q_wait'):
            all_came(q_ref.at[head(n_dev - 1)], q_rsem.at[0], at.partner)
            all_sent(block_total, q_ssem, at.partner)
            all_sent(far_ref.at[:, head(n_dev - 1), :, head(kv_cols)], kv_ssem, at.partner)
            all_sent(spot_ref.at[head(n_dev - 1)], p_ssem, at.partner)
        kt_ref[...] = k_all(n_dev).T
        vt_ref[...] = v_all(n_dev).T
        dk_ref[...] = jnp.zeros_like(dk_ref)
        dv_ref[...] = jnp.zeros_like(dv_ref)
        dys.own_across.wait_recv()

        def fetch(i, slot):
            return pltpu.make_async_copy(dy_all.at[block(chip_at(i), CORES), core], dyk.at[slot], mix_sem.at[slot])

        with scope('wo_wait'):
            fetch(0, 0).start()
            wo_in.wait()

        @pl.loop(0, chips)
        def _(i):
            slot = lax.rem(i, 2)

            @pl.when((i == 1) & (at.chip < chips - 1))
            def _():
                block_out()

            @pl.when(i == 1)
            def _():
                with scope('dy_wait'):
                    dys.share_second()
                    all_came(dy_all.at[head(2)], dy_rsem.at[7], at.partner)
                fetch(i, slot).start()

            @pl.when(i == chips - 1)
            def _():
                with scope('dy_far2'):
                    all_came(dy_all.at[0], dy_rsem.at[8], at.partner)
                fetch(i, slot).start()
                with scope('h_pass'):
                    hcols.pass_on()

            fetch(i, slot).wait()

            @pl.when((i > 0) & (i < chips - 2))
            def _():
                fetch(i + 1, 1 - slot).start()

            chip = chip_at(i)
            with scope('da'):
                da_ref[block(chip, tile), :] = dot_nt(dyk[slot].reshape(tile, width), wo_vm[...]).astype(BF16)
            with scope('attend_back'):
                for t in range(chips):
                    @pl.when(chip == t)
                    def _(t=t):
                        attend_back(t, i)

    pl.run_scoped(middle, pltpu.VMEM((n_rows, width), BF16), pltpu.VMEM((2, CORES, seq, width), BF16))
    all_sent(dy_all.at[head(n_dev - 1)], dy_ssem, at.partner)
    heads_across.start()
    g_ref[:, :, n_rows:n_rows + head_dim] = by_dev(rotate_back(dk_ref[...].T, cost_ref[...], sint_ref[...]).T)
    g_ref[:, :, n_rows + head_dim:] = by_dev(dv_ref[...])

    def span_of(q):
        return block(q, CORES)

    turn = [[at.ring(q) for q in (2, 1, 3, 0)], [at.ring(q) for q in (3, 0, 1, 2)]]
    direct = [[send(g_ref.at[span_of(turn[i][q])], g_all.at[me, span_of(turn[i][q])], kv_ssem, kv_rsem.at[i * chips + q], at.dev(steps[i], core)) for q in range(chips)] for i in PAIR]
    came = [[at.ring(q) for q in (1, 0, 2, 3)], [at.ring(q) for q in (0, 1, 2, 3)]]
    n_heads = group + 2
    late_heads = [range(n_heads), range(n_heads // 2 + 1), range(n_heads // 2 + 1, n_heads)]

    def columns(heads):
        return pl.ds(heads[0] * head_dim, len(heads) * head_dim)

    def late(ref, quarters):
        own = [ref.at[pl.ds(quarters[1] * CORES + min(c, 1), 1), :, columns(heads)] for c, heads in enumerate(late_heads)]
        return [ref.at[span_of(quarters[0])]] + own

    onward = [[send(src, dst, q_ssem, q_rsem.at[4 * i + q], at.dev(steps[i], core)) for q, (src, dst) in enumerate(zip(late(g_all.at[origin[i]], came[i]), late(far_ref.at[core], came[i])))] for i in PAIR]
    ends = [[at.ring(q) for q in (0, 3)], [at.ring(q) for q in (1, 2)]]
    g_across = send(g_ref, g_all.at[me], x_ssem, dy_rsem.at[0], at.partner)
    near_across = [[send(g_all.at[origin[i], span_of(came[i][q])], g_all.at[origin[i], span_of(came[i][q])], x_ssem, dy_rsem.at[1 + q // 2], at.partner) for q in range(chips)] for i in PAIR]
    end_across = [[send(ref, ref, x_ssem, dy_rsem.at[3 + (q or 4 * i)], at.partner) for q, ref in enumerate(late(far_ref.at[core], ends[i]))] for i in PAIR]
    for q in range(chips):
        for i in PAIR:
            direct[i][q].start()
    g_across.start()
    g_keep = pltpu.make_async_copy(g_ref, g_all.at[me], loc_sem.at[0])
    g_keep.start()
    at2_ref[:, block(core, n_seq)] = at_ref[block(core, half), :]

    @pl.when(at.chip == chips - 1)
    def _():
        block_out()

    dy_back = [pltpu.make_async_copy(dy_ref.at[b], h_ref.at[pl.ds(b * seq, seq)], loc_sem.at[2 + b]) for b in range(n_batch)]
    for copy in dy_back:
        copy.start()

    def wo_rows(dy_vm, sem):
        def dy_tile(s, slot):
            return [pltpu.make_async_copy(dy_all.at[:, :, :, block(s, COL_TILE)], dy_vm.at[slot], sem.at[slot])]

        def wo_tile(s, slot):
            pieces = [dy_vm[slot, d, b] for b in range(n_batch) for d in range(n_dev)]
            dwo_ref[:, block(s, COL_TILE)] = dot(at2_ref[...], jnp.concatenate(pieces, axis=0))

        ring = Ring(width // COL_TILE, dy_vm.shape[0], dy_tile)
        ring.prime()
        with scope('heads_wait'):
            heads_across.wait_recv()
        with scope('grad_wo'):
            ring.run(wo_tile)

    pl.run_scoped(wo_rows, pltpu.VMEM((4, n_dev, n_batch, seq, COL_TILE), BF16), pltpu.SemaphoreType.DMA((4,)))

    with scope('h_wait'):
        all_came(ht_all.at[head(n_dev - 1)], h_rsem.at[0], at.partner)
        all_sent(block_total, h_ssem, at.partner)
    h_keep.wait()
    lhs_in = [pltpu.make_async_copy(ht_all.at[d, :, pl.ds(b * seq, seq)], at2_ref.at[:, pl.ds((b * n_dev + d) * seq, seq)], lhs_sem.at[0]) for d in range(n_dev) for b in range(n_batch)]
    for copy in lhs_in:
        copy.start()
    with jax.named_scope('own_wait'):
        pltpu.make_async_copy(at2_ref, at2_ref, lhs_sem.at[0]).wait()
        g_keep.wait()
        g_across.wait_recv()
    pair_across = send(pair_ref.at[core], pair_ref.at[core], p_ssem, p_rsem.at[0], at.partner)
    rows_out = [send(row_ref.at[at.chip, core], row_ref.at[at.chip, core], p_ssem, p_rsem.at[1], at.dev(step, c)) for step in (1, -1, 2) for c in range(CORES)]
    all_rows = row_ref.at[head(chips - 1)]

    def weight_grads(wq_vm, wkv_vm, acc_ref, hat_ref, inv_ref, job_ref, mine_ref):
        n_slots = wq_vm.shape[0]
        chunk = wq_vm.shape[2]
        n_chunks = width // chunk
        total = n_chunks * chips

        def weights(s):
            slot = lax.rem(s, n_slots)
            chip = chip_at(lax.div(s, n_chunks))
            rows = block(lax.rem(s, n_chunks), chunk)
            return [
                pltpu.make_async_copy(wq_ref.at[block(chip, group), rows], wq_vm.at[slot], w_sem.at[slot, 0]),
                pltpu.make_async_copy(wkv_all.at[chip, rows], wkv_vm.at[slot], w_sem.at[slot, 1]),
            ]

        for s in range(n_slots):
            for copy in weights(s):
                copy.start()

        def grow(i, read):
            @pl.loop(0, n_chunks)
            def _(n):
                s = i * n_chunks + n
                slot = lax.rem(s, n_slots)
                for copy in weights(s):
                    copy.wait()
                rows = jnp.concatenate([read(b) for b in range(n_batch)], axis=0)
                part = dot_nt(rows, jnp.concatenate([wq_vm[slot, j] for j in range(group)] + [wkv_vm[slot]], axis=1))
                sl = block(n, chunk)

                @pl.when(i == 0)
                def _():
                    acc_ref[:, sl] = part

                @pl.when(i > 0)
                def _():
                    acc_ref[:, sl] += part

                @pl.when(s + n_slots < total)
                def _():
                    for copy in weights(s + n_slots):
                        copy.start()

        def mine_in(i):
            return [pltpu.make_async_copy(g_all.at[chip_at(i) * CORES + b, me], mine_ref.at[lax.rem(i, 2), b], job_sem.at[2 + lax.rem(i, 2)]) for b in range(n_batch)]

        def grow_near(i):
            here = mine_ref.at[lax.rem(i, 2)]
            pltpu.make_async_copy(here, here, job_sem.at[2 + lax.rem(i, 2)]).wait()
            grow(i, lambda b: mine_ref[lax.rem(i, 2), b])

        def job_in(chip, quarters, slot):
            return [pltpu.make_async_copy(g_all.at[chip * CORES + b, span_of(q)], job_ref.at[slot, b, n], job_sem.at[slot]) for b in range(n_batch) for n, q in enumerate(quarters)]

        def job(chip, pieces, read, add, heads=range(n_heads)):
            lhs = [at2_ref[:, pl.ds(pl.multiple_of(b * n_seq + d * seq, seq), seq)] for b in range(n_batch) for d in pieces]
            rhs = [read(b, n) for b in range(n_batch) for n in range(len(pieces))]
            y = dot(jnp.concatenate(lhs, axis=1), jnp.concatenate(rhs, axis=0))
            for n, j in enumerate(heads):
                v = y[:, n * head_dim:(n + 1) * head_dim]
                if j < group:
                    dwq_ref[chip * group + j] = dwq_ref[chip * group + j] + v if add else v
                else:
                    ref, rows = (dwk_ref, dwv_ref)[j - group], pl.ds(chip, half, stride=chips)
                    ref[rows, :] = ref[rows, :] + v if add else v

        def devs_of(quarters):
            return [q * CORES + c for q in quarters for c in range(CORES)]

        def near_pair(quarters, add):
            for slot, step in enumerate(steps):
                for copy in job_in(at.ring(step), quarters, slot):
                    copy.start()

            @pl.loop(0, 2)
            def _(slot):
                chip = at.ring(1 - 2 * slot)
                pltpu.make_async_copy(job_ref.at[slot], job_ref.at[slot], job_sem.at[slot]).wait()
                job(chip, devs_of(quarters), lambda b, n: job_ref[slot, b, n // CORES, n % CORES], add)

        halves = [[at.ring(q) for q in half_of] for half_of in ((0, 1), (2, 3))]
        for slot in PAIR:
            for copy in job_in(at.chip, [at.ring(2 * slot), at.ring(2 * slot + 1)], slot):
                copy.start()
        for copy in mine_in(0):
            copy.start()
        with jax.named_scope('own_job'):
            for slot in PAIR:
                quarters = [at.ring(2 * slot), at.ring(2 * slot + 1)]
                pltpu.make_async_copy(job_ref.at[slot], job_ref.at[slot], job_sem.at[slot]).wait()
                job(at.chip, devs_of(quarters), lambda b, n: job_ref[slot, b, n // CORES, n % CORES], slot == 1)

        with jax.named_scope('own_dh'):
            grow_near(0)

        with jax.named_scope('d01_wait'):
            for q in PAIR:
                for i in PAIR:
                    direct[i][q].wait_recv()
                for i in PAIR:
                    for copy in onward[i][:1] if q == 0 else onward[i][1:]:
                        copy.start()
                    near_across[i][q].start()
        with scope('d01_across'):
            all_came(g_all.at[0], dy_rsem.at[1], at.partner)
        for i in (1, 2):
            for copy in mine_in(i):
                copy.start()
        with scope('near_dh'):
            @pl.loop(1, chips - 1)
            def _(i):
                grow_near(i)

        with jax.named_scope('near_a'):
            near_pair(halves[0], False)
        with scope('d2_wait'):
            for i in PAIR:
                direct[i][2].wait_recv()
                near_across[i][2].start()
        with jax.named_scope('hat'):
            @pl.loop(0, n_tok // (2 * ROWS))
            def _(step):
                for i in PAIR:
                    sl = block(2 * step + i, ROWS)
                    hat, inv = layer_norm(dx_ref[sl, :].astype(F32))
                    hat_ref[sl, :] = hat
                    inv_ref[sl, :] = jnp.broadcast_to(inv, (ROWS, 128))

        with scope('d3_wait'):
            for i in PAIR:
                direct[i][3].wait_recv()
                near_across[i][3].start()
        with scope('d23_across'):
            all_came(g_all.at[0], dy_rsem.at[2], at.partner)
        with jax.named_scope('near_b'):
            near_pair(halves[1], True)
        far_chip = at.ring(2)
        end_total = [g_all.at[0, head(CORES), :, columns(heads)] for heads in late_heads]
        with jax.named_scope('far0_wait'):
            for i in PAIR:
                onward[i][0].wait_recv()
                end_across[i][0].start()
        with scope('far0_across'):
            all_came(end_total[0], dy_rsem.at[3], at.partner)
        with jax.named_scope('far_dh'):
            grow(chips - 1, lambda b: far_ref[b, me])
        for copy in dy_back:
            copy.wait()
        part_ref[...] = jnp.zeros_like(part_ref)

        with jax.named_scope('norm_back'):
            @pl.loop(0, n_tok // (2 * ROWS))
            def _(step):
                for i in PAIR:
                    sl = block(2 * step + i, ROWS)
                    hat, inv = hat_ref[sl, :], inv_ref[sl, 0:1]
                    dh = acc_ref[sl, :]
                    dg = dh * hat
                    gh = dh * gain
                    one = jnp.mean(gh, axis=-1, keepdims=True)
                    two = jnp.mean(dg * gain, axis=-1, keepdims=True)
                    dx_ref[sl, :] = (h_ref[sl, :].astype(F32) + inv * (gh - one - hat * two)).astype(BF16)
                    part_ref[0] += dg[0:8] + dg[8:16]
                    part_ref[1] += dh[0:8] + dh[8:16]

        for i in PAIR:
            pair_ref[core, i:i + 1, :] = jnp.sum(part_ref[i], axis=0, keepdims=True)
        pair_across.start()

        def hand_on(c):
            with scope('far1_wait'):
                for i in PAIR:
                    onward[i][1 + c].wait_recv()
                    end_across[i][1 + c].start()

        def far_rows(devs, add, heads=range(n_heads)):
            job(far_chip, devs, lambda b, n: far_ref[b, devs[n], :, heads[0] * head_dim:(heads[-1] + 1) * head_dim], add, heads)

        def last_half(c):
            with scope('far1_across'):
                all_came(end_total[c], dy_rsem.at[4 + c], at.partner)
            with scope('far_b'):
                far_rows([ends[i][1] * CORES + min(c, 1) for i in PAIR], True, late_heads[c])

        hand_on(0)
        with scope('far_a'):
            all_came(end_total[0], dy_rsem.at[7], at.partner)
            far_rows(devs_of([ends[0][0], ends[1][0]]), False)
        with scope('rows'):
            all_came(pair_ref.at[0], p_rsem.at[0], at.partner)
            all_sent(pair_ref.at[0], p_ssem, at.partner)
            for i in PAIR:
                row_ref[at.chip, i] = pair_ref[0, i:i + 1, :] + pair_ref[1, i:i + 1, :]
            for copy in rows_out:
                copy.start()
        hand_on(1)
        last_half(0)
        hand_on(2)
        last_half(1)
        last_half(2)

    pl.run_scoped(
        weight_grads,
        pltpu.VMEM((W_SLOTS, group, W_ROWS, head_dim), BF16), pltpu.VMEM((W_SLOTS, W_ROWS, 2 * head_dim), BF16), pltpu.VMEM((n_tok, width), F32),
        pltpu.VMEM((n_tok, width), F32), pltpu.VMEM((n_tok, 128), F32), pltpu.VMEM((2, n_batch, 2, CORES, seq, cols), BF16), pltpu.VMEM((2, n_batch, seq, cols), BF16),
    )

    with scope('sums'):
        all_came(all_rows, p_rsem.at[1], at.partner)
        for i, ref in enumerate((dgain_ref, dbias_ref)):
            total = row_ref[0, i]
            for n in range(1, chips):
                total = total + row_ref[n, i]
            ref[...] = total.reshape(width)
    with scope('done'):
        heads_across.wait_send()
        all_sent(far_ref, kv_ssem, at.partner)
        all_sent(g_ref, q_ssem, at.partner)
        all_sent(g_all.at[head(chips)], x_ssem, at.partner)
        all_sent(all_rows, p_ssem, at.partner)


def whole_block(n_dev, x, gain, bias, positions, freq, dy, wq, wk, wv, wo):
    n_batch, seq, width = dy.shape
    n_tok = n_batch * seq
    head_dim = wq.shape[2]
    chips = n_dev // CORES
    group = wq.shape[0] // chips
    cols = (group + 2) * head_dim
    n_rows = group * head_dim
    half = n_rows // CORES
    n_seq = n_dev * seq
    quarter = head_dim // 4
    dma = pltpu.SemaphoreType.DMA
    vm = pltpu.VMEM
    shapes = [((n_tok, width), BF16)] * 2 + [((chips * group, half, head_dim), F32)] + [((chips * half, head_dim), F32)] * 2 + [((half, width), F32), ((width,), F32), ((width,), F32)]
    held = [((n_dev, n_batch, seq, width), BF16), ((n_dev, half, n_tok), BF16), ((n_dev, n_dev, seq, cols), BF16), ((chips, width, 2 * head_dim), BF16)]
    return pl.pallas_call(
        functools.partial(block_body, n_dev, group),
        out_shape=tuple(pltpu.VMEM(*t) for t in shapes) + tuple(sds(*t) for t in held),
        in_specs=[HBM] * 10,
        out_specs=(VM,) * len(shapes) + (HBM,) * len(held),
        scratch_shapes=[
            vm((n_tok, width), BF16), vm((width, n_tok), BF16), vm((n_dev, seq, cols), BF16), vm((n_dev, seq, n_rows), BF16),
            vm((n_rows, n_seq), BF16), vm((half, n_batch * n_seq), BF16), vm((n_seq, n_rows), BF16),
            vm((head_dim, n_seq), BF16), vm((head_dim, n_seq), BF16), vm((n_seq, head_dim), F32), vm((n_seq, head_dim), F32),
            vm((quarter, n_seq), F32), vm((quarter, n_seq), F32), vm((3, n_tok, head_dim), F32), vm((n_dev, n_batch, seq), jnp.int32), vm((width,), F32), vm((width,), F32), vm((quarter, 1), F32),
            vm((2, seq, n_rows), BF16), vm((2, half, n_tok), BF16),
            vm((n_batch, n_dev, seq, cols), BF16), vm((2, 8, width), F32), vm((CORES, 2, width), F32), vm((chips, CORES, 1, width), F32),
            dma((6,)), dma((9,)), dma((8,)), dma((8,)), dma((3,)), dma((2,)), dma((2,)),
            dma((6,)), dma((3,)), dma((1,)), dma((W_SLOTS, 2)), dma((4,)),
        ],
        compiler_params=pltpu.CompilerParams(collective_id=0, has_side_effects=True, vmem_limit_bytes=VMEM_LIMIT),
        cost_estimate=pl.CostEstimate(flops=10 ** 11, bytes_accessed=10 ** 8, transcendentals=0),
        name='block',
    )(gain, bias, positions, freq, x.reshape(n_tok, width), dy, wq, wk, wv, wo)[:len(shapes)]


def settle_body(n, *refs):
    sem = refs[2 * n]
    copies = []
    for src, dst in zip(refs[:n], refs[n:2 * n]):
        pieces = SETTLE if len(src.shape) > 1 else 1
        size = src.shape[0] // pieces
        copies += [pltpu.make_async_copy(src.at[pl.ds(p * size, size)], dst.at[pl.ds(p * size, size)], sem) for p in range(pieces)]
    for copy in copies:
        copy.start()
    for copy in copies:
        copy.wait()


def settle(arrays):
    n = len(arrays)
    return pl.pallas_call(
        functools.partial(settle_body, n),
        out_shape=tuple(sds(t.shape, t.dtype) for t in arrays),
        in_specs=[ANY] * n,
        out_specs=(HBM,) * n,
        scratch_shapes=[pltpu.SemaphoreType.DMA],
        compiler_params=pltpu.CompilerParams(vmem_limit_bytes=1024 * 1024),
        name='settle',
    )(*arrays)


def solution(mesh):
    n_dev = mesh.shape['cp']

    def device_step(x_act, d_out, positions, ln_gain, ln_bias, w_query, w_key, w_value, w_out):
        n_batch, seq, width = x_act.shape
        q_heads, (kv_heads, head_dim) = w_query.shape[1], w_key.shape[1:]
        group = q_heads // kv_heads
        quarter = head_dim // 4
        assert n_batch == CORES and n_dev // CORES == kv_heads == 4 and q_heads * head_dim == width

        freq = np.exp(np.arange(quarter) * (-2.0 * math.log(ROPE_BASE) / (head_dim // 2))).astype(np.float32).reshape(quarter, 1)
        by_head = lambda t: jnp.transpose(t, (1, 0, 2))
        by_row = lambda t: t.reshape(width * kv_heads, head_dim)
        wq = by_head(w_query)

        results = whole_block(n_dev, x_act, ln_gain, ln_bias, positions, jnp.asarray(freq), d_out, wq, by_row(w_key), by_row(w_value), w_out)
        out, dx, dwq, dwk, dwv, dwo, dgain, dbias = settle(results)
        kv_rows = lambda t: t.reshape(width // n_dev, kv_heads, head_dim)
        return (out.reshape(x_act.shape), dx.reshape(x_act.shape), by_head(dwq), kv_rows(dwk), kv_rows(dwv), dwo, dgain, dbias)

    return jax.shard_map(device_step, mesh=mesh, in_specs=(P('dp', 'cp', None), P('dp', 'cp', None), P('dp', 'cp'), P(None), P(None), P(None, None, None), P(None, None, None), P(None, None, None), P(None, None)), out_specs=(P('dp', 'cp', None), P('dp', 'cp', None), P(('dp', 'cp'), None, None), P(('dp', 'cp'), None, None), P(('dp', 'cp'), None, None), P(('dp', 'cp'), None), P('dp'), P('dp')), check_vma=False)
```

```python
import functools
import math
import jax
import jax.numpy as jnp
import numpy as np
from jax import lax
from jax.experimental import pallas as pl
from jax.experimental.pallas import tpu as pltpu
from jax.sharding import PartitionSpec as P

EPS = 1e-5
ROPE_BASE = 10000.0
BF16 = jnp.bfloat16
F32 = jnp.float32
VMEM_LIMIT = 46 * 1024 * 1024
NT = (((1,), (1,)), ((), ()))
ANY = pl.BlockSpec(memory_space=pl.ANY)
VM = pl.BlockSpec(memory_space=pltpu.VMEM)
HBM = pl.BlockSpec(memory_space=pltpu.HBM)
CORES = 2
PAIR = range(2)
STEPS = (1, -1)
COL_TILE = 512
OUT_TILE = 256
ROWS = 16
W_SLOTS = 4
W_ROWS = 512
SETTLE = 4


def dot(a, b):
    return jnp.dot(a, b, preferred_element_type=F32)


def dot_nt(a, b):
    return lax.dot_general(a, b, NT, preferred_element_type=F32)


def sds(shape, dtype):
    return jax.ShapeDtypeStruct(shape, dtype)


def head(size):
    return pl.ds(0, size)


def block(i, size):
    return pl.ds(pl.multiple_of(i * size, size), size)


class Place:
    def __init__(self, n_dev):
        self.n_dev = n_dev
        self.chips = n_dev // CORES
        self.me = lax.axis_index('cp')
        self.chip = self.me // CORES
        self.core = self.me % CORES
        self.partner = self.chip * CORES + 1 - self.core

    def ring(self, step):
        return lax.rem(self.chip + self.chips + step, self.chips)

    def dev(self, step, core):
        return self.ring(step) * CORES + core

    def peers(self, far):
        near = [self.partner] + [self.dev(s, c) for s in STEPS for c in range(CORES)]
        return near + ([self.dev(2, c) for c in range(CORES)] if far else [])


def send(src, dst, ssem, rsem, to):
    return pltpu.make_async_remote_copy(src_ref=src, dst_ref=dst, send_sem=ssem, recv_sem=rsem, device_id={'cp': to}, device_id_type=pl.DeviceIdType.MESH)


def all_sent(total, ssem, to):
    send(total, total, ssem, ssem, to).wait_send()


def all_came(total, rsem, to):
    send(total, total, rsem, rsem, to).wait_recv()


def meet(peers):
    barrier = pltpu.get_barrier_semaphore()
    for peer in peers:
        pl.semaphore_signal(barrier, inc=1, device_id={'cp': peer}, device_id_type=pl.DeviceIdType.MESH)
    pl.semaphore_wait(barrier, len(peers))


class Ring:
    def __init__(self, n, slots, copies):
        self.n, self.slots, self.copies = n, slots, copies

    def prime(self):
        for s in range(self.slots):
            for copy in self.copies(s, s):
                copy.start()

    def run(self, use):
        @pl.loop(0, self.n)
        def _(s):
            slot = lax.rem(s, self.slots)
            for copy in self.copies(s, slot):
                copy.wait()
            use(s, slot)

            @pl.when(s + self.slots < self.n)
            def _():
                for copy in self.copies(s + self.slots, slot):
                    copy.start()


class Gather:
    def __init__(self, at, own, piece, both, ssem, rsem, across):
        steps = STEPS
        origin = [at.dev(-1, at.core), at.dev(1, at.core)]
        far = at.dev(2, at.core)
        link = lambda i, src, dst, to: send(src, dst, ssem, rsem.at[i], to)
        self.first = [link(b, own(b), piece(at.me, b), at.dev(steps[b], at.core)) for b in PAIR]
        self.second = [link(2 + b, own(1 - b), piece(at.me, 1 - b), at.dev(steps[b], at.core)) for b in PAIR]
        self.again = [link(4 + b, piece(origin[b], b), piece(origin[b], b), at.dev(steps[b], at.core)) for b in PAIR]
        self.own_across = link(across[0], both(None), both(at.me), at.partner)
        self.first_across = [link(across[1], piece(origin[b], b), piece(origin[b], b), at.partner) for b in PAIR]
        self.second_across = [link(across[1], piece(origin[b], 1 - b), piece(origin[b], 1 - b), at.partner) for b in PAIR]
        self.far_across = [link(across[2], piece(far, b), piece(far, b), at.partner) for b in PAIR]

    def start_first(self):
        for copy in self.first + [self.own_across]:
            copy.start()

    def start_second(self):
        for copy in self.second:
            copy.start()

    def pass_on(self):
        for copy, again, across in zip(self.first, self.again, self.first_across):
            copy.wait_recv()
            again.start()
            across.start()

    def share_second(self):
        for copy, across in zip(self.second, self.second_across):
            copy.wait_recv()
            across.start()

    def share_far(self):
        for copy, across in zip(self.again, self.far_across):
            copy.wait_recv()
            across.start()


class Exchange:
    def __init__(self, at, src, dst, relay, ssem, rsem):
        near = [(0, 1 - at.core)] + [(s, c) for s in STEPS for c in range(CORES)]
        self.near = [send(src(at.dev(s, c)), dst(at.me), ssem, rsem.at[0], at.dev(s, c)) for s, c in near]
        self.far = [send(src(at.dev(2, i)), relay.at[i], ssem, rsem.at[1 + i], at.dev(step, at.core)) for i, step in enumerate(STEPS)]
        self.on = [send(relay.at[i], dst(at.dev(-step, at.core)), ssem, rsem.at[0], at.dev(step, i)) for i, step in enumerate(STEPS)]

    def start(self):
        for copy in self.far + self.near:
            copy.start()

    def pass_on(self):
        for far, on in zip(self.far, self.on):
            far.wait_recv()
            on.start()


def layer_norm(x):
    cen = x - jnp.mean(x, axis=-1, keepdims=True)
    inv = lax.rsqrt(jnp.mean(cen * cen, axis=-1, keepdims=True) + EPS)
    return cen * inv, inv


def block_body(n_dev, group, gain_hbm, bias_hbm, pos_hbm, freq_hbm, x_hbm, dy_ref, wq_ref, wk_ref, wv_ref, wo_ref,
               out_ref, dx_ref, dwq_ref, dwk_ref, dwv_ref, dwo_ref, dgain_ref, dbias_ref, dy_all, ht_all, g_all, wkv_all,
               h_ref, ht_ref, g_ref, q_ref, at_ref, at2_ref, da_ref, kt_ref, vt_ref, dk_ref, dv_ref,
               cost_ref, sint_ref, tab_ref, spot_ref, gain_ref, bias_ref, freq_ref, relay_q, relay_h, far_ref, part_ref, pair_ref, row_ref,
               s_sem, dy_rsem, kv_rsem, q_rsem, h_rsem, p_rsem, t_sem, loc_sem, mix_sem, lhs_sem, w_sem, job_sem):
    at = Place(n_dev)
    n_batch, seq, width = dy_ref.shape
    n_tok = n_batch * seq
    head_dim = wq_ref.shape[2]
    cols = (group + 2) * head_dim
    n_rows = group * head_dim
    half = n_rows // CORES
    n_seq = n_dev * seq
    quarter = head_dim // 4
    scale = head_dim ** -0.5
    chips = at.chips
    tile = CORES * seq
    core, me = at.core, at.me
    steps = STEPS
    origin = [at.dev(-1, core), at.dev(1, core)]
    far_dev = at.dev(2, core)
    scope = jax.named_scope

    dy_ssem, kv_ssem, q_ssem, h_ssem, p_ssem, x_ssem = [s_sem.at[i] for i in range(6)]
    assert (n_dev + 1) * n_rows == (n_dev - 1) * cols
    block_total = far_ref.at[0, head(n_dev - 1)]

    with scope('meet'):
        meet(at.peers(True))

    kv_cols = 2 * head_dim * chips
    kv_piece = lambda d, b: far_ref.at[b, d, :, head(kv_cols)]
    kv_both = lambda d: far_ref.at[:, me if d is None else d, :, head(kv_cols)]
    dys = Gather(at, lambda b: dy_ref.at[b], lambda d, b: dy_all.at[d, b], lambda d: dy_ref if d is None else dy_all.at[d], dy_ssem, dy_rsem, (6, 7, 8))
    kvs = Gather(at, lambda b: kv_piece(me, b), kv_piece, kv_both, kv_ssem, kv_rsem, (6, 6, 6))
    q_part = head(n_rows)
    queries = Exchange(at, lambda d: g_ref.at[d, :, q_part], lambda d: q_ref.at[d], relay_q, q_ssem, q_rsem)
    hcols = Exchange(at, lambda d: ht_ref.at[block(d, half)], lambda d: ht_all.at[d], relay_h, h_ssem, h_rsem)
    heads_across = send(at_ref.at[block(1 - core, half)], at2_ref.at[:, block(core, n_seq)], t_sem.at[0], t_sem.at[1], at.partner)
    spots = [send(pos_hbm, spot_ref.at[me], p_ssem, p_rsem.at[0], peer) for peer in at.peers(True)]

    dys.start_first()
    x_in = pltpu.make_async_copy(x_hbm, dx_ref, loc_sem.at[1])
    x_in.start()
    for copy in spots:
        copy.start()
    small = [pltpu.make_async_copy(src, dst, loc_sem.at[2 + n]) for n, (src, dst) in enumerate(((gain_hbm, gain_ref), (bias_hbm, bias_ref), (freq_hbm, freq_ref), (pos_hbm, spot_ref.at[me])))]
    for copy in small:
        copy.start()
    for copy in small:
        copy.wait()

    freq = freq_ref[...]
    for b in range(n_batch):
        angle = freq * spot_ref[me, b:b + 1, :].astype(F32)
        cos, sin, none = jnp.cos(angle), jnp.sin(angle), jnp.zeros((quarter, seq), F32)
        rest = jnp.zeros((head_dim - 2 * quarter, seq), F32)
        for i, rows in enumerate(([cos, cos, rest + 1.0], [-sin, none, rest], [none, sin, rest])):
            tab_ref[i, b * seq:(b + 1) * seq, :] = jnp.concatenate(rows, axis=0).T

    gain = (1.0 + gain_ref[...]).reshape(1, width)
    bias = bias_ref[...].reshape(1, width)

    def project_all(wkv_ref, raw_ref, wq_vm, raw_sem, wq_sem, stage_sem):
        pieces = [(b, i) for b in range(n_batch) for i in range(width // n_rows)]
        there = lambda n: da_ref.at[pl.ds(n * seq, seq)]
        dy_in = [pltpu.make_async_copy(dy_ref.at[b, :, pl.ds(i * n_rows, n_rows)], there(n), stage_sem.at[n]) for n, (b, i) in enumerate(pieces)]
        dy_keep = [pltpu.make_async_copy(there(n), dy_all.at[me, b, :, pl.ds(i * n_rows, n_rows)], stage_sem.at[n]) for n, (b, i) in enumerate(pieces)]
        span = 64 * chips
        batch = raw_ref.shape[2] // span
        row = lax.broadcasted_iota(jnp.int32, (span, span), 0)
        col = lax.broadcasted_iota(jnp.int32, (span, span), 1)
        pick = jnp.where(col == lax.rem(row, 64) * chips + lax.div(row, 64), 1.0, 0.0).astype(BF16)

        def raw_in(s, slot):
            return [pltpu.make_async_copy(w.at[block(s, span * batch)], raw_ref.at[slot, i], raw_sem.at[slot, i]) for i, w in enumerate((wk_ref, wv_ref))]

        def wq_in(s, slot):
            return [pltpu.make_async_copy(wq_ref.at[block(s, 2)], wq_vm.at[slot], wq_sem.at[slot])]

        def part_heads(s, slot):
            for i in range(batch):
                sl = slice(i * span, (i + 1) * span)
                rows = dot(pick, jnp.concatenate([raw_ref[slot, 0, sl, :], raw_ref[slot, 1, sl, :]], axis=1)).astype(BF16)
                for n in range(chips):
                    wkv_ref[n, block(s * batch + i, 64), :] = rows[n * 64:(n + 1) * 64]

        def turned(v):
            return v * tab_ref[0] + pltpu.roll(v, head_dim - quarter, 1) * tab_ref[1] + pltpu.roll(v, quarter, 1) * tab_ref[2]

        def project(s, slot):
            y = dot(h_ref[...], jnp.concatenate([wq_vm[slot, 0], wq_vm[slot, 1]], axis=1))
            for i in PAIR:
                head = s * 2 + i
                v = turned(y[:, i * head_dim:(i + 1) * head_dim]).astype(BF16)
                for b in range(n_batch):
                    g_ref[lax.div(head, group) * n_batch + b, :, block(lax.rem(head, group), head_dim)] = v[b * seq:(b + 1) * seq]

        kv_ring = Ring(width // (64 * batch), raw_ref.shape[0], raw_in)
        q_ring = Ring(chips * group // 2, wq_vm.shape[0], wq_in)
        kv_ring.prime()
        q_ring.prime()
        for copy in dy_in:
            copy.start()
        x_in.wait()
        with scope('norm'):
            @pl.loop(0, n_tok // (2 * ROWS))
            def _(step):
                for i in PAIR:
                    sl = block(2 * step + i, ROWS)
                    hat, _ = layer_norm(dx_ref[sl, :].astype(F32))
                    h_ref[sl, :] = (hat * gain + bias).astype(BF16)

        with scope('heads_kv'):
            kv_ring.run(part_heads)
        keep = pltpu.make_async_copy(wkv_ref, wkv_all, mix_sem.at[2])
        keep.start()
        for come, go in zip(dy_in, dy_keep):
            come.wait()
            go.start()
        with scope('project_kv'):
            @pl.loop(0, chips)
            def _(n):
                y = dot(h_ref[...], wkv_ref[n])
                v = jnp.concatenate([turned(y[:, :head_dim]), y[:, head_dim:]], axis=1).astype(BF16)
                for b in range(n_batch):
                    far_ref[b, me, :, block(n, 2 * head_dim)] = v[b * seq:(b + 1) * seq]

        kvs.start_first()
        kvs.start_second()
        with scope('project_q'):
            q_ring.run(project)
        keep.wait()
        for copy in dy_keep:
            copy.wait()

    pl.run_scoped(
        project_all,
        pltpu.VMEM((chips, width, 2 * head_dim), BF16),
        pltpu.VMEM((3, 2, 4 * 64 * chips, head_dim), BF16), pltpu.VMEM((4, 2, width, head_dim), BF16),
        pltpu.SemaphoreType.DMA((3, 2)), pltpu.SemaphoreType.DMA((4,)), pltpu.SemaphoreType.DMA((n_batch * width // n_rows,)),
    )

    with scope('kv_pass'):
        kvs.pass_on()
    queries.start()
    q_ref[me] = g_ref[me, :, q_part]
    with scope('turn_h'):
        @pl.loop(0, width // 128)
        def _(step):
            sl = block(step, 128)
            ht_ref[sl, :] = h_ref[:, sl].T

    with scope('kv_wait'):
        kvs.share_second()
        kvs.share_far()
        all_came(far_ref.at[:, head(chips), :, head(kv_cols)], kv_rsem.at[6], at.partner)

    def chip_at(i):
        return at.ring(jnp.where(i == 0, 0, jnp.where(i == 1, 1, jnp.where(i == 2, 3, 2))))

    def soft(s, seen):
        s = s * scale
        clear = s.shape[0] - seen.shape[0]
        tail = jnp.where(seen, s[clear:], -1e30)
        s = tail if clear == 0 else jnp.concatenate([s[:clear], tail], axis=0)
        e = jnp.exp(s - jnp.max(s, axis=0, keepdims=True))
        return e * (1.0 / jnp.sum(e, axis=0, keepdims=True))

    def attend(limit, clear):
        @pl.loop(0, n_batch * chips)
        def _(i):
            @pl.when(i == 1)
            def _():
                with scope('q_pass'):
                    queries.pass_on()
                dys.start_second()
                dys.pass_on()
                hcols.start()

            b, n = lax.rem(i, n_batch), lax.div(i, n_batch)
            k = far_ref[b, 0:limit // seq, :, block(2 * n, head_dim)].reshape(limit, head_dim)
            vt = far_ref[b, 0:limit // seq, :, block(2 * n + 1, head_dim)].reshape(limit, head_dim).T
            q = jnp.concatenate([g_ref[n * n_batch + b, :, block(j, head_dim)] for j in range(group)], axis=0)
            row = lax.broadcasted_iota(jnp.int32, (limit - clear, n_rows), 0)
            col = lax.broadcasted_iota(jnp.int32, (limit - clear, n_rows), 1)
            p = soft(dot_nt(k, q), row <= lax.rem(col, seq) + (me * seq - clear))
            mixed = dot(vt, p.astype(BF16)).astype(BF16)
            for j in range(group):
                h_ref[block(b, seq), block(n * group + j, head_dim)] = mixed[:, j * seq:(j + 1) * seq].T

    with scope('attend'):
        @pl.when(at.chip == chips - 1)
        def _():
            attend(chips * tile, (chips - 1) * tile)

        @pl.when(at.chip < chips - 1)
        def _():
            attend((chips - 1) * tile, 0)

    h_keep = pltpu.make_async_copy(ht_ref.at[block(me, half)], ht_all.at[me], loc_sem.at[1])
    h_keep.start()

    def block_out():
        def stream(wo_vm, sem):
            def wo_in(s, slot):
                return [pltpu.make_async_copy(wo_ref.at[:, block(s, OUT_TILE)], wo_vm.at[slot], sem.at[slot])]

            def out_tile(s, slot):
                sl = block(s, OUT_TILE)
                out_ref[:, sl] = (dx_ref[:, sl].astype(F32) + dot(h_ref[...], wo_vm[slot])).astype(BF16)

            ring = Ring(width // OUT_TILE, wo_vm.shape[0], wo_in)
            ring.prime()
            ring.run(out_tile)

        with scope('output'):
            pl.run_scoped(stream, pltpu.VMEM((4, width, OUT_TILE), BF16), pltpu.SemaphoreType.DMA((4,)))

    k_all = lambda n: far_ref[core, 0:n, :, block(2 * at.chip, head_dim)].reshape(n * seq, head_dim)
    v_all = lambda n: far_ref[core, 0:n, :, block(2 * at.chip + 1, head_dim)].reshape(n * seq, head_dim)

    def rotate_back(t, cos, sin):
        u, w = t[:quarter], t[quarter:2 * quarter]
        return jnp.concatenate([u * cos + w * sin, w * cos - u * sin, t[2 * quarter:]], axis=0)

    def by_dev(t):
        return t.astype(BF16).reshape(t.shape[0] // seq, seq, head_dim)

    def attend_back(t, i):
        limit = (t + 1) * tile
        sl = slice(t * tile, limit)
        devs = slice(t * CORES, (t + 1) * CORES)

        def heads(first, count):
            each = range(count)
            q = jnp.concatenate([q_ref[devs, :, block(first + j, head_dim)].reshape(tile, head_dim) for j in each], axis=0)
            da = jnp.concatenate([da_ref[sl, block(first + j, head_dim)] for j in each], axis=0)
            k, v = k_all(limit // seq), v_all(limit // seq)
            row = lax.broadcasted_iota(jnp.int32, (tile, count * tile), 0)
            col = lax.broadcasted_iota(jnp.int32, (tile, count * tile), 1)
            p = soft(dot_nt(k, q), row <= lax.rem(col, tile))
            p_low = p.astype(BF16)
            mixed = dot(vt_ref[:, :limit], p_low).astype(BF16)
            dp = dot_nt(v, da)
            row_dot = jnp.sum(p * dp, axis=0, keepdims=True)
            ds = (p * (dp - row_dot) * scale).astype(BF16)
            dv_ref[:limit, :] += dot(p_low, da)
            dk_ref[:limit, :] += dot(ds, q)
            back = dot(kt_ref[:, :limit], ds)
            for j in each:
                part = slice(j * tile, (j + 1) * tile)
                at_ref[block(first + j, head_dim), sl] = mixed[:, part]
                g_ref[devs, :, block(first + j, head_dim)] = by_dev(rotate_back(back[:, part], cost_ref[:, sl], sint_ref[:, sl]).T)

        @pl.loop(0, group // 2)
        def _(j):
            heads(2 * j, 2)

        @pl.when(i == chips - 2)
        def _():
            with scope('dy_far'):
                dys.share_far()

        heads(group - 1, 1)

    def middle(wo_vm, dyk):
        wo_in = pltpu.make_async_copy(wo_ref.at[block(at.chip, n_rows)], wo_vm, mix_sem.at[2])
        wo_in.start()
        all_came(spot_ref.at[head(n_dev - 1)], p_rsem.at[0], at.partner)
        for d in range(n_dev):
            angle = freq * spot_ref[d, pl.ds(core, 1), :].astype(F32)
            cost_ref[:, d * seq:(d + 1) * seq] = jnp.cos(angle)
            sint_ref[:, d * seq:(d + 1) * seq] = jnp.sin(angle)
        with scope('q_wait'):
            all_came(q_ref.at[head(n_dev - 1)], q_rsem.at[0], at.partner)
            all_sent(block_total, q_ssem, at.partner)
            all_sent(far_ref.at[:, head(n_dev - 1), :, head(kv_cols)], kv_ssem, at.partner)
            all_sent(spot_ref.at[head(n_dev - 1)], p_ssem, at.partner)
        kt_ref[...] = k_all(n_dev).T
        vt_ref[...] = v_all(n_dev).T
        dk_ref[...] = jnp.zeros_like(dk_ref)
        dv_ref[...] = jnp.zeros_like(dv_ref)
        dys.own_across.wait_recv()

        def fetch(i, slot):
            return pltpu.make_async_copy(dy_all.at[block(chip_at(i), CORES), core], dyk.at[slot], mix_sem.at[slot])

        with scope('wo_wait'):
            fetch(0, 0).start()
            wo_in.wait()

        @pl.loop(0, chips)
        def _(i):
            slot = lax.rem(i, 2)

            @pl.when((i == 1) & (at.chip < chips - 1))
            def _():
                block_out()

            @pl.when(i == 1)
            def _():
                with scope('dy_wait'):
                    dys.share_second()
                    all_came(dy_all.at[head(2)], dy_rsem.at[7], at.partner)
                fetch(i, slot).start()

            @pl.when(i == chips - 1)
            def _():
                with scope('dy_far2'):
                    all_came(dy_all.at[0], dy_rsem.at[8], at.partner)
                fetch(i, slot).start()
                with scope('h_pass'):
                    hcols.pass_on()

            fetch(i, slot).wait()

            @pl.when((i > 0) & (i < chips - 2))
            def _():
                fetch(i + 1, 1 - slot).start()

            chip = chip_at(i)
            with scope('da'):
                da_ref[block(chip, tile), :] = dot_nt(dyk[slot].reshape(tile, width), wo_vm[...]).astype(BF16)
            with scope('attend_back'):
                for t in range(chips):
                    @pl.when(chip == t)
                    def _(t=t):
                        attend_back(t, i)

    pl.run_scoped(middle, pltpu.VMEM((n_rows, width), BF16), pltpu.VMEM((2, CORES, seq, width), BF16))
    all_sent(dy_all.at[head(n_dev - 1)], dy_ssem, at.partner)
    heads_across.start()
    g_ref[:, :, n_rows:n_rows + head_dim] = by_dev(rotate_back(dk_ref[...].T, cost_ref[...], sint_ref[...]).T)
    g_ref[:, :, n_rows + head_dim:] = by_dev(dv_ref[...])

    def span_of(q):
        return block(q, CORES)

    turn = [[at.ring(q) for q in (2, 1, 3, 0)], [at.ring(q) for q in (3, 0, 1, 2)]]
    direct = [[send(g_ref.at[span_of(turn[i][q])], g_all.at[me, span_of(turn[i][q])], kv_ssem, kv_rsem.at[i * chips + q], at.dev(steps[i], core)) for q in range(chips)] for i in PAIR]
    came = [[at.ring(q) for q in (1, 0, 2, 3)], [at.ring(q) for q in (0, 1, 2, 3)]]
    n_heads = group + 2
    late_heads = [range(n_heads), range(n_heads // 2 + 1), range(n_heads // 2 + 1, n_heads)]

    def columns(heads):
        return pl.ds(heads[0] * head_dim, len(heads) * head_dim)

    def late(ref, quarters):
        own = [ref.at[pl.ds(quarters[1] * CORES + min(c, 1), 1), :, columns(heads)] for c, heads in enumerate(late_heads)]
        return [ref.at[span_of(quarters[0])]] + own

    onward = [[send(src, dst, q_ssem, q_rsem.at[4 * i + q], at.dev(steps[i], core)) for q, (src, dst) in enumerate(zip(late(g_all.at[origin[i]], came[i]), late(far_ref.at[core], came[i])))] for i in PAIR]
    ends = [[at.ring(q) for q in (0, 3)], [at.ring(q) for q in (1, 2)]]
    g_across = send(g_ref, g_all.at[me], x_ssem, dy_rsem.at[0], at.partner)
    near_across = [[send(g_all.at[origin[i], span_of(came[i][q])], g_all.at[origin[i], span_of(came[i][q])], x_ssem, dy_rsem.at[1 + q // 2], at.partner) for q in range(chips)] for i in PAIR]
    end_across = [[send(ref, ref, x_ssem, dy_rsem.at[3 + (q or 4 * i)], at.partner) for q, ref in enumerate(late(far_ref.at[core], ends[i]))] for i in PAIR]
    for q in range(chips):
        for i in PAIR:
            direct[i][q].start()
    g_across.start()
    g_keep = pltpu.make_async_copy(g_ref, g_all.at[me], loc_sem.at[0])
    g_keep.start()
    at2_ref[:, block(core, n_seq)] = at_ref[block(core, half), :]

    @pl.when(at.chip == chips - 1)
    def _():
        block_out()

    dy_back = [pltpu.make_async_copy(dy_ref.at[b], h_ref.at[pl.ds(b * seq, seq)], loc_sem.at[2 + b]) for b in range(n_batch)]
    for copy in dy_back:
        copy.start()

    def wo_rows(dy_vm, sem):
        def dy_tile(s, slot):
            return [pltpu.make_async_copy(dy_all.at[:, :, :, block(s, COL_TILE)], dy_vm.at[slot], sem.at[slot])]

        def wo_tile(s, slot):
            pieces = [dy_vm[slot, d, b] for b in range(n_batch) for d in range(n_dev)]
            dwo_ref[:, block(s, COL_TILE)] = dot(at2_ref[...], jnp.concatenate(pieces, axis=0))

        ring = Ring(width // COL_TILE, dy_vm.shape[0], dy_tile)
        ring.prime()
        with scope('heads_wait'):
            heads_across.wait_recv()
        with scope('grad_wo'):
            ring.run(wo_tile)

    pl.run_scoped(wo_rows, pltpu.VMEM((4, n_dev, n_batch, seq, COL_TILE), BF16), pltpu.SemaphoreType.DMA((4,)))

    with scope('h_wait'):
        all_came(ht_all.at[head(n_dev - 1)], h_rsem.at[0], at.partner)
        all_sent(block_total, h_ssem, at.partner)
    h_keep.wait()
    lhs_in = [pltpu.make_async_copy(ht_all.at[d, :, pl.ds(b * seq, seq)], at2_ref.at[:, pl.ds((b * n_dev + d) * seq, seq)], lhs_sem.at[0]) for d in range(n_dev) for b in range(n_batch)]
    for copy in lhs_in:
        copy.start()
    with jax.named_scope('own_wait'):
        pltpu.make_async_copy(at2_ref, at2_ref, lhs_sem.at[0]).wait()
        g_keep.wait()
        g_across.wait_recv()
    pair_across = send(pair_ref.at[core], pair_ref.at[core], p_ssem, p_rsem.at[0], at.partner)
    rows_out = [send(row_ref.at[at.chip, core], row_ref.at[at.chip, core], p_ssem, p_rsem.at[1], at.dev(step, c)) for step in (1, -1, 2) for c in range(CORES)]
    all_rows = row_ref.at[head(chips - 1)]

    def weight_grads(wq_vm, wkv_vm, acc_ref, hat_ref, inv_ref, job_ref, mine_ref):
        n_slots = wq_vm.shape[0]
        chunk = wq_vm.shape[2]
        n_chunks = width // chunk
        total = n_chunks * chips

        def weights(s):
            slot = lax.rem(s, n_slots)
            chip = chip_at(lax.div(s, n_chunks))
            rows = block(lax.rem(s, n_chunks), chunk)
            return [
                pltpu.make_async_copy(wq_ref.at[block(chip, group), rows], wq_vm.at[slot], w_sem.at[slot, 0]),
                pltpu.make_async_copy(wkv_all.at[chip, rows], wkv_vm.at[slot], w_sem.at[slot, 1]),
            ]

        for s in range(n_slots):
            for copy in weights(s):
                copy.start()

        def grow(i, read):
            @pl.loop(0, n_chunks)
            def _(n):
                s = i * n_chunks + n
                slot = lax.rem(s, n_slots)
                for copy in weights(s):
                    copy.wait()
                rows = jnp.concatenate([read(b) for b in range(n_batch)], axis=0)
                part = dot_nt(rows, jnp.concatenate([wq_vm[slot, j] for j in range(group)] + [wkv_vm[slot]], axis=1))
                sl = block(n, chunk)

                @pl.when(i == 0)
                def _():
                    acc_ref[:, sl] = part

                @pl.when(i > 0)
                def _():
                    acc_ref[:, sl] += part

                @pl.when(s + n_slots < total)
                def _():
                    for copy in weights(s + n_slots):
                        copy.start()

        def mine_in(i):
            return [pltpu.make_async_copy(g_all.at[chip_at(i) * CORES + b, me], mine_ref.at[lax.rem(i, 2), b], job_sem.at[2 + lax.rem(i, 2)]) for b in range(n_batch)]

        def grow_near(i):
            here = mine_ref.at[lax.rem(i, 2)]
            pltpu.make_async_copy(here, here, job_sem.at[2 + lax.rem(i, 2)]).wait()
            grow(i, lambda b: mine_ref[lax.rem(i, 2), b])

        def job_in(chip, quarters, slot):
            return [pltpu.make_async_copy(g_all.at[chip * CORES + b, span_of(q)], job_ref.at[slot, b, n], job_sem.at[slot]) for b in range(n_batch) for n, q in enumerate(quarters)]

        def job(chip, pieces, read, add, heads=range(n_heads)):
            lhs = [at2_ref[:, pl.ds(pl.multiple_of(b * n_seq + d * seq, seq), seq)] for b in range(n_batch) for d in pieces]
            rhs = [read(b, n) for b in range(n_batch) for n in range(len(pieces))]
            y = dot(jnp.concatenate(lhs, axis=1), jnp.concatenate(rhs, axis=0))
            for n, j in enumerate(heads):
                v = y[:, n * head_dim:(n + 1) * head_dim]
                if j < group:
                    dwq_ref[chip * group + j] = dwq_ref[chip * group + j] + v if add else v
                else:
                    ref, rows = (dwk_ref, dwv_ref)[j - group], pl.ds(chip, half, stride=chips)
                    ref[rows, :] = ref[rows, :] + v if add else v

        def devs_of(quarters):
            return [q * CORES + c for q in quarters for c in range(CORES)]

        def near_pair(quarters, add):
            for slot, step in enumerate(steps):
                for copy in job_in(at.ring(step), quarters, slot):
                    copy.start()

            @pl.loop(0, 2)
            def _(slot):
                chip = at.ring(1 - 2 * slot)
                pltpu.make_async_copy(job_ref.at[slot], job_ref.at[slot], job_sem.at[slot]).wait()
                job(chip, devs_of(quarters), lambda b, n: job_ref[slot, b, n // CORES, n % CORES], add)

        halves = [[at.ring(q) for q in half_of] for half_of in ((0, 1), (2, 3))]
        for slot in PAIR:
            for copy in job_in(at.chip, [at.ring(2 * slot), at.ring(2 * slot + 1)], slot):
                copy.start()
        for copy in mine_in(0):
            copy.start()
        with jax.named_scope('own_job'):
            for slot in PAIR:
                quarters = [at.ring(2 * slot), at.ring(2 * slot + 1)]
                pltpu.make_async_copy(job_ref.at[slot], job_ref.at[slot], job_sem.at[slot]).wait()
                job(at.chip, devs_of(quarters), lambda b, n: job_ref[slot, b, n // CORES, n % CORES], slot == 1)

        with jax.named_scope('own_dh'):
            grow_near(0)

        with jax.named_scope('d01_wait'):
            for q in PAIR:
                for i in PAIR:
                    direct[i][q].wait_recv()
                for i in PAIR:
                    for copy in onward[i][:1] if q == 0 else onward[i][1:-1]:
                        copy.start()
                    near_across[i][q].start()
        with scope('d01_across'):
            all_came(g_all.at[0], dy_rsem.at[1], at.partner)
        for i in (1, 2):
            for copy in mine_in(i):
                copy.start()
        with scope('near_dh'):
            @pl.loop(1, chips - 1)
            def _(i):
                grow_near(i)

        with jax.named_scope('near_a'):
            near_pair(halves[0], False)
        with scope('d2_wait'):
            for i in PAIR:
                direct[i][2].wait_recv()
                near_across[i][2].start()
        with jax.named_scope('hat'):
            @pl.loop(0, n_tok // (2 * ROWS))
            def _(step):
                for i in PAIR:
                    sl = block(2 * step + i, ROWS)
                    hat, inv = layer_norm(dx_ref[sl, :].astype(F32))
                    hat_ref[sl, :] = hat
                    inv_ref[sl, :] = jnp.broadcast_to(inv, (ROWS, 128))

        with scope('d3_wait'):
            for i in PAIR:
                direct[i][3].wait_recv()
                near_across[i][3].start()
        with scope('d23_across'):
            all_came(g_all.at[0], dy_rsem.at[2], at.partner)
        with jax.named_scope('near_b'):
            near_pair(halves[1], True)
        far_chip = at.ring(2)
        end_total = [g_all.at[0, head(CORES), :, columns(heads)] for heads in late_heads]
        with jax.named_scope('far0_wait'):
            for i in PAIR:
                onward[i][0].wait_recv()
                end_across[i][0].start()
        with scope('far0_across'):
            all_came(end_total[0], dy_rsem.at[3], at.partner)
        with jax.named_scope('far_dh'):
            grow(chips - 1, lambda b: far_ref[b, me])
        for copy in dy_back:
            copy.wait()
        part_ref[...] = jnp.zeros_like(part_ref)

        with jax.named_scope('norm_back'):
            @pl.loop(0, n_tok // (2 * ROWS))
            def _(step):
                for i in PAIR:
                    sl = block(2 * step + i, ROWS)
                    hat, inv = hat_ref[sl, :], inv_ref[sl, 0:1]
                    dh = acc_ref[sl, :]
                    dg = dh * hat
                    gh = dh * gain
                    one = jnp.mean(gh, axis=-1, keepdims=True)
                    two = jnp.mean(dg * gain, axis=-1, keepdims=True)
                    dx_ref[sl, :] = (h_ref[sl, :].astype(F32) + inv * (gh - one - hat * two)).astype(BF16)
                    part_ref[0] += dg[0:8] + dg[8:16]
                    part_ref[1] += dh[0:8] + dh[8:16]

        for i in PAIR:
            pair_ref[core, i:i + 1, :] = jnp.sum(part_ref[i], axis=0, keepdims=True)
        pair_across.start()

        def hand_on(c):
            with scope('far1_wait'):
                for i in PAIR:
                    onward[i][1 + c].wait_recv()
                    end_across[i][1 + c].start()

        def far_rows(devs, add, heads=range(n_heads)):
            job(far_chip, devs, lambda b, n: far_ref[b, devs[n], :, heads[0] * head_dim:(heads[-1] + 1) * head_dim], add, heads)

        def last_half(c):
            with scope('far1_across'):
                all_came(end_total[c], dy_rsem.at[4 + c], at.partner)
            with scope('far_b'):
                far_rows([ends[i][1] * CORES + min(c, 1) for i in PAIR], True, late_heads[c])

        hand_on(0)
        with scope('far_a'):
            all_came(end_total[0], dy_rsem.at[7], at.partner)
            far_rows(devs_of([ends[0][0], ends[1][0]]), False)
        with scope('rows'):
            all_came(pair_ref.at[0], p_rsem.at[0], at.partner)
            all_sent(pair_ref.at[0], p_ssem, at.partner)
            for i in PAIR:
                row_ref[at.chip, i] = pair_ref[0, i:i + 1, :] + pair_ref[1, i:i + 1, :]
            for copy in rows_out + [onward[i][-1] for i in PAIR]:
                copy.start()
        hand_on(1)
        last_half(0)
        hand_on(2)
        last_half(1)
        last_half(2)

    pl.run_scoped(
        weight_grads,
        pltpu.VMEM((W_SLOTS, group, W_ROWS, head_dim), BF16), pltpu.VMEM((W_SLOTS, W_ROWS, 2 * head_dim), BF16), pltpu.VMEM((n_tok, width), F32),
        pltpu.VMEM((n_tok, width), F32), pltpu.VMEM((n_tok, 128), F32), pltpu.VMEM((2, n_batch, 2, CORES, seq, cols), BF16), pltpu.VMEM((2, n_batch, seq, cols), BF16),
    )

    with scope('sums'):
        all_came(all_rows, p_rsem.at[1], at.partner)
        for i, ref in enumerate((dgain_ref, dbias_ref)):
            total = row_ref[0, i]
            for n in range(1, chips):
                total = total + row_ref[n, i]
            ref[...] = total.reshape(width)
    with scope('done'):
        heads_across.wait_send()
        all_sent(far_ref, kv_ssem, at.partner)
        all_sent(g_ref, q_ssem, at.partner)
        all_sent(g_all.at[head(chips)], x_ssem, at.partner)
        all_sent(all_rows, p_ssem, at.partner)


def whole_block(n_dev, x, gain, bias, positions, freq, dy, wq, wk, wv, wo):
    n_batch, seq, width = dy.shape
    n_tok = n_batch * seq
    head_dim = wq.shape[2]
    chips = n_dev // CORES
    group = wq.shape[0] // chips
    cols = (group + 2) * head_dim
    n_rows = group * head_dim
    half = n_rows // CORES
    n_seq = n_dev * seq
    quarter = head_dim // 4
    dma = pltpu.SemaphoreType.DMA
    vm = pltpu.VMEM
    shapes = [((n_tok, width), BF16)] * 2 + [((chips * group, half, head_dim), F32)] + [((chips * half, head_dim), F32)] * 2 + [((half, width), F32), ((width,), F32), ((width,), F32)]
    held = [((n_dev, n_batch, seq, width), BF16), ((n_dev, half, n_tok), BF16), ((n_dev, n_dev, seq, cols), BF16), ((chips, width, 2 * head_dim), BF16)]
    return pl.pallas_call(
        functools.partial(block_body, n_dev, group),
        out_shape=tuple(pltpu.VMEM(*t) for t in shapes) + tuple(sds(*t) for t in held),
        in_specs=[HBM] * 10,
        out_specs=(VM,) * len(shapes) + (HBM,) * len(held),
        scratch_shapes=[
            vm((n_tok, width), BF16), vm((width, n_tok), BF16), vm((n_dev, seq, cols), BF16), vm((n_dev, seq, n_rows), BF16),
            vm((n_rows, n_seq), BF16), vm((half, n_batch * n_seq), BF16), vm((n_seq, n_rows), BF16),
            vm((head_dim, n_seq), BF16), vm((head_dim, n_seq), BF16), vm((n_seq, head_dim), F32), vm((n_seq, head_dim), F32),
            vm((quarter, n_seq), F32), vm((quarter, n_seq), F32), vm((3, n_tok, head_dim), F32), vm((n_dev, n_batch, seq), jnp.int32), vm((width,), F32), vm((width,), F32), vm((quarter, 1), F32),
            vm((2, seq, n_rows), BF16), vm((2, half, n_tok), BF16),
            vm((n_batch, n_dev, seq, cols), BF16), vm((2, 8, width), F32), vm((CORES, 2, width), F32), vm((chips, CORES, 1, width), F32),
            dma((6,)), dma((9,)), dma((8,)), dma((8,)), dma((3,)), dma((2,)), dma((2,)),
            dma((6,)), dma((3,)), dma((1,)), dma((W_SLOTS, 2)), dma((4,)),
        ],
        compiler_params=pltpu.CompilerParams(collective_id=0, has_side_effects=True, vmem_limit_bytes=VMEM_LIMIT),
        cost_estimate=pl.CostEstimate(flops=10 ** 11, bytes_accessed=10 ** 8, transcendentals=0),
        name='block',
    )(gain, bias, positions, freq, x.reshape(n_tok, width), dy, wq, wk, wv, wo)[:len(shapes)]


def settle_body(n, *refs):
    sem = refs[2 * n]
    copies = []
    for src, dst in zip(refs[:n], refs[n:2 * n]):
        pieces = SETTLE if len(src.shape) > 1 else 1
        size = src.shape[0] // pieces
        copies += [pltpu.make_async_copy(src.at[pl.ds(p * size, size)], dst.at[pl.ds(p * size, size)], sem) for p in range(pieces)]
    for copy in copies:
        copy.start()
    for copy in copies:
        copy.wait()


def settle(arrays):
    n = len(arrays)
    return pl.pallas_call(
        functools.partial(settle_body, n),
        out_shape=tuple(sds(t.shape, t.dtype) for t in arrays),
        in_specs=[ANY] * n,
        out_specs=(HBM,) * n,
        scratch_shapes=[pltpu.SemaphoreType.DMA],
        compiler_params=pltpu.CompilerParams(vmem_limit_bytes=1024 * 1024),
        name='settle',
    )(*arrays)


def solution(mesh):
    n_dev = mesh.shape['cp']

    def device_step(x_act, d_out, positions, ln_gain, ln_bias, w_query, w_key, w_value, w_out):
        n_batch, seq, width = x_act.shape
        q_heads, (kv_heads, head_dim) = w_query.shape[1], w_key.shape[1:]
        group = q_heads // kv_heads
        quarter = head_dim // 4
        assert n_batch == CORES and n_dev // CORES == kv_heads == 4 and q_heads * head_dim == width

        freq = np.exp(np.arange(quarter) * (-2.0 * math.log(ROPE_BASE) / (head_dim // 2))).astype(np.float32).reshape(quarter, 1)
        by_head = lambda t: jnp.transpose(t, (1, 0, 2))
        by_row = lambda t: t.reshape(width * kv_heads, head_dim)
        wq = by_head(w_query)

        results = whole_block(n_dev, x_act, ln_gain, ln_bias, positions, jnp.asarray(freq), d_out, wq, by_row(w_key), by_row(w_value), w_out)
        out, dx, dwq, dwk, dwv, dwo, dgain, dbias = settle(results)
        kv_rows = lambda t: t.reshape(width // n_dev, kv_heads, head_dim)
        return (out.reshape(x_act.shape), dx.reshape(x_act.shape), by_head(dwq), kv_rows(dwk), kv_rows(dwv), dwo, dgain, dbias)

    return jax.shard_map(device_step, mesh=mesh, in_specs=(P('dp', 'cp', None), P('dp', 'cp', None), P('dp', 'cp'), P(None), P(None), P(None, None, None), P(None, None, None), P(None, None, None), P(None, None)), out_specs=(P('dp', 'cp', None), P('dp', 'cp', None), P(('dp', 'cp'), None, None), P(('dp', 'cp'), None, None), P(('dp', 'cp'), None, None), P(('dp', 'cp'), None), P('dp'), P('dp')), check_vma=False)
```
